32 devices in a mesh: tp: 4 (over z), dp: 8 (over y, x, core).
Axes of the slice: x: 2, y: 2, z: 4, core: 2. Of those that a mesh axis runs over, the one named last changes fastest.
Arguments:
- w_query: bfloat16 [16, 1024, 1024], P(None, ('dp', 'tp'))
- w_key: bfloat16 [16, 1024, 1024], P(None, ('dp', 'tp'))
- w_value: bfloat16 [16, 1024, 1024], P(None, ('dp', 'tp'))
- w_out: bfloat16 [16, 1024, 1024], P(None, ('dp', 'tp'))
- w_gate: bfloat16 [16, 1024, 2816], P(None, ('dp', 'tp'))
- w_up: bfloat16 [16, 1024, 2816], P(None, ('dp', 'tp'))
- w_down: bfloat16 [16, 2816, 1024], P(None, ('dp', 'tp'))
- w_head: bfloat16 [1024, 151936], P(('dp', 'tp'))
Outputs:
- output 1: bfloat16 [16, 3072, 1024], P(None, 'tp')
- output 2: bfloat16 [16, 1024, 1024], P(None, None, 'tp')
- output 3: bfloat16 [16, 5632, 1024], P(None, 'tp')
- output 4: bfloat16 [16, 1024, 2816], P(None, None, 'tp')
- output 5: bfloat16 [151936, 1024], P('tp')
All inputs are finite; a program needn't handle non-finite values.
Results may differ from the reference program's by a relative error of at most 0.001.
Values are sent between devices in bfloat16 or wider.
A program may use at most 1 GiB of HBM per device.

```python
import jax
import jax.numpy as jnp

LAYERS = 16
D = 1024
HEADS = 16
KV_HEADS = 16
HEAD = 64
FF = 2816
VOCAB = 151936
TP = 4

Q_COLS = HEADS * HEAD
KV_COLS = KV_HEADS * HEAD


def draw_matrix(key, shape, fan_in):
    return (jax.random.normal(key, shape, jnp.float32) * fan_in ** -0.5).astype(jnp.bfloat16)


def setup_inputs(seed: int = 0) -> dict:
    sub_keys = jax.random.split(jax.random.key(seed), 8)
    return {
        "w_query": draw_matrix(sub_keys[0], (LAYERS, D, Q_COLS), D),
        "w_key": draw_matrix(sub_keys[1], (LAYERS, D, KV_COLS), D),
        "w_value": draw_matrix(sub_keys[2], (LAYERS, D, KV_COLS), D),
        "w_out": draw_matrix(sub_keys[3], (LAYERS, Q_COLS, D), Q_COLS),
        "w_gate": draw_matrix(sub_keys[4], (LAYERS, D, FF), D),
        "w_up": draw_matrix(sub_keys[5], (LAYERS, D, FF), D),
        "w_down": draw_matrix(sub_keys[6], (LAYERS, FF, D), FF),
        "w_head": draw_matrix(sub_keys[7], (D, VOCAB), D),
    }


def rank_rows(weights):
    layers, in_width, out_width = weights.shape
    return jnp.swapaxes(weights, 1, 2).reshape(layers, TP, out_width // TP, in_width)


def fuse_by_rank(weight_list):
    joined = jnp.concatenate([rank_rows(weights) for weights in weight_list], axis=2)
    return joined.reshape(joined.shape[0], joined.shape[1] * joined.shape[2], joined.shape[3])


def reference(w_query, w_key, w_value, w_out, w_gate, w_up, w_down, w_head):
    return (
        fuse_by_rank([w_query, w_key, w_value]),
        jnp.swapaxes(w_out, 1, 2),
        fuse_by_rank([w_gate, w_up]),
        jnp.swapaxes(w_down, 1, 2),
        jnp.transpose(w_head),
    )
```

```python
import functools

import jax
import jax.numpy as jnp
from jax import lax
from jax.experimental import pallas as pl
from jax.experimental.pallas import tpu as pltpu
from jax.sharding import PartitionSpec as P

MESH = pl.DeviceIdType.MESH
LANES = 128
AHEAD = 4
LAG = 2
SCRATCH_TILES = 3


class Plan:
    def __init__(self, tp, dp, w_query, w_gate, w_out, w_down, w_head):
        self.tp, self.dp = tp, dp
        self.layers, self.rows, columns = w_query.shape
        self.part = columns // tp
        self.wide = w_gate.shape[2] // tp
        self.vocab = w_head.shape[1] // tp
        self.head_tiles = w_head.shape[1] // LANES
        self.chunk = 3 * self.part + 2 * self.wide
        self.wide_window = -(-self.wide // LANES) * LANES
        self.layer_window = 3 * self.part + 2 * self.wide_window
        self.head_chunks = -(-self.vocab // self.chunk)
        self.tail = self.vocab - (self.head_chunks - 1) * self.chunk
        self.chunks = self.layers + self.head_chunks
        self.tail_window = -(-(self.tail + LANES) // LANES) * LANES
        self.window_tiles = (self.head_chunks - 1) * self.chunk // LANES + self.tail_window // LANES
        self.out_rows, self.down_rows = w_out.shape[1], w_down.shape[1]
        self.share = self.layers // dp

    def wide_base(self, rank):
        return (self.wide * rank) // LANES

    def head_base(self, rank):
        base = (self.vocab * rank) // LANES
        return base - (rank // (self.tp - 1)) * (self.vocab * (self.tp - 1) // LANES + self.window_tiles - self.head_tiles)


def gather_kernel(plan, q, k, v, o, g, u, d, h, slabs, outs, downs, zbuf, tbuf, z_recv, z_send, local, x_recv, y_recv,
                  a_recv, b_recv, pair_recv, send, share_recv, share_send):
    z, dp = lax.axis_index("tp"), lax.axis_index("dp")
    core, x, y = dp % 2, (dp // 2) % 2, dp // 4
    x_peer = y * 4 + (1 - x) * 2 + core
    y_peer = (1 - y) * 4 + x * 2 + core
    diagonal = (1 - y) * 4 + (1 - x) * 2 + core
    pair = dp + 1 - 2 * core
    rows, chunk, tail = plan.rows, plan.chunk, plan.tail
    layers, last = plan.layers, plan.chunks - 1
    my_rows = pl.ds(pl.multiple_of(z * rows, rows), rows)

    def lanes(first_tile, width):
        return pl.ds(pl.multiple_of(first_tile * LANES, LANES), width)

    def exchange(pieces, index):
        for step in range(1, plan.tp):
            rank = (z + step) % plan.tp
            for source, column, width in pieces(rank):
                pltpu.make_async_remote_copy(
                    source, zbuf.at[index, my_rows, pl.ds(column, width)], z_send.at[index], z_recv.at[index],
                    device_id={"tp": rank}, device_id_type=MESH,
                ).start()
        for source, column, width in pieces(z):
            pltpu.make_async_copy(source, zbuf.at[index, my_rows, pl.ds(column, width)], z_recv.at[index]).start()

    def layer_pieces(layer):
        def pieces(rank):
            part, wide = plan.part, plan.wide_window
            narrow = lanes(rank * (part // LANES), part)
            window = lanes(plan.wide_base(rank), wide)
            return [
                (q.at[layer, :, narrow], 0, part),
                (k.at[layer, :, narrow], part, part),
                (v.at[layer, :, narrow], 2 * part, part),
                (g.at[layer, :, window], 3 * part, wide),
                (u.at[layer, :, window], 3 * part + wide, wide),
            ]
        return pieces

    def head_pieces(step, width):
        def pieces(rank):
            return [(h.at[:, lanes(plan.head_base(rank) + step * (chunk // LANES), width)], 0, width)]
        return pieces

    def start_exchange(index):
        @pl.when(index < layers)
        def _():
            exchange(layer_pieces(index), index)

        @pl.when((index >= layers) & (index < last))
        def _():
            exchange(head_pieces(index - layers, chunk), index)

        @pl.when(index == last)
        def _():
            exchange(head_pieces(last - layers, plan.tail_window), last)

    def wait_for(ref, sem):
        pltpu.make_async_copy(ref, ref, sem).wait()

    def wait_exchange(index, width):
        wait_for(zbuf.at[index, :, pl.ds(0, width)], z_recv.at[index])

    def turn(slot, tile, index, source_tile):
        tbuf[slot, pl.ds(tile * LANES, LANES), :] = zbuf[index, :, pl.ds(source_tile * LANES, LANES)].T

    def store(slot, first, index, to, count):
        return pltpu.make_async_copy(
            tbuf.at[slot, pl.ds(first, count), :], slabs.at[dp, index, pl.ds(to, count), :], local.at[slot]
        )

    def make_layer(index, slot):
        wait_exchange(index, plan.layer_window)
        for tile in range(plan.layer_window // LANES):
            turn(slot, tile, index, tile)
        shift = plan.wide * z - plan.wide_base(z) * LANES
        narrow, wide, window = 3 * plan.part, plan.wide, plan.wide_window
        store(slot, 0, index, 0, narrow).start()
        store(slot, pl.multiple_of(narrow + shift, 16), index, narrow, wide).start()
        store(slot, pl.multiple_of(narrow + window + shift, 16), index, narrow + wide, wide).start()

    head_shift = plan.vocab * z - plan.head_base(z) * LANES

    def make_head(index, slot):
        @pl.when(index == layers)
        def _():
            wait_exchange(index, chunk)

        @pl.when(index < last - 1)
        def _():
            wait_exchange(index + 1, chunk)

        @pl.when(index == last - 1)
        def _():
            wait_exchange(last, plan.tail_window)

        tiles = chunk // LANES
        for tile in range(tiles):
            turn(slot, tile, index, tile)
        for tile in range(2):
            turn(slot, tiles + tile, index + 1, tile)
        store(slot, pl.multiple_of(head_shift, 16), index, 0, chunk).start()

    def make_tail(slot):
        for tile in range(plan.tail_window // LANES):
            turn(slot, tile, last, tile)
        store(slot, pl.multiple_of(head_shift, 16), last, 0, tail).start()

    def push(owner, index, first, count, recv, to):
        part = slabs.at[owner, index, pl.ds(first, count), :]
        pltpu.make_async_remote_copy(
            part, part, send.at[index], recv.at[index], device_id={"dp": to}, device_id_type=MESH
        ).start()

    def wait_slab(owner, index, first, count, sem):
        wait_for(slabs.at[owner, index, pl.ds(first, count), :], sem.at[index])

    def send_own(index, slot, count):
        wait_for(slabs.at[dp, index, pl.ds(0, count), :], local.at[slot])
        push(dp, index, 0, count, x_recv, x_peer)
        push(dp, index, 0, count, y_recv, y_peer)
        push(dp, index, 0, count, pair_recv, pair)

    def forward(index, count):
        half = count // 2
        wait_slab(x_peer, index, 0, count, x_recv)
        push(x_peer, index, half, half, b_recv, y_peer)
        push(x_peer, index, 0, count, pair_recv, pair)
        wait_slab(y_peer, index, 0, count, y_recv)
        push(y_peer, index, 0, half, a_recv, x_peer)
        push(y_peer, index, 0, count, pair_recv, pair)

    def forward_diagonal(index, count):
        half = count // 2
        wait_slab(diagonal, index, 0, half, a_recv)
        wait_slab(diagonal, index, half, half, b_recv)
        push(diagonal, index, 0, count, pair_recv, pair)

    def finish(index, count, window):
        wait_for(slabs.at[pl.ds(0, 7), index, pl.ds(0, count), :], send.at[index])
        wait_for(slabs.at[pl.ds(0, 4), index, pl.ds(0, count), :], pair_recv.at[index])
        wait_for(zbuf.at[index, pl.ds(0, (plan.tp - 1) * rows), pl.ds(0, window)], z_send.at[index])

    for index in range(AHEAD):
        start_exchange(index)

    rank = dp // 2
    place = (dp % 2) * plan.tp + z
    stays = rank == z
    shares = ((d, downs, plan.down_rows), (o, outs, plan.out_rows))
    for step in range(plan.dp):
        to = (dp + step) % plan.dp
        for n, (source, target, count) in enumerate(shares):
            piece = source.at[pl.ds(to * plan.share, plan.share), :, :]
            landing = target.at[:, pl.ds(pl.multiple_of(place * count, 8), count), :]

            def start_remote(piece=piece, landing=landing, n=n, to=to):
                pltpu.make_async_remote_copy(
                    piece, landing, share_send.at[n], share_recv.at[n],
                    device_id={"dp": to, "tp": rank}, device_id_type=MESH,
                ).start()

            if step:
                start_remote()
            else:
                pl.when(jnp.logical_not(stays))(start_remote)

                @pl.when(stays)
                def _(piece=piece, landing=landing, n=n):
                    pltpu.make_async_copy(piece, landing, share_recv.at[n]).start()

    def step(index, _):
        slot = index % 2

        @pl.when(index + AHEAD < plan.chunks)
        def _():
            start_exchange(index + AHEAD)

        @pl.when(index < layers)
        def _():
            make_layer(index, slot)

        @pl.when(index >= layers)
        def _():
            make_head(index, slot)

        send_own(index, slot, chunk)

        @pl.when(index >= LAG)
        def _():
            forward(index - LAG, chunk)

        @pl.when(index >= 2 * LAG)
        def _():
            forward_diagonal(index - 2 * LAG, chunk)

        return 0

    lax.fori_loop(0, last, step, 0)
    make_tail(last % 2)
    send_own(last, last % 2, tail)
    for index in range(last - LAG, last):
        forward(index, chunk)
    forward(last, tail)
    for index in range(last - 2 * LAG, last):
        forward_diagonal(index, chunk)
    forward_diagonal(last, tail)

    def drain(index, _):
        @pl.when(index < layers)
        def _():
            finish(index, chunk, plan.layer_window)

        @pl.when(index >= layers)
        def _():
            finish(index, chunk, chunk)

        return 0

    lax.fori_loop(0, last, drain, 0)
    finish(last, tail, plan.tail_window)
    for n, (_, target, count) in enumerate(shares):
        wait_for(target, share_recv.at[n])
        wait_for(target.at[:, pl.ds(0, (plan.dp - 1) * count), :], share_send.at[n])

        @pl.when(jnp.logical_not(stays))
        def _(target=target, count=count, n=n):
            wait_for(target.at[:, pl.ds(0, count), :], share_send.at[n])


def gather(plan, *args):
    dma = pltpu.SemaphoreType.DMA
    per_chunk = dma((plan.chunks,))
    columns = args[3].shape[2]
    hbm = pl.BlockSpec(memory_space=pltpu.HBM)
    return pl.pallas_call(
        functools.partial(gather_kernel, plan),
        out_shape=(
            jax.ShapeDtypeStruct((plan.dp, plan.chunks, plan.chunk, LANES), jnp.bfloat16),
            jax.ShapeDtypeStruct((plan.share, 8 * plan.out_rows, columns), jnp.bfloat16),
            jax.ShapeDtypeStruct((plan.share, 8 * plan.down_rows, columns), jnp.bfloat16),
        ),
        in_specs=[hbm] * 8,
        out_specs=(hbm,) * 3,
        scratch_shapes=[
            pltpu.VMEM((plan.chunks, plan.tp * plan.rows, plan.layer_window), jnp.bfloat16),
            pltpu.VMEM((2, plan.chunk + 2 * LANES, LANES), jnp.bfloat16),
            per_chunk, per_chunk, dma((2,)),
            per_chunk, per_chunk, per_chunk, per_chunk, per_chunk, per_chunk,
            dma((2,)), dma((2,)),
        ],
        compiler_params=pltpu.CompilerParams(has_side_effects=True),
        name="gather",
    )(*args)


def place_layers(plan, slabs):
    narrow, wide = 3 * plan.part, 2 * plan.wide

    def body(slab, qkv, gate_up):
        for i in range(plan.dp):
            lanes = pl.ds(i * LANES, LANES)
            qkv[0, :, lanes] = slab[i, 0, :narrow, :]
            gate_up[0, :, lanes] = slab[i, 0, narrow:, :]

    width = plan.dp * LANES
    bytes_moved = 4 * plan.layers * plan.chunk * width
    return pl.pallas_call(
        body,
        grid=(plan.layers,),
        in_specs=[pl.BlockSpec((plan.dp, 1, plan.chunk, LANES), lambda i: (0, i, 0, 0))],
        out_specs=(
            pl.BlockSpec((1, narrow, width), lambda i: (i, 0, 0)),
            pl.BlockSpec((1, wide, width), lambda i: (i, 0, 0)),
        ),
        out_shape=(
            jax.ShapeDtypeStruct((plan.layers, narrow, width), jnp.bfloat16),
            jax.ShapeDtypeStruct((plan.layers, wide, width), jnp.bfloat16),
        ),
        cost_estimate=pl.CostEstimate(flops=10**10, bytes_accessed=bytes_moved, transcendentals=0),
        name="place_layers",
    )(slabs)


def place_head(plan, slabs):
    def body(slab, head):
        for i in range(plan.dp):
            head[:, pl.ds(i * LANES, LANES)] = slab[i, 0]

    width = plan.dp * LANES
    return pl.pallas_call(
        body,
        grid=(plan.head_chunks,),
        in_specs=[pl.BlockSpec((plan.dp, 1, plan.chunk, LANES), lambda i: (0, plan.layers + i, 0, 0))],
        out_specs=pl.BlockSpec((plan.chunk, width), lambda i: (i, 0)),
        out_shape=jax.ShapeDtypeStruct((plan.vocab, width), jnp.bfloat16),
        cost_estimate=pl.CostEstimate(flops=10**10, bytes_accessed=4 * plan.vocab * width, transcendentals=0),
        name="place_head",
    )(slabs)


def solution(mesh):
    train_stack = P(None, ("dp", "tp"), None)
    train_head = P(("dp", "tp"), None)
    fused_stack = P(None, "tp", None)
    last_stack = P(None, None, "tp")
    head_rows = P("tp", None)

    def local_sync(w_query, w_key, w_value, w_out, w_gate, w_up, w_down, w_head):
        plan = Plan(mesh.shape["tp"], mesh.shape["dp"], w_query, w_gate, w_out, w_down, w_head)
        slabs, outs, downs = gather(plan, w_query, w_key, w_value, w_out, w_gate, w_up, w_down, w_head)
        o_block = lax.all_gather(outs, "dp", axis=0, tiled=True)
        down_block = lax.all_gather(downs, "dp", axis=0, tiled=True)
        qkv_block, gate_up_block = place_layers(plan, slabs)
        head_block = place_head(plan, slabs)
        return (
            qkv_block,
            jnp.swapaxes(o_block, 1, 2),
            gate_up_block,
            jnp.swapaxes(down_block, 1, 2),
            head_block,
        )

    return jax.shard_map(
        local_sync,
        mesh=mesh,
        in_specs=(train_stack,) * 7 + (train_head,),
        out_specs=(fused_stack, last_stack, fused_stack, last_stack, head_rows),
        check_vma=False,
    )
```

```python
import functools

import jax
import jax.numpy as jnp
from jax import lax
from jax.experimental import pallas as pl
from jax.experimental.pallas import tpu as pltpu
from jax.sharding import PartitionSpec as P

MESH = pl.DeviceIdType.MESH
LANES = 128
VMEM = 67_000_000
AHEAD = 4
LAG = 2
SHARE_AT = 3


class Plan:
    def __init__(self, tp, dp, w_query, w_gate, w_out, w_down, w_head):
        self.tp, self.dp = tp, dp
        self.layers, self.rows, columns = w_query.shape
        self.part = columns // tp
        self.wide = w_gate.shape[2] // tp
        self.vocab = w_head.shape[1] // tp
        self.head_tiles = w_head.shape[1] // LANES
        self.chunk = 3 * self.part + 2 * self.wide
        self.wide_window = -(-self.wide // LANES) * LANES
        self.layer_window = 3 * self.part + 2 * self.wide_window
        self.head_chunks = -(-self.vocab // self.chunk)
        self.tail = self.vocab - (self.head_chunks - 1) * self.chunk
        self.chunks = self.layers + self.head_chunks
        self.tail_window = -(-(self.tail + LANES) // LANES) * LANES
        self.window_tiles = (self.head_chunks - 1) * self.chunk // LANES + self.tail_window // LANES
        self.out_rows, self.down_rows = w_out.shape[1], w_down.shape[1]
        self.share = self.layers // dp

    def wide_base(self, rank):
        return (self.wide * rank) // LANES

    def head_base(self, rank):
        base = (self.vocab * rank) // LANES
        return base - (rank // (self.tp - 1)) * (self.vocab * (self.tp - 1) // LANES + self.window_tiles - self.head_tiles)


def gather_kernel(plan, q, k, v, o, g, u, d, h, slabs, turned, down_0, down_1, outs, down_stop, out_stop, zbuf, tbuf, obuf,
                  otbuf, z_recv, z_send, local, x_recv, y_recv, a_recv, b_recv, pair_recv, send, stop_recv, share_recv,
                  share_send, out_load):
    z, dp = lax.axis_index("tp"), lax.axis_index("dp")
    core, x, y = dp % 2, (dp // 2) % 2, dp // 4
    x_peer = y * 4 + (1 - x) * 2 + core
    y_peer = (1 - y) * 4 + x * 2 + core
    diagonal = (1 - y) * 4 + (1 - x) * 2 + core
    pair = dp + 1 - 2 * core
    rows, chunk, tail = plan.rows, plan.chunk, plan.tail
    layers, last = plan.layers, plan.chunks - 1
    my_rows = pl.ds(pl.multiple_of(z * rows, rows), rows)

    def lanes(first_tile, width):
        return pl.ds(pl.multiple_of(first_tile * LANES, LANES), width)

    def remote(source, target, send_sem, recv_sem, **to):
        pltpu.make_async_remote_copy(source, target, send_sem, recv_sem, device_id=to, device_id_type=MESH).start()

    def wait_for(ref, sem):
        pltpu.make_async_copy(ref, ref, sem).wait()


    def exchange(pieces, index):
        for step in range(1, plan.tp):
            rank = (z + step) % plan.tp
            for source, column, width in pieces(rank):
                target = zbuf.at[index, my_rows, pl.ds(column, width)]
                remote(source, target, z_send.at[index], z_recv.at[index], tp=rank)
        for source, column, width in pieces(z):
            pltpu.make_async_copy(source, zbuf.at[index, my_rows, pl.ds(column, width)], z_recv.at[index]).start()

    def layer_pieces(layer):
        def pieces(rank):
            part, wide = plan.part, plan.wide_window
            narrow = lanes(rank * (part // LANES), part)
            window = lanes(plan.wide_base(rank), wide)
            return [
                (q.at[layer, :, narrow], 0, part),
                (k.at[layer, :, narrow], part, part),
                (v.at[layer, :, narrow], 2 * part, part),
                (g.at[layer, :, window], 3 * part, wide),
                (u.at[layer, :, window], 3 * part + wide, wide),
            ]
        return pieces

    def head_pieces(step, width):
        def pieces(rank):
            return [(h.at[:, lanes(plan.head_base(rank) + step * (chunk // LANES), width)], 0, width)]
        return pieces

    def start_exchange(index):
        @pl.when(index < layers)
        def _():
            exchange(layer_pieces(index), index)

        @pl.when((index >= layers) & (index < last))
        def _():
            exchange(head_pieces(index - layers, chunk), index)

        @pl.when(index == last)
        def _():
            exchange(head_pieces(last - layers, plan.tail_window), last)

    def wait_exchange(index, width):
        wait_for(zbuf.at[index, :, pl.ds(0, width)], z_recv.at[index])


    def turn(slot, tile, index, source_tile):
        tbuf[slot, pl.ds(tile * LANES, LANES), :] = zbuf[index, :, pl.ds(source_tile * LANES, LANES)].T

    def store(slot, first, index, to, count):
        pltpu.make_async_copy(
            tbuf.at[slot, pl.ds(first, count), :], slabs.at[dp, index, pl.ds(to, count), :], local.at[slot]
        ).start()

    def make_layer(index, slot):
        wait_exchange(index, plan.layer_window)
        for tile in range(plan.layer_window // LANES):
            turn(slot, tile, index, tile)
        shift = plan.wide * z - plan.wide_base(z) * LANES
        narrow, wide, window = 3 * plan.part, plan.wide, plan.wide_window
        store(slot, 0, index, 0, narrow)
        store(slot, pl.multiple_of(narrow + shift, 16), index, narrow, wide)
        store(slot, pl.multiple_of(narrow + window + shift, 16), index, narrow + wide, wide)

    head_shift = plan.vocab * z - plan.head_base(z) * LANES

    def make_head(index, slot):
        @pl.when(index == layers)
        def _():
            wait_exchange(index, chunk)

        @pl.when(index < last - 1)
        def _():
            wait_exchange(index + 1, chunk)

        @pl.when(index == last - 1)
        def _():
            wait_exchange(last, plan.tail_window)

        tiles = chunk // LANES
        for tile in range(tiles):
            turn(slot, tile, index, tile)
        for tile in range(2):
            turn(slot, tiles + tile, index + 1, tile)
        store(slot, pl.multiple_of(head_shift, 16), index, 0, chunk)

    def make_tail(slot):
        for tile in range(plan.tail_window // LANES):
            turn(slot, tile, last, tile)
        store(slot, pl.multiple_of(head_shift, 16), last, 0, tail)

    def make_out(layer):
        for i in range(plan.tp * 2 * plan.out_rows // LANES):
            for j in range(plan.dp):
                otbuf[layer, pl.ds(j * LANES, LANES), pl.ds(i * LANES, LANES)] = obuf[
                    layer, pl.ds(i * LANES, LANES), pl.ds(j * LANES, LANES)
                ].T
        pltpu.make_async_copy(otbuf.at[layer], turned.at[dp, layer], local.at[layer % 2]).start()


    def slab_view(index):
        return lambda owner, first, count: slabs.at[owner, index, pl.ds(first, count), :]

    def out_view(layer):
        return lambda owner, first, count: turned.at[owner, layer, pl.ds(first, count), :]

    def push(part, index, recv, to):
        remote(part, part, send.at[index], recv.at[index], dp=to)

    def send_own(view, index, slot, count):
        own = view(dp, 0, count)
        wait_for(own, local.at[slot])
        push(own, index, x_recv, x_peer)
        push(own, index, y_recv, y_peer)
        push(own, index, pair_recv, pair)

    def forward(view, index, count):
        half = count // 2
        wait_for(view(x_peer, 0, count), x_recv.at[index])
        push(view(x_peer, half, half), index, b_recv, y_peer)
        push(view(x_peer, 0, count), index, pair_recv, pair)
        wait_for(view(y_peer, 0, count), y_recv.at[index])
        push(view(y_peer, 0, half), index, a_recv, x_peer)
        push(view(y_peer, 0, count), index, pair_recv, pair)

    def forward_diagonal(view, index, count):
        half = count // 2
        wait_for(view(diagonal, 0, half), a_recv.at[index])
        wait_for(view(diagonal, half, half), b_recv.at[index])
        push(view(diagonal, 0, count), index, pair_recv, pair)

    def finish(view, index, count):
        wait_for(view(pl.ds(0, 7), 0, count), send.at[index])
        wait_for(view(pl.ds(0, 4), 0, count), pair_recv.at[index])

    def finish_exchange(index, window):
        wait_for(zbuf.at[index, pl.ds(0, (plan.tp - 1) * rows), pl.ds(0, window)], z_send.at[index])


    def pieces(source_dp, to, place):
        home = pl.ds(pl.multiple_of(place * plan.down_rows, 8), plan.down_rows)
        out_home = pl.ds(pl.multiple_of(place * plan.out_rows, 8), plan.out_rows)
        return [
            (d.at[to * plan.share], down_stop.at[source_dp, 0], down_0.at[home, :], 0),
            (d.at[to * plan.share + plan.share - 1], down_stop.at[source_dp, 1], down_1.at[home, :], 1),
            (o.at[pl.ds(to * plan.share, plan.share), :, :], out_stop.at[source_dp], outs.at[:, out_home, :], 2),
        ]

    my_rank = dp // 2
    my_place = (dp % 2) * plan.tp + z
    stays = my_rank == z

    def share_in_plane():
        for step in range(1, plan.dp):
            to = (dp + step) % plan.dp

            @pl.when(stays)
            def _(to=to):
                for part, _, final, n in pieces(dp, to, my_place):
                    remote(part, final, share_send.at[n], share_recv.at[n], dp=to)

            @pl.when(jnp.logical_not(stays))
            def _(to=to):
                for part, stop, _, n in pieces(dp, to, my_place):
                    remote(part, stop, share_send.at[n], stop_recv.at[n, dp], dp=to)

        @pl.when(stays)
        def _():
            for part, _, final, n in pieces(dp, dp, my_place):
                pltpu.make_async_copy(part, final, share_recv.at[n]).start()

    def share_to_rank(source_dp):
        rank, place = source_dp // 2, (source_dp % 2) * plan.tp + z

        @pl.when((rank != z) & (source_dp == dp))
        def _():
            for part, _, final, n in pieces(dp, dp, place):
                remote(part, final, share_send.at[n], share_recv.at[n], tp=rank)

        @pl.when((rank != z) & (source_dp != dp))
        def _():
            for _, stop, final, n in pieces(source_dp, dp, place):
                wait_for(stop, stop_recv.at[n, source_dp])
                remote(stop, final, share_send.at[n], share_recv.at[n], tp=rank)

    for index in range(2):
        start_exchange(index)
    share_in_plane()
    for index in range(2, AHEAD):
        start_exchange(index)

    def step(index, _):
        slot = index % 2

        @pl.when(index + AHEAD < plan.chunks)
        def _():
            start_exchange(index + AHEAD)

        @pl.when((index >= SHARE_AT) & (index < SHARE_AT + plan.dp))
        def _():
            share_to_rank(index - SHARE_AT)

        @pl.when(index < layers)
        def _():
            make_layer(index, slot)

        @pl.when(index >= layers)
        def _():
            make_head(index, slot)

        send_own(slab_view(index), index, slot, chunk)

        @pl.when(index >= LAG)
        def _():
            forward(slab_view(index - LAG), index - LAG, chunk)

        @pl.when(index >= 2 * LAG)
        def _():
            forward_diagonal(slab_view(index - 2 * LAG), index - 2 * LAG, chunk)

        return 0

    lax.fori_loop(0, last, step, 0)

    wait_for(outs, share_recv.at[2])
    load = pltpu.make_async_copy(outs, obuf, out_load)
    load.start()
    load.wait()
    final = [(out_view(i), plan.chunks + i, otbuf.shape[1], functools.partial(make_out, i)) for i in range(plan.share)]
    final.append((slab_view(last), last, tail, functools.partial(make_tail, plan.share % 2)))
    ended = [(slab_view(i), i, chunk) for i in range(last - 2 * LAG, last)] + [f[:3] for f in final]
    forwards, diagonals = ended[LAG:], list(ended)
    for slot, (view, index, count, make) in enumerate(final):
        make()
        send_own(view, index, slot % 2, count)
        forward(*forwards.pop(0))
        forward_diagonal(*diagonals.pop(0))
    for item in forwards:
        forward(*item)
    for item in diagonals:
        forward_diagonal(*item)

    def drain(index, _):
        finish(slab_view(index), index, chunk)

        @pl.when(index < layers)
        def _():
            finish_exchange(index, plan.layer_window)

        @pl.when(index >= layers)
        def _():
            finish_exchange(index, chunk)

        return 0

    lax.fori_loop(0, last, drain, 0)
    finish_exchange(last, plan.tail_window)
    for view, index, count, _ in final:
        finish(view, index, count)
    for n, target in enumerate((down_0, down_1)):
        wait_for(target, share_recv.at[n])
    for n, (target, count) in enumerate(((down_0, plan.down_rows), (down_1, plan.down_rows), (outs, plan.out_rows))):
        for parts in (8, 5):
            part = pl.ds(0, parts * count)
            wait_for(target.at[:, part, :] if n == 2 else target.at[part, :], share_send.at[n])


def gather(plan, *args):
    dma = pltpu.SemaphoreType.DMA
    per_chunk = dma((plan.chunks + plan.share,))
    columns = args[3].shape[2]
    out_rows, down_rows = plan.out_rows, plan.down_rows
    hbm = pl.BlockSpec(memory_space=pltpu.HBM)
    shapes = [
        (plan.dp, plan.chunks, plan.chunk, LANES),
        (plan.dp, plan.share, columns, 8 * out_rows),
        (8 * down_rows, columns),
        (8 * down_rows, columns),
        (plan.share, 8 * out_rows, columns),
        (plan.dp, 2, down_rows, columns),
        (plan.dp, plan.share, out_rows, columns),
    ]
    return pl.pallas_call(
        functools.partial(gather_kernel, plan),
        out_shape=[jax.ShapeDtypeStruct(shape, jnp.bfloat16) for shape in shapes],
        in_specs=[hbm] * 8,
        out_specs=[hbm] * len(shapes),
        scratch_shapes=[
            pltpu.VMEM((plan.chunks, plan.tp * plan.rows, plan.layer_window), jnp.bfloat16),
            pltpu.VMEM((2, plan.chunk + 2 * LANES, LANES), jnp.bfloat16),
            pltpu.VMEM((plan.share, 8 * out_rows, columns), jnp.bfloat16),
            pltpu.VMEM((plan.share, columns, 8 * out_rows), jnp.bfloat16),
            per_chunk, per_chunk, dma((2,)),
            per_chunk, per_chunk, per_chunk, per_chunk, per_chunk, per_chunk,
            dma((3, plan.dp)), dma((3,)), dma((3,)), dma,
        ],
        compiler_params=pltpu.CompilerParams(has_side_effects=True),
        name="gather",
    )(*args)[:4]


def place_layers(plan, slabs):
    narrow, wide = 3 * plan.part, 2 * plan.wide

    def body(slab, qkv, gate_up):
        for i in range(plan.dp):
            lanes = pl.ds(i * LANES, LANES)
            qkv[0, :, lanes] = slab[i, 0, :narrow, :]
            gate_up[0, :, lanes] = slab[i, 0, narrow:, :]

    width = plan.dp * LANES
    bytes_moved = 4 * plan.layers * plan.chunk * width
    return pl.pallas_call(
        body,
        grid=(plan.layers,),
        in_specs=[pl.BlockSpec((plan.dp, 1, plan.chunk, LANES), lambda i: (0, i, 0, 0))],
        out_specs=(
            pl.BlockSpec((1, narrow, width), lambda i: (i, 0, 0)),
            pl.BlockSpec((1, wide, width), lambda i: (i, 0, 0)),
        ),
        out_shape=(
            jax.ShapeDtypeStruct((plan.layers, narrow, width), jnp.bfloat16),
            jax.ShapeDtypeStruct((plan.layers, wide, width), jnp.bfloat16),
        ),
        cost_estimate=pl.CostEstimate(flops=10**10, bytes_accessed=bytes_moved, transcendentals=0),
        compiler_params=pltpu.CompilerParams(vmem_limit_bytes=VMEM),
        name="place_layers",
    )(slabs)


def place_head(plan, slabs, first, count, head=None):
    def body(slab, *rest):
        for i in range(plan.dp):
            rest[-1][:, pl.ds(i * LANES, LANES)] = slab[i, 0]

    width = plan.dp * LANES
    return pl.pallas_call(
        body,
        grid=(count,),
        in_specs=[pl.BlockSpec((plan.dp, 1, plan.chunk, LANES), lambda i: (0, plan.layers + first + i, 0, 0))]
        + ([] if head is None else [pl.BlockSpec(memory_space=pltpu.HBM)]),
        out_specs=pl.BlockSpec((plan.chunk, width), lambda i: (first + i, 0)),
        out_shape=jax.ShapeDtypeStruct((plan.vocab, width), jnp.bfloat16),
        input_output_aliases={} if head is None else {1: 0},
        cost_estimate=pl.CostEstimate(flops=10**10, bytes_accessed=4 * count * plan.chunk * width, transcendentals=0),
        compiler_params=pltpu.CompilerParams(vmem_limit_bytes=VMEM),
        name="place_head" if head is None else "place_head_end",
    )(slabs, *([] if head is None else [head]))


def place_pieces(plan, pieces, total, outs=None):
    owners = list(pieces)
    arrays = [array for owner in owners for array in pieces[owner]]
    shape = arrays[0].shape

    def body(*refs):
        sources, target = refs[: len(arrays)], refs[len(arrays) + (outs is not None)]
        buffers, loads, stores = refs[-3:]
        dp = lax.axis_index("dp")
        core, x, y = dp % 2, (dp // 2) % 2, dp // 4

        def layer(owner):
            flip_x, flip_y, flip_core = owner
            at = (y + flip_y * (1 - 2 * y)) * 4 + (x + flip_x * (1 - 2 * x)) * 2 + core + flip_core * (1 - 2 * core)
            return at * plan.share

        moves = []
        for n, source in enumerate(sources):
            moves.append((
                pltpu.make_async_copy(source, buffers.at[n], loads.at[n]),
                pltpu.make_async_copy(
                    buffers.at[n], target.at[layer(owners[n // plan.share]) + n % plan.share], stores.at[n]
                ),
            ))
            moves[-1][0].start()
        for load, store in moves:
            load.wait()
            store.start()
        for _, store in moves:
            store.wait()

    hbm = pl.BlockSpec(memory_space=pltpu.HBM)
    operands = arrays + ([outs] if outs is not None else [])
    return pl.pallas_call(
        body,
        out_shape=jax.ShapeDtypeStruct((total, *shape), jnp.bfloat16),
        in_specs=[hbm] * len(operands),
        out_specs=hbm,
        scratch_shapes=[
            pltpu.VMEM((len(arrays), *shape), jnp.bfloat16),
            pltpu.SemaphoreType.DMA((len(arrays),)),
            pltpu.SemaphoreType.DMA((len(arrays),)),
        ],
        input_output_aliases={len(arrays): 0} if outs is not None else {},
        cost_estimate=pl.CostEstimate(
            flops=10**9, bytes_accessed=4 * len(arrays) * shape[0] * shape[1], transcendentals=0
        ),
        compiler_params=pltpu.CompilerParams(vmem_limit_bytes=VMEM),
        name="place_down" + ("_end" if outs is not None else ""),
    )(*operands)


def place_out(plan, turned):
    _, share, height, width = turned.shape

    def body(block, out):
        out[...] = block[0]

    return pl.pallas_call(
        body,
        grid=(plan.dp,),
        in_specs=[pl.BlockSpec((1, share, height, width), lambda i: (i, 0, 0, 0))],
        out_specs=pl.BlockSpec((share, height, width), lambda i: (i, 0, 0)),
        out_shape=jax.ShapeDtypeStruct((plan.dp * share, height, width), jnp.bfloat16),
        cost_estimate=pl.CostEstimate(flops=10**9, bytes_accessed=4 * turned.size, transcendentals=0),
        name="place_out",
    )(turned)


def solution(mesh):
    train_stack = P(None, ("dp", "tp"), None)
    train_head = P(("dp", "tp"), None)
    fused_stack = P(None, "tp", None)
    last_stack = P(None, None, "tp")
    head_rows = P("tp", None)

    def local_sync(w_query, w_key, w_value, w_out, w_gate, w_up, w_down, w_head):
        plan = Plan(mesh.shape["tp"], mesh.shape["dp"], w_query, w_gate, w_out, w_down, w_head)
        slabs, turned, own_0, own_1 = gather(plan, w_query, w_key, w_value, w_out, w_gate, w_up, w_down, w_head)

        def swap(bit, array):
            return lax.ppermute(array, "dp", [(i, i ^ bit) for i in range(plan.dp)])

        pair, along_x, along_y = (functools.partial(swap, bit) for bit in (1, 2, 4))
        hold = lax.optimization_barrier

        x_1, y_0 = along_x(own_1), along_y(own_0)
        x_0, y_1 = along_x(own_0), along_y(own_1)
        pair_own = [pair(own_0), pair(own_1)]
        qkv_block, gate_up_block = place_layers(plan, slabs)
        x_1, y_0, qkv_block, slabs = hold((x_1, y_0, qkv_block, slabs))
        diagonal = [along_x(y_0), along_y(x_1)]
        pair_x_1, pair_y_0 = pair(x_1), pair(y_0)
        early = plan.head_chunks // 2
        head_block = place_head(plan, slabs, early, plan.head_chunks - early)
        x_0, y_1, head_block, slabs, turned = hold((x_0, y_1, head_block, slabs, turned))
        pair_x_0, pair_y_1 = pair(x_0), pair(y_1)
        head_block = place_head(plan, slabs, 0, early, head_block)
        o_block = place_out(plan, turned)
        *diagonal, head_block, o_block = hold((*diagonal, head_block, o_block))
        pair_diagonal = [pair(array) for array in diagonal]
        near = {
            (0, 0, 0): [own_0, own_1], (0, 0, 1): pair_own, (1, 0, 0): [x_0, x_1], (1, 0, 1): [pair_x_0, pair_x_1],
            (0, 1, 0): [y_0, y_1], (0, 1, 1): [pair_y_0, pair_y_1],
        }
        down_block = place_pieces(plan, near, plan.layers)
        down_block = place_pieces(plan, {(1, 1, 0): diagonal, (1, 1, 1): pair_diagonal}, plan.layers, down_block)
        return (
            qkv_block,
            o_block,
            gate_up_block,
            jnp.swapaxes(down_block, 1, 2),
            head_block,
        )

    return jax.shard_map(
        local_sync,
        mesh=mesh,
        in_specs=(train_stack,) * 7 + (train_head,),
        out_specs=(fused_stack, last_stack, fused_stack, last_stack, head_rows),
        check_vma=False,
    )
```

```python
import functools

import jax
import jax.numpy as jnp
from jax import lax
from jax.experimental import pallas as pl
from jax.experimental.pallas import tpu as pltpu
from jax.sharding import PartitionSpec as P

MESH = pl.DeviceIdType.MESH
LANES = 128
VMEM = 67_000_000
AHEAD = 4
BUFFERS = 6
LAG = 2
SHARE_AT = 3


class Plan:
    def __init__(self, tp, dp, w_query, w_gate, w_out, w_down, w_head):
        self.tp, self.dp = tp, dp
        self.layers, self.rows, columns = w_query.shape
        self.part = columns // tp
        self.wide = w_gate.shape[2] // tp
        self.vocab = w_head.shape[1] // tp
        self.head_tiles = w_head.shape[1] // LANES
        self.chunk = 3 * self.part + 2 * self.wide
        self.wide_window = -(-self.wide // LANES) * LANES
        self.layer_window = 3 * self.part + 2 * self.wide_window
        self.head_chunks = -(-self.vocab // self.chunk)
        self.tail = self.vocab - (self.head_chunks - 1) * self.chunk
        self.chunks = self.layers + self.head_chunks
        self.tail_window = -(-(self.tail + LANES) // LANES) * LANES
        self.window_tiles = (self.head_chunks - 1) * self.chunk // LANES + self.tail_window // LANES
        self.out_rows, self.down_rows = w_out.shape[1], w_down.shape[1]
        self.share = self.layers // dp

    def wide_base(self, rank):
        return (self.wide * rank) // LANES

    def head_base(self, rank):
        base = (self.vocab * rank) // LANES
        return base - (rank // (self.tp - 1)) * (self.vocab * (self.tp - 1) // LANES + self.window_tiles - self.head_tiles)


def gather_kernel(plan, q, k, v, o, g, u, d, h, slabs, own_0, own_1, stop_0, stop_1, zbuf, tbuf, z_recv, z_send,
                  local, x_recv, y_recv, a_recv, b_recv, pair_recv, send, stop_recv, share_recv, share_send):
    z, dp = lax.axis_index("tp"), lax.axis_index("dp")
    core, x, y = dp % 2, (dp // 2) % 2, dp // 4
    x_peer = y * 4 + (1 - x) * 2 + core
    y_peer = (1 - y) * 4 + x * 2 + core
    diagonal = (1 - y) * 4 + (1 - x) * 2 + core
    pair = dp + 1 - 2 * core
    rows, chunk, tail = plan.rows, plan.chunk, plan.tail
    layers, last = plan.layers, plan.chunks - 1
    my_rows = pl.ds(pl.multiple_of(z * rows, rows), rows)

    def lanes(first_tile, width):
        return pl.ds(pl.multiple_of(first_tile * LANES, LANES), width)

    def remote(source, target, send_sem, recv_sem, **to):
        pltpu.make_async_remote_copy(source, target, send_sem, recv_sem, device_id=to, device_id_type=MESH).start()

    def wait_for(ref, sem):
        pltpu.make_async_copy(ref, ref, sem).wait()


    def exchange(pieces, index):
        for step in range(1, plan.tp):
            rank = (z + step) % plan.tp
            for source, column, width in pieces(rank):
                target = zbuf.at[index, my_rows, pl.ds(column, width)]
                remote(source, target, z_send.at[index], z_recv.at[index], tp=rank)
        for source, column, width in pieces(z):
            pltpu.make_async_copy(source, zbuf.at[index, my_rows, pl.ds(column, width)], z_recv.at[index]).start()

    def layer_pieces(layer):
        def pieces(rank):
            part, wide = plan.part, plan.wide_window
            narrow = lanes(rank * (part // LANES), part)
            window = lanes(plan.wide_base(rank), wide)
            return [
                (q.at[layer, :, narrow], 0, part),
                (k.at[layer, :, narrow], part, part),
                (v.at[layer, :, narrow], 2 * part, part),
                (g.at[layer, :, window], 3 * part, wide),
                (u.at[layer, :, window], 3 * part + wide, wide),
            ]
        return pieces

    def head_pieces(step, width):
        def pieces(rank):
            return [(h.at[:, lanes(plan.head_base(rank) + step * (chunk // LANES), width)], 0, width)]
        return pieces

    def start_exchange(index):
        @pl.when(index < layers)
        def _():
            exchange(layer_pieces(index), index)

        @pl.when((index >= layers) & (index < last))
        def _():
            exchange(head_pieces(index - layers, chunk), index)

        @pl.when(index == last)
        def _():
            exchange(head_pieces(last - layers, plan.tail_window), last)

    def wait_exchange(index, width):
        with jax.named_scope("zwait"):
            wait_for(zbuf.at[index, :, pl.ds(0, width)], z_recv.at[index])


    def turn(slot, tile, index, source_tile):
        tbuf[slot, pl.ds(tile * LANES, LANES), :] = zbuf[index, :, pl.ds(source_tile * LANES, LANES)].T

    def store(slot, first, index, to, count):
        pltpu.make_async_copy(
            tbuf.at[slot, pl.ds(first, count), :], slabs.at[dp, index, pl.ds(to, count), :], local.at[slot]
        ).start()

    def make_layer(index, slot):
        wait_exchange(index, plan.layer_window)
        for tile in range(plan.layer_window // LANES):
            turn(slot, tile, index, tile)
        shift = plan.wide * z - plan.wide_base(z) * LANES
        narrow, wide, window = 3 * plan.part, plan.wide, plan.wide_window
        store(slot, 0, index, 0, narrow)
        store(slot, pl.multiple_of(narrow + shift, 16), index, narrow, wide)
        store(slot, pl.multiple_of(narrow + window + shift, 16), index, narrow + wide, wide)

    head_shift = plan.vocab * z - plan.head_base(z) * LANES

    def make_head(index, slot):
        @pl.when(index == layers)
        def _():
            wait_exchange(index, chunk)

        @pl.when(index < last - 1)
        def _():
            wait_exchange(index + 1, chunk)

        @pl.when(index == last - 1)
        def _():
            wait_exchange(last, plan.tail_window)

        tiles = chunk // LANES
        for tile in range(tiles):
            turn(slot, tile, index, tile)
        for tile in range(2):
            turn(slot, tiles + tile, index + 1, tile)
        store(slot, pl.multiple_of(head_shift, 16), index, 0, chunk)

    def make_tail(slot):
        for tile in range(plan.tail_window // LANES):
            turn(slot, tile, last, tile)
        store(slot, pl.multiple_of(head_shift, 16), last, 0, tail)


    def slab_view(index):
        return lambda owner, first, count: slabs.at[owner, index, pl.ds(first, count), :]

    def push(part, index, recv, to):
        remote(part, part, send.at[index], recv.at[index], dp=to)

    def send_own(view, index, slot, count):
        own = view(dp, 0, count)
        with jax.named_scope("lwait"):
            wait_for(own, local.at[slot])
        push(own, index, x_recv, x_peer)
        push(own, index, y_recv, y_peer)
        push(own, index, pair_recv, pair)

    def forward(view, index, count):
        half = count // 2
        with jax.named_scope("xwait"):
            wait_for(view(x_peer, 0, count), x_recv.at[index])
        push(view(x_peer, half, half), index, b_recv, y_peer)
        push(view(x_peer, 0, count), index, pair_recv, pair)
        with jax.named_scope("ywait"):
            wait_for(view(y_peer, 0, count), y_recv.at[index])
        push(view(y_peer, 0, half), index, a_recv, x_peer)
        push(view(y_peer, 0, count), index, pair_recv, pair)

    def forward_diagonal(view, index, count):
        half = count // 2
        with jax.named_scope("await"):
            wait_for(view(diagonal, 0, half), a_recv.at[index])
        with jax.named_scope("bwait"):
            wait_for(view(diagonal, half, half), b_recv.at[index])
        push(view(diagonal, 0, count), index, pair_recv, pair)

    def finish(view, index, count):
        wait_for(view(pl.ds(0, 7), 0, count), send.at[index])
        wait_for(view(pl.ds(0, 4), 0, count), pair_recv.at[index])

    def finish_exchange(index, window):
        wait_for(zbuf.at[index, pl.ds(0, (plan.tp - 1) * rows), pl.ds(0, window)], z_send.at[index])


    def pieces(source_dp, to, place):
        all_rows = plan.tp * 2 * plan.down_rows
        downs = pl.ds(pl.multiple_of(place * plan.down_rows, 8), plan.down_rows)
        outs = pl.ds(pl.multiple_of(all_rows + place * plan.out_rows, 8), plan.out_rows)
        stop_downs, stop_outs = pl.ds(0, plan.down_rows), pl.ds(plan.down_rows, plan.out_rows)
        found = []
        for n, (stop, own) in enumerate(((stop_0, own_0), (stop_1, own_1))):
            layer = to * 2 + n
            found.append((d.at[layer], stop.at[source_dp, stop_downs, :], own.at[downs, :], n))
            found.append((o.at[layer], stop.at[source_dp, stop_outs, :], own.at[outs, :], n))
        return found

    my_rank = dp // 2
    my_place = (dp % 2) * plan.tp + z
    stays = my_rank == z

    def share_in_plane():
        for step in range(1, plan.dp):
            to = (dp + step) % plan.dp

            @pl.when(stays)
            def _(to=to):
                for part, _, final, n in pieces(dp, to, my_place):
                    remote(part, final, share_send.at[n], share_recv.at[n], dp=to)

            @pl.when(jnp.logical_not(stays))
            def _(to=to):
                for part, stop, _, n in pieces(dp, to, my_place):
                    remote(part, stop, share_send.at[n], stop_recv.at[n, dp], dp=to)

        @pl.when(stays)
        def _():
            for part, _, final, n in pieces(dp, dp, my_place):
                pltpu.make_async_copy(part, final, share_recv.at[n]).start()

    def share_to_rank(source_dp):
        rank, place = source_dp // 2, (source_dp % 2) * plan.tp + z

        @pl.when((rank != z) & (source_dp == dp))
        def _():
            for part, _, final, n in pieces(dp, dp, place):
                remote(part, final, share_send.at[n], share_recv.at[n], tp=rank)

        @pl.when((rank != z) & (source_dp != dp))
        def _():
            with jax.named_scope("stopwait"):
                for n, stop in enumerate((stop_0, stop_1)):
                    wait_for(stop.at[source_dp], stop_recv.at[n, source_dp])
            for _, stop, final, n in pieces(source_dp, dp, place):
                remote(stop, final, share_send.at[n], share_recv.at[n], tp=rank)

    for index in range(2):
        start_exchange(index)
    share_in_plane()
    for index in range(2, AHEAD):
        start_exchange(index)

    def step(index, _):
        slot = index % 2

        @pl.when(index + AHEAD < plan.chunks)
        def _():
            start_exchange(index + AHEAD)

        @pl.when((index >= SHARE_AT) & (index < SHARE_AT + plan.dp))
        def _():
            share_to_rank(index - SHARE_AT)

        @pl.when(index < layers)
        def _():
            make_layer(index, slot)

        @pl.when(index >= layers)
        def _():
            make_head(index, slot)

        send_own(slab_view(index), index, slot, chunk)

        @pl.when(index >= LAG)
        def _():
            forward(slab_view(index - LAG), index - LAG, chunk)

        @pl.when(index >= 2 * LAG)
        def _():
            forward_diagonal(slab_view(index - 2 * LAG), index - 2 * LAG, chunk)

        return 0

    lax.fori_loop(0, last, step, 0)

    make_tail(last % 2)
    send_own(slab_view(last), last, last % 2, tail)
    for index in range(last - LAG, last):
        forward(slab_view(index), index, chunk)
    forward(slab_view(last), last, tail)
    for index in range(last - 2 * LAG, last):
        forward_diagonal(slab_view(index), index, chunk)
    forward_diagonal(slab_view(last), last, tail)

    def drain(index, _):
        finish(slab_view(index), index, chunk)

        @pl.when(index < layers)
        def _():
            finish_exchange(index, plan.layer_window)

        @pl.when(index >= layers)
        def _():
            finish_exchange(index, chunk)

        return 0

    with jax.named_scope("drain"):
        lax.fori_loop(0, last, drain, 0)
        finish(slab_view(last), last, tail)
        finish_exchange(last, plan.tail_window)
    with jax.named_scope("sharewait"):
        for n, own in enumerate((own_0, own_1)):
            wait_for(own, share_recv.at[n])
            for parts in (8, 5):
                wait_for(own.at[pl.ds(0, parts * (plan.down_rows + plan.out_rows)), :], share_send.at[n])


def gather(plan, *args):
    dma = pltpu.SemaphoreType.DMA
    per_chunk = dma((plan.chunks,))
    columns = args[3].shape[2]
    share_rows = plan.down_rows + plan.out_rows
    hbm = pl.BlockSpec(memory_space=pltpu.HBM)
    shapes = [(plan.dp, plan.chunks, plan.chunk, LANES)]
    shapes += [(plan.tp * 2 * share_rows, columns)] * 2 + [(plan.dp, share_rows, columns)] * 2
    return pl.pallas_call(
        functools.partial(gather_kernel, plan),
        out_shape=[jax.ShapeDtypeStruct(shape, jnp.bfloat16) for shape in shapes],
        in_specs=[hbm] * 8,
        out_specs=[hbm] * len(shapes),
        scratch_shapes=[
            pltpu.VMEM((plan.chunks, plan.tp * plan.rows, plan.layer_window), jnp.bfloat16),
            pltpu.VMEM((2, plan.chunk + 2 * LANES, LANES), jnp.bfloat16),
            per_chunk, per_chunk, dma((2,)),
            per_chunk, per_chunk, per_chunk, per_chunk, per_chunk, per_chunk,
            dma((2, plan.dp)), dma((2,)), dma((2,)),
        ],
        compiler_params=pltpu.CompilerParams(has_side_effects=True),
        name="gather",
    )(*args)[:3]


def place_slabs(plan, slabs, first, count, shapes, store, held=(), name="place"):
    hbm = pl.BlockSpec(memory_space=pltpu.HBM)
    depth = min(BUFFERS, count)
    ahead = depth // 2

    def body(slab, *refs):
        outs, (buffers, loads, stores) = refs[len(held):-3], refs[-3:]

        def each_size(chunk, act):
            if first + count == plan.chunks:
                pl.when(chunk < plan.chunks - 1)(lambda: act(plan.chunk))
                pl.when(chunk == plan.chunks - 1)(lambda: act(plan.tail))
            else:
                act(plan.chunk)

        def load(i, rows):
            for owner in range(plan.dp):
                pltpu.make_async_copy(
                    slab.at[owner, first + i, pl.ds(0, rows), :],
                    buffers.at[i % depth, pl.ds(0, rows), pl.ds(owner * LANES, LANES)],
                    loads.at[i % depth],
                ).start()

        def wait(i, rows, sem):
            buffer = buffers.at[i % depth, pl.ds(0, rows), :]
            pltpu.make_async_copy(buffer, buffer, sem.at[i % depth]).wait()

        def write(i, rows):
            wait(i, rows, loads)
            for source, target in store(buffers.at[i % depth], first + i, rows, outs):
                pltpu.make_async_copy(source, target, stores.at[i % depth]).start()

        def step(i, _):
            @pl.when(i >= depth)
            def _():
                each_size(first + i - depth, lambda rows: wait(i - depth, rows, stores))

            @pl.when(i < count)
            def _():
                each_size(first + i, lambda rows: load(i, rows))

            @pl.when((i >= ahead) & (i < count + ahead))
            def _():
                each_size(first + i - ahead, lambda rows: write(i - ahead, rows))

            return 0

        lax.fori_loop(0, count + depth, step, 0)

    outs = [jax.ShapeDtypeStruct(shape, jnp.bfloat16) for shape in shapes]
    return pl.pallas_call(
        body,
        in_specs=[hbm] * (1 + len(held)),
        out_specs=[hbm] * len(outs),
        out_shape=outs,
        scratch_shapes=[
            pltpu.VMEM((depth, plan.chunk, plan.dp * LANES), jnp.bfloat16),
            pltpu.SemaphoreType.DMA((depth,)),
            pltpu.SemaphoreType.DMA((depth,)),
        ],
        input_output_aliases={1 + n: n for n in range(len(held))},
        cost_estimate=pl.CostEstimate(
            flops=10**10, bytes_accessed=4 * count * plan.chunk * plan.dp * LANES, transcendentals=0
        ),
        compiler_params=pltpu.CompilerParams(vmem_limit_bytes=VMEM),
        name=name,
    )(slabs, *held)


def place_layers(plan, slabs):
    narrow, wide, width = 3 * plan.part, 2 * plan.wide, plan.dp * LANES

    def store(buffer, chunk, rows, outs):
        return [
            (buffer.at[pl.ds(0, narrow), :], outs[0].at[chunk]),
            (buffer.at[pl.ds(narrow, wide), :], outs[1].at[chunk]),
        ]

    shapes = [(plan.layers, narrow, width), (plan.layers, wide, width)]
    return place_slabs(plan, slabs, 0, plan.layers, shapes, store, name="place_layers")


def place_head(plan, slabs, first, count, *held):
    def store(buffer, chunk, rows, outs):
        at = pl.multiple_of((chunk - plan.layers) * plan.chunk, 16)
        return [(buffer.at[pl.ds(0, rows), :], outs[0].at[pl.ds(at, rows), :])]

    shapes = [(plan.vocab, plan.dp * LANES)]
    return place_slabs(plan, slabs, plan.layers + first, count, shapes, store, held, name="place_head")[0]


def place_pieces(plan, pieces, held=()):
    owners = list(pieces)
    arrays = [array for owner in owners for array in pieces[owner]]
    rows, columns = arrays[0].shape
    downs, outs = plan.tp * 2 * plan.down_rows, plan.tp * 2 * plan.out_rows

    def body(*refs):
        sources, (down, out) = refs[: len(arrays)], refs[len(arrays) + len(held): -5]
        buffers, turned, loads, stores, out_stores = refs[-5:]
        dp = lax.axis_index("dp")
        core, x, y = dp % 2, (dp // 2) % 2, dp // 4

        def layer(n):
            flip_x, flip_y, flip_core = owners[n // plan.share]
            at = (y + flip_y * (1 - 2 * y)) * 4 + (x + flip_x * (1 - 2 * x)) * 2 + core + flip_core * (1 - 2 * core)
            return at * plan.share + n % plan.share

        loading = [pltpu.make_async_copy(source, buffers.at[n], loads.at[n]) for n, source in enumerate(sources)]
        storing = []
        for load in loading:
            load.start()
        for n, load in enumerate(loading):
            load.wait()
            storing.append(pltpu.make_async_copy(buffers.at[n, pl.ds(0, downs), :], down.at[layer(n)], stores.at[n]))
            storing[-1].start()
        for n in range(len(arrays)):
            for i in range(outs // LANES):
                for j in range(columns // LANES):
                    turned[n, pl.ds(j * LANES, LANES), pl.ds(i * LANES, LANES)] = buffers[
                        n, pl.ds(downs + i * LANES, LANES), pl.ds(j * LANES, LANES)
                    ].T
            storing.append(pltpu.make_async_copy(turned.at[n], out.at[layer(n)], out_stores.at[n]))
            storing[-1].start()
        for store in storing:
            store.wait()

    hbm = pl.BlockSpec(memory_space=pltpu.HBM)
    dma = pltpu.SemaphoreType.DMA((len(arrays),))
    shapes = [(plan.layers, downs, columns), (plan.layers, columns, outs)]
    return pl.pallas_call(
        body,
        out_shape=[jax.ShapeDtypeStruct(shape, jnp.bfloat16) for shape in shapes],
        in_specs=[hbm] * (len(arrays) + len(held)),
        out_specs=[hbm] * 2,
        scratch_shapes=[
            pltpu.VMEM((len(arrays), rows, columns), jnp.bfloat16),
            pltpu.VMEM((len(arrays), columns, outs), jnp.bfloat16),
            dma, dma, dma,
        ],
        input_output_aliases={len(arrays) + n: n for n in range(len(held))},
        cost_estimate=pl.CostEstimate(flops=10**9, bytes_accessed=4 * len(arrays) * rows * columns, transcendentals=0),
        compiler_params=pltpu.CompilerParams(vmem_limit_bytes=VMEM),
        name="place_pieces_end" if held else "place_pieces",
    )(*arrays, *held)


def solution(mesh):
    train_stack = P(None, ("dp", "tp"), None)
    train_head = P(("dp", "tp"), None)
    fused_stack = P(None, "tp", None)
    last_stack = P(None, None, "tp")
    head_rows = P("tp", None)

    def local_sync(w_query, w_key, w_value, w_out, w_gate, w_up, w_down, w_head):
        plan = Plan(mesh.shape["tp"], mesh.shape["dp"], w_query, w_gate, w_out, w_down, w_head)
        slabs, own_0, own_1 = gather(plan, w_query, w_key, w_value, w_out, w_gate, w_up, w_down, w_head)

        def swap(bit, array):
            return lax.ppermute(array, "dp", [(i, i ^ bit) for i in range(plan.dp)])

        pair, along_x, along_y = (functools.partial(swap, bit) for bit in (1, 2, 4))
        hold = lax.optimization_barrier

        x_1, y_0 = along_x(own_1), along_y(own_0)
        x_0, y_1 = along_x(own_0), along_y(own_1)
        pair_own = [pair(own_0), pair(own_1)]
        qkv_block, gate_up_block = place_layers(plan, slabs)
        x_1, y_0, qkv_block, slabs = hold((x_1, y_0, qkv_block, slabs))
        diagonal = [along_x(y_0), along_y(x_1)]
        pair_x_1, pair_y_0 = pair(x_1), pair(y_0)
        early = plan.head_chunks // 2
        head_block = place_head(plan, slabs, early, plan.head_chunks - early)
        x_0, y_1, head_block, slabs = hold((x_0, y_1, head_block, slabs))
        pair_x_0, pair_y_1 = pair(x_0), pair(y_1)
        head_block = place_head(plan, slabs, 0, early, head_block)
        *diagonal, head_block = hold((*diagonal, head_block))
        pair_diagonal = [pair(array) for array in diagonal]
        near = {
            (0, 0, 0): [own_0, own_1], (0, 0, 1): pair_own, (1, 0, 0): [x_0, x_1], (1, 0, 1): [pair_x_0, pair_x_1],
            (0, 1, 0): [y_0, y_1], (0, 1, 1): [pair_y_0, pair_y_1],
        }
        placed = place_pieces(plan, near)
        down_block, o_block = place_pieces(plan, {(1, 1, 0): diagonal, (1, 1, 1): pair_diagonal}, placed)
        return (
            qkv_block,
            o_block,
            gate_up_block,
            jnp.swapaxes(down_block, 1, 2),
            head_block,
        )

    return jax.shard_map(
        local_sync,
        mesh=mesh,
        in_specs=(train_stack,) * 7 + (train_head,),
        out_specs=(fused_stack, last_stack, fused_stack, last_stack, head_rows),
        check_vma=False,
    )
```

```python
import functools

import jax
import jax.numpy as jnp
from jax import lax
from jax.experimental import pallas as pl
from jax.experimental.pallas import tpu as pltpu
from jax.sharding import PartitionSpec as P


MESH = pl.DeviceIdType.MESH
LANES = 128
VMEM = 67_000_000
AHEAD = 4
BUFFERS = 6
LAG = 2
SHARE_AT = 14
GROUP = 2


class Plan:
    def __init__(self, tp, dp, w_query, w_gate, w_out, w_down, w_head):
        self.tp, self.dp = tp, dp
        self.layers, self.rows, columns = w_query.shape
        self.part = columns // tp
        self.wide = w_gate.shape[2] // tp
        self.vocab = w_head.shape[1] // tp
        self.head_tiles = w_head.shape[1] // LANES
        self.chunk = 3 * self.part + 2 * self.wide
        self.wide_window = -(-self.wide // LANES) * LANES
        self.layer_window = 3 * self.part + 2 * self.wide_window
        self.head_chunks = -(-self.vocab // self.chunk)
        self.tail = self.vocab - (self.head_chunks - 1) * self.chunk
        self.chunks = self.layers + self.head_chunks
        self.tail_window = -(-(self.tail + LANES) // LANES) * LANES
        self.window_tiles = (self.head_chunks - 1) * self.chunk // LANES + self.tail_window // LANES
        self.out_rows, self.down_rows = w_out.shape[1], w_down.shape[1]
        self.share = self.layers // dp

    def wide_base(self, rank):
        return (self.wide * rank) // LANES

    def head_base(self, rank):
        base = (self.vocab * rank) // LANES
        return base - (rank // (self.tp - 1)) * (self.vocab * (self.tp - 1) // LANES + self.window_tiles - self.head_tiles)


def gather_kernel(plan, q, k, v, o, g, u, d, h, slabs, own_0, own_1, stop_0, stop_1, zbuf, tbuf, z_recv, z_send,
                  local, x_recv, y_recv, a_recv, b_recv, pair_recv, send, stop_recv, share_recv, share_send):
    z, dp = lax.axis_index("tp"), lax.axis_index("dp")
    core, x, y = dp % 2, (dp // 2) % 2, dp // 4
    x_peer = y * 4 + (1 - x) * 2 + core
    y_peer = (1 - y) * 4 + x * 2 + core
    diagonal = (1 - y) * 4 + (1 - x) * 2 + core
    pair = dp + 1 - 2 * core
    rows, chunk, tail = plan.rows, plan.chunk, plan.tail
    layers, last = plan.layers, plan.chunks - 1
    my_rows = pl.ds(pl.multiple_of(z * rows, rows), rows)

    def lanes(first_tile, width):
        return pl.ds(pl.multiple_of(first_tile * LANES, LANES), width)

    def remote(source, target, send_sem, recv_sem, **to):
        pltpu.make_async_remote_copy(source, target, send_sem, recv_sem, device_id=to, device_id_type=MESH).start()

    def wait_for(ref, sem):
        pltpu.make_async_copy(ref, ref, sem).wait()


    def exchange(pieces, chunks, index):
        for step in range(1, plan.tp):
            rank = (z + step + core * (plan.tp - 2 * step)) % plan.tp
            for source, column, width in pieces(rank):
                target = zbuf.at[chunks, my_rows, pl.ds(column, width)]
                remote(source, target, z_send.at[index], z_recv.at[index], tp=rank)
        for source, column, width in pieces(z):
            target = zbuf.at[chunks, my_rows, pl.ds(column, width)]
            pltpu.make_async_copy(source, target, z_recv.at[index]).start()

    def layer_pieces(some):
        def pieces(rank):
            part, wide = plan.part, plan.wide_window
            narrow = lanes(rank * (part // LANES), part)
            window = lanes(plan.wide_base(rank), wide)
            return [
                (q.at[some, :, narrow], 0, part),
                (k.at[some, :, narrow], part, part),
                (v.at[some, :, narrow], 2 * part, part),
                (g.at[some, :, window], 3 * part, wide),
                (u.at[some, :, window], 3 * part + wide, wide),
            ]

        return pieces

    def head_pieces(step, width):
        def pieces(rank):
            return [(h.at[:, lanes(plan.head_base(rank) + step * (chunk // LANES), width)], 0, width)]

        return pieces

    def start_exchange(index):
        @pl.when((index < layers) & (index % GROUP == 0))
        def _():
            some = pl.ds(index, GROUP)
            exchange(layer_pieces(some), some, index)

        @pl.when((index >= layers) & (index < last))
        def _():
            exchange(head_pieces(index - layers, chunk), index, index)

        @pl.when(index == last)
        def _():
            exchange(head_pieces(last - layers, plan.tail_window), last, last)

    def wait_exchange(index, width):
        wait_for(zbuf.at[index, :, pl.ds(0, width)], z_recv.at[index])


    def turn(slot, tile, index, source_tile):
        tbuf[slot, pl.ds(tile * LANES, LANES), :] = zbuf[index, :, pl.ds(source_tile * LANES, LANES)].T

    def store(slot, first, index, to, count):
        pltpu.make_async_copy(
            tbuf.at[slot, pl.ds(first, count), :], slabs.at[dp, index, pl.ds(to, count), :], local.at[slot]
        ).start()

    def make_layer(index, slot):
        @pl.when(index % GROUP == 0)
        def _():
            wait_for(zbuf.at[pl.ds(index, GROUP), :, pl.ds(0, plan.layer_window)], z_recv.at[index])

        for tile in range(plan.layer_window // LANES):
            turn(slot, tile, index, tile)
        shift = plan.wide * z - plan.wide_base(z) * LANES
        narrow, wide, window = 3 * plan.part, plan.wide, plan.wide_window
        store(slot, 0, index, 0, narrow)
        store(slot, pl.multiple_of(narrow + shift, 16), index, narrow, wide)
        store(slot, pl.multiple_of(narrow + window + shift, 16), index, narrow + wide, wide)

    head_shift = plan.vocab * z - plan.head_base(z) * LANES

    def make_head(index, slot):
        @pl.when(index == layers)
        def _():
            wait_exchange(index, chunk)

        @pl.when(index < last - 1)
        def _():
            wait_exchange(index + 1, chunk)

        @pl.when(index == last - 1)
        def _():
            wait_exchange(last, plan.tail_window)

        tiles = chunk // LANES
        for tile in range(tiles):
            turn(slot, tile, index, tile)
        for tile in range(2):
            turn(slot, tiles + tile, index + 1, tile)
        store(slot, pl.multiple_of(head_shift, 16), index, 0, chunk)

    def make_tail(slot):
        for tile in range(plan.tail_window // LANES):
            turn(slot, tile, last, tile)
        store(slot, pl.multiple_of(head_shift, 16), last, 0, tail)


    def slab_view(index):
        return lambda owner, first, count: slabs.at[owner, index, pl.ds(first, count), :]

    def push(part, index, recv, to):
        remote(part, part, send.at[index], recv.at[index], dp=to)

    def send_own(view, index, slot, count):
        own = view(dp, 0, count)
        wait_for(own, local.at[slot])
        push(own, index, x_recv, x_peer)
        push(own, index, y_recv, y_peer)
        push(own, index, pair_recv, pair)

    def forward(view, index, count):
        half = count // 2
        wait_for(view(x_peer, 0, count), x_recv.at[index])
        push(view(x_peer, half, half), index, b_recv, y_peer)
        push(view(x_peer, 0, count), index, pair_recv, pair)
        wait_for(view(y_peer, 0, count), y_recv.at[index])
        push(view(y_peer, 0, half), index, a_recv, x_peer)
        push(view(y_peer, 0, count), index, pair_recv, pair)

    def forward_diagonal(view, index, count):
        half = count // 2
        wait_for(view(diagonal, 0, half), a_recv.at[index])
        wait_for(view(diagonal, half, half), b_recv.at[index])
        push(view(diagonal, 0, count), index, pair_recv, pair)

    def finish(view, index, count):
        wait_for(view(pl.ds(0, 7), 0, count), send.at[index])
        wait_for(view(pl.ds(0, 4), 0, count), pair_recv.at[index])

    def finish_exchange(index, window):
        wait_for(zbuf.at[index, pl.ds(0, (plan.tp - 1) * rows), pl.ds(0, window)], z_send.at[index])


    def pieces(source_dp, to, place):
        all_rows = plan.tp * 2 * plan.down_rows
        downs = pl.ds(pl.multiple_of(place * plan.down_rows, 8), plan.down_rows)
        outs = pl.ds(pl.multiple_of(all_rows + place * plan.out_rows, 8), plan.out_rows)
        stop_downs, stop_outs = pl.ds(0, plan.down_rows), pl.ds(plan.down_rows, plan.out_rows)
        found = []
        for n, (stop, own) in enumerate(((stop_0, own_0), (stop_1, own_1))):
            layer = to * 2 + n
            found.append((d.at[layer], stop.at[source_dp, stop_downs, :], own.at[downs, :], n))
            found.append((o.at[layer], stop.at[source_dp, stop_outs, :], own.at[outs, :], n))
        return found

    my_rank = dp // 2
    my_place = (dp % 2) * plan.tp + z
    stays = my_rank == z

    def share_in_plane():
        for step in range(1, plan.dp):
            to = (dp + step) % plan.dp

            @pl.when(stays)
            def _(to=to):
                for part, _, final, n in pieces(dp, to, my_place):
                    remote(part, final, share_send.at[n], share_recv.at[n], dp=to)

            @pl.when(jnp.logical_not(stays))
            def _(to=to):
                for part, stop, _, n in pieces(dp, to, my_place):
                    remote(part, stop, share_send.at[n], stop_recv.at[n, dp], dp=to)

        @pl.when(stays)
        def _():
            for part, _, final, n in pieces(dp, dp, my_place):
                pltpu.make_async_copy(part, final, share_recv.at[n]).start()

    def share_to_rank(source_dp):
        rank, place = source_dp // 2, (source_dp % 2) * plan.tp + z

        @pl.when((rank != z) & (source_dp == dp))
        def _():
            for part, _, final, n in pieces(dp, dp, place):
                remote(part, final, share_send.at[n], share_recv.at[n], tp=rank)

        @pl.when((rank != z) & (source_dp != dp))
        def _():
            for n, stop in enumerate((stop_0, stop_1)):
                wait_for(stop.at[source_dp], stop_recv.at[n, source_dp])
            for _, stop, final, n in pieces(source_dp, dp, place):
                remote(stop, final, share_send.at[n], share_recv.at[n], tp=rank)

    start_exchange(0)
    share_in_plane()
    for index in range(GROUP, AHEAD):
        start_exchange(index)

    def step(index, _):
        slot = index % 2

        @pl.when(index + AHEAD < plan.chunks)
        def _():
            start_exchange(index + AHEAD)

        @pl.when((index >= SHARE_AT) & (index < SHARE_AT + 2 * plan.dp) & (index % 2 == SHARE_AT % 2))
        def _():
            share_to_rank((index - SHARE_AT) // 2)

        @pl.when(index < layers)
        def _():
            make_layer(index, slot)

        @pl.when(index >= layers)
        def _():
            make_head(index, slot)

        send_own(slab_view(index), index, slot, chunk)

        @pl.when(index >= LAG)
        def _():
            forward(slab_view(index - LAG), index - LAG, chunk)

        @pl.when(index >= 2 * LAG)
        def _():
            forward_diagonal(slab_view(index - 2 * LAG), index - 2 * LAG, chunk)

        return 0

    lax.fori_loop(0, last, step, 0)

    make_tail(last % 2)
    send_own(slab_view(last), last, last % 2, tail)
    for index in range(last - LAG, last):
        forward(slab_view(index), index, chunk)
    forward(slab_view(last), last, tail)
    for index in range(last - 2 * LAG, last):
        forward_diagonal(slab_view(index), index, chunk)
    forward_diagonal(slab_view(last), last, tail)

    def drain(index, _):
        finish(slab_view(index), index, chunk)

        @pl.when((index < layers) & (index % GROUP == 0))
        def _():
            sent = pl.ds(0, (plan.tp - 1) * rows)
            wait_for(zbuf.at[pl.ds(index, GROUP), sent, pl.ds(0, plan.layer_window)], z_send.at[index])

        @pl.when(index >= layers)
        def _():
            finish_exchange(index, chunk)

        return 0

    lax.fori_loop(0, last, drain, 0)
    finish(slab_view(last), last, tail)
    finish_exchange(last, plan.tail_window)
    for n, own in enumerate((own_0, own_1)):
        wait_for(own, share_recv.at[n])
        for parts in (8, 5):
            wait_for(own.at[pl.ds(0, parts * (plan.down_rows + plan.out_rows)), :], share_send.at[n])


def gather(plan, *args):
    dma = pltpu.SemaphoreType.DMA
    per_chunk = dma((plan.chunks,))
    columns = args[3].shape[2]
    share_rows = plan.down_rows + plan.out_rows
    hbm = pl.BlockSpec(memory_space=pltpu.HBM)
    shapes = [(plan.dp, plan.chunks, plan.chunk, LANES)]
    shapes += [(plan.tp * 2 * share_rows, columns)] * 2 + [(plan.dp, share_rows, columns)] * 2
    return pl.pallas_call(
        functools.partial(gather_kernel, plan),
        out_shape=[jax.ShapeDtypeStruct(shape, jnp.bfloat16) for shape in shapes],
        in_specs=[hbm] * 8,
        out_specs=[hbm] * len(shapes),
        scratch_shapes=[
            pltpu.VMEM((plan.chunks, plan.tp * plan.rows, plan.layer_window), jnp.bfloat16),
            pltpu.VMEM((2, plan.chunk + 2 * LANES, LANES), jnp.bfloat16),
            per_chunk, per_chunk, dma((2,)),
            per_chunk, per_chunk, per_chunk, per_chunk, per_chunk, per_chunk,
            dma((2, plan.dp)), dma((2,)), dma((2,)),
        ],
        compiler_params=pltpu.CompilerParams(has_side_effects=True),
        name="gather",
    )(*args)[:3]


def place_slabs(plan, slabs, first, count, shapes, store, held=()):
    hbm = pl.BlockSpec(memory_space=pltpu.HBM)
    depth = min(BUFFERS, count)
    ahead = depth // 2

    def body(slab, *refs):
        outs, (buffers, loads, stores) = refs[len(held):-3], refs[-3:]

        def each_size(chunk, act):
            if first + count == plan.chunks:
                pl.when(chunk < plan.chunks - 1)(lambda: act(plan.chunk))
                pl.when(chunk == plan.chunks - 1)(lambda: act(plan.tail))
            else:
                act(plan.chunk)

        def load(i, rows):
            for owner in range(plan.dp):
                pltpu.make_async_copy(
                    slab.at[owner, first + i, pl.ds(0, rows), :],
                    buffers.at[i % depth, pl.ds(0, rows), pl.ds(owner * LANES, LANES)],
                    loads.at[i % depth],
                ).start()

        def wait(i, rows, sem):
            buffer = buffers.at[i % depth, pl.ds(0, rows), :]
            pltpu.make_async_copy(buffer, buffer, sem.at[i % depth]).wait()

        def write(i, rows):
            wait(i, rows, loads)
            for source, target in store(buffers.at[i % depth], first + i, rows, outs):
                pltpu.make_async_copy(source, target, stores.at[i % depth]).start()

        def step(i, _):
            @pl.when(i >= depth)
            def _():
                each_size(first + i - depth, lambda rows: wait(i - depth, rows, stores))

            @pl.when(i < count)
            def _():
                each_size(first + i, lambda rows: load(i, rows))

            @pl.when((i >= ahead) & (i < count + ahead))
            def _():
                each_size(first + i - ahead, lambda rows: write(i - ahead, rows))

            return 0

        lax.fori_loop(0, count + depth, step, 0)

    outs = [jax.ShapeDtypeStruct(shape, jnp.bfloat16) for shape in shapes]
    return pl.pallas_call(
        body,
        in_specs=[hbm] * (1 + len(held)),
        out_specs=[hbm] * len(outs),
        out_shape=outs,
        scratch_shapes=[
            pltpu.VMEM((depth, plan.chunk, plan.dp * LANES), jnp.bfloat16),
            pltpu.SemaphoreType.DMA((depth,)),
            pltpu.SemaphoreType.DMA((depth,)),
        ],
        input_output_aliases={1 + n: n for n in range(len(held))},
        cost_estimate=pl.CostEstimate(
            flops=10**7, bytes_accessed=4 * count * plan.chunk * plan.dp * LANES, transcendentals=0
        ),
        compiler_params=pltpu.CompilerParams(vmem_limit_bytes=VMEM),
    )(slabs, *held)


def place_layers(plan, slabs):
    narrow, wide, width = 3 * plan.part, 2 * plan.wide, plan.dp * LANES

    def store(buffer, chunk, rows, outs):
        return [
            (buffer.at[pl.ds(0, narrow), :], outs[0].at[chunk]),
            (buffer.at[pl.ds(narrow, wide), :], outs[1].at[chunk]),
        ]

    shapes = [(plan.layers, narrow, width), (plan.layers, wide, width)]
    return place_slabs(plan, slabs, 0, plan.layers, shapes, store)


def place_head(plan, slabs, first, count, *held):
    def store(buffer, chunk, rows, outs):
        at = pl.multiple_of((chunk - plan.layers) * plan.chunk, 16)
        return [(buffer.at[pl.ds(0, rows), :], outs[0].at[pl.ds(at, rows), :])]

    shapes = [(plan.vocab, plan.dp * LANES)]
    return place_slabs(plan, slabs, plan.layers + first, count, shapes, store, held)[0]


def place_pieces(plan, pieces, held=()):
    owners = list(pieces)
    arrays = [array for owner in owners for array in pieces[owner]]
    rows, columns = arrays[0].shape
    downs, outs = plan.tp * 2 * plan.down_rows, plan.tp * 2 * plan.out_rows

    def body(*refs):
        sources, (down, out) = refs[: len(arrays)], refs[len(arrays) + len(held): -5]
        buffers, turned, loads, stores, out_stores = refs[-5:]
        dp = lax.axis_index("dp")
        core, x, y = dp % 2, (dp // 2) % 2, dp // 4

        def layer(n):
            flip_x, flip_y, flip_core = owners[n // plan.share]
            at = (y + flip_y * (1 - 2 * y)) * 4 + (x + flip_x * (1 - 2 * x)) * 2 + core + flip_core * (1 - 2 * core)
            return at * plan.share + n % plan.share

        loading = [pltpu.make_async_copy(source, buffers.at[n], loads.at[n]) for n, source in enumerate(sources)]
        storing = []
        for load in loading:
            load.start()
        for n, load in enumerate(loading):
            load.wait()
            storing.append(pltpu.make_async_copy(buffers.at[n, pl.ds(0, downs), :], down.at[layer(n)], stores.at[n]))
            storing[-1].start()
        for n in range(len(arrays)):
            for i in range(outs // LANES):
                for j in range(columns // LANES):
                    turned[n, pl.ds(j * LANES, LANES), pl.ds(i * LANES, LANES)] = buffers[
                        n, pl.ds(downs + i * LANES, LANES), pl.ds(j * LANES, LANES)
                    ].T
            storing.append(pltpu.make_async_copy(turned.at[n], out.at[layer(n)], out_stores.at[n]))
            storing[-1].start()
        for store in storing:
            store.wait()

    hbm = pl.BlockSpec(memory_space=pltpu.HBM)
    dma = pltpu.SemaphoreType.DMA((len(arrays),))
    shapes = [(plan.layers, downs, columns), (plan.layers, columns, outs)]
    return pl.pallas_call(
        body,
        out_shape=[jax.ShapeDtypeStruct(shape, jnp.bfloat16) for shape in shapes],
        in_specs=[hbm] * (len(arrays) + len(held)),
        out_specs=[hbm] * 2,
        scratch_shapes=[
            pltpu.VMEM((len(arrays), rows, columns), jnp.bfloat16),
            pltpu.VMEM((len(arrays), columns, outs), jnp.bfloat16),
            dma, dma, dma,
        ],
        input_output_aliases={len(arrays) + n: n for n in range(len(held))},
        cost_estimate=pl.CostEstimate(flops=10**7, bytes_accessed=4 * len(arrays) * rows * columns, transcendentals=0),
        compiler_params=pltpu.CompilerParams(vmem_limit_bytes=VMEM),
        name="place_pieces_end" if held else "place_pieces",
    )(*arrays, *held)


def solution(mesh):
    train_stack = P(None, ("dp", "tp"), None)
    train_head = P(("dp", "tp"), None)
    fused_stack = P(None, "tp", None)
    last_stack = P(None, None, "tp")
    head_rows = P("tp", None)

    def local_sync(w_query, w_key, w_value, w_out, w_gate, w_up, w_down, w_head):
        plan = Plan(mesh.shape["tp"], mesh.shape["dp"], w_query, w_gate, w_out, w_down, w_head)
        slabs, own_0, own_1 = gather(plan, w_query, w_key, w_value, w_out, w_gate, w_up, w_down, w_head)

        def swap(bit, array):
            return lax.ppermute(array, "dp", [(i, i ^ bit) for i in range(plan.dp)])

        pair, along_x, along_y = (functools.partial(swap, bit) for bit in (1, 2, 4))
        hold = lax.optimization_barrier

        x_1, y_0 = along_x(own_1), along_y(own_0)
        x_0, y_1 = along_x(own_0), along_y(own_1)
        pair_own = [pair(own_0), pair(own_1)]
        qkv_block, gate_up_block = place_layers(plan, slabs)
        x_1, y_0, qkv_block, slabs = hold((x_1, y_0, qkv_block, slabs))
        diagonal_0 = along_x(y_0)
        diagonal_1 = along_y(x_1)
        pair_x_1, pair_y_0 = pair(x_1), pair(y_0)
        early = plan.head_chunks // 2
        head_block = place_head(plan, slabs, early, plan.head_chunks - early)
        x_0, y_1, head_block, slabs = hold((x_0, y_1, head_block, slabs))
        pair_x_0, pair_y_1 = pair(x_0), pair(y_1)
        head_block = place_head(plan, slabs, 0, early, head_block)
        own_0, own_1, head_block = hold((own_0, own_1, head_block))
        near = {
            (0, 0, 0): [own_0, own_1], (0, 0, 1): pair_own, (1, 0, 0): [x_0, x_1], (1, 0, 1): [pair_x_0, pair_x_1],
            (0, 1, 0): [y_0, y_1], (0, 1, 1): [pair_y_0, pair_y_1],
        }
        placed = place_pieces(plan, near)
        diagonal_0, diagonal_1, down_block, o_block = hold((diagonal_0, diagonal_1, *placed))
        pair_diagonal = [pair(diagonal_0), pair(diagonal_1)]
        placed = place_pieces(plan, {(1, 1, 0): [diagonal_0, diagonal_1]}, (down_block, o_block))
        down_block, o_block = place_pieces(plan, {(1, 1, 1): pair_diagonal}, placed)
        return (
            qkv_block,
            o_block,
            gate_up_block,
            jnp.swapaxes(down_block, 1, 2),
            head_block,
        )

    return jax.shard_map(
        local_sync,
        mesh=mesh,
        in_specs=(train_stack,) * 7 + (train_head,),
        out_specs=(fused_stack, last_stack, fused_stack, last_stack, head_rows),
        check_vma=False,
    )
```

```python
import functools

import jax
import jax.numpy as jnp
from jax import lax
from jax.experimental import pallas as pl
from jax.experimental.pallas import tpu as pltpu
from jax.sharding import PartitionSpec as P


MESH = pl.DeviceIdType.MESH
LANES = 128
VMEM = 67_000_000
AHEAD = 4
BUFFERS = 6
LAG = 2
SHARE_AT = 14
RETIRE = 8
GROUP = 2


class Plan:
    def __init__(self, tp, dp, w_query, w_gate, w_out, w_down, w_head):
        self.tp, self.dp = tp, dp
        self.layers, self.rows, columns = w_query.shape
        self.part = columns // tp
        self.wide = w_gate.shape[2] // tp
        self.vocab = w_head.shape[1] // tp
        self.head_tiles = w_head.shape[1] // LANES
        self.chunk = 3 * self.part + 2 * self.wide
        self.wide_window = -(-self.wide // LANES) * LANES
        self.layer_window = 3 * self.part + 2 * self.wide_window
        self.head_chunks = -(-self.vocab // self.chunk)
        self.tail = self.vocab - (self.head_chunks - 1) * self.chunk
        self.chunks = self.layers + self.head_chunks
        self.tail_window = -(-(self.tail + LANES) // LANES) * LANES
        self.window_tiles = (self.head_chunks - 1) * self.chunk // LANES + self.tail_window // LANES
        self.out_rows, self.down_rows = w_out.shape[1], w_down.shape[1]
        self.share = self.layers // dp

    def wide_base(self, rank):
        return (self.wide * rank) // LANES

    def head_base(self, rank):
        base = (self.vocab * rank) // LANES
        return base - (rank // (self.tp - 1)) * (self.vocab * (self.tp - 1) // LANES + self.window_tiles - self.head_tiles)


def gather_kernel(plan, q, k, v, o, g, u, d, h, slabs, own_0, own_1, stop_0, stop_1, zbuf, tbuf, z_recv, z_send,
                  local, x_recv, y_recv, a_recv, b_recv, pair_recv, send, stop_recv, share_recv, share_send):
    z, dp = lax.axis_index("tp"), lax.axis_index("dp")
    core, x, y = dp % 2, (dp // 2) % 2, dp // 4
    x_peer = y * 4 + (1 - x) * 2 + core
    y_peer = (1 - y) * 4 + x * 2 + core
    diagonal = (1 - y) * 4 + (1 - x) * 2 + core
    pair = dp + 1 - 2 * core
    rows, chunk, tail = plan.rows, plan.chunk, plan.tail
    layers, last = plan.layers, plan.chunks - 1
    my_rows = pl.ds(pl.multiple_of(z * rows, rows), rows)

    def lanes(first_tile, width):
        return pl.ds(pl.multiple_of(first_tile * LANES, LANES), width)

    def remote(source, target, send_sem, recv_sem, **to):
        pltpu.make_async_remote_copy(source, target, send_sem, recv_sem, device_id=to, device_id_type=MESH).start()

    def wait_for(ref, sem):
        pltpu.make_async_copy(ref, ref, sem).wait()


    def exchange(pieces, chunks, index):
        for step in range(1, plan.tp):
            rank = (z + step + core * (plan.tp - 2 * step)) % plan.tp
            for source, column, width in pieces(rank):
                target = zbuf.at[chunks, my_rows, pl.ds(column, width)]
                remote(source, target, z_send.at[index], z_recv.at[index], tp=rank)
        for source, column, width in pieces(z):
            target = zbuf.at[chunks, my_rows, pl.ds(column, width)]
            pltpu.make_async_copy(source, target, z_recv.at[index]).start()

    def layer_pieces(some):
        def pieces(rank):
            part, wide = plan.part, plan.wide_window
            narrow = lanes(rank * (part // LANES), part)
            window = lanes(plan.wide_base(rank), wide)
            return [
                (q.at[some, :, narrow], 0, part),
                (k.at[some, :, narrow], part, part),
                (v.at[some, :, narrow], 2 * part, part),
                (g.at[some, :, window], 3 * part, wide),
                (u.at[some, :, window], 3 * part + wide, wide),
            ]

        return pieces

    def head_pieces(step, width):
        def pieces(rank):
            return [(h.at[:, lanes(plan.head_base(rank) + step * (chunk // LANES), width)], 0, width)]

        return pieces

    def start_exchange(index):
        @pl.when((index < layers) & (index % GROUP == 0))
        def _():
            some = pl.ds(index, GROUP)
            exchange(layer_pieces(some), some, index)

        @pl.when((index >= layers) & (index < last))
        def _():
            exchange(head_pieces(index - layers, chunk), index, index)

        @pl.when(index == last)
        def _():
            exchange(head_pieces(last - layers, plan.tail_window), last, last)

    def wait_exchange(index, width):
        wait_for(zbuf.at[index, :, pl.ds(0, width)], z_recv.at[index])


    def turn(slot, tile, index, source_tile):
        tbuf[slot, pl.ds(tile * LANES, LANES), :] = zbuf[index, :, pl.ds(source_tile * LANES, LANES)].T

    def store(slot, first, index, to, count):
        pltpu.make_async_copy(
            tbuf.at[slot, pl.ds(first, count), :], slabs.at[dp, index, pl.ds(to, count), :], local.at[slot]
        ).start()

    def make_layer(index, slot):
        @pl.when(index % GROUP == 0)
        def _():
            wait_for(zbuf.at[pl.ds(index, GROUP), :, pl.ds(0, plan.layer_window)], z_recv.at[index])

        for tile in range(plan.layer_window // LANES):
            turn(slot, tile, index, tile)
        shift = plan.wide * z - plan.wide_base(z) * LANES
        narrow, wide, window = 3 * plan.part, plan.wide, plan.wide_window
        store(slot, 0, index, 0, narrow)
        store(slot, pl.multiple_of(narrow + shift, 16), index, narrow, wide)
        store(slot, pl.multiple_of(narrow + window + shift, 16), index, narrow + wide, wide)

    head_shift = plan.vocab * z - plan.head_base(z) * LANES

    def make_head(index, slot):
        @pl.when(index == layers)
        def _():
            wait_exchange(index, chunk)

        @pl.when(index < last - 1)
        def _():
            wait_exchange(index + 1, chunk)

        @pl.when(index == last - 1)
        def _():
            wait_exchange(last, plan.tail_window)

        tiles = chunk // LANES
        for tile in range(tiles):
            turn(slot, tile, index, tile)
        for tile in range(2):
            turn(slot, tiles + tile, index + 1, tile)
        store(slot, pl.multiple_of(head_shift, 16), index, 0, chunk)

    def make_tail(slot):
        for tile in range(plan.tail_window // LANES):
            turn(slot, tile, last, tile)
        store(slot, pl.multiple_of(head_shift, 16), last, 0, tail)


    def slab_view(index):
        return lambda owner, first, count: slabs.at[owner, index, pl.ds(first, count), :]

    def push(part, index, recv, to):
        remote(part, part, send.at[index], recv.at[index], dp=to)

    def send_own(view, index, slot, count):
        own = view(dp, 0, count)
        wait_for(own, local.at[slot])
        push(own, index, x_recv, x_peer)
        push(own, index, y_recv, y_peer)
        push(own, index, pair_recv, pair)

    def forward(view, index, count):
        half = count // 2
        wait_for(view(x_peer, 0, count), x_recv.at[index])
        push(view(x_peer, half, half), index, b_recv, y_peer)
        push(view(x_peer, 0, count), index, pair_recv, pair)
        wait_for(view(y_peer, 0, count), y_recv.at[index])
        push(view(y_peer, 0, half), index, a_recv, x_peer)
        push(view(y_peer, 0, count), index, pair_recv, pair)

    def forward_diagonal(view, index, count):
        half = count // 2
        wait_for(view(diagonal, 0, half), a_recv.at[index])
        wait_for(view(diagonal, half, half), b_recv.at[index])
        push(view(diagonal, 0, count), index, pair_recv, pair)

    def finish(view, index, count):
        wait_for(view(pl.ds(0, 7), 0, count), send.at[index])
        wait_for(view(pl.ds(0, 4), 0, count), pair_recv.at[index])

    def finish_exchange(index, window):
        wait_for(zbuf.at[index, pl.ds(0, (plan.tp - 1) * rows), pl.ds(0, window)], z_send.at[index])


    def pieces(source_dp, to, place):
        all_rows = plan.tp * 2 * plan.down_rows
        downs = pl.ds(pl.multiple_of(place * plan.down_rows, 8), plan.down_rows)
        outs = pl.ds(pl.multiple_of(all_rows + place * plan.out_rows, 8), plan.out_rows)
        stop_downs, stop_outs = pl.ds(0, plan.down_rows), pl.ds(plan.down_rows, plan.out_rows)
        found = []
        for n, (stop, own) in enumerate(((stop_0, own_0), (stop_1, own_1))):
            layer = to * 2 + n
            found.append((d.at[layer], stop.at[source_dp, stop_downs, :], own.at[downs, :], n))
            found.append((o.at[layer], stop.at[source_dp, stop_outs, :], own.at[outs, :], n))
        return found

    my_rank = dp // 2
    my_place = (dp % 2) * plan.tp + z
    stays = my_rank == z

    def share_in_plane():
        for step in range(1, plan.dp):
            to = (dp + step) % plan.dp

            @pl.when(stays)
            def _(to=to):
                for part, _, final, n in pieces(dp, to, my_place):
                    remote(part, final, share_send.at[n], share_recv.at[n], dp=to)

            @pl.when(jnp.logical_not(stays))
            def _(to=to):
                for part, stop, _, n in pieces(dp, to, my_place):
                    remote(part, stop, share_send.at[n], stop_recv.at[n, dp], dp=to)

        @pl.when(stays)
        def _():
            for part, _, final, n in pieces(dp, dp, my_place):
                pltpu.make_async_copy(part, final, share_recv.at[n]).start()

    def share_to_rank(source_dp):
        rank, place = source_dp // 2, (source_dp % 2) * plan.tp + z

        @pl.when((rank != z) & (source_dp == dp))
        def _():
            for part, _, final, n in pieces(dp, dp, place):
                remote(part, final, share_send.at[n], share_recv.at[n], tp=rank)

        @pl.when((rank != z) & (source_dp != dp))
        def _():
            for n, stop in enumerate((stop_0, stop_1)):
                wait_for(stop.at[source_dp], stop_recv.at[n, source_dp])
            for _, stop, final, n in pieces(source_dp, dp, place):
                remote(stop, final, share_send.at[n], share_recv.at[n], tp=rank)

    barrier = pltpu.get_barrier_semaphore()
    peers = [{"tp": (z + step) % plan.tp} for step in range(1, plan.tp)]
    peers += [{"dp": (dp + step) % plan.dp} for step in range(1, plan.dp)]
    for peer in peers:
        pl.semaphore_signal(barrier, inc=1, device_id=peer, device_id_type=MESH)
    pl.semaphore_wait(barrier, len(peers))

    start_exchange(0)
    share_in_plane()
    for index in range(GROUP, AHEAD):
        start_exchange(index)

    def retire(index):
        finish(slab_view(index), index, chunk)

        @pl.when((index < layers) & (index % GROUP == 0))
        def _():
            sent = pl.ds(0, (plan.tp - 1) * rows)
            wait_for(zbuf.at[pl.ds(index, GROUP), sent, pl.ds(0, plan.layer_window)], z_send.at[index])

        @pl.when(index >= layers)
        def _():
            finish_exchange(index, chunk)

    def step(index, _):
        slot = index % 2

        @pl.when(index + AHEAD < plan.chunks)
        def _():
            start_exchange(index + AHEAD)

        @pl.when((index >= SHARE_AT) & (index < SHARE_AT + 2 * plan.dp) & (index % 2 == SHARE_AT % 2))
        def _():
            share_to_rank((index - SHARE_AT) // 2)

        @pl.when(index < layers)
        def _():
            make_layer(index, slot)

        @pl.when(index >= layers)
        def _():
            make_head(index, slot)

        send_own(slab_view(index), index, slot, chunk)

        @pl.when(index >= LAG)
        def _():
            forward(slab_view(index - LAG), index - LAG, chunk)

        @pl.when(index >= 2 * LAG)
        def _():
            forward_diagonal(slab_view(index - 2 * LAG), index - 2 * LAG, chunk)

        @pl.when(index >= RETIRE)
        def _():
            retire(index - RETIRE)

        return 0

    lax.fori_loop(0, last, step, 0)

    make_tail(last % 2)
    send_own(slab_view(last), last, last % 2, tail)
    for index in range(last - LAG, last):
        forward(slab_view(index), index, chunk)
    forward(slab_view(last), last, tail)
    for index in range(last - 2 * LAG, last):
        forward_diagonal(slab_view(index), index, chunk)
    forward_diagonal(slab_view(last), last, tail)

    for index in range(last - RETIRE, last):
        retire(index)
    finish(slab_view(last), last, tail)
    finish_exchange(last, plan.tail_window)
    for n, own in enumerate((own_0, own_1)):
        wait_for(own, share_recv.at[n])
        for parts in (8, 5):
            wait_for(own.at[pl.ds(0, parts * (plan.down_rows + plan.out_rows)), :], share_send.at[n])


def gather(plan, *args):
    dma = pltpu.SemaphoreType.DMA
    per_chunk = dma((plan.chunks,))
    columns = args[3].shape[2]
    share_rows = plan.down_rows + plan.out_rows
    hbm = pl.BlockSpec(memory_space=pltpu.HBM)
    shapes = [(plan.dp, plan.chunks, plan.chunk, LANES)]
    shapes += [(plan.tp * 2 * share_rows, columns)] * 2 + [(plan.dp, share_rows, columns)] * 2
    return pl.pallas_call(
        functools.partial(gather_kernel, plan),
        out_shape=[jax.ShapeDtypeStruct(shape, jnp.bfloat16) for shape in shapes],
        in_specs=[hbm] * 8,
        out_specs=[hbm] * len(shapes),
        scratch_shapes=[
            pltpu.VMEM((plan.chunks, plan.tp * plan.rows, plan.layer_window), jnp.bfloat16),
            pltpu.VMEM((2, plan.chunk + 2 * LANES, LANES), jnp.bfloat16),
            per_chunk, per_chunk, dma((2,)),
            per_chunk, per_chunk, per_chunk, per_chunk, per_chunk, per_chunk,
            dma((2, plan.dp)), dma((2,)), dma((2,)),
        ],
        compiler_params=pltpu.CompilerParams(collective_id=0, has_side_effects=True),
        name="gather",
    )(*args)[:3]


def place_slabs(plan, slabs, first, count, shapes, store, held=()):
    hbm = pl.BlockSpec(memory_space=pltpu.HBM)
    depth = min(BUFFERS, count)
    ahead = depth // 2

    def body(slab, *refs):
        outs, (buffers, loads, stores) = refs[len(held):-3], refs[-3:]

        def each_size(chunk, act):
            if first + count == plan.chunks:
                pl.when(chunk < plan.chunks - 1)(lambda: act(plan.chunk))
                pl.when(chunk == plan.chunks - 1)(lambda: act(plan.tail))
            else:
                act(plan.chunk)

        def load(i, rows):
            for owner in range(plan.dp):
                pltpu.make_async_copy(
                    slab.at[owner, first + i, pl.ds(0, rows), :],
                    buffers.at[i % depth, pl.ds(0, rows), pl.ds(owner * LANES, LANES)],
                    loads.at[i % depth],
                ).start()

        def wait(i, rows, sem):
            buffer = buffers.at[i % depth, pl.ds(0, rows), :]
            pltpu.make_async_copy(buffer, buffer, sem.at[i % depth]).wait()

        def write(i, rows):
            wait(i, rows, loads)
            for source, target in store(buffers.at[i % depth], first + i, rows, outs):
                pltpu.make_async_copy(source, target, stores.at[i % depth]).start()

        def step(i, _):
            @pl.when(i >= depth)
            def _():
                each_size(first + i - depth, lambda rows: wait(i - depth, rows, stores))

            @pl.when(i < count)
            def _():
                each_size(first + i, lambda rows: load(i, rows))

            @pl.when((i >= ahead) & (i < count + ahead))
            def _():
                each_size(first + i - ahead, lambda rows: write(i - ahead, rows))

            return 0

        lax.fori_loop(0, count + depth, step, 0)

    outs = [jax.ShapeDtypeStruct(shape, jnp.bfloat16) for shape in shapes]
    return pl.pallas_call(
        body,
        in_specs=[hbm] * (1 + len(held)),
        out_specs=[hbm] * len(outs),
        out_shape=outs,
        scratch_shapes=[
            pltpu.VMEM((depth, plan.chunk, plan.dp * LANES), jnp.bfloat16),
            pltpu.SemaphoreType.DMA((depth,)),
            pltpu.SemaphoreType.DMA((depth,)),
        ],
        input_output_aliases={1 + n: n for n in range(len(held))},
        cost_estimate=pl.CostEstimate(
            flops=10**7, bytes_accessed=4 * count * plan.chunk * plan.dp * LANES, transcendentals=0
        ),
        compiler_params=pltpu.CompilerParams(vmem_limit_bytes=VMEM),
    )(slabs, *held)


def place_layers(plan, slabs):
    narrow, wide, width = 3 * plan.part, 2 * plan.wide, plan.dp * LANES

    def store(buffer, chunk, rows, outs):
        return [
            (buffer.at[pl.ds(0, narrow), :], outs[0].at[chunk]),
            (buffer.at[pl.ds(narrow, wide), :], outs[1].at[chunk]),
        ]

    shapes = [(plan.layers, narrow, width), (plan.layers, wide, width)]
    return place_slabs(plan, slabs, 0, plan.layers, shapes, store)


def place_head(plan, slabs, first, count, *held):
    def store(buffer, chunk, rows, outs):
        at = pl.multiple_of((chunk - plan.layers) * plan.chunk, 16)
        return [(buffer.at[pl.ds(0, rows), :], outs[0].at[pl.ds(at, rows), :])]

    shapes = [(plan.vocab, plan.dp * LANES)]
    return place_slabs(plan, slabs, plan.layers + first, count, shapes, store, held)[0]


def place_pieces(plan, pieces, held=()):
    owners = list(pieces)
    arrays = [array for owner in owners for array in pieces[owner]]
    rows, columns = arrays[0].shape
    downs, outs = plan.tp * 2 * plan.down_rows, plan.tp * 2 * plan.out_rows

    def body(*refs):
        sources, (down, out) = refs[: len(arrays)], refs[len(arrays) + len(held): -5]
        buffers, turned, loads, stores, out_stores = refs[-5:]
        dp = lax.axis_index("dp")
        core, x, y = dp % 2, (dp // 2) % 2, dp // 4

        def layer(n):
            flip_x, flip_y, flip_core = owners[n // plan.share]
            at = (y + flip_y * (1 - 2 * y)) * 4 + (x + flip_x * (1 - 2 * x)) * 2 + core + flip_core * (1 - 2 * core)
            return at * plan.share + n % plan.share

        loading = [pltpu.make_async_copy(source, buffers.at[n], loads.at[n]) for n, source in enumerate(sources)]
        storing = []
        for load in loading:
            load.start()
        for n, load in enumerate(loading):
            load.wait()
            storing.append(pltpu.make_async_copy(buffers.at[n, pl.ds(0, downs), :], down.at[layer(n)], stores.at[n]))
            storing[-1].start()
        for n in range(len(arrays)):
            for i in range(outs // LANES):
                for j in range(columns // LANES):
                    turned[n, pl.ds(j * LANES, LANES), pl.ds(i * LANES, LANES)] = buffers[
                        n, pl.ds(downs + i * LANES, LANES), pl.ds(j * LANES, LANES)
                    ].T
            storing.append(pltpu.make_async_copy(turned.at[n], out.at[layer(n)], out_stores.at[n]))
            storing[-1].start()
        for store in storing:
            store.wait()

    hbm = pl.BlockSpec(memory_space=pltpu.HBM)
    dma = pltpu.SemaphoreType.DMA((len(arrays),))
    shapes = [(plan.layers, downs, columns), (plan.layers, columns, outs)]
    return pl.pallas_call(
        body,
        out_shape=[jax.ShapeDtypeStruct(shape, jnp.bfloat16) for shape in shapes],
        in_specs=[hbm] * (len(arrays) + len(held)),
        out_specs=[hbm] * 2,
        scratch_shapes=[
            pltpu.VMEM((len(arrays), rows, columns), jnp.bfloat16),
            pltpu.VMEM((len(arrays), columns, outs), jnp.bfloat16),
            dma, dma, dma,
        ],
        input_output_aliases={len(arrays) + n: n for n in range(len(held))},
        cost_estimate=pl.CostEstimate(flops=10**7, bytes_accessed=4 * len(arrays) * rows * columns, transcendentals=0),
        compiler_params=pltpu.CompilerParams(vmem_limit_bytes=VMEM),
        name="place_pieces_end" if held else "place_pieces",
    )(*arrays, *held)


def solution(mesh):
    train_stack = P(None, ("dp", "tp"), None)
    train_head = P(("dp", "tp"), None)
    fused_stack = P(None, "tp", None)
    last_stack = P(None, None, "tp")
    head_rows = P("tp", None)

    def local_sync(w_query, w_key, w_value, w_out, w_gate, w_up, w_down, w_head):
        plan = Plan(mesh.shape["tp"], mesh.shape["dp"], w_query, w_gate, w_out, w_down, w_head)
        slabs, own_0, own_1 = gather(plan, w_query, w_key, w_value, w_out, w_gate, w_up, w_down, w_head)

        def swap(bit, array):
            return lax.ppermute(array, "dp", [(i, i ^ bit) for i in range(plan.dp)])

        pair, along_x, along_y = (functools.partial(swap, bit) for bit in (1, 2, 4))
        hold = lax.optimization_barrier

        x_1, y_0 = along_x(own_1), along_y(own_0)
        x_0, y_1 = along_x(own_0), along_y(own_1)
        pair_own = [pair(own_0), pair(own_1)]
        qkv_block, gate_up_block = place_layers(plan, slabs)
        x_1, y_0, qkv_block, slabs = hold((x_1, y_0, qkv_block, slabs))
        diagonal_0 = along_x(y_0)
        diagonal_1 = along_y(x_1)
        pair_x_1, pair_y_0 = pair(x_1), pair(y_0)
        early = plan.head_chunks * 5 // 18
        head_block = place_head(plan, slabs, early, plan.head_chunks - early)
        x_0, y_1, head_block, slabs = hold((x_0, y_1, head_block, slabs))
        pair_x_0, pair_y_1 = pair(x_0), pair(y_1)
        head_block = place_head(plan, slabs, 0, early, head_block)
        own_0, own_1, head_block = hold((own_0, own_1, head_block))
        near = {
            (0, 0, 0): [own_0, own_1], (0, 0, 1): pair_own, (1, 0, 0): [x_0, x_1], (1, 0, 1): [pair_x_0, pair_x_1],
            (0, 1, 0): [y_0, y_1], (0, 1, 1): [pair_y_0, pair_y_1],
        }
        placed = place_pieces(plan, near)
        diagonal_0, diagonal_1, down_block, o_block = hold((diagonal_0, diagonal_1, *placed))
        pair_diagonal = [pair(diagonal_0), pair(diagonal_1)]
        placed = place_pieces(plan, {(1, 1, 0): [diagonal_0, diagonal_1]}, (down_block, o_block))
        down_block, o_block = place_pieces(plan, {(1, 1, 1): pair_diagonal}, placed)
        return (
            qkv_block,
            o_block,
            gate_up_block,
            jnp.swapaxes(down_block, 1, 2),
            head_block,
        )

    return jax.shard_map(
        local_sync,
        mesh=mesh,
        in_specs=(train_stack,) * 7 + (train_head,),
        out_specs=(fused_stack, last_stack, fused_stack, last_stack, head_rows),
        check_vma=False,
    )
```

```python
import functools

import jax
import jax.numpy as jnp
from jax import lax
from jax.experimental import pallas as pl
from jax.experimental.pallas import tpu as pltpu
from jax.sharding import PartitionSpec as P


MESH = pl.DeviceIdType.MESH
LANES = 128
VMEM = 67_000_000
AHEAD = 4
BUFFERS = 6
LAG = 2
SHARE_AT = 14
RETIRE = 8
WHOLE = 3
WHOLE_AT = 2
PARTS = 4
GROUP = 2


class Plan:
    def __init__(self, tp, dp, w_query, w_gate, w_out, w_down, w_head):
        self.tp, self.dp = tp, dp
        self.layers, self.rows, columns = w_query.shape
        self.part = columns // tp
        self.wide = w_gate.shape[2] // tp
        self.vocab = w_head.shape[1] // tp
        self.head_tiles = w_head.shape[1] // LANES
        self.chunk = 3 * self.part + 2 * self.wide
        self.wide_window = -(-self.wide // LANES) * LANES
        self.layer_window = 3 * self.part + 2 * self.wide_window
        self.head_chunks = -(-self.vocab // self.chunk)
        self.chunks = self.layers + self.head_chunks
        end = self.vocab - (self.head_chunks - 1) * self.chunk
        self.tail_window = -(-(end + LANES) // LANES) * LANES
        self.window_tiles = (self.head_chunks - 1) * self.chunk // LANES + self.tail_window // LANES
        self.shift = max(self.vocab * r - self.head_base(r) * LANES for r in range(tp))
        self.out_rows, self.down_rows = w_out.shape[1], w_down.shape[1]
        self.downs, self.outs = 2 * tp * self.down_rows, 2 * tp * self.out_rows
        self.piece = self.downs + self.outs
        self.share = self.layers // dp
        self.columns = w_out.shape[2]
        self.whole = WHOLE * LANES
        self.cut = self.columns - self.whole
        self.extra_first = self.vocab - self.share * WHOLE * self.piece
        self.ring = self.layers + self.extra_first // self.chunk
        self.tail = self.extra_first % self.chunk

    def wide_base(self, rank):
        return (self.wide * rank) // LANES

    def head_base(self, rank):
        base = (self.vocab * rank) // LANES
        return base - (rank // (self.tp - 1)) * (self.vocab * (self.tp - 1) // LANES + self.window_tiles - self.head_tiles)


def gather_kernel(plan, q, k, v, o, g, u, d, h, slabs, own_0, own_1, whole, stop_0, stop_1, land_d, land_o, zbuf, tbuf,
                  z_recv, z_send, local, x_recv, y_recv, a_recv, b_recv, pair_recv, send, stop_recv, share_recv,
                  share_send, land_recv, land_send, whole_recv, whole_send, whole_pair_recv, whole_pair_send):
    z, dp = lax.axis_index("tp"), lax.axis_index("dp")
    core, x, y = dp % 2, (dp // 2) % 2, dp // 4
    x_peer = y * 4 + (1 - x) * 2 + core
    y_peer = (1 - y) * 4 + x * 2 + core
    diagonal = (1 - y) * 4 + (1 - x) * 2 + core
    pair = dp + 1 - 2 * core
    rows, chunk, tail = plan.rows, plan.chunk, plan.tail
    layers, ring, last = plan.layers, plan.ring, plan.chunks - 1
    my_rows = pl.ds(pl.multiple_of(z * rows, rows), rows)

    def lanes(first_tile, width):
        return pl.ds(pl.multiple_of(first_tile * LANES, LANES), width)

    def remote(source, target, send_sem, recv_sem, **to):
        pltpu.make_async_remote_copy(source, target, send_sem, recv_sem, device_id=to, device_id_type=MESH).start()

    def wait_for(ref, sem):
        pltpu.make_async_copy(ref, ref, sem).wait()


    def exchange(pieces, chunks, index):
        for step in range(1, plan.tp):
            rank = (z + step + core * (plan.tp - 2 * step)) % plan.tp
            for source, column, width in pieces(rank):
                target = zbuf.at[chunks, my_rows, pl.ds(column, width)]
                remote(source, target, z_send.at[index], z_recv.at[index], tp=rank)
        for source, column, width in pieces(z):
            target = zbuf.at[chunks, my_rows, pl.ds(column, width)]
            pltpu.make_async_copy(source, target, z_recv.at[index]).start()

    def layer_pieces(some):
        def pieces(rank):
            part, wide = plan.part, plan.wide_window
            narrow = lanes(rank * (part // LANES), part)
            window = lanes(plan.wide_base(rank), wide)
            return [
                (q.at[some, :, narrow], 0, part),
                (k.at[some, :, narrow], part, part),
                (v.at[some, :, narrow], 2 * part, part),
                (g.at[some, :, window], 3 * part, wide),
                (u.at[some, :, window], 3 * part + wide, wide),
            ]

        return pieces

    def head_pieces(step, width):
        def pieces(rank):
            return [(h.at[:, lanes(plan.head_base(rank) + step * (chunk // LANES), width)], 0, width)]

        return pieces

    def start_exchange(index):
        @pl.when((index < layers) & (index % GROUP == 0))
        def _():
            some = pl.ds(index, GROUP)
            exchange(layer_pieces(some), some, index)

        @pl.when((index >= layers) & (index < last))
        def _():
            exchange(head_pieces(index - layers, chunk), index, index)

        @pl.when(index == last)
        def _():
            exchange(head_pieces(last - layers, plan.tail_window), last, last)

    def wait_exchange(index, width):
        wait_for(zbuf.at[index, :, pl.ds(0, width)], z_recv.at[index])


    def turn(slot, tile, index, source_tile):
        tbuf[slot, pl.ds(tile * LANES, LANES), :] = zbuf[index, :, pl.ds(source_tile * LANES, LANES)].T

    def store(slot, first, index, to, count):
        pltpu.make_async_copy(
            tbuf.at[slot, pl.ds(first, count), :], slabs.at[dp, index, pl.ds(to, count), :], local.at[slot]
        ).start()

    def make_layer(index, slot):
        @pl.when(index % GROUP == 0)
        def _():
            wait_for(zbuf.at[pl.ds(index, GROUP), :, pl.ds(0, plan.layer_window)], z_recv.at[index])

        for tile in range(plan.layer_window // LANES):
            turn(slot, tile, index, tile)
        shift = plan.wide * z - plan.wide_base(z) * LANES
        narrow, wide, window = 3 * plan.part, plan.wide, plan.wide_window
        store(slot, 0, index, 0, narrow)
        store(slot, pl.multiple_of(narrow + shift, 16), index, narrow, wide)
        store(slot, pl.multiple_of(narrow + window + shift, 16), index, narrow + wide, wide)

    head_shift = plan.vocab * z - plan.head_base(z) * LANES

    def make_head(index, slot):
        @pl.when(index == layers)
        def _():
            wait_exchange(index, chunk)

        wait_exchange(index + 1, chunk)
        tiles = chunk // LANES
        for tile in range(tiles):
            turn(slot, tile, index, tile)
        for tile in range(2):
            turn(slot, tiles + tile, index + 1, tile)
        store(slot, pl.multiple_of(head_shift, 16), index, 0, chunk)

    def turn_rows(slot, first, count):
        start = first // LANES
        for tile in range(-(-(first % LANES + plan.shift + count) // LANES)):
            at = start + tile
            turn(slot, tile, layers + at // (chunk // LANES), at % (chunk // LANES))
        return pl.multiple_of(first % LANES + head_shift, 16)

    def make_tail(slot):
        wait_exchange(ring + 1, chunk)
        store(slot, turn_rows(slot, (ring - layers) * chunk, tail), ring, 0, tail)

    def make_extra():
        for index in range(ring + 2, last):
            wait_exchange(index, chunk)
        wait_exchange(last, plan.tail_window)
        blocks = plan.share * WHOLE

        def stored(n, own):
            wait_for(own.at[:, pl.ds(plan.cut, LANES)], local.at[n % 2])

        for n in range(blocks):
            own = (own_0, own_1)[n // WHOLE]
            if n >= 2:
                stored(n, own)
            at = turn_rows(n % 2, plan.extra_first + n * plan.piece, plan.piece)
            pltpu.make_async_copy(
                tbuf.at[n % 2, pl.ds(at, plan.piece), :],
                own.at[:, pl.ds(plan.cut + n % WHOLE * LANES, LANES)], local.at[n % 2],
            ).start()
        for n in range(blocks - min(2, blocks), blocks):
            stored(n, own_0)


    def slab_view(index):
        return lambda owner, first, count: slabs.at[owner, index, pl.ds(first, count), :]

    def push(part, index, recv, to):
        remote(part, part, send.at[index], recv.at[index], dp=to)

    def send_own(view, index, slot, count):
        own = view(dp, 0, count)
        wait_for(own, local.at[slot])
        push(own, index, x_recv, x_peer)
        push(own, index, y_recv, y_peer)
        push(own, index, pair_recv, pair)

    def forward(view, index, count):
        half = count // 2
        wait_for(view(x_peer, 0, count), x_recv.at[index])
        push(view(x_peer, half, half), index, b_recv, y_peer)
        push(view(x_peer, 0, count), index, pair_recv, pair)
        wait_for(view(y_peer, 0, count), y_recv.at[index])
        push(view(y_peer, 0, half), index, a_recv, x_peer)
        push(view(y_peer, 0, count), index, pair_recv, pair)

    def forward_diagonal(view, index, count):
        half = count // 2
        wait_for(view(diagonal, 0, half), a_recv.at[index])
        wait_for(view(diagonal, half, half), b_recv.at[index])
        push(view(diagonal, 0, count), index, pair_recv, pair)

    def finish(view, index, count):
        wait_for(view(pl.ds(0, 7), 0, count), send.at[index])
        wait_for(view(pl.ds(0, 4), 0, count), pair_recv.at[index])

    def finish_exchange(index, window):
        wait_for(zbuf.at[index, pl.ds(0, (plan.tp - 1) * rows), pl.ds(0, window)], z_send.at[index])


    def pieces(source_dp, to, place):
        all_rows = plan.downs
        downs = pl.ds(pl.multiple_of(place * plan.down_rows, 8), plan.down_rows)
        outs = pl.ds(pl.multiple_of(all_rows + place * plan.out_rows, 8), plan.out_rows)
        stop_downs, stop_outs = pl.ds(0, plan.down_rows), pl.ds(plan.down_rows, plan.out_rows)
        cut, home = pl.ds(plan.whole, plan.cut), pl.ds(0, plan.cut)
        found = []
        for n, (stop, own) in enumerate(((stop_0, own_0), (stop_1, own_1))):
            layer = to * 2 + n
            found.append((d.at[layer, :, cut], stop.at[source_dp, stop_downs, :], own.at[downs, home], n))
            found.append((o.at[layer, :, cut], stop.at[source_dp, stop_outs, :], own.at[outs, home], n))
        return found

    my_rank = dp // 2
    my_place = (dp % 2) * plan.tp + z
    stays = my_rank == z

    def share_in_plane():
        for step in range(1, plan.dp):
            to = (dp + step) % plan.dp

            @pl.when(stays)
            def _(to=to):
                for part, _, final, n in pieces(dp, to, my_place):
                    remote(part, final, share_send.at[n], share_recv.at[n], dp=to)

            @pl.when(jnp.logical_not(stays))
            def _(to=to):
                for part, stop, _, n in pieces(dp, to, my_place):
                    remote(part, stop, share_send.at[n], stop_recv.at[n, dp], dp=to)

        @pl.when(stays)
        def _():
            for part, _, final, n in pieces(dp, dp, my_place):
                pltpu.make_async_copy(part, final, share_recv.at[n]).start()

    def share_to_rank(source_dp):
        rank, place = source_dp // 2, (source_dp % 2) * plan.tp + z

        @pl.when((rank != z) & (source_dp == dp))
        def _():
            for part, _, final, n in pieces(dp, dp, place):
                remote(part, final, share_send.at[n], share_recv.at[n], tp=rank)

        @pl.when((rank != z) & (source_dp != dp))
        def _():
            for n, stop in enumerate((stop_0, stop_1)):
                wait_for(stop.at[source_dp], stop_recv.at[n, source_dp])
            for _, stop, final, n in pieces(source_dp, dp, place):
                remote(stop, final, share_send.at[n], share_recv.at[n], tp=rank)


    whole_columns = pl.ds(0, plan.whole)
    mine = ((d, land_d, plan.down_rows, 0), (o, land_o, plan.out_rows, plan.downs))
    half = layers // 2

    def whole_out():
        for n, (source, land, _, _) in enumerate(mine):
            for to, at in ((x_peer, 0), (y_peer, 2)):
                target = land.at[my_rank]
                remote(source.at[:, :, whole_columns], target, land_send.at[n], land_recv.at[at + n], dp=to)

    def whole_forward():
        for owner, at, first, to, then in ((x_peer, 0, half, y_peer, 6), (y_peer, 2, 0, x_peer, 4)):
            for n, (_, land, _, _) in enumerate(mine):
                wait_for(land.at[owner // 2], land_recv.at[at + n])
                part = land.at[owner // 2, pl.ds(first, half)]
                remote(part, part, land_send.at[n], land_recv.at[then + n], dp=to)

    def whole_arrive():
        for first, at in ((0, 4), (half, 6)):
            for n, (_, land, _, _) in enumerate(mine):
                wait_for(land.at[diagonal // 2, pl.ds(first, half)], land_recv.at[at + n])

    def whole_home(n, row):
        _, _, count, first = mine[n]
        return pl.ds(pl.multiple_of(first + row * count, 8), count)

    def whole_to_rank(block, part):
        flip_x, flip_y = block % 2, block // 2
        rank = (y + flip_y * (1 - 2 * y)) * 2 + x + flip_x * (1 - 2 * x)
        some = pl.ds(part * (layers // PARTS), layers // PARTS)

        def move(sources):
            for n, source in enumerate(sources):
                target = whole.at[some, whole_home(n, core * plan.tp + z), :]

                @pl.when(rank != z)
                def _(source=source, target=target, n=n):
                    remote(source, target, whole_send.at[n], whole_recv.at[n], tp=rank)

                @pl.when(rank == z)
                def _(source=source, target=target, n=n):
                    pltpu.make_async_copy(source, target, whole_recv.at[n]).start()

        pl.when(block == 0)(lambda: move([source.at[some, :, whole_columns] for source, _, _, _ in mine]))
        pl.when(block != 0)(lambda: move([land.at[rank, some] for _, land, _, _ in mine]))

    def whole_rows(which):
        return [
            whole.at[:, pl.ds(pl.multiple_of(first + which * plan.tp * count, 8), plan.tp * count), :]
            for _, _, count, first in mine
        ]

    def whole_to_pair():
        for n, part in enumerate(whole_rows(core)):
            wait_for(part, whole_recv.at[n])
            remote(part, part, whole_pair_send.at[n], whole_pair_recv.at[n], dp=pair)

    def whole_finish():
        for n, (_, land, count, first) in enumerate(mine):
            wait_for(land.at[pl.ds(0, 3)], land_send.at[n])
            wait_for(whole.at[:, pl.ds(first, (plan.tp - 1) * count), :], whole_send.at[n])
            wait_for(whole_rows(core)[n], whole_pair_send.at[n])
            wait_for(whole_rows(1 - core)[n], whole_pair_recv.at[n])

    barrier = pltpu.get_barrier_semaphore()
    peers = [{"tp": (z + step) % plan.tp} for step in range(1, plan.tp)]
    peers += [{"dp": (dp + step) % plan.dp} for step in range(1, plan.dp)]
    for peer in peers:
        pl.semaphore_signal(barrier, inc=1, device_id=peer, device_id_type=MESH)
    pl.semaphore_wait(barrier, len(peers))

    start_exchange(0)
    whole_out()
    share_in_plane()
    for index in range(GROUP, AHEAD):
        start_exchange(index)

    def retire(index):
        finish(slab_view(index), index, chunk)

        @pl.when((index < layers) & (index % GROUP == 0))
        def _():
            sent = pl.ds(0, (plan.tp - 1) * rows)
            wait_for(zbuf.at[pl.ds(index, GROUP), sent, pl.ds(0, plan.layer_window)], z_send.at[index])

        @pl.when(index >= layers)
        def _():
            finish_exchange(index, chunk)

    def step(index, _):
        slot = index % 2

        @pl.when(index + AHEAD < plan.chunks)
        def _():
            start_exchange(index + AHEAD)

        @pl.when((index >= SHARE_AT) & (index < SHARE_AT + 2 * plan.dp) & (index % 2 == SHARE_AT % 2))
        def _():
            share_to_rank((index - SHARE_AT) // 2)

        @pl.when(index == WHOLE_AT)
        def _():
            whole_forward()

        @pl.when(index == WHOLE_AT + 3)
        def _():
            whole_arrive()

        @pl.when((index >= WHOLE_AT) & (index < WHOLE_AT + 4 * PARTS))
        def _():
            whole_to_rank((index - WHOLE_AT) // PARTS, (index - WHOLE_AT) % PARTS)

        @pl.when(index == ring - 2)
        def _():
            whole_to_pair()

        @pl.when(index < layers)
        def _():
            make_layer(index, slot)

        @pl.when(index >= layers)
        def _():
            make_head(index, slot)

        send_own(slab_view(index), index, slot, chunk)

        @pl.when(index >= LAG)
        def _():
            forward(slab_view(index - LAG), index - LAG, chunk)

        @pl.when(index >= 2 * LAG)
        def _():
            forward_diagonal(slab_view(index - 2 * LAG), index - 2 * LAG, chunk)

        @pl.when(index >= RETIRE)
        def _():
            retire(index - RETIRE)

        return 0

    lax.fori_loop(0, ring, step, 0)

    make_tail(ring % 2)
    send_own(slab_view(ring), ring, ring % 2, tail)
    make_extra()
    for index in range(ring - LAG, ring):
        forward(slab_view(index), index, chunk)
    forward(slab_view(ring), ring, tail)
    for index in range(ring - 2 * LAG, ring):
        forward_diagonal(slab_view(index), index, chunk)
    forward_diagonal(slab_view(ring), ring, tail)

    for index in range(ring - RETIRE, ring):
        retire(index)
    finish(slab_view(ring), ring, tail)
    for index in range(ring, last):
        finish_exchange(index, chunk)
    finish_exchange(last, plan.tail_window)
    whole_finish()
    for n, own in enumerate((own_0, own_1)):
        wait_for(own.at[:, pl.ds(0, plan.cut)], share_recv.at[n])
        for parts in (8, 5):
            sent = pl.ds(0, parts * (plan.down_rows + plan.out_rows))
            wait_for(own.at[sent, pl.ds(0, plan.cut)], share_send.at[n])


def gather(plan, *args):
    dma = pltpu.SemaphoreType.DMA
    per_chunk = dma((plan.chunks,))
    share_rows = plan.down_rows + plan.out_rows
    hbm = pl.BlockSpec(memory_space=pltpu.HBM)
    shapes = [(plan.dp, plan.ring + 1, plan.chunk, LANES), (plan.piece, plan.columns), (plan.piece, plan.columns)]
    shapes += [(plan.layers, plan.piece, plan.whole)] + [(plan.dp, share_rows, plan.cut)] * 2
    shapes += [(plan.tp, plan.layers, count, plan.whole) for count in (plan.down_rows, plan.out_rows)]
    return pl.pallas_call(
        functools.partial(gather_kernel, plan),
        out_shape=[jax.ShapeDtypeStruct(shape, jnp.bfloat16) for shape in shapes],
        in_specs=[hbm] * 8,
        out_specs=[hbm] * len(shapes),
        scratch_shapes=[
            pltpu.VMEM((plan.chunks, plan.tp * plan.rows, plan.layer_window), jnp.bfloat16),
            pltpu.VMEM((2, plan.chunk + 2 * LANES, LANES), jnp.bfloat16),
            per_chunk, per_chunk, dma((2,)),
            per_chunk, per_chunk, per_chunk, per_chunk, per_chunk, per_chunk,
            dma((2, plan.dp)), dma((2,)), dma((2,)),
            dma((8,)), dma((2,)), dma((2,)), dma((2,)), dma((2,)), dma((2,)),
        ],
        compiler_params=pltpu.CompilerParams(collective_id=0, has_side_effects=True),
        name="gather",
    )(*args)[:4]


def place_slabs(plan, slabs, first, count, shapes, store, held=()):
    hbm = pl.BlockSpec(memory_space=pltpu.HBM)
    depth = min(BUFFERS, count)
    ahead = depth // 2

    def body(slab, *refs):
        outs, (buffers, loads, stores) = refs[len(held):-3], refs[-3:]

        def each_size(chunk, act):
            if first + count > plan.ring:
                pl.when(chunk < plan.ring)(lambda: act(plan.chunk))
                pl.when(chunk == plan.ring)(lambda: act(plan.tail))
            else:
                act(plan.chunk)

        def load(i, rows):
            for owner in range(plan.dp):
                pltpu.make_async_copy(
                    slab.at[owner, first + i, pl.ds(0, rows), :],
                    buffers.at[i % depth, pl.ds(0, rows), pl.ds(owner * LANES, LANES)],
                    loads.at[i % depth],
                ).start()

        def wait(i, rows, sem):
            buffer = buffers.at[i % depth, pl.ds(0, rows), :]
            pltpu.make_async_copy(buffer, buffer, sem.at[i % depth]).wait()

        def write(i, rows):
            wait(i, rows, loads)
            for source, target in store(buffers.at[i % depth], first + i, rows, outs):
                pltpu.make_async_copy(source, target, stores.at[i % depth]).start()

        def step(i, _):
            @pl.when(i >= depth)
            def _():
                each_size(first + i - depth, lambda rows: wait(i - depth, rows, stores))

            @pl.when(i < count)
            def _():
                each_size(first + i, lambda rows: load(i, rows))

            @pl.when((i >= ahead) & (i < count + ahead))
            def _():
                each_size(first + i - ahead, lambda rows: write(i - ahead, rows))

            return 0

        lax.fori_loop(0, count + depth, step, 0)

    outs = [jax.ShapeDtypeStruct(shape, jnp.bfloat16) for shape in shapes]
    return pl.pallas_call(
        body,
        in_specs=[hbm] * (1 + len(held)),
        out_specs=[hbm] * len(outs),
        out_shape=outs,
        scratch_shapes=[
            pltpu.VMEM((depth, plan.chunk, plan.dp * LANES), jnp.bfloat16),
            pltpu.SemaphoreType.DMA((depth,)),
            pltpu.SemaphoreType.DMA((depth,)),
        ],
        input_output_aliases={1 + n: n for n in range(len(held))},
        cost_estimate=pl.CostEstimate(
            flops=10**7, bytes_accessed=4 * count * plan.chunk * plan.dp * LANES, transcendentals=0
        ),
        compiler_params=pltpu.CompilerParams(vmem_limit_bytes=VMEM),
    )(slabs, *held)


def place_layers(plan, slabs):
    narrow, wide, width = 3 * plan.part, 2 * plan.wide, plan.dp * LANES

    def store(buffer, chunk, rows, outs):
        return [
            (buffer.at[pl.ds(0, narrow), :], outs[0].at[chunk]),
            (buffer.at[pl.ds(narrow, wide), :], outs[1].at[chunk]),
        ]

    shapes = [(plan.layers, narrow, width), (plan.layers, wide, width)]
    return place_slabs(plan, slabs, 0, plan.layers, shapes, store)


def place_head(plan, slabs, first, count, *held):
    def store(buffer, chunk, rows, outs):
        at = pl.multiple_of((chunk - plan.layers) * plan.chunk, 16)
        return [(buffer.at[pl.ds(0, rows), :], outs[0].at[pl.ds(at, rows), :])]

    shapes = [(plan.vocab, plan.dp * LANES)]
    return place_slabs(plan, slabs, plan.layers + first, count, shapes, store, held)[0]


def place_rows(plan, arrays, spots, width, column, held):
    count = len(spots([array for array in arrays], 0))
    columns = arrays[0].shape[-1]
    outs = [
        jax.ShapeDtypeStruct((plan.layers, plan.downs, plan.columns), jnp.bfloat16),
        jax.ShapeDtypeStruct((plan.layers, plan.columns, plan.outs), jnp.bfloat16),
        jax.ShapeDtypeStruct((plan.vocab, plan.dp * LANES), jnp.bfloat16),
    ]
    with_head = columns > width
    kept = [n for n in range(3) if n in held]
    made = [n for n in range(3 if with_head else 2)]

    def body(*refs):
        targets = dict(zip(made, refs[len(arrays) + len(kept):-6], strict=True))
        buffers, turned, loads, stores, out_stores, head_stores = refs[-6:]
        moves = spots(refs[: len(arrays)], lax.axis_index("dp"))
        loading = [pltpu.make_async_copy(move[0], buffers.at[n], loads.at[n]) for n, move in enumerate(moves)]
        storing = []
        for load in loading:
            load.start()

        def put(source, target, sem):
            storing.append(pltpu.make_async_copy(source, target, sem))
            storing[-1].start()

        place = pl.ds(column, width)
        for n, (load, (_, layer, owner, part)) in enumerate(zip(loading, moves, strict=True)):
            load.wait()
            put(buffers.at[n, pl.ds(0, plan.downs), pl.ds(0, width)], targets[0].at[layer, :, place], stores.at[n])
            for j in range((columns - width) // LANES):
                row = plan.extra_first + (part * WHOLE + j) * plan.piece
                put(
                    buffers.at[n, :, pl.ds(width + j * LANES, LANES)],
                    targets[2].at[pl.ds(row, plan.piece), pl.ds(pl.multiple_of(owner * LANES, LANES), LANES)],
                    head_stores.at[n, j],
                )
        for n, (_, layer, _, _) in enumerate(moves):
            for i in range(plan.outs // LANES):
                for j in range(width // LANES):
                    turned[n, pl.ds(j * LANES, LANES), pl.ds(i * LANES, LANES)] = buffers[
                        n, pl.ds(plan.downs + i * LANES, LANES), pl.ds(j * LANES, LANES)
                    ].T
            put(turned.at[n], targets[1].at[layer, place, :], out_stores.at[n])
        for store in storing:
            store.wait()

    hbm = pl.BlockSpec(memory_space=pltpu.HBM)
    dma = pltpu.SemaphoreType.DMA((count,))
    result = pl.pallas_call(
        body,
        out_shape=[outs[n] for n in made],
        in_specs=[hbm] * (len(arrays) + len(kept)),
        out_specs=[hbm] * len(made),
        scratch_shapes=[
            pltpu.VMEM((count, plan.piece, columns), jnp.bfloat16),
            pltpu.VMEM((count, width, plan.outs), jnp.bfloat16),
            dma, dma, dma, pltpu.SemaphoreType.DMA((count, max(WHOLE, 1))),
        ],
        input_output_aliases={len(arrays) + i: n for i, n in enumerate(kept)},
        cost_estimate=pl.CostEstimate(flops=10**7, bytes_accessed=4 * count * plan.piece * columns, transcendentals=0),
        compiler_params=pltpu.CompilerParams(vmem_limit_bytes=VMEM),
    )(*arrays, *(held[n] for n in kept))
    return dict(zip(made, result, strict=True))


def place_whole(plan, whole):
    def spots(refs, dp):
        return [(refs[0].at[layer], layer, 0, 0) for layer in range(plan.layers)]

    return place_rows(plan, [whole], spots, plan.whole, 0, {})


def place_shares(plan, shares, held):
    owners = list(shares)
    arrays = [array for owner in owners for array in shares[owner]]

    def spots(refs, dp):
        core, x, y = dp % 2, (dp // 2) % 2, dp // 4
        found = []
        for n, ref in enumerate(refs):
            flip_x, flip_y, flip_core = owners[n // plan.share]
            owner = (y + flip_y * (1 - 2 * y)) * 4 + (x + flip_x * (1 - 2 * x)) * 2 + core + flip_core * (1 - 2 * core)
            found.append((ref, owner * plan.share + n % plan.share, owner, n % plan.share))
        return found

    return place_rows(plan, arrays, spots, plan.cut, plan.whole, held)


def solution(mesh):
    train_stack = P(None, ("dp", "tp"), None)
    train_head = P(("dp", "tp"), None)
    fused_stack = P(None, "tp", None)
    last_stack = P(None, None, "tp")
    head_rows = P("tp", None)

    def local_sync(w_query, w_key, w_value, w_out, w_gate, w_up, w_down, w_head):
        plan = Plan(mesh.shape["tp"], mesh.shape["dp"], w_query, w_gate, w_out, w_down, w_head)
        slabs, own_0, own_1, whole = gather(plan, w_query, w_key, w_value, w_out, w_gate, w_up, w_down, w_head)

        def swap(bit, array):
            return lax.ppermute(array, "dp", [(i, i ^ bit) for i in range(plan.dp)])

        pair, along_x, along_y = (functools.partial(swap, bit) for bit in (1, 2, 4))
        hold = lax.optimization_barrier

        x_1, y_0 = along_x(own_1), along_y(own_0)
        x_0, y_1 = along_x(own_0), along_y(own_1)
        pair_own = [pair(own_0), pair(own_1)]
        qkv_block, gate_up_block = place_layers(plan, slabs)
        x_1, y_0, qkv_block, slabs = hold((x_1, y_0, qkv_block, slabs))
        diagonal_0 = along_x(y_0)
        diagonal_1 = along_y(x_1)
        pair_x_1, pair_y_0 = pair(x_1), pair(y_0)
        head_chunks = plan.ring + 1 - plan.layers
        early = head_chunks // 4
        head_block = place_head(plan, slabs, early, head_chunks - early)
        x_0, y_1, head_block, slabs, whole = hold((x_0, y_1, head_block, slabs, whole))
        pair_x_0, pair_y_1 = pair(x_0), pair(y_1)
        placed = place_whole(plan, whole)
        slabs, *placed = hold((slabs, placed[0], placed[1]))
        head_block = place_head(plan, slabs, 0, early, head_block)
        own_0, own_1, head_block = hold((own_0, own_1, head_block))
        near = {
            (0, 0, 0): [own_0, own_1], (0, 0, 1): pair_own, (1, 0, 0): [x_0, x_1], (1, 0, 1): [pair_x_0, pair_x_1],
            (0, 1, 0): [y_0, y_1], (0, 1, 1): [pair_y_0, pair_y_1],
        }
        placed = place_shares(plan, near, {0: placed[0], 1: placed[1], 2: head_block})
        diagonal_0, diagonal_1, *placed = hold((diagonal_0, diagonal_1, placed[0], placed[1], placed[2]))
        pair_diagonal = [pair(diagonal_0), pair(diagonal_1)]
        placed = place_shares(plan, {(1, 1, 0): [diagonal_0, diagonal_1]}, dict(enumerate(placed)))
        placed = place_shares(plan, {(1, 1, 1): pair_diagonal}, placed)
        down_block, o_block, head_block = placed[0], placed[1], placed[2]
        return (
            qkv_block,
            o_block,
            gate_up_block,
            jnp.swapaxes(down_block, 1, 2),
            head_block,
        )

    return jax.shard_map(
        local_sync,
        mesh=mesh,
        in_specs=(train_stack,) * 7 + (train_head,),
        out_specs=(fused_stack, last_stack, fused_stack, last_stack, head_rows),
        check_vma=False,
    )
```

```python
import functools

import jax
import jax.numpy as jnp
from jax import lax
from jax.experimental import pallas as pl
from jax.experimental.pallas import tpu as pltpu
from jax.sharding import PartitionSpec as P


MESH = pl.DeviceIdType.MESH
LANES = 128
VMEM = 67_000_000
AHEAD = 8
BUFFERS = 6
LAG = 2
SHARE_AT = 12
RETIRE = 8
WHOLE = 2
WHOLE_AT = 2
PARTS = 4
GROUP = 2


class Plan:
    def __init__(self, tp, dp, w_query, w_gate, w_out, w_down, w_head):
        self.tp, self.dp = tp, dp
        self.layers, self.rows, columns = w_query.shape
        self.part = columns // tp
        self.wide = w_gate.shape[2] // tp
        self.vocab = w_head.shape[1] // tp
        self.head_tiles = w_head.shape[1] // LANES
        self.chunk = 3 * self.part + 2 * self.wide
        self.wide_window = -(-self.wide // LANES) * LANES
        self.layer_window = 3 * self.part + 2 * self.wide_window
        self.head_chunks = -(-self.vocab // self.chunk)
        self.chunks = self.layers + self.head_chunks
        end = self.vocab - (self.head_chunks - 1) * self.chunk
        self.tail_window = -(-(end + LANES) // LANES) * LANES
        self.window_tiles = (self.head_chunks - 1) * self.chunk // LANES + self.tail_window // LANES
        self.shift = max(self.vocab * r - self.head_base(r) * LANES for r in range(tp))
        self.out_rows, self.down_rows = w_out.shape[1], w_down.shape[1]
        self.downs, self.outs = 2 * tp * self.down_rows, 2 * tp * self.out_rows
        self.piece = self.downs + self.outs
        self.share = self.layers // dp
        self.columns = w_out.shape[2]
        self.whole = WHOLE * LANES
        self.cut = self.columns - self.whole
        self.extra_first = self.vocab - self.share * WHOLE * self.piece
        self.ring = self.layers + self.extra_first // self.chunk
        self.tail = self.extra_first % self.chunk

    def wide_base(self, rank):
        return (self.wide * rank) // LANES

    def head_base(self, rank):
        base = (self.vocab * rank) // LANES
        return base - (rank // (self.tp - 1)) * (self.vocab * (self.tp - 1) // LANES + self.window_tiles - self.head_tiles)


def gather_kernel(plan, q, k, v, o, g, u, d, h, slabs, own_0, own_1, whole, stop_0, stop_1, land_d, land_o, zbuf, tbuf,
                  z_recv, z_send, local, x_recv, y_recv, a_recv, b_recv, pair_recv, send, stop_recv, share_recv,
                  share_send, land_recv, land_send, whole_recv, whole_send, whole_pair_recv, whole_pair_send,
                  keep_d, keep_o, keep_sem):
    z, dp = lax.axis_index("tp"), lax.axis_index("dp")
    core, x, y = dp % 2, (dp // 2) % 2, dp // 4
    x_peer = y * 4 + (1 - x) * 2 + core
    y_peer = (1 - y) * 4 + x * 2 + core
    diagonal = (1 - y) * 4 + (1 - x) * 2 + core
    pair = dp + 1 - 2 * core
    rows, chunk, tail = plan.rows, plan.chunk, plan.tail
    layers, ring, last = plan.layers, plan.ring, plan.chunks - 1
    my_rows = pl.ds(pl.multiple_of(z * rows, rows), rows)

    def lanes(first_tile, width):
        return pl.ds(pl.multiple_of(first_tile * LANES, LANES), width)

    def remote(source, target, send_sem, recv_sem, **to):
        pltpu.make_async_remote_copy(source, target, send_sem, recv_sem, device_id=to, device_id_type=MESH).start()

    def wait_for(ref, sem):
        pltpu.make_async_copy(ref, ref, sem).wait()


    def exchange(pieces, chunks, index):
        for step in range(1, plan.tp):
            rank = (z + step + core * (plan.tp - 2 * step)) % plan.tp
            for source, column, width in pieces(rank):
                target = zbuf.at[chunks, my_rows, pl.ds(column, width)]
                remote(source, target, z_send.at[index], z_recv.at[index], tp=rank)
        for source, column, width in pieces(z):
            target = zbuf.at[chunks, my_rows, pl.ds(column, width)]
            pltpu.make_async_copy(source, target, z_recv.at[index]).start()

    def layer_pieces(some):
        def pieces(rank):
            part, wide = plan.part, plan.wide_window
            narrow = lanes(rank * (part // LANES), part)
            window = lanes(plan.wide_base(rank), wide)
            return [
                (q.at[some, :, narrow], 0, part),
                (k.at[some, :, narrow], part, part),
                (v.at[some, :, narrow], 2 * part, part),
                (g.at[some, :, window], 3 * part, wide),
                (u.at[some, :, window], 3 * part + wide, wide),
            ]

        return pieces

    def head_pieces(step, width):
        def pieces(rank):
            return [(h.at[:, lanes(plan.head_base(rank) + step * (chunk // LANES), width)], 0, width)]

        return pieces

    def start_exchange(index):
        @pl.when((index < layers) & (index % GROUP == 0))
        def _():
            some = pl.ds(index, GROUP)
            exchange(layer_pieces(some), some, index)

        @pl.when((index >= layers) & (index < last))
        def _():
            exchange(head_pieces(index - layers, chunk), index, index)

        @pl.when(index == last)
        def _():
            exchange(head_pieces(last - layers, plan.tail_window), last, last)

    def wait_exchange(index, width):
        wait_for(zbuf.at[index, :, pl.ds(0, width)], z_recv.at[index])


    def turn(slot, tile, index, source_tile):
        tbuf[slot, pl.ds(tile * LANES, LANES), :] = zbuf[index, :, pl.ds(source_tile * LANES, LANES)].T

    def store(slot, first, index, to, count):
        pltpu.make_async_copy(
            tbuf.at[slot, pl.ds(first, count), :], slabs.at[dp, index, pl.ds(to, count), :], local.at[slot]
        ).start()

    def make_layer(index, slot):
        @pl.when(index % GROUP == 0)
        def _():
            wait_for(zbuf.at[pl.ds(index, GROUP), :, pl.ds(0, plan.layer_window)], z_recv.at[index])

        for tile in range(plan.layer_window // LANES):
            turn(slot, tile, index, tile)
        shift = plan.wide * z - plan.wide_base(z) * LANES
        narrow, wide, window = 3 * plan.part, plan.wide, plan.wide_window
        store(slot, 0, index, 0, narrow)
        store(slot, pl.multiple_of(narrow + shift, 16), index, narrow, wide)
        store(slot, pl.multiple_of(narrow + window + shift, 16), index, narrow + wide, wide)

    head_shift = plan.vocab * z - plan.head_base(z) * LANES

    def make_head(index, slot):
        @pl.when(index == layers)
        def _():
            wait_exchange(index, chunk)

        wait_exchange(index + 1, chunk)
        tiles = chunk // LANES
        for tile in range(tiles):
            turn(slot, tile, index, tile)
        for tile in range(2):
            turn(slot, tiles + tile, index + 1, tile)
        store(slot, pl.multiple_of(head_shift, 16), index, 0, chunk)

    def turn_rows(slot, first, count):
        start = first // LANES
        for tile in range(-(-(first % LANES + plan.shift + count) // LANES)):
            at = start + tile
            turn(slot, tile, layers + at // (chunk // LANES), at % (chunk // LANES))
        return pl.multiple_of(first % LANES + head_shift, 16)

    def make_tail(slot):
        wait_exchange(ring + 1, chunk)
        store(slot, turn_rows(slot, (ring - layers) * chunk, tail), ring, 0, tail)

    def make_extra():
        for index in range(ring + 2, last):
            wait_exchange(index, chunk)
        wait_exchange(last, plan.tail_window)
        blocks = plan.share * WHOLE

        def stored(n, own):
            wait_for(own.at[:, pl.ds(plan.cut, LANES)], local.at[n % 2])

        for n in range(blocks):
            own = (own_0, own_1)[n // WHOLE]
            if n >= 2:
                stored(n, own)
            at = turn_rows(n % 2, plan.extra_first + n * plan.piece, plan.piece)
            pltpu.make_async_copy(
                tbuf.at[n % 2, pl.ds(at, plan.piece), :],
                own.at[:, pl.ds(plan.cut + n % WHOLE * LANES, LANES)], local.at[n % 2],
            ).start()
        for n in range(blocks - min(2, blocks), blocks):
            stored(n, own_0)


    def slab_view(index):
        return lambda owner, first, count: slabs.at[owner, index, pl.ds(first, count), :]

    def push(part, index, recv, to):
        remote(part, part, send.at[index], recv.at[index], dp=to)

    def send_own(view, index, slot, count):
        own = view(dp, 0, count)
        wait_for(own, local.at[slot])
        push(own, index, x_recv, x_peer)
        push(own, index, y_recv, y_peer)
        push(own, index, pair_recv, pair)

    def forward(view, index, count):
        half = count // 2
        wait_for(view(x_peer, 0, count), x_recv.at[index])
        push(view(x_peer, half, half), index, b_recv, y_peer)
        push(view(x_peer, 0, count), index, pair_recv, pair)
        wait_for(view(y_peer, 0, count), y_recv.at[index])
        push(view(y_peer, 0, half), index, a_recv, x_peer)
        push(view(y_peer, 0, count), index, pair_recv, pair)

    def forward_diagonal(view, index, count):
        half = count // 2
        wait_for(view(diagonal, 0, half), a_recv.at[index])
        wait_for(view(diagonal, half, half), b_recv.at[index])
        push(view(diagonal, 0, count), index, pair_recv, pair)

    def finish(view, index, count):
        wait_for(view(pl.ds(0, 7), 0, count), send.at[index])
        wait_for(view(pl.ds(0, 4), 0, count), pair_recv.at[index])

    def finish_exchange(index, window):
        wait_for(zbuf.at[index, pl.ds(0, (plan.tp - 1) * rows), pl.ds(0, window)], z_send.at[index])


    def pieces(source_dp, to, place):
        all_rows = plan.downs
        downs = pl.ds(pl.multiple_of(place * plan.down_rows, 8), plan.down_rows)
        outs = pl.ds(pl.multiple_of(all_rows + place * plan.out_rows, 8), plan.out_rows)
        stop_downs, stop_outs = pl.ds(0, plan.down_rows), pl.ds(plan.down_rows, plan.out_rows)
        cut, home = pl.ds(plan.whole, plan.cut), pl.ds(0, plan.cut)
        found = []
        for n, (stop, own) in enumerate(((stop_0, own_0), (stop_1, own_1))):
            layer = to * 2 + n
            found.append((d.at[layer, :, cut], stop.at[source_dp, stop_downs, :], own.at[downs, home], n))
            found.append((o.at[layer, :, cut], stop.at[source_dp, stop_outs, :], own.at[outs, home], n))
        return found

    my_rank = dp // 2
    my_place = (dp % 2) * plan.tp + z
    stays = my_rank == z

    def share_in_plane():
        for step in range(1, plan.dp):
            to = (dp + step) % plan.dp

            @pl.when(stays)
            def _(to=to):
                for part, _, final, n in pieces(dp, to, my_place):
                    remote(part, final, share_send.at[n], share_recv.at[n], dp=to)

            @pl.when(jnp.logical_not(stays))
            def _(to=to):
                for part, stop, _, n in pieces(dp, to, my_place):
                    remote(part, stop, share_send.at[n], stop_recv.at[n, dp], dp=to)

        @pl.when(stays)
        def _():
            for part, _, final, n in pieces(dp, dp, my_place):
                pltpu.make_async_copy(part, final, share_recv.at[n]).start()

    def share_to_rank(source_dp):
        rank, place = source_dp // 2, (source_dp % 2) * plan.tp + z

        @pl.when((rank != z) & (source_dp == dp))
        def _():
            for part, _, final, n in pieces(dp, dp, place):
                remote(part, final, share_send.at[n], share_recv.at[n], tp=rank)

        @pl.when((rank != z) & (source_dp != dp))
        def _():
            for n, stop in enumerate((stop_0, stop_1)):
                wait_for(stop.at[source_dp], stop_recv.at[n, source_dp])
            for _, stop, final, n in pieces(source_dp, dp, place):
                remote(stop, final, share_send.at[n], share_recv.at[n], tp=rank)


    whole_columns = pl.ds(0, plan.whole)
    keep = (keep_d, keep_o)
    mine = ((d, land_d, plan.down_rows, 0), (o, land_o, plan.out_rows, plan.downs))
    half = layers // 2

    def whole_home(n, row):
        _, _, count, first = mine[n]
        return pl.ds(pl.multiple_of(first + row * count, 8), count)

    def landing(rank, some, act):
        pl.when(rank == z)(lambda: act([whole.at[some, whole_home(n, core * plan.tp + z), :] for n in range(2)]))
        pl.when(rank != z)(lambda: act([land.at[rank, some] for _, land, _, _ in mine]))

    every = pl.ds(0, layers)

    def whole_out():
        def act(places):
            for n, (source, _, _, _) in enumerate(mine):
                for to, at in ((x_peer, 0), (y_peer, 2)):
                    remote(source.at[:, :, whole_columns], places[n], land_send.at[n], land_recv.at[at + n], dp=to)

        landing(my_rank, every, act)

        @pl.when(stays)
        def _():
            for n, (source, _, _, _) in enumerate(mine):
                pltpu.make_async_copy(source.at[:, :, whole_columns], keep[n], keep_sem.at[n]).start()

    def whole_keep():
        @pl.when(stays)
        def _():
            for n in range(2):
                wait_for(keep[n], keep_sem.at[n])
                target = whole.at[:, whole_home(n, core * plan.tp + z), :]
                pltpu.make_async_copy(keep[n], target, keep_sem.at[2 + n]).start()

    def whole_forward():
        for owner, at, first, to, then in ((x_peer, 0, half, y_peer, 6), (y_peer, 2, 0, x_peer, 4)):
            def arrived(places, at=at):
                for n in range(2):
                    wait_for(places[n], land_recv.at[at + n])

            def on(places, to=to, then=then):
                for n in range(2):
                    remote(places[n], places[n], land_send.at[n], land_recv.at[then + n], dp=to)

            landing(owner // 2, every, arrived)
            landing(owner // 2, pl.ds(first, half), on)

    def whole_arrive():
        for first, at in ((0, 4), (half, 6)):
            def arrived(places, at=at):
                for n in range(2):
                    wait_for(places[n], land_recv.at[at + n])

            landing(diagonal // 2, pl.ds(first, half), arrived)

    def whole_to_rank(shift, part):
        rank = (z + shift + core * (plan.tp - 2 * shift)) % plan.tp
        some = pl.ds(part * (layers // PARTS), layers // PARTS)

        def move(sources):
            for n, source in enumerate(sources):
                target = whole.at[some, whole_home(n, core * plan.tp + z), :]
                remote(source, target, whole_send.at[n], whole_recv.at[n], tp=rank)

        pl.when(rank == my_rank)(lambda: move([source.at[some, :, whole_columns] for source, _, _, _ in mine]))
        pl.when(rank != my_rank)(lambda: move([land.at[rank, some] for _, land, _, _ in mine]))

    def whole_rows(which):
        return [
            whole.at[:, pl.ds(pl.multiple_of(first + which * plan.tp * count, 8), plan.tp * count), :]
            for _, _, count, first in mine
        ]

    def whole_to_pair():
        for n, part in enumerate(whole_rows(core)):
            away = pl.ds(0, (plan.tp - 1) * mine[n][2])
            wait_for(whole.at[:, away, :], whole_recv.at[n])

            @pl.when(stays)
            def _(n=n):
                wait_for(keep[n], keep_sem.at[2 + n])

            remote(part, part, whole_pair_send.at[n], whole_pair_recv.at[n], dp=pair)

    def whole_finish():
        for n, (_, land, count, first) in enumerate(mine):
            wait_for(land.at[pl.ds(0, 3)], land_send.at[n])
            wait_for(whole.at[:, pl.ds(first, (plan.tp - 1) * count), :], whole_send.at[n])
            wait_for(whole_rows(core)[n], whole_pair_send.at[n])
            wait_for(whole_rows(1 - core)[n], whole_pair_recv.at[n])

    barrier = pltpu.get_barrier_semaphore()
    peers = [{"tp": (z + step) % plan.tp} for step in range(1, plan.tp)]
    peers += [{"dp": (dp + step) % plan.dp} for step in range(1, plan.dp)]
    for peer in peers:
        pl.semaphore_signal(barrier, inc=1, device_id=peer, device_id_type=MESH)
    pl.semaphore_wait(barrier, len(peers))

    start_exchange(0)
    whole_out()
    share_in_plane()
    for index in range(GROUP, AHEAD):
        start_exchange(index)

    def retire(index):
        finish(slab_view(index), index, chunk)

        @pl.when((index < layers) & (index % GROUP == 0))
        def _():
            sent = pl.ds(0, (plan.tp - 1) * rows)
            wait_for(zbuf.at[pl.ds(index, GROUP), sent, pl.ds(0, plan.layer_window)], z_send.at[index])

        @pl.when(index >= layers)
        def _():
            finish_exchange(index, chunk)

    def step(index, _):
        slot = index % 2

        @pl.when(index + AHEAD < plan.chunks)
        def _():
            start_exchange(index + AHEAD)

        @pl.when((index >= SHARE_AT) & (index < SHARE_AT + 2 * plan.dp) & (index % 2 == SHARE_AT % 2))
        def _():
            share_to_rank((index - SHARE_AT) // 2)

        @pl.when(index == WHOLE_AT)
        def _():
            whole_keep()
            whole_forward()

        @pl.when(index == WHOLE_AT + 3)
        def _():
            whole_arrive()

        @pl.when((index >= WHOLE_AT + 4) & (index < WHOLE_AT + 4 + (plan.tp - 1) * PARTS))
        def _():
            whole_to_rank((index - WHOLE_AT - 4) % (plan.tp - 1) + 1, (index - WHOLE_AT - 4) // (plan.tp - 1))

        @pl.when(index == ring - 2)
        def _():
            whole_to_pair()

        @pl.when(index < layers)
        def _():
            make_layer(index, slot)

        @pl.when(index >= layers)
        def _():
            make_head(index, slot)

        send_own(slab_view(index), index, slot, chunk)

        @pl.when(index >= LAG)
        def _():
            forward(slab_view(index - LAG), index - LAG, chunk)

        @pl.when(index >= 2 * LAG)
        def _():
            forward_diagonal(slab_view(index - 2 * LAG), index - 2 * LAG, chunk)

        @pl.when(index >= RETIRE)
        def _():
            retire(index - RETIRE)

        return 0

    lax.fori_loop(0, ring, step, 0)

    make_tail(ring % 2)
    send_own(slab_view(ring), ring, ring % 2, tail)
    make_extra()
    for index in range(ring - LAG, ring):
        forward(slab_view(index), index, chunk)
    forward(slab_view(ring), ring, tail)
    for index in range(ring - 2 * LAG, ring):
        forward_diagonal(slab_view(index), index, chunk)
    forward_diagonal(slab_view(ring), ring, tail)

    for index in range(ring - RETIRE, ring):
        retire(index)
    finish(slab_view(ring), ring, tail)
    for index in range(ring, last):
        finish_exchange(index, chunk)
    finish_exchange(last, plan.tail_window)
    whole_finish()
    for n, own in enumerate((own_0, own_1)):
        wait_for(own.at[:, pl.ds(0, plan.cut)], share_recv.at[n])
        for parts in (8, 5):
            sent = pl.ds(0, parts * (plan.down_rows + plan.out_rows))
            wait_for(own.at[sent, pl.ds(0, plan.cut)], share_send.at[n])


def gather(plan, *args):
    dma = pltpu.SemaphoreType.DMA
    per_chunk = dma((plan.chunks,))
    share_rows = plan.down_rows + plan.out_rows
    hbm = pl.BlockSpec(memory_space=pltpu.HBM)
    shapes = [(plan.dp, plan.ring + 1, plan.chunk, LANES), (plan.piece, plan.columns), (plan.piece, plan.columns)]
    shapes += [(plan.layers, plan.piece, plan.whole)] + [(plan.dp, share_rows, plan.cut)] * 2
    shapes += [(plan.tp, plan.layers, count, plan.whole) for count in (plan.down_rows, plan.out_rows)]
    return pl.pallas_call(
        functools.partial(gather_kernel, plan),
        out_shape=[jax.ShapeDtypeStruct(shape, jnp.bfloat16) for shape in shapes],
        in_specs=[hbm] * 8,
        out_specs=[hbm] * len(shapes),
        scratch_shapes=[
            pltpu.VMEM((plan.chunks, plan.tp * plan.rows, plan.layer_window), jnp.bfloat16),
            pltpu.VMEM((2, plan.chunk + 2 * LANES, LANES), jnp.bfloat16),
            per_chunk, per_chunk, dma((2,)),
            per_chunk, per_chunk, per_chunk, per_chunk, per_chunk, per_chunk,
            dma((2, plan.dp)), dma((2,)), dma((2,)),
            dma((8,)), dma((2,)), dma((2,)), dma((2,)), dma((2,)), dma((2,)),
            pltpu.VMEM((plan.layers, plan.down_rows, plan.whole), jnp.bfloat16),
            pltpu.VMEM((plan.layers, plan.out_rows, plan.whole), jnp.bfloat16),
            dma((4,)),
        ],
        compiler_params=pltpu.CompilerParams(collective_id=0, has_side_effects=True),
        name="gather",
    )(*args)[:4]


def place_slabs(plan, slabs, first, count, shapes, store, held=()):
    hbm = pl.BlockSpec(memory_space=pltpu.HBM)
    depth = min(BUFFERS, count)
    ahead = depth // 2

    def body(slab, *refs):
        outs, (buffers, loads, stores) = refs[len(held):-3], refs[-3:]

        def each_size(chunk, act):
            if first + count > plan.ring:
                pl.when(chunk < plan.ring)(lambda: act(plan.chunk))
                pl.when(chunk == plan.ring)(lambda: act(plan.tail))
            else:
                act(plan.chunk)

        def load(i, rows):
            for owner in range(plan.dp):
                pltpu.make_async_copy(
                    slab.at[owner, first + i, pl.ds(0, rows), :],
                    buffers.at[i % depth, pl.ds(0, rows), pl.ds(owner * LANES, LANES)],
                    loads.at[i % depth],
                ).start()

        def wait(i, rows, sem):
            buffer = buffers.at[i % depth, pl.ds(0, rows), :]
            pltpu.make_async_copy(buffer, buffer, sem.at[i % depth]).wait()

        def write(i, rows):
            wait(i, rows, loads)
            for source, target in store(buffers.at[i % depth], first + i, rows, outs):
                pltpu.make_async_copy(source, target, stores.at[i % depth]).start()

        def step(i, _):
            @pl.when(i >= depth)
            def _():
                each_size(first + i - depth, lambda rows: wait(i - depth, rows, stores))

            @pl.when(i < count)
            def _():
                each_size(first + i, lambda rows: load(i, rows))

            @pl.when((i >= ahead) & (i < count + ahead))
            def _():
                each_size(first + i - ahead, lambda rows: write(i - ahead, rows))

            return 0

        lax.fori_loop(0, count + depth, step, 0)

    outs = [jax.ShapeDtypeStruct(shape, jnp.bfloat16) for shape in shapes]
    return pl.pallas_call(
        body,
        in_specs=[hbm] * (1 + len(held)),
        out_specs=[hbm] * len(outs),
        out_shape=outs,
        scratch_shapes=[
            pltpu.VMEM((depth, plan.chunk, plan.dp * LANES), jnp.bfloat16),
            pltpu.SemaphoreType.DMA((depth,)),
            pltpu.SemaphoreType.DMA((depth,)),
        ],
        input_output_aliases={1 + n: n for n in range(len(held))},
        cost_estimate=pl.CostEstimate(
            flops=10**7, bytes_accessed=4 * count * plan.chunk * plan.dp * LANES, transcendentals=0
        ),
        compiler_params=pltpu.CompilerParams(vmem_limit_bytes=VMEM),
    )(slabs, *held)


def place_layers(plan, slabs):
    narrow, wide, width = 3 * plan.part, 2 * plan.wide, plan.dp * LANES

    def store(buffer, chunk, rows, outs):
        return [
            (buffer.at[pl.ds(0, narrow), :], outs[0].at[chunk]),
            (buffer.at[pl.ds(narrow, wide), :], outs[1].at[chunk]),
        ]

    shapes = [(plan.layers, narrow, width), (plan.layers, wide, width)]
    return place_slabs(plan, slabs, 0, plan.layers, shapes, store)


def place_head(plan, slabs, first, count, *held):
    def store(buffer, chunk, rows, outs):
        at = pl.multiple_of((chunk - plan.layers) * plan.chunk, 16)
        return [(buffer.at[pl.ds(0, rows), :], outs[0].at[pl.ds(at, rows), :])]

    shapes = [(plan.vocab, plan.dp * LANES)]
    return place_slabs(plan, slabs, plan.layers + first, count, shapes, store, held)[0]


def place_rows(plan, arrays, spots, width, column, held):
    count = len(spots([array for array in arrays], 0))
    columns = arrays[0].shape[-1]
    outs = [
        jax.ShapeDtypeStruct((plan.layers, plan.downs, plan.columns), jnp.bfloat16),
        jax.ShapeDtypeStruct((plan.layers, plan.columns, plan.outs), jnp.bfloat16),
        jax.ShapeDtypeStruct((plan.vocab, plan.dp * LANES), jnp.bfloat16),
    ]
    with_head = columns > width
    kept = [n for n in range(3) if n in held]
    made = [n for n in range(3 if with_head else 2)]

    def body(*refs):
        targets = dict(zip(made, refs[len(arrays) + len(kept):-6], strict=True))
        buffers, turned, loads, stores, out_stores, head_stores = refs[-6:]
        moves = spots(refs[: len(arrays)], lax.axis_index("dp"))
        loading = [pltpu.make_async_copy(move[0], buffers.at[n], loads.at[n]) for n, move in enumerate(moves)]
        storing = []
        for load in loading:
            load.start()

        def put(source, target, sem):
            storing.append(pltpu.make_async_copy(source, target, sem))
            storing[-1].start()

        place = pl.ds(column, width)
        for n, (load, (_, layer, owner, part)) in enumerate(zip(loading, moves, strict=True)):
            load.wait()
            put(buffers.at[n, pl.ds(0, plan.downs), pl.ds(0, width)], targets[0].at[layer, :, place], stores.at[n])
            for j in range((columns - width) // LANES):
                row = plan.extra_first + (part * WHOLE + j) * plan.piece
                put(
                    buffers.at[n, :, pl.ds(width + j * LANES, LANES)],
                    targets[2].at[pl.ds(row, plan.piece), pl.ds(pl.multiple_of(owner * LANES, LANES), LANES)],
                    head_stores.at[n, j],
                )
        for n, (_, layer, _, _) in enumerate(moves):
            for i in range(plan.outs // LANES):
                for j in range(width // LANES):
                    turned[n, pl.ds(j * LANES, LANES), pl.ds(i * LANES, LANES)] = buffers[
                        n, pl.ds(plan.downs + i * LANES, LANES), pl.ds(j * LANES, LANES)
                    ].T
            put(turned.at[n], targets[1].at[layer, place, :], out_stores.at[n])
        for store in storing:
            store.wait()

    hbm = pl.BlockSpec(memory_space=pltpu.HBM)
    dma = pltpu.SemaphoreType.DMA((count,))
    result = pl.pallas_call(
        body,
        out_shape=[outs[n] for n in made],
        in_specs=[hbm] * (len(arrays) + len(kept)),
        out_specs=[hbm] * len(made),
        scratch_shapes=[
            pltpu.VMEM((count, plan.piece, columns), jnp.bfloat16),
            pltpu.VMEM((count, width, plan.outs), jnp.bfloat16),
            dma, dma, dma, pltpu.SemaphoreType.DMA((count, max(WHOLE, 1))),
        ],
        input_output_aliases={len(arrays) + i: n for i, n in enumerate(kept)},
        cost_estimate=pl.CostEstimate(flops=10**7, bytes_accessed=4 * count * plan.piece * columns, transcendentals=0),
        compiler_params=pltpu.CompilerParams(vmem_limit_bytes=VMEM),
    )(*arrays, *(held[n] for n in kept))
    return dict(zip(made, result, strict=True))


def place_whole(plan, whole):
    def spots(refs, dp):
        return [(refs[0].at[layer], layer, 0, 0) for layer in range(plan.layers)]

    return place_rows(plan, [whole], spots, plan.whole, 0, {})


def place_shares(plan, shares, held):
    owners = list(shares)
    arrays = [array for owner in owners for array in shares[owner]]

    def spots(refs, dp):
        core, x, y = dp % 2, (dp // 2) % 2, dp // 4
        found = []
        for n, ref in enumerate(refs):
            flip_x, flip_y, flip_core = owners[n // plan.share]
            owner = (y + flip_y * (1 - 2 * y)) * 4 + (x + flip_x * (1 - 2 * x)) * 2 + core + flip_core * (1 - 2 * core)
            found.append((ref, owner * plan.share + n % plan.share, owner, n % plan.share))
        return found

    return place_rows(plan, arrays, spots, plan.cut, plan.whole, held)


def solution(mesh):
    train_stack = P(None, ("dp", "tp"), None)
    train_head = P(("dp", "tp"), None)
    fused_stack = P(None, "tp", None)
    last_stack = P(None, None, "tp")
    head_rows = P("tp", None)

    def local_sync(w_query, w_key, w_value, w_out, w_gate, w_up, w_down, w_head):
        plan = Plan(mesh.shape["tp"], mesh.shape["dp"], w_query, w_gate, w_out, w_down, w_head)
        slabs, own_0, own_1, whole = gather(plan, w_query, w_key, w_value, w_out, w_gate, w_up, w_down, w_head)

        def swap(bit, array):
            return lax.ppermute(array, "dp", [(i, i ^ bit) for i in range(plan.dp)])

        pair, along_x, along_y = (functools.partial(swap, bit) for bit in (1, 2, 4))
        hold = lax.optimization_barrier

        x_1, y_0 = along_x(own_1), along_y(own_0)
        x_0, y_1 = along_x(own_0), along_y(own_1)
        pair_own = [pair(own_0), pair(own_1)]
        qkv_block, gate_up_block = place_layers(plan, slabs)
        x_1, y_0, qkv_block, slabs = hold((x_1, y_0, qkv_block, slabs))
        diagonal_0 = along_x(y_0)
        diagonal_1 = along_y(x_1)
        pair_x_1, pair_y_0 = pair(x_1), pair(y_0)
        head_chunks = plan.ring + 1 - plan.layers
        early = head_chunks // 4
        head_block = place_head(plan, slabs, early, head_chunks - early)
        x_0, y_1, head_block, slabs, whole = hold((x_0, y_1, head_block, slabs, whole))
        pair_x_0, pair_y_1 = pair(x_0), pair(y_1)
        placed = place_whole(plan, whole)
        slabs, *placed = hold((slabs, placed[0], placed[1]))
        head_block = place_head(plan, slabs, 0, early, head_block)
        own_0, own_1, head_block = hold((own_0, own_1, head_block))
        near = {
            (0, 0, 0): [own_0, own_1], (0, 0, 1): pair_own, (1, 0, 0): [x_0, x_1], (1, 0, 1): [pair_x_0, pair_x_1],
            (0, 1, 0): [y_0, y_1], (0, 1, 1): [pair_y_0, pair_y_1],
        }
        placed = place_shares(plan, near, {0: placed[0], 1: placed[1], 2: head_block})
        diagonal_0, diagonal_1, *placed = hold((diagonal_0, diagonal_1, placed[0], placed[1], placed[2]))
        pair_diagonal = [pair(diagonal_0), pair(diagonal_1)]
        placed = place_shares(plan, {(1, 1, 0): [diagonal_0, diagonal_1]}, dict(enumerate(placed)))
        placed = place_shares(plan, {(1, 1, 1): pair_diagonal}, placed)
        down_block, o_block, head_block = placed[0], placed[1], placed[2]
        return (
            qkv_block,
            o_block,
            gate_up_block,
            jnp.swapaxes(down_block, 1, 2),
            head_block,
        )

    return jax.shard_map(
        local_sync,
        mesh=mesh,
        in_specs=(train_stack,) * 7 + (train_head,),
        out_specs=(fused_stack, last_stack, fused_stack, last_stack, head_rows),
        check_vma=False,
    )
```

```python
import functools

import jax
import jax.numpy as jnp
from jax import lax
from jax.experimental import pallas as pl
from jax.experimental.pallas import tpu as pltpu
from jax.sharding import PartitionSpec as P


MESH = pl.DeviceIdType.MESH
LANES = 128
VMEM = 67_000_000
AHEAD = 14
BUFFERS = 6
LAG = 2
SHARE_AT = 20
RETIRE = 8
WHOLE = 3
WHOLE_AT = 2
RANKS_AT = 10
PARTS = 4
GROUP = 4


class Plan:
    def __init__(self, tp, dp, w_query, w_gate, w_out, w_down, w_head):
        self.tp, self.dp = tp, dp
        self.layers, self.rows, columns = w_query.shape
        self.part = columns // tp
        self.wide = w_gate.shape[2] // tp
        self.vocab = w_head.shape[1] // tp
        self.head_tiles = w_head.shape[1] // LANES
        self.chunk = 3 * self.part + 2 * self.wide
        self.wide_window = -(-self.wide // LANES) * LANES
        self.layer_window = 3 * self.part + 2 * self.wide_window
        self.head_chunks = -(-self.vocab // self.chunk)
        self.chunks = self.layers + self.head_chunks
        end = self.vocab - (self.head_chunks - 1) * self.chunk
        self.tail_window = -(-(end + LANES) // LANES) * LANES
        self.window_tiles = (self.head_chunks - 1) * self.chunk // LANES + self.tail_window // LANES
        self.shift = max(self.vocab * r - self.head_base(r) * LANES for r in range(tp))
        self.out_rows, self.down_rows = w_out.shape[1], w_down.shape[1]
        self.downs, self.outs = 2 * tp * self.down_rows, 2 * tp * self.out_rows
        self.piece = self.downs + self.outs
        self.share = self.layers // dp
        self.columns = w_out.shape[2]
        self.whole = WHOLE * LANES
        self.cut = self.columns - self.whole
        self.extra_first = self.vocab - self.share * WHOLE * self.piece
        self.ring = self.layers + self.extra_first // self.chunk
        self.tail = self.extra_first % self.chunk

    def wide_base(self, rank):
        return (self.wide * rank) // LANES

    def head_base(self, rank):
        base = (self.vocab * rank) // LANES
        return base - (rank // (self.tp - 1)) * (self.vocab * (self.tp - 1) // LANES + self.window_tiles - self.head_tiles)


def gather_kernel(plan, q, k, v, o, g, u, d, h, slabs, own_0, own_1, whole, stop_0, stop_1, land_d, land_o, zbuf, tbuf,
                  z_recv, z_send, local, x_recv, y_recv, a_recv, b_recv, pair_recv, send, stop_recv, share_recv,
                  share_send, land_recv, land_send, whole_recv, whole_send, whole_pair_recv, whole_pair_send,
                  keep_d, keep_o, keep_sem):
    z, dp = lax.axis_index("tp"), lax.axis_index("dp")
    core, x, y = dp % 2, (dp // 2) % 2, dp // 4
    x_peer = y * 4 + (1 - x) * 2 + core
    y_peer = (1 - y) * 4 + x * 2 + core
    diagonal = (1 - y) * 4 + (1 - x) * 2 + core
    pair = dp + 1 - 2 * core
    rows, chunk, tail = plan.rows, plan.chunk, plan.tail
    layers, ring, last = plan.layers, plan.ring, plan.chunks - 1
    my_rows = pl.ds(pl.multiple_of(z * rows, rows), rows)

    def lanes(first_tile, width):
        return pl.ds(pl.multiple_of(first_tile * LANES, LANES), width)

    def remote(source, target, send_sem, recv_sem, **to):
        pltpu.make_async_remote_copy(source, target, send_sem, recv_sem, device_id=to, device_id_type=MESH).start()

    def wait_for(ref, sem):
        pltpu.make_async_copy(ref, ref, sem).wait()


    def exchange(pieces, chunks, index):
        for step in range(1, plan.tp):
            rank = (z + step + core * (plan.tp - 2 * step)) % plan.tp
            for source, column, width in pieces(rank):
                target = zbuf.at[chunks, my_rows, pl.ds(column, width)]
                remote(source, target, z_send.at[index], z_recv.at[index], tp=rank)
        for source, column, width in pieces(z):
            target = zbuf.at[chunks, my_rows, pl.ds(column, width)]
            pltpu.make_async_copy(source, target, z_recv.at[index]).start()

    def layer_pieces(some):
        def pieces(rank):
            part, wide = plan.part, plan.wide_window
            narrow = lanes(rank * (part // LANES), part)
            window = lanes(plan.wide_base(rank), wide)
            return [
                (q.at[some, :, narrow], 0, part),
                (k.at[some, :, narrow], part, part),
                (v.at[some, :, narrow], 2 * part, part),
                (g.at[some, :, window], 3 * part, wide),
                (u.at[some, :, window], 3 * part + wide, wide),
            ]

        return pieces

    def head_pieces(step, width):
        def pieces(rank):
            return [(h.at[:, lanes(plan.head_base(rank) + step * (chunk // LANES), width)], 0, width)]

        return pieces

    def start_exchange(index):
        @pl.when((index < layers) & (index % GROUP == 0))
        def _():
            some = pl.ds(index, GROUP)
            exchange(layer_pieces(some), some, index)

        @pl.when((index >= layers) & (index < last))
        def _():
            exchange(head_pieces(index - layers, chunk), index, index)

        @pl.when(index == last)
        def _():
            exchange(head_pieces(last - layers, plan.tail_window), last, last)

    def wait_exchange(index, width):
        wait_for(zbuf.at[index, :, pl.ds(0, width)], z_recv.at[index])


    def turn(slot, tile, index, source_tile):
        tbuf[slot, pl.ds(tile * LANES, LANES), :] = zbuf[index, :, pl.ds(source_tile * LANES, LANES)].T

    def store(slot, first, index, to, count):
        pltpu.make_async_copy(
            tbuf.at[slot, pl.ds(first, count), :], slabs.at[dp, index, pl.ds(to, count), :], local.at[slot]
        ).start()

    def make_layer(index, slot):
        @pl.when(index % GROUP == 0)
        def _():
            wait_for(zbuf.at[pl.ds(index, GROUP), :, pl.ds(0, plan.layer_window)], z_recv.at[index])

        for tile in range(plan.layer_window // LANES):
            turn(slot, tile, index, tile)
        shift = plan.wide * z - plan.wide_base(z) * LANES
        narrow, wide, window = 3 * plan.part, plan.wide, plan.wide_window
        store(slot, 0, index, 0, narrow)
        store(slot, pl.multiple_of(narrow + shift, 16), index, narrow, wide)
        store(slot, pl.multiple_of(narrow + window + shift, 16), index, narrow + wide, wide)

    head_shift = plan.vocab * z - plan.head_base(z) * LANES

    def make_head(index, slot):
        @pl.when(index == layers)
        def _():
            wait_exchange(index, chunk)

        wait_exchange(index + 1, chunk)
        tiles = chunk // LANES
        for tile in range(tiles):
            turn(slot, tile, index, tile)
        for tile in range(2):
            turn(slot, tiles + tile, index + 1, tile)
        store(slot, pl.multiple_of(head_shift, 16), index, 0, chunk)

    def turn_rows(slot, first, count):
        start = first // LANES
        for tile in range(-(-(first % LANES + plan.shift + count) // LANES)):
            at = start + tile
            turn(slot, tile, layers + at // (chunk // LANES), at % (chunk // LANES))
        return pl.multiple_of(first % LANES + head_shift, 16)

    def make_tail(slot):
        wait_exchange(ring + 1, chunk)
        store(slot, turn_rows(slot, (ring - layers) * chunk, tail), ring, 0, tail)

    def make_extra():
        for index in range(ring + 2, last):
            wait_exchange(index, chunk)
        wait_exchange(last, plan.tail_window)
        blocks = plan.share * WHOLE

        def stored(n, own):
            wait_for(own.at[:, pl.ds(plan.cut, LANES)], local.at[n % 2])

        for n in range(blocks):
            own = (own_0, own_1)[n // WHOLE]
            if n >= 2:
                stored(n, own)
            at = turn_rows(n % 2, plan.extra_first + n * plan.piece, plan.piece)
            pltpu.make_async_copy(
                tbuf.at[n % 2, pl.ds(at, plan.piece), :],
                own.at[:, pl.ds(plan.cut + n % WHOLE * LANES, LANES)], local.at[n % 2],
            ).start()
        for n in range(blocks - min(2, blocks), blocks):
            stored(n, own_0)


    def slab_view(index):
        return lambda owner, first, count: slabs.at[owner, index, pl.ds(first, count), :]

    def push(part, index, recv, to):
        remote(part, part, send.at[index], recv.at[index], dp=to)

    def send_own(view, index, slot, count):
        own = view(dp, 0, count)
        wait_for(own, local.at[slot])
        push(own, index, x_recv, x_peer)
        push(own, index, y_recv, y_peer)
        push(own, index, pair_recv, pair)

    def forward(view, index, count):
        half = count // 2
        wait_for(view(x_peer, 0, count), x_recv.at[index])
        push(view(x_peer, half, half), index, b_recv, y_peer)
        push(view(x_peer, 0, count), index, pair_recv, pair)
        wait_for(view(y_peer, 0, count), y_recv.at[index])
        push(view(y_peer, 0, half), index, a_recv, x_peer)
        push(view(y_peer, 0, count), index, pair_recv, pair)

    def forward_diagonal(view, index, count):
        half = count // 2
        wait_for(view(diagonal, 0, half), a_recv.at[index])
        wait_for(view(diagonal, half, half), b_recv.at[index])
        push(view(diagonal, 0, count), index, pair_recv, pair)

    def finish(view, index, count):
        wait_for(view(pl.ds(0, 7), 0, count), send.at[index])
        wait_for(view(pl.ds(0, 4), 0, count), pair_recv.at[index])

    def finish_exchange(index, window):
        wait_for(zbuf.at[index, pl.ds(0, (plan.tp - 1) * rows), pl.ds(0, window)], z_send.at[index])


    def pieces(source_dp, to, place):
        all_rows = plan.downs
        downs = pl.ds(pl.multiple_of(place * plan.down_rows, 8), plan.down_rows)
        outs = pl.ds(pl.multiple_of(all_rows + place * plan.out_rows, 8), plan.out_rows)
        stop_downs, stop_outs = pl.ds(0, plan.down_rows), pl.ds(plan.down_rows, plan.out_rows)
        cut, home = pl.ds(plan.whole, plan.cut), pl.ds(0, plan.cut)
        found = []
        for n, (stop, own) in enumerate(((stop_0, own_0), (stop_1, own_1))):
            layer = to * 2 + n
            found.append((d.at[layer, :, cut], stop.at[source_dp, stop_downs, :], own.at[downs, home], n))
            found.append((o.at[layer, :, cut], stop.at[source_dp, stop_outs, :], own.at[outs, home], n))
        return found

    my_rank = dp // 2
    my_place = (dp % 2) * plan.tp + z
    stays = my_rank == z

    def share_in_plane():
        for step in range(1, plan.dp):
            to = (dp + step) % plan.dp

            @pl.when(stays)
            def _(to=to):
                for part, _, final, n in pieces(dp, to, my_place):
                    remote(part, final, share_send.at[n], share_recv.at[n], dp=to)

            @pl.when(jnp.logical_not(stays))
            def _(to=to):
                for part, stop, _, n in pieces(dp, to, my_place):
                    remote(part, stop, share_send.at[n], stop_recv.at[n, dp], dp=to)

        @pl.when(stays)
        def _():
            for part, _, final, n in pieces(dp, dp, my_place):
                pltpu.make_async_copy(part, final, share_recv.at[n]).start()

    def share_to_rank(source_dp):
        rank, place = source_dp // 2, (source_dp % 2) * plan.tp + z

        @pl.when((rank != z) & (source_dp == dp))
        def _():
            for part, _, final, n in pieces(dp, dp, place):
                remote(part, final, share_send.at[n], share_recv.at[n], tp=rank)

        @pl.when((rank != z) & (source_dp != dp))
        def _():
            for n, stop in enumerate((stop_0, stop_1)):
                wait_for(stop.at[source_dp], stop_recv.at[n, source_dp])
            for _, stop, final, n in pieces(source_dp, dp, place):
                remote(stop, final, share_send.at[n], share_recv.at[n], tp=rank)


    whole_columns = pl.ds(0, plan.whole)
    keep = (keep_d, keep_o)
    mine = ((d, land_d, plan.down_rows, 0), (o, land_o, plan.out_rows, plan.downs))
    half = layers // 2

    def whole_home(n, row):
        _, _, count, first = mine[n]
        return pl.ds(pl.multiple_of(first + row * count, 8), count)

    def landing(rank, some, act):
        pl.when(rank == z)(lambda: act([whole.at[some, whole_home(n, core * plan.tp + z), :] for n in range(2)]))
        pl.when(rank != z)(lambda: act([land.at[rank, some] for _, land, _, _ in mine]))

    every = pl.ds(0, layers)

    def whole_out():
        def act(places):
            for n, (source, _, _, _) in enumerate(mine):
                for to, at in ((x_peer, 0), (y_peer, 2)):
                    remote(source.at[:, :, whole_columns], places[n], land_send.at[n], land_recv.at[at + n], dp=to)

        landing(my_rank, every, act)

        @pl.when(stays)
        def _():
            for n, (source, _, _, _) in enumerate(mine):
                pltpu.make_async_copy(source.at[:, :, whole_columns], keep[n], keep_sem.at[n]).start()

    def whole_keep():
        @pl.when(stays)
        def _():
            for n in range(2):
                wait_for(keep[n], keep_sem.at[n])
                target = whole.at[:, whole_home(n, core * plan.tp + z), :]
                pltpu.make_async_copy(keep[n], target, keep_sem.at[2 + n]).start()

    def whole_forward():
        for owner, at, first, to, then in ((x_peer, 0, half, y_peer, 6), (y_peer, 2, 0, x_peer, 4)):
            def arrived(places, at=at):
                for n in range(2):
                    wait_for(places[n], land_recv.at[at + n])

            def on(places, to=to, then=then):
                for n in range(2):
                    remote(places[n], places[n], land_send.at[n], land_recv.at[then + n], dp=to)

            landing(owner // 2, every, arrived)
            landing(owner // 2, pl.ds(first, half), on)

    def whole_arrive():
        for first, at in ((0, 4), (half, 6)):
            def arrived(places, at=at):
                for n in range(2):
                    wait_for(places[n], land_recv.at[at + n])

            landing(diagonal // 2, pl.ds(first, half), arrived)

    def whole_to_rank(shift, part):
        rank = (z + shift + core * (plan.tp - 2 * shift)) % plan.tp
        some = pl.ds(part * (layers // PARTS), layers // PARTS)

        def move(sources):
            for n, source in enumerate(sources):
                target = whole.at[some, whole_home(n, core * plan.tp + z), :]
                remote(source, target, whole_send.at[n], whole_recv.at[n], tp=rank)

        pl.when(rank == my_rank)(lambda: move([source.at[some, :, whole_columns] for source, _, _, _ in mine]))
        pl.when(rank != my_rank)(lambda: move([land.at[rank, some] for _, land, _, _ in mine]))

    def whole_rows(which):
        return [
            whole.at[:, pl.ds(pl.multiple_of(first + which * plan.tp * count, 8), plan.tp * count), :]
            for _, _, count, first in mine
        ]

    def whole_to_pair():
        for n, part in enumerate(whole_rows(core)):
            away = pl.ds(0, (plan.tp - 1) * mine[n][2])
            wait_for(whole.at[:, away, :], whole_recv.at[n])

            @pl.when(stays)
            def _(n=n):
                wait_for(keep[n], keep_sem.at[2 + n])

            remote(part, part, whole_pair_send.at[n], whole_pair_recv.at[n], dp=pair)

    def whole_finish():
        for n, (_, land, count, first) in enumerate(mine):
            wait_for(land.at[pl.ds(0, 3)], land_send.at[n])
            wait_for(whole.at[:, pl.ds(first, (plan.tp - 1) * count), :], whole_send.at[n])
            wait_for(whole_rows(core)[n], whole_pair_send.at[n])
            wait_for(whole_rows(1 - core)[n], whole_pair_recv.at[n])

    barrier = pltpu.get_barrier_semaphore()
    peers = [{"tp": (z + step) % plan.tp} for step in range(1, plan.tp)]
    peers += [{"dp": (dp + step) % plan.dp} for step in range(1, plan.dp)]
    for peer in peers:
        pl.semaphore_signal(barrier, inc=1, device_id=peer, device_id_type=MESH)
    pl.semaphore_wait(barrier, len(peers))

    start_exchange(0)
    whole_out()
    share_in_plane()
    for index in range(GROUP, AHEAD):
        start_exchange(index)

    def retire(index):
        finish(slab_view(index), index, chunk)

        @pl.when((index < layers) & (index % GROUP == 0))
        def _():
            sent = pl.ds(0, (plan.tp - 1) * rows)
            wait_for(zbuf.at[pl.ds(index, GROUP), sent, pl.ds(0, plan.layer_window)], z_send.at[index])

        @pl.when(index >= layers)
        def _():
            finish_exchange(index, chunk)

    def step(index, _):
        slot = index % 2

        @pl.when(index + AHEAD < plan.chunks)
        def _():
            start_exchange(index + AHEAD)

        @pl.when((index >= SHARE_AT) & (index < SHARE_AT + plan.dp))
        def _():
            share_to_rank(index - SHARE_AT)

        @pl.when(index == WHOLE_AT)
        def _():
            whole_keep()
            whole_forward()

        @pl.when(index == WHOLE_AT + 3)
        def _():
            whole_arrive()

        @pl.when((index >= RANKS_AT) & (index < RANKS_AT + (plan.tp - 1) * PARTS))
        def _():
            whole_to_rank((index - RANKS_AT) % (plan.tp - 1) + 1, (index - RANKS_AT) // (plan.tp - 1))

        @pl.when(index == ring - 2)
        def _():
            whole_to_pair()

        @pl.when(index < layers)
        def _():
            make_layer(index, slot)

        @pl.when(index >= layers)
        def _():
            make_head(index, slot)

        send_own(slab_view(index), index, slot, chunk)

        @pl.when(index >= LAG)
        def _():
            forward(slab_view(index - LAG), index - LAG, chunk)

        @pl.when(index >= 2 * LAG)
        def _():
            forward_diagonal(slab_view(index - 2 * LAG), index - 2 * LAG, chunk)

        @pl.when(index >= RETIRE)
        def _():
            retire(index - RETIRE)

        return 0

    lax.fori_loop(0, ring, step, 0)

    make_tail(ring % 2)
    send_own(slab_view(ring), ring, ring % 2, tail)
    make_extra()
    for index in range(ring - LAG, ring):
        forward(slab_view(index), index, chunk)
    forward(slab_view(ring), ring, tail)
    for index in range(ring - 2 * LAG, ring):
        forward_diagonal(slab_view(index), index, chunk)
    forward_diagonal(slab_view(ring), ring, tail)

    for index in range(ring - RETIRE, ring):
        retire(index)
    finish(slab_view(ring), ring, tail)
    for index in range(ring, last):
        finish_exchange(index, chunk)
    finish_exchange(last, plan.tail_window)
    whole_finish()
    for n, own in enumerate((own_0, own_1)):
        wait_for(own.at[:, pl.ds(0, plan.cut)], share_recv.at[n])
        for parts in (8, 5):
            sent = pl.ds(0, parts * (plan.down_rows + plan.out_rows))
            wait_for(own.at[sent, pl.ds(0, plan.cut)], share_send.at[n])


def gather(plan, *args):
    dma = pltpu.SemaphoreType.DMA
    per_chunk = dma((plan.chunks,))
    share_rows = plan.down_rows + plan.out_rows
    hbm = pl.BlockSpec(memory_space=pltpu.HBM)
    shapes = [(plan.dp, plan.ring + 1, plan.chunk, LANES), (plan.piece, plan.columns), (plan.piece, plan.columns)]
    shapes += [(plan.layers, plan.piece, plan.whole)] + [(plan.dp, share_rows, plan.cut)] * 2
    shapes += [(plan.tp, plan.layers, count, plan.whole) for count in (plan.down_rows, plan.out_rows)]
    return pl.pallas_call(
        functools.partial(gather_kernel, plan),
        out_shape=[jax.ShapeDtypeStruct(shape, jnp.bfloat16) for shape in shapes],
        in_specs=[hbm] * 8,
        out_specs=[hbm] * len(shapes),
        scratch_shapes=[
            pltpu.VMEM((plan.chunks, plan.tp * plan.rows, plan.layer_window), jnp.bfloat16),
            pltpu.VMEM((2, plan.chunk + 2 * LANES, LANES), jnp.bfloat16),
            per_chunk, per_chunk, dma((2,)),
            per_chunk, per_chunk, per_chunk, per_chunk, per_chunk, per_chunk,
            dma((2, plan.dp)), dma((2,)), dma((2,)),
            dma((8,)), dma((2,)), dma((2,)), dma((2,)), dma((2,)), dma((2,)),
            pltpu.VMEM((plan.layers, plan.down_rows, plan.whole), jnp.bfloat16),
            pltpu.VMEM((plan.layers, plan.out_rows, plan.whole), jnp.bfloat16),
            dma((4,)),
        ],
        compiler_params=pltpu.CompilerParams(collective_id=0, has_side_effects=True),
        name="gather",
    )(*args)[:4]


def place_slabs(plan, slabs, first, count, shapes, store, held=()):
    hbm = pl.BlockSpec(memory_space=pltpu.HBM)
    depth = min(BUFFERS, count)
    ahead = depth // 2

    def body(slab, *refs):
        outs, (buffers, loads, stores) = refs[len(held):-3], refs[-3:]

        def each_size(chunk, act):
            if first + count > plan.ring:
                pl.when(chunk < plan.ring)(lambda: act(plan.chunk))
                pl.when(chunk == plan.ring)(lambda: act(plan.tail))
            else:
                act(plan.chunk)

        def load(i, rows):
            for owner in range(plan.dp):
                pltpu.make_async_copy(
                    slab.at[owner, first + i, pl.ds(0, rows), :],
                    buffers.at[i % depth, pl.ds(0, rows), pl.ds(owner * LANES, LANES)],
                    loads.at[i % depth],
                ).start()

        def wait(i, rows, sem):
            buffer = buffers.at[i % depth, pl.ds(0, rows), :]
            pltpu.make_async_copy(buffer, buffer, sem.at[i % depth]).wait()

        def write(i, rows):
            wait(i, rows, loads)
            for source, target in store(buffers.at[i % depth], first + i, rows, outs):
                pltpu.make_async_copy(source, target, stores.at[i % depth]).start()

        def step(i, _):
            @pl.when(i >= depth)
            def _():
                each_size(first + i - depth, lambda rows: wait(i - depth, rows, stores))

            @pl.when(i < count)
            def _():
                each_size(first + i, lambda rows: load(i, rows))

            @pl.when((i >= ahead) & (i < count + ahead))
            def _():
                each_size(first + i - ahead, lambda rows: write(i - ahead, rows))

            return 0

        lax.fori_loop(0, count + depth, step, 0)

    outs = [jax.ShapeDtypeStruct(shape, jnp.bfloat16) for shape in shapes]
    return pl.pallas_call(
        body,
        in_specs=[hbm] * (1 + len(held)),
        out_specs=[hbm] * len(outs),
        out_shape=outs,
        scratch_shapes=[
            pltpu.VMEM((depth, plan.chunk, plan.dp * LANES), jnp.bfloat16),
            pltpu.SemaphoreType.DMA((depth,)),
            pltpu.SemaphoreType.DMA((depth,)),
        ],
        input_output_aliases={1 + n: n for n in range(len(held))},
        cost_estimate=pl.CostEstimate(
            flops=10**7, bytes_accessed=4 * count * plan.chunk * plan.dp * LANES, transcendentals=0
        ),
        compiler_params=pltpu.CompilerParams(vmem_limit_bytes=VMEM),
    )(slabs, *held)


def place_layers(plan, slabs):
    narrow, wide, width = 3 * plan.part, 2 * plan.wide, plan.dp * LANES

    def store(buffer, chunk, rows, outs):
        return [
            (buffer.at[pl.ds(0, narrow), :], outs[0].at[chunk]),
            (buffer.at[pl.ds(narrow, wide), :], outs[1].at[chunk]),
        ]

    shapes = [(plan.layers, narrow, width), (plan.layers, wide, width)]
    return place_slabs(plan, slabs, 0, plan.layers, shapes, store)


def place_head(plan, slabs, first, count, *held):
    def store(buffer, chunk, rows, outs):
        at = pl.multiple_of((chunk - plan.layers) * plan.chunk, 16)
        return [(buffer.at[pl.ds(0, rows), :], outs[0].at[pl.ds(at, rows), :])]

    shapes = [(plan.vocab, plan.dp * LANES)]
    return place_slabs(plan, slabs, plan.layers + first, count, shapes, store, held)[0]


def place_rows(plan, arrays, spots, width, column, held):
    count = len(spots([array for array in arrays], 0))
    columns = arrays[0].shape[-1]
    outs = [
        jax.ShapeDtypeStruct((plan.layers, plan.downs, plan.columns), jnp.bfloat16),
        jax.ShapeDtypeStruct((plan.layers, plan.columns, plan.outs), jnp.bfloat16),
        jax.ShapeDtypeStruct((plan.vocab, plan.dp * LANES), jnp.bfloat16),
    ]
    with_head = columns > width
    kept = [n for n in range(3) if n in held]
    made = [n for n in range(3 if with_head else 2)]

    def body(*refs):
        targets = dict(zip(made, refs[len(arrays) + len(kept):-6], strict=True))
        buffers, turned, loads, stores, out_stores, head_stores = refs[-6:]
        moves = spots(refs[: len(arrays)], lax.axis_index("dp"))
        loading = [pltpu.make_async_copy(move[0], buffers.at[n], loads.at[n]) for n, move in enumerate(moves)]
        storing = []
        for load in loading:
            load.start()

        def put(source, target, sem):
            storing.append(pltpu.make_async_copy(source, target, sem))
            storing[-1].start()

        place = pl.ds(column, width)
        for n, (load, (_, layer, owner, part)) in enumerate(zip(loading, moves, strict=True)):
            load.wait()
            put(buffers.at[n, pl.ds(0, plan.downs), pl.ds(0, width)], targets[0].at[layer, :, place], stores.at[n])
            for j in range((columns - width) // LANES):
                row = plan.extra_first + (part * WHOLE + j) * plan.piece
                put(
                    buffers.at[n, :, pl.ds(width + j * LANES, LANES)],
                    targets[2].at[pl.ds(row, plan.piece), pl.ds(pl.multiple_of(owner * LANES, LANES), LANES)],
                    head_stores.at[n, j],
                )
        for n, (_, layer, _, _) in enumerate(moves):
            for i in range(plan.outs // LANES):
                for j in range(width // LANES):
                    turned[n, pl.ds(j * LANES, LANES), pl.ds(i * LANES, LANES)] = buffers[
                        n, pl.ds(plan.downs + i * LANES, LANES), pl.ds(j * LANES, LANES)
                    ].T
            put(turned.at[n], targets[1].at[layer, place, :], out_stores.at[n])
        for store in storing:
            store.wait()

    hbm = pl.BlockSpec(memory_space=pltpu.HBM)
    dma = pltpu.SemaphoreType.DMA((count,))
    result = pl.pallas_call(
        body,
        out_shape=[outs[n] for n in made],
        in_specs=[hbm] * (len(arrays) + len(kept)),
        out_specs=[hbm] * len(made),
        scratch_shapes=[
            pltpu.VMEM((count, plan.piece, columns), jnp.bfloat16),
            pltpu.VMEM((count, width, plan.outs), jnp.bfloat16),
            dma, dma, dma, pltpu.SemaphoreType.DMA((count, max(WHOLE, 1))),
        ],
        input_output_aliases={len(arrays) + i: n for i, n in enumerate(kept)},
        cost_estimate=pl.CostEstimate(flops=10**7, bytes_accessed=4 * count * plan.piece * columns, transcendentals=0),
        compiler_params=pltpu.CompilerParams(vmem_limit_bytes=VMEM),
    )(*arrays, *(held[n] for n in kept))
    return dict(zip(made, result, strict=True))


def place_whole(plan, whole):
    def spots(refs, dp):
        return [(refs[0].at[layer], layer, 0, 0) for layer in range(plan.layers)]

    return place_rows(plan, [whole], spots, plan.whole, 0, {})


def place_shares(plan, shares, held):
    owners = list(shares)
    arrays = [array for owner in owners for array in shares[owner]]

    def spots(refs, dp):
        core, x, y = dp % 2, (dp // 2) % 2, dp // 4
        found = []
        for n, ref in enumerate(refs):
            flip_x, flip_y, flip_core = owners[n // plan.share]
            owner = (y + flip_y * (1 - 2 * y)) * 4 + (x + flip_x * (1 - 2 * x)) * 2 + core + flip_core * (1 - 2 * core)
            found.append((ref, owner * plan.share + n % plan.share, owner, n % plan.share))
        return found

    return place_rows(plan, arrays, spots, plan.cut, plan.whole, held)


def solution(mesh):
    train_stack = P(None, ("dp", "tp"), None)
    train_head = P(("dp", "tp"), None)
    fused_stack = P(None, "tp", None)
    last_stack = P(None, None, "tp")
    head_rows = P("tp", None)

    def local_sync(w_query, w_key, w_value, w_out, w_gate, w_up, w_down, w_head):
        plan = Plan(mesh.shape["tp"], mesh.shape["dp"], w_query, w_gate, w_out, w_down, w_head)
        slabs, own_0, own_1, whole = gather(plan, w_query, w_key, w_value, w_out, w_gate, w_up, w_down, w_head)

        def swap(bit, array):
            return lax.ppermute(array, "dp", [(i, i ^ bit) for i in range(plan.dp)])

        pair, along_x, along_y = (functools.partial(swap, bit) for bit in (1, 2, 4))
        hold = lax.optimization_barrier

        x_1, y_0 = along_x(own_1), along_y(own_0)
        x_0, y_1 = along_x(own_0), along_y(own_1)
        pair_own = [pair(own_0), pair(own_1)]
        qkv_block, gate_up_block = place_layers(plan, slabs)
        x_1, y_0, qkv_block, slabs = hold((x_1, y_0, qkv_block, slabs))
        diagonal_0 = along_x(y_0)
        diagonal_1 = along_y(x_1)
        pair_x_1, pair_y_0 = pair(x_1), pair(y_0)
        head_chunks = plan.ring + 1 - plan.layers
        early = head_chunks // 4
        head_block = place_head(plan, slabs, early, head_chunks - early)
        x_0, y_1, head_block, slabs, whole = hold((x_0, y_1, head_block, slabs, whole))
        pair_x_0, pair_y_1 = pair(x_0), pair(y_1)
        placed = place_whole(plan, whole)
        slabs, *placed = hold((slabs, placed[0], placed[1]))
        head_block = place_head(plan, slabs, 0, early, head_block)
        own_0, own_1, head_block = hold((own_0, own_1, head_block))
        near = {
            (0, 0, 0): [own_0, own_1], (0, 0, 1): pair_own, (1, 0, 0): [x_0, x_1], (1, 0, 1): [pair_x_0, pair_x_1],
            (0, 1, 0): [y_0, y_1], (0, 1, 1): [pair_y_0, pair_y_1],
        }
        placed = place_shares(plan, near, {0: placed[0], 1: placed[1], 2: head_block})
        diagonal_0, diagonal_1, *placed = hold((diagonal_0, diagonal_1, placed[0], placed[1], placed[2]))
        pair_diagonal = [pair(diagonal_0), pair(diagonal_1)]
        placed = place_shares(plan, {(1, 1, 0): [diagonal_0, diagonal_1]}, dict(enumerate(placed)))
        placed = place_shares(plan, {(1, 1, 1): pair_diagonal}, placed)
        down_block, o_block, head_block = placed[0], placed[1], placed[2]
        return (
            qkv_block,
            o_block,
            gate_up_block,
            jnp.swapaxes(down_block, 1, 2),
            head_block,
        )

    return jax.shard_map(
        local_sync,
        mesh=mesh,
        in_specs=(train_stack,) * 7 + (train_head,),
        out_specs=(fused_stack, last_stack, fused_stack, last_stack, head_rows),
        check_vma=False,
    )
```

```python
import functools

import jax
import jax.numpy as jnp
from jax import lax
from jax.experimental import pallas as pl
from jax.experimental.pallas import tpu as pltpu
from jax.sharding import PartitionSpec as P


MESH = pl.DeviceIdType.MESH
LANES = 128
VMEM = 67_000_000
AHEAD = 14
BUFFERS = 6
LAG = 2
SHARE_AT = 20
RETIRE = 8
WHOLE = 3
WHOLE_AT = 2
RANKS_AT = 10
PARTS = 4
GROUP = 4


class Plan:
    def __init__(self, tp, dp, w_query, w_gate, w_out, w_down, w_head):
        self.tp, self.dp = tp, dp
        self.layers, self.rows, columns = w_query.shape
        self.part = columns // tp
        self.wide = w_gate.shape[2] // tp
        self.vocab = w_head.shape[1] // tp
        self.head_tiles = w_head.shape[1] // LANES
        self.chunk = 3 * self.part + 2 * self.wide
        self.wide_window = -(-self.wide // LANES) * LANES
        self.layer_window = 3 * self.part + 2 * self.wide_window
        self.head_chunks = -(-self.vocab // self.chunk)
        self.chunks = self.layers + self.head_chunks
        end = self.vocab - (self.head_chunks - 1) * self.chunk
        self.tail_window = -(-(end + LANES) // LANES) * LANES
        self.window_tiles = (self.head_chunks - 1) * self.chunk // LANES + self.tail_window // LANES
        self.shift = max(self.vocab * r - self.head_base(r) * LANES for r in range(tp))
        self.out_rows, self.down_rows = w_out.shape[1], w_down.shape[1]
        self.downs, self.outs = 2 * tp * self.down_rows, 2 * tp * self.out_rows
        self.piece = self.downs + self.outs
        self.share = self.layers // dp
        self.columns = w_out.shape[2]
        self.whole = WHOLE * LANES
        self.cut = self.columns - self.whole
        self.extra_first = self.vocab - self.share * WHOLE * self.piece
        self.ring = self.layers + self.extra_first // self.chunk
        self.tail = self.extra_first % self.chunk

    def wide_base(self, rank):
        return (self.wide * rank) // LANES

    def head_base(self, rank):
        base = (self.vocab * rank) // LANES
        return base - (rank // (self.tp - 1)) * (self.vocab * (self.tp - 1) // LANES + self.window_tiles - self.head_tiles)


def gather_kernel(plan, q, k, v, o, g, u, d, h, slabs, own_0, own_1, whole, stop_0, stop_1, land_d, land_o, zbuf, tbuf,
                  z_recv, z_send, local, x_recv, y_recv, a_recv, b_recv, pair_recv, send, stop_recv, share_recv,
                  share_send, land_recv, land_send, whole_recv, whole_send, whole_pair_recv, whole_pair_send,
                  keep_d, keep_o, keep_sem, packed, pack_sem):
    z, dp = lax.axis_index("tp"), lax.axis_index("dp")
    core, x, y = dp % 2, (dp // 2) % 2, dp // 4
    x_peer = y * 4 + (1 - x) * 2 + core
    y_peer = (1 - y) * 4 + x * 2 + core
    diagonal = (1 - y) * 4 + (1 - x) * 2 + core
    pair = dp + 1 - 2 * core
    rows, chunk, tail = plan.rows, plan.chunk, plan.tail
    layers, ring, last = plan.layers, plan.ring, plan.chunks - 1
    my_rows = pl.ds(pl.multiple_of(z * rows, rows), rows)

    def lanes(first_tile, width):
        return pl.ds(pl.multiple_of(first_tile * LANES, LANES), width)

    def remote(source, target, send_sem, recv_sem, **to):
        pltpu.make_async_remote_copy(source, target, send_sem, recv_sem, device_id=to, device_id_type=MESH).start()

    def wait_for(ref, sem):
        pltpu.make_async_copy(ref, ref, sem).wait()


    def rank_at(step):
        return (z + step + core * (plan.tp - 2 * step)) % plan.tp

    def layer_pieces(first, rank):
        some, part, wide = pl.ds(first, GROUP), plan.part, plan.wide_window
        narrow = lanes(rank * (part // LANES), part)
        window = lanes(plan.wide_base(rank), wide)
        return [
            (q.at[some, :, narrow], 0, part),
            (k.at[some, :, narrow], part, part),
            (v.at[some, :, narrow], 2 * part, part),
            (g.at[some, :, window], 3 * part, wide),
            (u.at[some, :, window], 3 * part + wide, wide),
        ]

    def collect(group):
        for step in range(1, plan.tp):
            for source, column, width in layer_pieces(group * GROUP, rank_at(step)):
                target = packed.at[group, step - 1, :, :, pl.ds(column, width)]
                pltpu.make_async_copy(source, target, pack_sem.at[group]).start()
        for source, column, width in layer_pieces(group * GROUP, z):
            target = zbuf.at[pl.ds(group * GROUP, GROUP), my_rows, pl.ds(column, width)]
            pltpu.make_async_copy(source, target, z_recv.at[group * GROUP]).start()

    def exchange_layers(group):
        wait_for(packed.at[group], pack_sem.at[group])
        for step in range(1, plan.tp):
            index = group * GROUP
            target = zbuf.at[pl.ds(index, GROUP), my_rows, :]
            remote(packed.at[group, step - 1], target, z_send.at[index], z_recv.at[index], tp=rank_at(step))

    def exchange_head(index, width):
        def piece(rank):
            return h.at[:, lanes(plan.head_base(rank) + (index - layers) * (chunk // LANES), width)]

        target = zbuf.at[index, my_rows, pl.ds(0, width)]
        for step in range(1, plan.tp):
            remote(piece(rank_at(step)), target, z_send.at[index], z_recv.at[index], tp=rank_at(step))
        pltpu.make_async_copy(piece(z), target, z_recv.at[index]).start()

    def start_exchange(index):
        @pl.when((index >= layers) & (index < last))
        def _():
            exchange_head(index, chunk)

        @pl.when(index == last)
        def _():
            exchange_head(last, plan.tail_window)

    def wait_exchange(index, width):
        wait_for(zbuf.at[index, :, pl.ds(0, width)], z_recv.at[index])


    def turn(slot, tile, index, source_tile):
        tbuf[slot, pl.ds(tile * LANES, LANES), :] = zbuf[index, :, pl.ds(source_tile * LANES, LANES)].T

    def store(slot, first, index, to, count):
        pltpu.make_async_copy(
            tbuf.at[slot, pl.ds(first, count), :], slabs.at[dp, index, pl.ds(to, count), :], local.at[slot]
        ).start()

    def make_layer(index, slot):
        @pl.when(index % GROUP == 0)
        def _():
            wait_for(zbuf.at[pl.ds(index, GROUP), :, pl.ds(0, plan.layer_window)], z_recv.at[index])

        for tile in range(plan.layer_window // LANES):
            turn(slot, tile, index, tile)
        shift = plan.wide * z - plan.wide_base(z) * LANES
        narrow, wide, window = 3 * plan.part, plan.wide, plan.wide_window
        store(slot, 0, index, 0, narrow)
        store(slot, pl.multiple_of(narrow + shift, 16), index, narrow, wide)
        store(slot, pl.multiple_of(narrow + window + shift, 16), index, narrow + wide, wide)

    head_shift = plan.vocab * z - plan.head_base(z) * LANES

    def make_head(index, slot):
        @pl.when(index == layers)
        def _():
            wait_exchange(index, chunk)

        wait_exchange(index + 1, chunk)
        tiles = chunk // LANES
        for tile in range(tiles):
            turn(slot, tile, index, tile)
        for tile in range(2):
            turn(slot, tiles + tile, index + 1, tile)
        store(slot, pl.multiple_of(head_shift, 16), index, 0, chunk)

    def turn_rows(slot, first, count):
        start = first // LANES
        for tile in range(-(-(first % LANES + plan.shift + count) // LANES)):
            at = start + tile
            turn(slot, tile, layers + at // (chunk // LANES), at % (chunk // LANES))
        return pl.multiple_of(first % LANES + head_shift, 16)

    def make_tail(slot):
        wait_exchange(ring + 1, chunk)
        store(slot, turn_rows(slot, (ring - layers) * chunk, tail), ring, 0, tail)

    def make_extra():
        for index in range(ring + 2, last):
            wait_exchange(index, chunk)
        wait_exchange(last, plan.tail_window)
        blocks = plan.share * WHOLE

        def stored(n, own):
            wait_for(own.at[:, pl.ds(plan.cut, LANES)], local.at[n % 2])

        for n in range(blocks):
            own = (own_0, own_1)[n // WHOLE]
            if n >= 2:
                stored(n, own)
            at = turn_rows(n % 2, plan.extra_first + n * plan.piece, plan.piece)
            pltpu.make_async_copy(
                tbuf.at[n % 2, pl.ds(at, plan.piece), :],
                own.at[:, pl.ds(plan.cut + n % WHOLE * LANES, LANES)], local.at[n % 2],
            ).start()
        for n in range(blocks - min(2, blocks), blocks):
            stored(n, own_0)


    def slab_view(index):
        return lambda owner, first, count: slabs.at[owner, index, pl.ds(first, count), :]

    def push(part, index, recv, to):
        remote(part, part, send.at[index], recv.at[index], dp=to)

    def send_own(view, index, slot, count):
        own = view(dp, 0, count)
        wait_for(own, local.at[slot])
        push(own, index, x_recv, x_peer)
        push(own, index, y_recv, y_peer)
        push(own, index, pair_recv, pair)

    def forward(view, index, count):
        half = count // 2
        wait_for(view(x_peer, 0, count), x_recv.at[index])
        push(view(x_peer, half, half), index, b_recv, y_peer)
        push(view(x_peer, 0, count), index, pair_recv, pair)
        wait_for(view(y_peer, 0, count), y_recv.at[index])
        push(view(y_peer, 0, half), index, a_recv, x_peer)
        push(view(y_peer, 0, count), index, pair_recv, pair)

    def forward_diagonal(view, index, count):
        half = count // 2
        wait_for(view(diagonal, 0, half), a_recv.at[index])
        wait_for(view(diagonal, half, half), b_recv.at[index])
        push(view(diagonal, 0, count), index, pair_recv, pair)

    def finish(view, index, count):
        wait_for(view(pl.ds(0, 7), 0, count), send.at[index])
        wait_for(view(pl.ds(0, 4), 0, count), pair_recv.at[index])

    def finish_exchange(index, window):
        wait_for(zbuf.at[index, pl.ds(0, (plan.tp - 1) * rows), pl.ds(0, window)], z_send.at[index])


    def pieces(source_dp, to, place):
        all_rows = plan.downs
        downs = pl.ds(pl.multiple_of(place * plan.down_rows, 8), plan.down_rows)
        outs = pl.ds(pl.multiple_of(all_rows + place * plan.out_rows, 8), plan.out_rows)
        stop_downs, stop_outs = pl.ds(0, plan.down_rows), pl.ds(plan.down_rows, plan.out_rows)
        cut, home = pl.ds(plan.whole, plan.cut), pl.ds(0, plan.cut)
        found = []
        for n, (stop, own) in enumerate(((stop_0, own_0), (stop_1, own_1))):
            layer = to * 2 + n
            found.append((d.at[layer, :, cut], stop.at[source_dp, stop_downs, :], own.at[downs, home], n))
            found.append((o.at[layer, :, cut], stop.at[source_dp, stop_outs, :], own.at[outs, home], n))
        return found

    my_rank = dp // 2
    my_place = (dp % 2) * plan.tp + z
    stays = my_rank == z

    def share_in_plane():
        for step in range(1, plan.dp):
            to = (dp + step) % plan.dp

            @pl.when(stays)
            def _(to=to):
                for part, _, final, n in pieces(dp, to, my_place):
                    remote(part, final, share_send.at[n], share_recv.at[n], dp=to)

            @pl.when(jnp.logical_not(stays))
            def _(to=to):
                for part, stop, _, n in pieces(dp, to, my_place):
                    remote(part, stop, share_send.at[n], stop_recv.at[n, dp], dp=to)

        @pl.when(stays)
        def _():
            for part, _, final, n in pieces(dp, dp, my_place):
                pltpu.make_async_copy(part, final, share_recv.at[n]).start()

    def share_to_rank(source_dp):
        rank, place = source_dp // 2, (source_dp % 2) * plan.tp + z

        @pl.when((rank != z) & (source_dp == dp))
        def _():
            for part, _, final, n in pieces(dp, dp, place):
                remote(part, final, share_send.at[n], share_recv.at[n], tp=rank)

        @pl.when((rank != z) & (source_dp != dp))
        def _():
            for n, stop in enumerate((stop_0, stop_1)):
                wait_for(stop.at[source_dp], stop_recv.at[n, source_dp])
            for _, stop, final, n in pieces(source_dp, dp, place):
                remote(stop, final, share_send.at[n], share_recv.at[n], tp=rank)


    whole_columns = pl.ds(0, plan.whole)
    keep = (keep_d, keep_o)
    mine = ((d, land_d, plan.down_rows, 0), (o, land_o, plan.out_rows, plan.downs))
    half = layers // 2

    def whole_home(n, row):
        _, _, count, first = mine[n]
        return pl.ds(pl.multiple_of(first + row * count, 8), count)

    def landing(rank, some, act):
        pl.when(rank == z)(lambda: act([whole.at[some, whole_home(n, core * plan.tp + z), :] for n in range(2)]))
        pl.when(rank != z)(lambda: act([land.at[rank, some] for _, land, _, _ in mine]))

    every = pl.ds(0, layers)

    def whole_out():
        def act(places):
            for n, (source, _, _, _) in enumerate(mine):
                for to, at in ((x_peer, 0), (y_peer, 2)):
                    remote(source.at[:, :, whole_columns], places[n], land_send.at[n], land_recv.at[at + n], dp=to)

        landing(my_rank, every, act)

        @pl.when(stays)
        def _():
            for n, (source, _, _, _) in enumerate(mine):
                pltpu.make_async_copy(source.at[:, :, whole_columns], keep[n], keep_sem.at[n]).start()

    def whole_keep():
        @pl.when(stays)
        def _():
            for n in range(2):
                wait_for(keep[n], keep_sem.at[n])
                target = whole.at[:, whole_home(n, core * plan.tp + z), :]
                pltpu.make_async_copy(keep[n], target, keep_sem.at[2 + n]).start()

    def whole_forward():
        for owner, at, first, to, then in ((x_peer, 0, half, y_peer, 6), (y_peer, 2, 0, x_peer, 4)):
            def arrived(places, at=at):
                for n in range(2):
                    wait_for(places[n], land_recv.at[at + n])

            def on(places, to=to, then=then):
                for n in range(2):
                    remote(places[n], places[n], land_send.at[n], land_recv.at[then + n], dp=to)

            landing(owner // 2, every, arrived)
            landing(owner // 2, pl.ds(first, half), on)

    def whole_arrive():
        for first, at in ((0, 4), (half, 6)):
            def arrived(places, at=at):
                for n in range(2):
                    wait_for(places[n], land_recv.at[at + n])

            landing(diagonal // 2, pl.ds(first, half), arrived)

    def whole_to_rank(shift, part):
        rank = (z + shift + core * (plan.tp - 2 * shift)) % plan.tp
        some = pl.ds(part * (layers // PARTS), layers // PARTS)

        def move(sources):
            for n, source in enumerate(sources):
                target = whole.at[some, whole_home(n, core * plan.tp + z), :]
                remote(source, target, whole_send.at[n], whole_recv.at[n], tp=rank)

        pl.when(rank == my_rank)(lambda: move([source.at[some, :, whole_columns] for source, _, _, _ in mine]))
        pl.when(rank != my_rank)(lambda: move([land.at[rank, some] for _, land, _, _ in mine]))

    def whole_rows(which):
        return [
            whole.at[:, pl.ds(pl.multiple_of(first + which * plan.tp * count, 8), plan.tp * count), :]
            for _, _, count, first in mine
        ]

    def whole_to_pair():
        for n, part in enumerate(whole_rows(core)):
            away = pl.ds(0, (plan.tp - 1) * mine[n][2])
            wait_for(whole.at[:, away, :], whole_recv.at[n])

            @pl.when(stays)
            def _(n=n):
                wait_for(keep[n], keep_sem.at[2 + n])

            remote(part, part, whole_pair_send.at[n], whole_pair_recv.at[n], dp=pair)

    def whole_finish():
        for n, (_, land, count, first) in enumerate(mine):
            wait_for(land.at[pl.ds(0, 3)], land_send.at[n])
            wait_for(whole.at[:, pl.ds(first, (plan.tp - 1) * count), :], whole_send.at[n])
            wait_for(whole_rows(core)[n], whole_pair_send.at[n])
            wait_for(whole_rows(1 - core)[n], whole_pair_recv.at[n])

    groups = layers // GROUP
    barrier = pltpu.get_barrier_semaphore()
    peers = [{"tp": (z + step) % plan.tp} for step in range(1, plan.tp)]
    peers += [{"dp": (dp + step) % plan.dp} for step in range(1, plan.dp)]
    for peer in peers:
        pl.semaphore_signal(barrier, inc=1, device_id=peer, device_id_type=MESH)
    for group in range(groups):
        collect(group)
    pl.semaphore_wait(barrier, len(peers))

    whole_out()
    exchange_layers(0)
    share_in_plane()
    for group in range(1, groups):
        exchange_layers(group)
    for index in range(layers, AHEAD):
        start_exchange(index)

    def retire(index):
        finish(slab_view(index), index, chunk)

        @pl.when((index < layers) & (index % GROUP == 0))
        def _():
            sent = pl.ds(0, (plan.tp - 1) * rows)
            wait_for(zbuf.at[pl.ds(index, GROUP), sent, pl.ds(0, plan.layer_window)], z_send.at[index])

        @pl.when(index >= layers)
        def _():
            finish_exchange(index, chunk)

    def step(index, _):
        slot = index % 2

        @pl.when(index + AHEAD < plan.chunks)
        def _():
            start_exchange(index + AHEAD)

        @pl.when((index >= SHARE_AT) & (index < SHARE_AT + plan.dp))
        def _():
            share_to_rank(index - SHARE_AT)

        @pl.when(index == WHOLE_AT)
        def _():
            whole_keep()
            whole_forward()

        @pl.when(index == WHOLE_AT + 3)
        def _():
            whole_arrive()

        @pl.when((index >= RANKS_AT) & (index < RANKS_AT + (plan.tp - 1) * PARTS))
        def _():
            whole_to_rank((index - RANKS_AT) % (plan.tp - 1) + 1, (index - RANKS_AT) // (plan.tp - 1))

        @pl.when(index < layers)
        def _():
            make_layer(index, slot)

        @pl.when(index >= layers)
        def _():
            make_head(index, slot)

        send_own(slab_view(index), index, slot, chunk)

        @pl.when(index >= LAG)
        def _():
            forward(slab_view(index - LAG), index - LAG, chunk)

        @pl.when(index >= 2 * LAG)
        def _():
            forward_diagonal(slab_view(index - 2 * LAG), index - 2 * LAG, chunk)

        @pl.when(index >= RETIRE)
        def _():
            retire(index - RETIRE)

        return 0

    lax.fori_loop(0, ring, step, 0)

    make_tail(ring % 2)
    send_own(slab_view(ring), ring, ring % 2, tail)
    make_extra()
    for index in range(ring - LAG, ring):
        forward(slab_view(index), index, chunk)
        if index == ring - LAG:
            whole_to_pair()
    forward(slab_view(ring), ring, tail)
    for index in range(ring - 2 * LAG, ring):
        forward_diagonal(slab_view(index), index, chunk)
    forward_diagonal(slab_view(ring), ring, tail)

    for index in range(ring - RETIRE, ring):
        retire(index)
    finish(slab_view(ring), ring, tail)
    for index in range(ring, last):
        finish_exchange(index, chunk)
    finish_exchange(last, plan.tail_window)
    whole_finish()
    for n, own in enumerate((own_0, own_1)):
        wait_for(own.at[:, pl.ds(0, plan.cut)], share_recv.at[n])
        for parts in (8, 5):
            sent = pl.ds(0, parts * (plan.down_rows + plan.out_rows))
            wait_for(own.at[sent, pl.ds(0, plan.cut)], share_send.at[n])


def gather(plan, *args):
    dma = pltpu.SemaphoreType.DMA
    per_chunk = dma((plan.chunks,))
    share_rows = plan.down_rows + plan.out_rows
    hbm = pl.BlockSpec(memory_space=pltpu.HBM)
    shapes = [(plan.dp, plan.ring + 1, plan.chunk, LANES), (plan.piece, plan.columns), (plan.piece, plan.columns)]
    shapes += [(plan.layers, plan.piece, plan.whole)] + [(plan.dp, share_rows, plan.cut)] * 2
    shapes += [(plan.tp, plan.layers, count, plan.whole) for count in (plan.down_rows, plan.out_rows)]
    return pl.pallas_call(
        functools.partial(gather_kernel, plan),
        out_shape=[jax.ShapeDtypeStruct(shape, jnp.bfloat16) for shape in shapes],
        in_specs=[hbm] * 8,
        out_specs=[hbm] * len(shapes),
        scratch_shapes=[
            pltpu.VMEM((plan.chunks, plan.tp * plan.rows, plan.layer_window), jnp.bfloat16),
            pltpu.VMEM((2, plan.chunk + 2 * LANES, LANES), jnp.bfloat16),
            per_chunk, per_chunk, dma((2,)),
            per_chunk, per_chunk, per_chunk, per_chunk, per_chunk, per_chunk,
            dma((2, plan.dp)), dma((2,)), dma((2,)),
            dma((8,)), dma((2,)), dma((2,)), dma((2,)), dma((2,)), dma((2,)),
            pltpu.VMEM((plan.layers, plan.down_rows, plan.whole), jnp.bfloat16),
            pltpu.VMEM((plan.layers, plan.out_rows, plan.whole), jnp.bfloat16),
            dma((4,)),
            pltpu.VMEM((plan.layers // GROUP, plan.tp - 1, GROUP, plan.rows, plan.layer_window), jnp.bfloat16),
            dma((plan.layers // GROUP,)),
        ],
        compiler_params=pltpu.CompilerParams(collective_id=0, has_side_effects=True),
        name="gather",
    )(*args)[:4]


def place_slabs(plan, slabs, first, count, shapes, store, held=()):
    hbm = pl.BlockSpec(memory_space=pltpu.HBM)
    depth = min(BUFFERS, count)
    ahead = depth // 2

    def body(slab, *refs):
        outs, (buffers, loads, stores) = refs[len(held):-3], refs[-3:]

        def each_size(chunk, act):
            if first + count > plan.ring:
                pl.when(chunk < plan.ring)(lambda: act(plan.chunk))
                pl.when(chunk == plan.ring)(lambda: act(plan.tail))
            else:
                act(plan.chunk)

        def load(i, rows):
            for owner in range(plan.dp):
                pltpu.make_async_copy(
                    slab.at[owner, first + i, pl.ds(0, rows), :],
                    buffers.at[i % depth, pl.ds(0, rows), pl.ds(owner * LANES, LANES)],
                    loads.at[i % depth],
                ).start()

        def wait(i, rows, sem):
            buffer = buffers.at[i % depth, pl.ds(0, rows), :]
            pltpu.make_async_copy(buffer, buffer, sem.at[i % depth]).wait()

        def write(i, rows):
            wait(i, rows, loads)
            for source, target in store(buffers.at[i % depth], first + i, rows, outs):
                pltpu.make_async_copy(source, target, stores.at[i % depth]).start()

        def step(i, _):
            @pl.when(i >= depth)
            def _():
                each_size(first + i - depth, lambda rows: wait(i - depth, rows, stores))

            @pl.when(i < count)
            def _():
                each_size(first + i, lambda rows: load(i, rows))

            @pl.when((i >= ahead) & (i < count + ahead))
            def _():
                each_size(first + i - ahead, lambda rows: write(i - ahead, rows))

            return 0

        lax.fori_loop(0, count + depth, step, 0)

    outs = [jax.ShapeDtypeStruct(shape, jnp.bfloat16) for shape in shapes]
    return pl.pallas_call(
        body,
        in_specs=[hbm] * (1 + len(held)),
        out_specs=[hbm] * len(outs),
        out_shape=outs,
        scratch_shapes=[
            pltpu.VMEM((depth, plan.chunk, plan.dp * LANES), jnp.bfloat16),
            pltpu.SemaphoreType.DMA((depth,)),
            pltpu.SemaphoreType.DMA((depth,)),
        ],
        input_output_aliases={1 + n: n for n in range(len(held))},
        cost_estimate=pl.CostEstimate(
            flops=10**7, bytes_accessed=4 * count * plan.chunk * plan.dp * LANES, transcendentals=0
        ),
        compiler_params=pltpu.CompilerParams(vmem_limit_bytes=VMEM),
    )(slabs, *held)


def place_layers(plan, slabs):
    narrow, wide, width = 3 * plan.part, 2 * plan.wide, plan.dp * LANES

    def store(buffer, chunk, rows, outs):
        return [
            (buffer.at[pl.ds(0, narrow), :], outs[0].at[chunk]),
            (buffer.at[pl.ds(narrow, wide), :], outs[1].at[chunk]),
        ]

    shapes = [(plan.layers, narrow, width), (plan.layers, wide, width)]
    return place_slabs(plan, slabs, 0, plan.layers, shapes, store)


def place_head(plan, slabs, first, count, *held):
    def store(buffer, chunk, rows, outs):
        at = pl.multiple_of((chunk - plan.layers) * plan.chunk, 16)
        return [(buffer.at[pl.ds(0, rows), :], outs[0].at[pl.ds(at, rows), :])]

    shapes = [(plan.vocab, plan.dp * LANES)]
    return place_slabs(plan, slabs, plan.layers + first, count, shapes, store, held)[0]


def place_rows(plan, arrays, spots, width, column, held):
    count = len(spots([array for array in arrays], 0))
    columns = arrays[0].shape[-1]
    outs = [
        jax.ShapeDtypeStruct((plan.layers, plan.downs, plan.columns), jnp.bfloat16),
        jax.ShapeDtypeStruct((plan.layers, plan.columns, plan.outs), jnp.bfloat16),
        jax.ShapeDtypeStruct((plan.vocab, plan.dp * LANES), jnp.bfloat16),
    ]
    with_head = columns > width
    kept = [n for n in range(3) if n in held]
    made = [n for n in range(3 if with_head else 2)]

    def body(*refs):
        targets = dict(zip(made, refs[len(arrays) + len(kept):-6], strict=True))
        buffers, turned, loads, stores, out_stores, head_stores = refs[-6:]
        moves = spots(refs[: len(arrays)], lax.axis_index("dp"))
        loading = [pltpu.make_async_copy(move[0], buffers.at[n], loads.at[n]) for n, move in enumerate(moves)]
        storing = []
        for load in loading:
            load.start()

        def put(source, target, sem):
            storing.append(pltpu.make_async_copy(source, target, sem))
            storing[-1].start()

        place = pl.ds(column, width)
        for n, (load, (_, layer, owner, part)) in enumerate(zip(loading, moves, strict=True)):
            load.wait()
            put(buffers.at[n, pl.ds(0, plan.downs), pl.ds(0, width)], targets[0].at[layer, :, place], stores.at[n])
            for j in range((columns - width) // LANES):
                row = plan.extra_first + (part * WHOLE + j) * plan.piece
                put(
                    buffers.at[n, :, pl.ds(width + j * LANES, LANES)],
                    targets[2].at[pl.ds(row, plan.piece), pl.ds(pl.multiple_of(owner * LANES, LANES), LANES)],
                    head_stores.at[n, j],
                )
        for n, (_, layer, _, _) in enumerate(moves):
            for i in range(plan.outs // LANES):
                for j in range(width // LANES):
                    turned[n, pl.ds(j * LANES, LANES), pl.ds(i * LANES, LANES)] = buffers[
                        n, pl.ds(plan.downs + i * LANES, LANES), pl.ds(j * LANES, LANES)
                    ].T
            put(turned.at[n], targets[1].at[layer, place, :], out_stores.at[n])
        for store in storing:
            store.wait()

    hbm = pl.BlockSpec(memory_space=pltpu.HBM)
    dma = pltpu.SemaphoreType.DMA((count,))
    result = pl.pallas_call(
        body,
        out_shape=[outs[n] for n in made],
        in_specs=[hbm] * (len(arrays) + len(kept)),
        out_specs=[hbm] * len(made),
        scratch_shapes=[
            pltpu.VMEM((count, plan.piece, columns), jnp.bfloat16),
            pltpu.VMEM((count, width, plan.outs), jnp.bfloat16),
            dma, dma, dma, pltpu.SemaphoreType.DMA((count, max(WHOLE, 1))),
        ],
        input_output_aliases={len(arrays) + i: n for i, n in enumerate(kept)},
        cost_estimate=pl.CostEstimate(flops=10**7, bytes_accessed=4 * count * plan.piece * columns, transcendentals=0),
        compiler_params=pltpu.CompilerParams(vmem_limit_bytes=VMEM),
    )(*arrays, *(held[n] for n in kept))
    return dict(zip(made, result, strict=True))


def place_whole(plan, whole):
    def spots(refs, dp):
        return [(refs[0].at[layer], layer, 0, 0) for layer in range(plan.layers)]

    return place_rows(plan, [whole], spots, plan.whole, 0, {})


def place_shares(plan, shares, held):
    owners = list(shares)
    arrays = [array for owner in owners for array in shares[owner]]

    def spots(refs, dp):
        core, x, y = dp % 2, (dp // 2) % 2, dp // 4
        found = []
        for n, ref in enumerate(refs):
            flip_x, flip_y, flip_core = owners[n // plan.share]
            owner = (y + flip_y * (1 - 2 * y)) * 4 + (x + flip_x * (1 - 2 * x)) * 2 + core + flip_core * (1 - 2 * core)
            found.append((ref, owner * plan.share + n % plan.share, owner, n % plan.share))
        return found

    return place_rows(plan, arrays, spots, plan.cut, plan.whole, held)


def solution(mesh):
    train_stack = P(None, ("dp", "tp"), None)
    train_head = P(("dp", "tp"), None)
    fused_stack = P(None, "tp", None)
    last_stack = P(None, None, "tp")
    head_rows = P("tp", None)

    def local_sync(w_query, w_key, w_value, w_out, w_gate, w_up, w_down, w_head):
        plan = Plan(mesh.shape["tp"], mesh.shape["dp"], w_query, w_gate, w_out, w_down, w_head)
        slabs, own_0, own_1, whole = gather(plan, w_query, w_key, w_value, w_out, w_gate, w_up, w_down, w_head)

        def swap(bit, array):
            return lax.ppermute(array, "dp", [(i, i ^ bit) for i in range(plan.dp)])

        pair, along_x, along_y = (functools.partial(swap, bit) for bit in (1, 2, 4))
        hold = lax.optimization_barrier

        x_1, y_0 = along_x(own_1), along_y(own_0)
        x_0, y_1 = along_x(own_0), along_y(own_1)
        pair_own = [pair(own_0), pair(own_1)]
        qkv_block, gate_up_block = place_layers(plan, slabs)
        x_1, y_0, qkv_block, slabs = hold((x_1, y_0, qkv_block, slabs))
        diagonal_0 = along_x(y_0)
        diagonal_1 = along_y(x_1)
        pair_x_1, pair_y_0 = pair(x_1), pair(y_0)
        head_chunks = plan.ring + 1 - plan.layers
        early = head_chunks // 4
        head_block = place_head(plan, slabs, early, head_chunks - early)
        x_0, y_1, head_block, slabs, whole = hold((x_0, y_1, head_block, slabs, whole))
        pair_x_0, pair_y_1 = pair(x_0), pair(y_1)
        placed = place_whole(plan, whole)
        slabs, *placed = hold((slabs, placed[0], placed[1]))
        head_block = place_head(plan, slabs, 0, early, head_block)
        own_0, own_1, head_block = hold((own_0, own_1, head_block))
        near = {
            (0, 0, 0): [own_0, own_1], (0, 0, 1): pair_own, (1, 0, 0): [x_0, x_1], (1, 0, 1): [pair_x_0, pair_x_1],
            (0, 1, 0): [y_0, y_1], (0, 1, 1): [pair_y_0, pair_y_1],
        }
        placed = place_shares(plan, near, {0: placed[0], 1: placed[1], 2: head_block})
        diagonal_0, diagonal_1, *placed = hold((diagonal_0, diagonal_1, placed[0], placed[1], placed[2]))
        pair_diagonal = [pair(diagonal_0), pair(diagonal_1)]
        placed = place_shares(plan, {(1, 1, 0): [diagonal_0, diagonal_1]}, dict(enumerate(placed)))
        placed = place_shares(plan, {(1, 1, 1): pair_diagonal}, placed)
        down_block, o_block, head_block = placed[0], placed[1], placed[2]
        return (
            qkv_block,
            o_block,
            gate_up_block,
            jnp.swapaxes(down_block, 1, 2),
            head_block,
        )

    return jax.shard_map(
        local_sync,
        mesh=mesh,
        in_specs=(train_stack,) * 7 + (train_head,),
        out_specs=(fused_stack, last_stack, fused_stack, last_stack, head_rows),
        check_vma=False,
    )
```

```python
import functools

import jax
import jax.numpy as jnp
from jax import lax
from jax.experimental import pallas as pl
from jax.experimental.pallas import tpu as pltpu
from jax.sharding import PartitionSpec as P


MESH = pl.DeviceIdType.MESH
LANES = 128
VMEM = 67_000_000
AHEAD = 14
BUFFERS = 6
LAG = 2
SHARE_AT = 20
RETIRE = 8
WHOLE = 3
WHOLE_AT = 2
RANKS_AT = 10
PARTS = 4
GROUP = 4


class Plan:
    def __init__(self, tp, dp, w_query, w_gate, w_out, w_down, w_head):
        self.tp, self.dp = tp, dp
        self.layers, self.rows, columns = w_query.shape
        self.part = columns // tp
        self.wide = w_gate.shape[2] // tp
        self.vocab = w_head.shape[1] // tp
        self.head_tiles = w_head.shape[1] // LANES
        self.chunk = 3 * self.part + 2 * self.wide
        self.wide_window = -(-self.wide // LANES) * LANES
        self.layer_window = 3 * self.part + 2 * self.wide_window
        self.head_chunks = -(-self.vocab // self.chunk)
        self.chunks = self.layers + self.head_chunks
        end = self.vocab - (self.head_chunks - 1) * self.chunk
        self.tail_window = -(-(end + LANES) // LANES) * LANES
        self.window_tiles = (self.head_chunks - 1) * self.chunk // LANES + self.tail_window // LANES
        self.shift = max(self.vocab * r - self.head_base(r) * LANES for r in range(tp))
        self.out_rows, self.down_rows = w_out.shape[1], w_down.shape[1]
        self.downs, self.outs = 2 * tp * self.down_rows, 2 * tp * self.out_rows
        self.piece = self.downs + self.outs
        self.share = self.layers // dp
        self.columns = w_out.shape[2]
        self.whole = WHOLE * LANES
        self.cut = self.columns - self.whole
        self.extra_first = self.vocab - self.share * WHOLE * self.piece
        self.ring = self.layers + self.extra_first // self.chunk
        self.tail = self.extra_first % self.chunk

    def wide_base(self, rank):
        return (self.wide * rank) // LANES

    def head_base(self, rank):
        base = (self.vocab * rank) // LANES
        return base - (rank // (self.tp - 1)) * (self.vocab * (self.tp - 1) // LANES + self.window_tiles - self.head_tiles)


def gather_kernel(plan, q, k, v, o, g, u, d, h, slabs, own_0, own_1, whole, stop_0, stop_1, land_d, land_o, zbuf, tbuf,
                  z_recv, z_send, local, x_recv, y_recv, a_recv, b_recv, pair_recv, send, stop_recv, share_recv,
                  share_send, land_recv, land_send, whole_recv, whole_send, whole_pair_recv, whole_pair_send,
                  keep_d, keep_o, keep_sem, packed, pack_sem):
    z, dp = lax.axis_index("tp"), lax.axis_index("dp")
    core, x, y = dp % 2, (dp // 2) % 2, dp // 4
    x_peer = y * 4 + (1 - x) * 2 + core
    y_peer = (1 - y) * 4 + x * 2 + core
    diagonal = (1 - y) * 4 + (1 - x) * 2 + core
    pair = dp + 1 - 2 * core
    rows, chunk, tail = plan.rows, plan.chunk, plan.tail
    layers, ring, last = plan.layers, plan.ring, plan.chunks - 1
    my_rows = pl.ds(pl.multiple_of(z * rows, rows), rows)

    def lanes(first_tile, width):
        return pl.ds(pl.multiple_of(first_tile * LANES, LANES), width)

    def remote(source, target, send_sem, recv_sem, **to):
        pltpu.make_async_remote_copy(source, target, send_sem, recv_sem, device_id=to, device_id_type=MESH).start()

    def wait_for(ref, sem):
        pltpu.make_async_copy(ref, ref, sem).wait()


    def rank_at(step):
        return (z + step + core * (plan.tp - 2 * step)) % plan.tp

    def layer_pieces(first, rank):
        some, part, wide = pl.ds(first, GROUP), plan.part, plan.wide_window
        narrow = lanes(rank * (part // LANES), part)
        window = lanes(plan.wide_base(rank), wide)
        return [
            (q.at[some, :, narrow], 0, part),
            (k.at[some, :, narrow], part, part),
            (v.at[some, :, narrow], 2 * part, part),
            (g.at[some, :, window], 3 * part, wide),
            (u.at[some, :, window], 3 * part + wide, wide),
        ]

    def collect(group):
        for step in range(1, plan.tp):
            for source, column, width in layer_pieces(group * GROUP, rank_at(step)):
                target = packed.at[group, step - 1, :, :, pl.ds(column, width)]
                pltpu.make_async_copy(source, target, pack_sem.at[group]).start()
        for source, column, width in layer_pieces(group * GROUP, z):
            target = zbuf.at[pl.ds(group * GROUP, GROUP), my_rows, pl.ds(column, width)]
            pltpu.make_async_copy(source, target, z_recv.at[group * GROUP]).start()

    def exchange_layers(group):
        wait_for(packed.at[group], pack_sem.at[group])
        for step in range(1, plan.tp):
            index = group * GROUP
            target = zbuf.at[pl.ds(index, GROUP), my_rows, :]
            remote(packed.at[group, step - 1], target, z_send.at[index], z_recv.at[index], tp=rank_at(step))

    def exchange_head(index, width):
        def piece(rank):
            return h.at[:, lanes(plan.head_base(rank) + (index - layers) * (chunk // LANES), width)]

        target = zbuf.at[index, my_rows, pl.ds(0, width)]
        for step in range(1, plan.tp):
            remote(piece(rank_at(step)), target, z_send.at[index], z_recv.at[index], tp=rank_at(step))
        pltpu.make_async_copy(piece(z), target, z_recv.at[index]).start()

    def start_exchange(index):
        @pl.when((index >= layers) & (index < last))
        def _():
            exchange_head(index, chunk)

        @pl.when(index == last)
        def _():
            exchange_head(last, plan.tail_window)

    def wait_exchange(index, width):
        wait_for(zbuf.at[index, :, pl.ds(0, width)], z_recv.at[index])


    def turn(slot, tile, index, source_tile):
        tbuf[slot, pl.ds(tile * LANES, LANES), :] = zbuf[index, :, pl.ds(source_tile * LANES, LANES)].T

    def store(slot, first, index, to, count):
        pltpu.make_async_copy(
            tbuf.at[slot, pl.ds(first, count), :], slabs.at[dp, index, pl.ds(to, count), :], local.at[slot]
        ).start()

    def make_layer(index, slot):
        @pl.when(index % GROUP == 0)
        def _():
            wait_for(zbuf.at[pl.ds(index, GROUP), :, pl.ds(0, plan.layer_window)], z_recv.at[index])

        for tile in range(plan.layer_window // LANES):
            turn(slot, tile, index, tile)
        shift = plan.wide * z - plan.wide_base(z) * LANES
        narrow, wide, window = 3 * plan.part, plan.wide, plan.wide_window
        store(slot, 0, index, 0, narrow)
        store(slot, pl.multiple_of(narrow + shift, 16), index, narrow, wide)
        store(slot, pl.multiple_of(narrow + window + shift, 16), index, narrow + wide, wide)

    head_shift = plan.vocab * z - plan.head_base(z) * LANES

    def make_head(index, slot):
        @pl.when(index == layers)
        def _():
            wait_exchange(index, chunk)

        wait_exchange(index + 1, chunk)
        tiles = chunk // LANES
        for tile in range(tiles):
            turn(slot, tile, index, tile)
        for tile in range(2):
            turn(slot, tiles + tile, index + 1, tile)
        store(slot, pl.multiple_of(head_shift, 16), index, 0, chunk)

    def turn_rows(slot, first, count):
        start = first // LANES
        for tile in range(-(-(first % LANES + plan.shift + count) // LANES)):
            at = start + tile
            turn(slot, tile, layers + at // (chunk // LANES), at % (chunk // LANES))
        return pl.multiple_of(first % LANES + head_shift, 16)

    def make_tail(slot):
        wait_exchange(ring + 1, chunk)
        store(slot, turn_rows(slot, (ring - layers) * chunk, tail), ring, 0, tail)

    def make_extra():
        for index in range(ring + 2, last):
            wait_exchange(index, chunk)
        wait_exchange(last, plan.tail_window)
        blocks = plan.share * WHOLE

        def stored(n, own):
            wait_for(own.at[:, pl.ds(plan.cut, LANES)], local.at[n % 2])

        for n in range(blocks):
            own = (own_0, own_1)[n // WHOLE]
            if n >= 2:
                stored(n, own)
            at = turn_rows(n % 2, plan.extra_first + n * plan.piece, plan.piece)
            pltpu.make_async_copy(
                tbuf.at[n % 2, pl.ds(at, plan.piece), :],
                own.at[:, pl.ds(plan.cut + n % WHOLE * LANES, LANES)], local.at[n % 2],
            ).start()
        for n in range(blocks - min(2, blocks), blocks):
            stored(n, own_0)


    def slab_view(index):
        return lambda owner, first, count: slabs.at[owner, index, pl.ds(first, count), :]

    def push(part, index, recv, to):
        remote(part, part, send.at[index], recv.at[index], dp=to)

    def send_own(view, index, slot, count):
        own = view(dp, 0, count)
        wait_for(own, local.at[slot])
        push(own, index, x_recv, x_peer)
        push(own, index, y_recv, y_peer)
        push(own, index, pair_recv, pair)

    def forward(view, index, count):
        half = count // 2
        wait_for(view(x_peer, 0, count), x_recv.at[index])
        push(view(x_peer, half, half), index, b_recv, y_peer)
        push(view(x_peer, 0, count), index, pair_recv, pair)
        wait_for(view(y_peer, 0, count), y_recv.at[index])
        push(view(y_peer, 0, half), index, a_recv, x_peer)
        push(view(y_peer, 0, count), index, pair_recv, pair)

    def forward_diagonal(view, index, count):
        half = count // 2
        wait_for(view(diagonal, 0, half), a_recv.at[index])
        wait_for(view(diagonal, half, half), b_recv.at[index])
        push(view(diagonal, 0, count), index, pair_recv, pair)

    def finish(view, index, count):
        wait_for(view(pl.ds(0, 7), 0, count), send.at[index])
        wait_for(view(pl.ds(0, 4), 0, count), pair_recv.at[index])

    def finish_exchange(index, window):
        wait_for(zbuf.at[index, pl.ds(0, (plan.tp - 1) * rows), pl.ds(0, window)], z_send.at[index])


    def pieces(source_dp, to, place):
        all_rows = plan.downs
        downs = pl.ds(pl.multiple_of(place * plan.down_rows, 8), plan.down_rows)
        outs = pl.ds(pl.multiple_of(all_rows + place * plan.out_rows, 8), plan.out_rows)
        stop_downs, stop_outs = pl.ds(0, plan.down_rows), pl.ds(plan.down_rows, plan.out_rows)
        cut, home = pl.ds(plan.whole, plan.cut), pl.ds(0, plan.cut)
        found = []
        for n, (stop, own) in enumerate(((stop_0, own_0), (stop_1, own_1))):
            layer = to * 2 + n
            found.append((d.at[layer, :, cut], stop.at[source_dp, stop_downs, :], own.at[downs, home], n))
            found.append((o.at[layer, :, cut], stop.at[source_dp, stop_outs, :], own.at[outs, home], n))
        return found

    my_rank = dp // 2
    my_place = (dp % 2) * plan.tp + z
    stays = my_rank == z

    def share_in_plane():
        for step in range(1, plan.dp):
            to = (dp + step) % plan.dp

            @pl.when(stays)
            def _(to=to):
                for part, _, final, n in pieces(dp, to, my_place):
                    remote(part, final, share_send.at[n], share_recv.at[n], dp=to)

            @pl.when(jnp.logical_not(stays))
            def _(to=to):
                for part, stop, _, n in pieces(dp, to, my_place):
                    remote(part, stop, share_send.at[n], stop_recv.at[n, dp], dp=to)

        @pl.when(stays)
        def _():
            for part, _, final, n in pieces(dp, dp, my_place):
                pltpu.make_async_copy(part, final, share_recv.at[n]).start()

    def share_to_rank(source_dp):
        rank, place = source_dp // 2, (source_dp % 2) * plan.tp + z

        @pl.when((rank != z) & (source_dp == dp))
        def _():
            for part, _, final, n in pieces(dp, dp, place):
                remote(part, final, share_send.at[n], share_recv.at[n], tp=rank)

        @pl.when((rank != z) & (source_dp != dp))
        def _():
            for n, stop in enumerate((stop_0, stop_1)):
                wait_for(stop.at[source_dp], stop_recv.at[n, source_dp])
            for _, stop, final, n in pieces(source_dp, dp, place):
                remote(stop, final, share_send.at[n], share_recv.at[n], tp=rank)


    whole_columns = pl.ds(0, plan.whole)
    keep = (keep_d, keep_o)
    mine = ((d, land_d, plan.down_rows, 0), (o, land_o, plan.out_rows, plan.downs))
    half = layers // 2

    def whole_home(n, row):
        _, _, count, first = mine[n]
        return pl.ds(pl.multiple_of(first + row * count, 8), count)

    def landing(rank, some, act):
        pl.when(rank == z)(lambda: act([whole.at[some, whole_home(n, core * plan.tp + z), :] for n in range(2)]))
        pl.when(rank != z)(lambda: act([land.at[rank, some] for _, land, _, _ in mine]))

    every = pl.ds(0, layers)

    def whole_out():
        def act(places):
            for n, (source, _, _, _) in enumerate(mine):
                for to, at in ((x_peer, 0), (y_peer, 2)):
                    remote(source.at[:, :, whole_columns], places[n], land_send.at[n], land_recv.at[at + n], dp=to)

        landing(my_rank, every, act)

        @pl.when(stays)
        def _():
            for n, (source, _, _, _) in enumerate(mine):
                pltpu.make_async_copy(source.at[:, :, whole_columns], keep[n], keep_sem.at[n]).start()

    def whole_keep():
        @pl.when(stays)
        def _():
            for n in range(2):
                wait_for(keep[n], keep_sem.at[n])
                target = whole.at[:, whole_home(n, core * plan.tp + z), :]
                pltpu.make_async_copy(keep[n], target, keep_sem.at[2 + n]).start()

    def whole_forward():
        for owner, at, first, to, then in ((x_peer, 0, half, y_peer, 6), (y_peer, 2, 0, x_peer, 4)):
            def arrived(places, at=at):
                for n in range(2):
                    wait_for(places[n], land_recv.at[at + n])

            def on(places, to=to, then=then):
                for n in range(2):
                    remote(places[n], places[n], land_send.at[n], land_recv.at[then + n], dp=to)

            landing(owner // 2, every, arrived)
            landing(owner // 2, pl.ds(first, half), on)

    def whole_arrive():
        for first, at in ((0, 4), (half, 6)):
            def arrived(places, at=at):
                for n in range(2):
                    wait_for(places[n], land_recv.at[at + n])

            landing(diagonal // 2, pl.ds(first, half), arrived)

    def whole_to_rank(shift, part):
        rank = (z + shift + core * (plan.tp - 2 * shift)) % plan.tp
        some = pl.ds(part * (layers // PARTS), layers // PARTS)

        def move(sources):
            for n, source in enumerate(sources):
                target = whole.at[some, whole_home(n, core * plan.tp + z), :]
                remote(source, target, whole_send.at[n], whole_recv.at[n], tp=rank)

        pl.when(rank == my_rank)(lambda: move([source.at[some, :, whole_columns] for source, _, _, _ in mine]))
        pl.when(rank != my_rank)(lambda: move([land.at[rank, some] for _, land, _, _ in mine]))

    def whole_rows(which):
        return [
            whole.at[:, pl.ds(pl.multiple_of(first + which * plan.tp * count, 8), plan.tp * count), :]
            for _, _, count, first in mine
        ]

    def whole_to_pair():
        for n, part in enumerate(whole_rows(core)):
            away = pl.ds(0, (plan.tp - 1) * mine[n][2])
            wait_for(whole.at[:, away, :], whole_recv.at[n])

            @pl.when(stays)
            def _(n=n):
                wait_for(keep[n], keep_sem.at[2 + n])

            remote(part, part, whole_pair_send.at[n], whole_pair_recv.at[n], dp=pair)

    def whole_finish():
        for n, (_, land, count, first) in enumerate(mine):
            wait_for(land.at[pl.ds(0, 3)], land_send.at[n])
            wait_for(whole.at[:, pl.ds(first, (plan.tp - 1) * count), :], whole_send.at[n])
            wait_for(whole_rows(core)[n], whole_pair_send.at[n])
            wait_for(whole_rows(1 - core)[n], whole_pair_recv.at[n])

    groups = layers // GROUP
    barrier = pltpu.get_barrier_semaphore()
    peers = [{"tp": (z + step) % plan.tp} for step in range(1, plan.tp)]
    peers += [{"dp": (dp + step) % plan.dp} for step in range(1, plan.dp)]
    for peer in peers:
        pl.semaphore_signal(barrier, inc=1, device_id=peer, device_id_type=MESH)
    for group in range(groups):
        collect(group)
    pl.semaphore_wait(barrier, len(peers))

    whole_out()
    exchange_layers(0)
    share_in_plane()
    for group in range(1, groups):
        exchange_layers(group)
    for index in range(layers, AHEAD):
        start_exchange(index)

    def retire(index):
        finish(slab_view(index), index, chunk)

        @pl.when((index < layers) & (index % GROUP == 0))
        def _():
            sent = pl.ds(0, (plan.tp - 1) * rows)
            wait_for(zbuf.at[pl.ds(index, GROUP), sent, pl.ds(0, plan.layer_window)], z_send.at[index])

        @pl.when(index >= layers)
        def _():
            finish_exchange(index, chunk)

    def step(index, _):
        slot = index % 2

        @pl.when(index + AHEAD < plan.chunks)
        def _():
            start_exchange(index + AHEAD)

        @pl.when((index >= SHARE_AT) & (index < SHARE_AT + plan.dp))
        def _():
            share_to_rank(index - SHARE_AT)

        @pl.when(index == WHOLE_AT)
        def _():
            whole_keep()
            whole_forward()

        @pl.when(index == WHOLE_AT + 3)
        def _():
            whole_arrive()

        @pl.when((index >= RANKS_AT) & (index < RANKS_AT + (plan.tp - 1) * PARTS))
        def _():
            whole_to_rank((index - RANKS_AT) % (plan.tp - 1) + 1, (index - RANKS_AT) // (plan.tp - 1))

        @pl.when(index < layers)
        def _():
            make_layer(index, slot)

        @pl.when(index >= layers)
        def _():
            make_head(index, slot)

        send_own(slab_view(index), index, slot, chunk)

        @pl.when(index >= LAG)
        def _():
            forward(slab_view(index - LAG), index - LAG, chunk)

        @pl.when(index >= 2 * LAG)
        def _():
            forward_diagonal(slab_view(index - 2 * LAG), index - 2 * LAG, chunk)

        @pl.when(index >= RETIRE)
        def _():
            retire(index - RETIRE)

        return 0

    lax.fori_loop(0, ring, step, 0)

    make_tail(ring % 2)
    send_own(slab_view(ring), ring, ring % 2, tail)
    make_extra()
    for index in range(ring - LAG, ring):
        forward(slab_view(index), index, chunk)
        if index == ring - LAG:
            whole_to_pair()
    forward(slab_view(ring), ring, tail)
    for index in range(ring - 2 * LAG, ring):
        forward_diagonal(slab_view(index), index, chunk)
        if index == ring - 2:
            for older in range(ring - RETIRE, ring - LAG):
                retire(older)
            for older in range(ring, last):
                finish_exchange(older, chunk)
            finish_exchange(last, plan.tail_window)
            whole_finish()
            for n, own in enumerate((own_0, own_1)):
                wait_for(own.at[:, pl.ds(0, plan.cut)], share_recv.at[n])
                for parts in (8, 5):
                    sent = pl.ds(0, parts * (plan.down_rows + plan.out_rows))
                    wait_for(own.at[sent, pl.ds(0, plan.cut)], share_send.at[n])
    forward_diagonal(slab_view(ring), ring, tail)
    for index in range(ring - LAG, ring):
        retire(index)
    finish(slab_view(ring), ring, tail)


def gather(plan, *args):
    dma = pltpu.SemaphoreType.DMA
    per_chunk = dma((plan.chunks,))
    share_rows = plan.down_rows + plan.out_rows
    hbm = pl.BlockSpec(memory_space=pltpu.HBM)
    shapes = [(plan.dp, plan.ring + 1, plan.chunk, LANES), (plan.piece, plan.columns), (plan.piece, plan.columns)]
    shapes += [(plan.layers, plan.piece, plan.whole)] + [(plan.dp, share_rows, plan.cut)] * 2
    shapes += [(plan.tp, plan.layers, count, plan.whole) for count in (plan.down_rows, plan.out_rows)]
    return pl.pallas_call(
        functools.partial(gather_kernel, plan),
        out_shape=[jax.ShapeDtypeStruct(shape, jnp.bfloat16) for shape in shapes],
        in_specs=[hbm] * 8,
        out_specs=[hbm] * len(shapes),
        scratch_shapes=[
            pltpu.VMEM((plan.chunks, plan.tp * plan.rows, plan.layer_window), jnp.bfloat16),
            pltpu.VMEM((2, plan.chunk + 2 * LANES, LANES), jnp.bfloat16),
            per_chunk, per_chunk, dma((2,)),
            per_chunk, per_chunk, per_chunk, per_chunk, per_chunk, per_chunk,
            dma((2, plan.dp)), dma((2,)), dma((2,)),
            dma((8,)), dma((2,)), dma((2,)), dma((2,)), dma((2,)), dma((2,)),
            pltpu.VMEM((plan.layers, plan.down_rows, plan.whole), jnp.bfloat16),
            pltpu.VMEM((plan.layers, plan.out_rows, plan.whole), jnp.bfloat16),
            dma((4,)),
            pltpu.VMEM((plan.layers // GROUP, plan.tp - 1, GROUP, plan.rows, plan.layer_window), jnp.bfloat16),
            dma((plan.layers // GROUP,)),
        ],
        compiler_params=pltpu.CompilerParams(collective_id=0, has_side_effects=True),
        name="gather",
    )(*args)[:4]


def place_slabs(plan, slabs, first, count, shapes, store, held=()):
    hbm = pl.BlockSpec(memory_space=pltpu.HBM)
    depth = min(BUFFERS, count)
    ahead = depth // 2

    def body(slab, *refs):
        outs, (buffers, loads, stores) = refs[len(held):-3], refs[-3:]

        def each_size(chunk, act):
            if first + count > plan.ring:
                pl.when(chunk < plan.ring)(lambda: act(plan.chunk))
                pl.when(chunk == plan.ring)(lambda: act(plan.tail))
            else:
                act(plan.chunk)

        def load(i, rows):
            for owner in range(plan.dp):
                pltpu.make_async_copy(
                    slab.at[owner, first + i, pl.ds(0, rows), :],
                    buffers.at[i % depth, pl.ds(0, rows), pl.ds(owner * LANES, LANES)],
                    loads.at[i % depth],
                ).start()

        def wait(i, rows, sem):
            buffer = buffers.at[i % depth, pl.ds(0, rows), :]
            pltpu.make_async_copy(buffer, buffer, sem.at[i % depth]).wait()

        def write(i, rows):
            wait(i, rows, loads)
            for source, target in store(buffers.at[i % depth], first + i, rows, outs):
                pltpu.make_async_copy(source, target, stores.at[i % depth]).start()

        def step(i, _):
            @pl.when(i >= depth)
            def _():
                each_size(first + i - depth, lambda rows: wait(i - depth, rows, stores))

            @pl.when(i < count)
            def _():
                each_size(first + i, lambda rows: load(i, rows))

            @pl.when((i >= ahead) & (i < count + ahead))
            def _():
                each_size(first + i - ahead, lambda rows: write(i - ahead, rows))

            return 0

        lax.fori_loop(0, count + depth, step, 0)

    outs = [jax.ShapeDtypeStruct(shape, jnp.bfloat16) for shape in shapes]
    return pl.pallas_call(
        body,
        in_specs=[hbm] * (1 + len(held)),
        out_specs=[hbm] * len(outs),
        out_shape=outs,
        scratch_shapes=[
            pltpu.VMEM((depth, plan.chunk, plan.dp * LANES), jnp.bfloat16),
            pltpu.SemaphoreType.DMA((depth,)),
            pltpu.SemaphoreType.DMA((depth,)),
        ],
        input_output_aliases={1 + n: n for n in range(len(held))},
        cost_estimate=pl.CostEstimate(
            flops=10**7, bytes_accessed=4 * count * plan.chunk * plan.dp * LANES, transcendentals=0
        ),
        compiler_params=pltpu.CompilerParams(vmem_limit_bytes=VMEM),
    )(slabs, *held)


def place_layers(plan, slabs):
    narrow, wide, width = 3 * plan.part, 2 * plan.wide, plan.dp * LANES

    def store(buffer, chunk, rows, outs):
        return [
            (buffer.at[pl.ds(0, narrow), :], outs[0].at[chunk]),
            (buffer.at[pl.ds(narrow, wide), :], outs[1].at[chunk]),
        ]

    shapes = [(plan.layers, narrow, width), (plan.layers, wide, width)]
    return place_slabs(plan, slabs, 0, plan.layers, shapes, store)


def place_head(plan, slabs, first, count, *held):
    def store(buffer, chunk, rows, outs):
        at = pl.multiple_of((chunk - plan.layers) * plan.chunk, 16)
        return [(buffer.at[pl.ds(0, rows), :], outs[0].at[pl.ds(at, rows), :])]

    shapes = [(plan.vocab, plan.dp * LANES)]
    return place_slabs(plan, slabs, plan.layers + first, count, shapes, store, held)[0]


def place_rows(plan, arrays, spots, width, column, held):
    count = len(spots([array for array in arrays], 0))
    columns = arrays[0].shape[-1]
    outs = [
        jax.ShapeDtypeStruct((plan.layers, plan.downs, plan.columns), jnp.bfloat16),
        jax.ShapeDtypeStruct((plan.layers, plan.columns, plan.outs), jnp.bfloat16),
        jax.ShapeDtypeStruct((plan.vocab, plan.dp * LANES), jnp.bfloat16),
    ]
    with_head = columns > width
    kept = [n for n in range(3) if n in held]
    made = [n for n in range(3 if with_head else 2)]

    def body(*refs):
        targets = dict(zip(made, refs[len(arrays) + len(kept):-6], strict=True))
        buffers, turned, loads, stores, out_stores, head_stores = refs[-6:]
        moves = spots(refs[: len(arrays)], lax.axis_index("dp"))
        loading = [pltpu.make_async_copy(move[0], buffers.at[n], loads.at[n]) for n, move in enumerate(moves)]
        storing = []
        for load in loading:
            load.start()

        def put(source, target, sem):
            storing.append(pltpu.make_async_copy(source, target, sem))
            storing[-1].start()

        place = pl.ds(column, width)
        for n, (load, (_, layer, owner, part)) in enumerate(zip(loading, moves, strict=True)):
            load.wait()
            put(buffers.at[n, pl.ds(0, plan.downs), pl.ds(0, width)], targets[0].at[layer, :, place], stores.at[n])
            for j in range((columns - width) // LANES):
                row = plan.extra_first + (part * WHOLE + j) * plan.piece
                put(
                    buffers.at[n, :, pl.ds(width + j * LANES, LANES)],
                    targets[2].at[pl.ds(row, plan.piece), pl.ds(pl.multiple_of(owner * LANES, LANES), LANES)],
                    head_stores.at[n, j],
                )
        for n, (_, layer, _, _) in enumerate(moves):
            for i in range(plan.outs // LANES):
                for j in range(width // LANES):
                    turned[n, pl.ds(j * LANES, LANES), pl.ds(i * LANES, LANES)] = buffers[
                        n, pl.ds(plan.downs + i * LANES, LANES), pl.ds(j * LANES, LANES)
                    ].T
            put(turned.at[n], targets[1].at[layer, place, :], out_stores.at[n])
        for store in storing:
            store.wait()

    hbm = pl.BlockSpec(memory_space=pltpu.HBM)
    dma = pltpu.SemaphoreType.DMA((count,))
    result = pl.pallas_call(
        body,
        out_shape=[outs[n] for n in made],
        in_specs=[hbm] * (len(arrays) + len(kept)),
        out_specs=[hbm] * len(made),
        scratch_shapes=[
            pltpu.VMEM((count, plan.piece, columns), jnp.bfloat16),
            pltpu.VMEM((count, width, plan.outs), jnp.bfloat16),
            dma, dma, dma, pltpu.SemaphoreType.DMA((count, max(WHOLE, 1))),
        ],
        input_output_aliases={len(arrays) + i: n for i, n in enumerate(kept)},
        cost_estimate=pl.CostEstimate(flops=10**7, bytes_accessed=4 * count * plan.piece * columns, transcendentals=0),
        compiler_params=pltpu.CompilerParams(vmem_limit_bytes=VMEM),
    )(*arrays, *(held[n] for n in kept))
    return dict(zip(made, result, strict=True))


def place_whole(plan, whole):
    def spots(refs, dp):
        return [(refs[0].at[layer], layer, 0, 0) for layer in range(plan.layers)]

    return place_rows(plan, [whole], spots, plan.whole, 0, {})


def place_shares(plan, shares, held):
    which = [(owner, part) for owner, arrays in shares.items() for part in arrays]
    arrays = [shares[owner][part] for owner, part in which]

    def spots(refs, dp):
        core, x, y = dp % 2, (dp // 2) % 2, dp // 4
        found = []
        for ref, ((flip_x, flip_y, flip_core), part) in zip(refs, which, strict=True):
            owner = (y + flip_y * (1 - 2 * y)) * 4 + (x + flip_x * (1 - 2 * x)) * 2 + core + flip_core * (1 - 2 * core)
            found.append((ref, owner * plan.share + part, owner, part))
        return found

    return place_rows(plan, arrays, spots, plan.cut, plan.whole, held)


def solution(mesh):
    train_stack = P(None, ("dp", "tp"), None)
    train_head = P(("dp", "tp"), None)
    fused_stack = P(None, "tp", None)
    last_stack = P(None, None, "tp")
    head_rows = P("tp", None)

    def local_sync(w_query, w_key, w_value, w_out, w_gate, w_up, w_down, w_head):
        plan = Plan(mesh.shape["tp"], mesh.shape["dp"], w_query, w_gate, w_out, w_down, w_head)
        slabs, own_0, own_1, whole = gather(plan, w_query, w_key, w_value, w_out, w_gate, w_up, w_down, w_head)

        def swap(bit, array):
            return lax.ppermute(array, "dp", [(i, i ^ bit) for i in range(plan.dp)])

        pair, along_x, along_y = (functools.partial(swap, bit) for bit in (1, 2, 4))
        hold = lax.optimization_barrier

        x_1, y_0 = along_x(own_1), along_y(own_0)
        x_0, y_1 = along_x(own_0), along_y(own_1)
        pair_own = [pair(own_0), pair(own_1)]
        qkv_block, gate_up_block = place_layers(plan, slabs)
        x_1, y_0, qkv_block, slabs = hold((x_1, y_0, qkv_block, slabs))
        diagonal_0 = along_x(y_0)
        diagonal_1 = along_y(x_1)
        pair_x_1, pair_y_0 = pair(x_1), pair(y_0)
        head_chunks = plan.ring + 1 - plan.layers
        early = head_chunks // 4
        head_block = place_head(plan, slabs, early, head_chunks - early)
        x_0, y_1, head_block, slabs, whole = hold((x_0, y_1, head_block, slabs, whole))
        pair_x_0, pair_y_1 = pair(x_0), pair(y_1)
        placed = place_whole(plan, whole)
        slabs, *placed = hold((slabs, placed[0], placed[1]))
        head_block = place_head(plan, slabs, 0, early, head_block)
        own_0, own_1, head_block = hold((own_0, own_1, head_block))
        near = {
            (0, 0, 0): {0: own_0, 1: own_1}, (0, 0, 1): dict(enumerate(pair_own)),
            (1, 0, 0): {0: x_0, 1: x_1}, (1, 0, 1): {0: pair_x_0, 1: pair_x_1},
            (0, 1, 0): {0: y_0, 1: y_1}, (0, 1, 1): {0: pair_y_0, 1: pair_y_1},
        }
        placed = place_shares(plan, near, {0: placed[0], 1: placed[1], 2: head_block})
        diagonal_0, head_block = hold((diagonal_0, placed[2]))
        pair_diagonal_0 = pair(diagonal_0)
        diagonal_1, down_block = hold((diagonal_1, placed[0]))
        pair_diagonal_1 = pair(diagonal_1)
        placed = {0: down_block, 1: placed[1], 2: head_block}
        placed = place_shares(plan, {(1, 1, 0): {0: diagonal_0, 1: diagonal_1}}, placed)
        placed = place_shares(plan, {(1, 1, 1): {0: pair_diagonal_0}}, placed)
        placed = place_shares(plan, {(1, 1, 1): {1: pair_diagonal_1}}, placed)
        down_block, o_block, head_block = placed[0], placed[1], placed[2]
        return (
            qkv_block,
            o_block,
            gate_up_block,
            jnp.swapaxes(down_block, 1, 2),
            head_block,
        )

    return jax.shard_map(
        local_sync,
        mesh=mesh,
        in_specs=(train_stack,) * 7 + (train_head,),
        out_specs=(fused_stack, last_stack, fused_stack, last_stack, head_rows),
        check_vma=False,
    )
```

```python
import functools

import jax
import jax.numpy as jnp
from jax import lax
from jax.experimental import pallas as pl
from jax.experimental.pallas import tpu as pltpu
from jax.sharding import PartitionSpec as P


MESH = pl.DeviceIdType.MESH
LANES = 128
VMEM = 67_000_000
AHEAD = 14
BUFFERS = 6
LAG = 2
SHARE_AT = 20
SLOTS = 8
COUNTED = 4
WHOLE = 3
WHOLE_AT = 2
RANKS_AT = 10
PARTS = 4
GROUP = 4


class Plan:
    def __init__(self, tp, dp, w_query, w_gate, w_out, w_down, w_head):
        self.tp, self.dp = tp, dp
        self.layers, self.rows, columns = w_query.shape
        self.part = columns // tp
        self.wide = w_gate.shape[2] // tp
        self.vocab = w_head.shape[1] // tp
        self.head_tiles = w_head.shape[1] // LANES
        self.chunk = 3 * self.part + 2 * self.wide
        self.wide_window = -(-self.wide // LANES) * LANES
        self.layer_window = 3 * self.part + 2 * self.wide_window
        self.head_chunks = -(-self.vocab // self.chunk)
        self.chunks = self.layers + self.head_chunks
        end = self.vocab - (self.head_chunks - 1) * self.chunk
        self.tail_window = -(-(end + LANES) // LANES) * LANES
        self.window_tiles = (self.head_chunks - 1) * self.chunk // LANES + self.tail_window // LANES
        self.shift = max(self.vocab * r - self.head_base(r) * LANES for r in range(tp))
        self.out_rows, self.down_rows = w_out.shape[1], w_down.shape[1]
        self.downs, self.outs = 2 * tp * self.down_rows, 2 * tp * self.out_rows
        self.piece = self.downs + self.outs
        self.share = self.layers // dp
        self.columns = w_out.shape[2]
        self.whole = WHOLE * LANES
        self.cut = self.columns - self.whole
        self.extra_first = self.vocab - self.share * WHOLE * self.piece
        self.ring = self.layers + self.extra_first // self.chunk
        self.tail = self.extra_first % self.chunk
        self.counts = -(-self.ring // COUNTED) + 1

    def wide_base(self, rank):
        return (self.wide * rank) // LANES

    def head_base(self, rank):
        base = (self.vocab * rank) // LANES
        return base - (rank // (self.tp - 1)) * (self.vocab * (self.tp - 1) // LANES + self.window_tiles - self.head_tiles)


def gather_kernel(plan, q, k, v, o, g, u, d, h, slabs, own_0, own_1, whole, stop_0, stop_1, land_d, land_o, zbuf, tbuf,
                  z_recv, z_send, local, x_recv, y_recv, a_recv, b_recv, pair_recv, send, stop_recv, share_recv,
                  share_send, land_recv, land_send, whole_recv, whole_send, whole_pair_recv, whole_pair_send,
                  keep_d, keep_o, keep_sem, packed, pack_sem):
    z, dp = lax.axis_index("tp"), lax.axis_index("dp")
    core, x, y = dp % 2, (dp // 2) % 2, dp // 4
    x_peer = y * 4 + (1 - x) * 2 + core
    y_peer = (1 - y) * 4 + x * 2 + core
    diagonal = (1 - y) * 4 + (1 - x) * 2 + core
    pair = dp + 1 - 2 * core
    rows, chunk, tail = plan.rows, plan.chunk, plan.tail
    layers, ring, last = plan.layers, plan.ring, plan.chunks - 1
    my_rows = pl.ds(pl.multiple_of(z * rows, rows), rows)

    def lanes(first_tile, width):
        return pl.ds(pl.multiple_of(first_tile * LANES, LANES), width)

    def remote(source, target, send_sem, recv_sem, **to):
        pltpu.make_async_remote_copy(source, target, send_sem, recv_sem, device_id=to, device_id_type=MESH).start()

    def wait_for(ref, sem):
        pltpu.make_async_copy(ref, ref, sem).wait()


    def z_slot(index):
        return index - layers + layers // GROUP

    def rank_at(step):
        return (z + step + core * (plan.tp - 2 * step)) % plan.tp

    def layer_pieces(first, rank):
        some, part, wide = pl.ds(first, GROUP), plan.part, plan.wide_window
        narrow = lanes(rank * (part // LANES), part)
        window = lanes(plan.wide_base(rank), wide)
        return [
            (q.at[some, :, narrow], 0, part),
            (k.at[some, :, narrow], part, part),
            (v.at[some, :, narrow], 2 * part, part),
            (g.at[some, :, window], 3 * part, wide),
            (u.at[some, :, window], 3 * part + wide, wide),
        ]

    def collect(group):
        for step in range(1, plan.tp):
            for source, column, width in layer_pieces(group * GROUP, rank_at(step)):
                target = packed.at[group, step - 1, :, :, pl.ds(column, width)]
                pltpu.make_async_copy(source, target, pack_sem.at[group]).start()
        for source, column, width in layer_pieces(group * GROUP, z):
            target = zbuf.at[pl.ds(group * GROUP, GROUP), my_rows, pl.ds(column, width)]
            pltpu.make_async_copy(source, target, z_recv.at[group]).start()

    def exchange_layers(group):
        wait_for(packed.at[group], pack_sem.at[group])
        for step in range(1, plan.tp):
            index = group * GROUP
            target = zbuf.at[pl.ds(index, GROUP), my_rows, :]
            remote(packed.at[group, step - 1], target, z_send.at[0], z_recv.at[group], tp=rank_at(step))

    def exchange_head(index, width):
        def piece(rank):
            return h.at[:, lanes(plan.head_base(rank) + (index - layers) * (chunk // LANES), width)]

        target = zbuf.at[index, my_rows, pl.ds(0, width)]
        sent = z_send.at[1 if width == chunk else 2]
        for step in range(1, plan.tp):
            remote(piece(rank_at(step)), target, sent, z_recv.at[z_slot(index)], tp=rank_at(step))
        pltpu.make_async_copy(piece(z), target, z_recv.at[z_slot(index)]).start()

    def start_exchange(index):
        @pl.when((index >= layers) & (index < last))
        def _():
            exchange_head(index, chunk)

        @pl.when(index == last)
        def _():
            exchange_head(last, plan.tail_window)

    def wait_exchange(index, width):
        wait_for(zbuf.at[index, :, pl.ds(0, width)], z_recv.at[z_slot(index)])


    def turn(slot, tile, index, source_tile):
        tbuf[slot, pl.ds(tile * LANES, LANES), :] = zbuf[index, :, pl.ds(source_tile * LANES, LANES)].T

    def store(slot, first, index, to, count):
        pltpu.make_async_copy(
            tbuf.at[slot, pl.ds(first, count), :], slabs.at[dp, index, pl.ds(to, count), :], local.at[slot]
        ).start()

    def make_layer(index, slot):
        @pl.when(index % GROUP == 0)
        def _():
            wait_for(zbuf.at[pl.ds(index, GROUP), :, pl.ds(0, plan.layer_window)], z_recv.at[index // GROUP])

        for tile in range(plan.layer_window // LANES):
            turn(slot, tile, index, tile)
        shift = plan.wide * z - plan.wide_base(z) * LANES
        narrow, wide, window = 3 * plan.part, plan.wide, plan.wide_window
        store(slot, 0, index, 0, narrow)
        store(slot, pl.multiple_of(narrow + shift, 16), index, narrow, wide)
        store(slot, pl.multiple_of(narrow + window + shift, 16), index, narrow + wide, wide)

    head_shift = plan.vocab * z - plan.head_base(z) * LANES

    def make_head(index, slot):
        @pl.when(index == layers)
        def _():
            wait_exchange(index, chunk)

        wait_exchange(index + 1, chunk)
        tiles = chunk // LANES
        for tile in range(tiles):
            turn(slot, tile, index, tile)
        for tile in range(2):
            turn(slot, tiles + tile, index + 1, tile)
        store(slot, pl.multiple_of(head_shift, 16), index, 0, chunk)

    def turn_rows(slot, first, count):
        start = first // LANES
        for tile in range(-(-(first % LANES + plan.shift + count) // LANES)):
            at = start + tile
            turn(slot, tile, layers + at // (chunk // LANES), at % (chunk // LANES))
        return pl.multiple_of(first % LANES + head_shift, 16)

    def make_tail(slot):
        wait_exchange(ring + 1, chunk)
        store(slot, turn_rows(slot, (ring - layers) * chunk, tail), ring, 0, tail)

    def make_extra():
        for index in range(ring + 2, last):
            wait_exchange(index, chunk)
        wait_exchange(last, plan.tail_window)
        blocks = plan.share * WHOLE

        def stored(n, own):
            wait_for(own.at[:, pl.ds(plan.cut, LANES)], local.at[n % 2])

        for n in range(blocks):
            own = (own_0, own_1)[n // WHOLE]
            if n >= 2:
                stored(n, own)
            at = turn_rows(n % 2, plan.extra_first + n * plan.piece, plan.piece)
            pltpu.make_async_copy(
                tbuf.at[n % 2, pl.ds(at, plan.piece), :],
                own.at[:, pl.ds(plan.cut + n % WHOLE * LANES, LANES)], local.at[n % 2],
            ).start()
        for n in range(blocks - min(2, blocks), blocks):
            stored(n, own_0)


    def slab_view(index):
        return lambda owner, first, count: slabs.at[owner, index, pl.ds(first, count), :]

    def push(part, index, recv, to):
        remote(part, part, send.at[counted(index)], recv.at[index % SLOTS], dp=to)

    def push_pair(part, index):
        remote(part, part, send.at[counted(index)], pair_recv.at[counted(index)], dp=pair)

    def counted(index):
        return index // COUNTED if index is not ring else plan.counts - 1

    def send_own(view, index, slot, count):
        own = view(dp, 0, count)
        wait_for(own, local.at[slot])
        push(own, index, x_recv, x_peer)
        push(own, index, y_recv, y_peer)
        push_pair(own, index)

    def forward(view, index, count):
        half = count // 2
        slot = index % SLOTS
        wait_for(view(x_peer, 0, count), x_recv.at[slot])
        push(view(x_peer, half, half), index, b_recv, y_peer)
        push_pair(view(x_peer, 0, count), index)
        wait_for(view(y_peer, 0, count), y_recv.at[slot])
        push(view(y_peer, 0, half), index, a_recv, x_peer)
        push_pair(view(y_peer, 0, count), index)

    def forward_diagonal(view, index, count):
        half = count // 2
        slot = index % SLOTS
        wait_for(view(diagonal, 0, half), a_recv.at[slot])
        wait_for(view(diagonal, half, half), b_recv.at[slot])
        push_pair(view(diagonal, 0, count), index)

    def finish(index, some, count):
        wait_for(slabs.at[pl.ds(0, 7), some, pl.ds(0, count), :], send.at[index])
        wait_for(slabs.at[pl.ds(0, 4), some, pl.ds(0, count), :], pair_recv.at[index])


    def pieces(source_dp, to, place):
        all_rows = plan.downs
        downs = pl.ds(pl.multiple_of(place * plan.down_rows, 8), plan.down_rows)
        outs = pl.ds(pl.multiple_of(all_rows + place * plan.out_rows, 8), plan.out_rows)
        stop_downs, stop_outs = pl.ds(0, plan.down_rows), pl.ds(plan.down_rows, plan.out_rows)
        cut, home = pl.ds(plan.whole, plan.cut), pl.ds(0, plan.cut)
        found = []
        for n, (stop, own) in enumerate(((stop_0, own_0), (stop_1, own_1))):
            layer = to * 2 + n
            found.append((d.at[layer, :, cut], stop.at[source_dp, stop_downs, :], own.at[downs, home], n))
            found.append((o.at[layer, :, cut], stop.at[source_dp, stop_outs, :], own.at[outs, home], n))
        return found

    my_rank = dp // 2
    my_place = (dp % 2) * plan.tp + z
    stays = my_rank == z

    def share_in_plane():
        for step in range(1, plan.dp):
            to = (dp + step) % plan.dp

            @pl.when(stays)
            def _(to=to):
                for part, _, final, n in pieces(dp, to, my_place):
                    remote(part, final, share_send.at[n], share_recv.at[n], dp=to)

            @pl.when(jnp.logical_not(stays))
            def _(to=to):
                for part, stop, _, n in pieces(dp, to, my_place):
                    remote(part, stop, share_send.at[n], stop_recv.at[n, dp], dp=to)

        @pl.when(stays)
        def _():
            for part, _, final, n in pieces(dp, dp, my_place):
                pltpu.make_async_copy(part, final, share_recv.at[n]).start()

    def share_to_rank(source_dp):
        rank, place = source_dp // 2, (source_dp % 2) * plan.tp + z

        @pl.when((rank != z) & (source_dp == dp))
        def _():
            for part, _, final, n in pieces(dp, dp, place):
                remote(part, final, share_send.at[n], share_recv.at[n], tp=rank)

        @pl.when((rank != z) & (source_dp != dp))
        def _():
            for n, stop in enumerate((stop_0, stop_1)):
                wait_for(stop.at[source_dp], stop_recv.at[n, source_dp])
            for _, stop, final, n in pieces(source_dp, dp, place):
                remote(stop, final, share_send.at[n], share_recv.at[n], tp=rank)


    whole_columns = pl.ds(0, plan.whole)
    keep = (keep_d, keep_o)
    mine = ((d, land_d, plan.down_rows, 0), (o, land_o, plan.out_rows, plan.downs))
    half = layers // 2

    def whole_home(n, row):
        _, _, count, first = mine[n]
        return pl.ds(pl.multiple_of(first + row * count, 8), count)

    def landing(rank, some, act):
        pl.when(rank == z)(lambda: act([whole.at[some, whole_home(n, core * plan.tp + z), :] for n in range(2)]))
        pl.when(rank != z)(lambda: act([land.at[rank, some] for _, land, _, _ in mine]))

    every = pl.ds(0, layers)

    def whole_out():
        def act(places):
            for n, (source, _, _, _) in enumerate(mine):
                for to, at in ((x_peer, 0), (y_peer, 2)):
                    remote(source.at[:, :, whole_columns], places[n], land_send.at[n], land_recv.at[at + n], dp=to)

        landing(my_rank, every, act)

        @pl.when(stays)
        def _():
            for n, (source, _, _, _) in enumerate(mine):
                pltpu.make_async_copy(source.at[:, :, whole_columns], keep[n], keep_sem.at[n]).start()

    def whole_keep():
        @pl.when(stays)
        def _():
            for n in range(2):
                wait_for(keep[n], keep_sem.at[n])
                target = whole.at[:, whole_home(n, core * plan.tp + z), :]
                pltpu.make_async_copy(keep[n], target, keep_sem.at[2 + n]).start()

    def whole_forward():
        for owner, at, first, to, then in ((x_peer, 0, half, y_peer, 6), (y_peer, 2, 0, x_peer, 4)):
            def arrived(places, at=at):
                for n in range(2):
                    wait_for(places[n], land_recv.at[at + n])

            def on(places, to=to, then=then):
                for n in range(2):
                    remote(places[n], places[n], land_send.at[n], land_recv.at[then + n], dp=to)

            landing(owner // 2, every, arrived)
            landing(owner // 2, pl.ds(first, half), on)

    def whole_arrive():
        for first, at in ((0, 4), (half, 6)):
            def arrived(places, at=at):
                for n in range(2):
                    wait_for(places[n], land_recv.at[at + n])

            landing(diagonal // 2, pl.ds(first, half), arrived)

    def whole_to_rank(shift, part):
        rank = (z + shift + core * (plan.tp - 2 * shift)) % plan.tp
        some = pl.ds(part * (layers // PARTS), layers // PARTS)

        def move(sources):
            for n, source in enumerate(sources):
                target = whole.at[some, whole_home(n, core * plan.tp + z), :]
                remote(source, target, whole_send.at[n], whole_recv.at[n], tp=rank)

        pl.when(rank == my_rank)(lambda: move([source.at[some, :, whole_columns] for source, _, _, _ in mine]))
        pl.when(rank != my_rank)(lambda: move([land.at[rank, some] for _, land, _, _ in mine]))

    def whole_rows(which):
        return [
            whole.at[:, pl.ds(pl.multiple_of(first + which * plan.tp * count, 8), plan.tp * count), :]
            for _, _, count, first in mine
        ]

    def whole_to_pair():
        for n, part in enumerate(whole_rows(core)):
            away = pl.ds(0, (plan.tp - 1) * mine[n][2])
            wait_for(whole.at[:, away, :], whole_recv.at[n])

            @pl.when(stays)
            def _(n=n):
                wait_for(keep[n], keep_sem.at[2 + n])

            remote(part, part, whole_pair_send.at[n], whole_pair_recv.at[n], dp=pair)

    def whole_finish():
        for n, (_, land, count, first) in enumerate(mine):
            wait_for(land.at[pl.ds(0, 3)], land_send.at[n])
            wait_for(whole.at[:, pl.ds(first, (plan.tp - 1) * count), :], whole_send.at[n])
            wait_for(whole_rows(core)[n], whole_pair_send.at[n])
            wait_for(whole_rows(1 - core)[n], whole_pair_recv.at[n])

    groups = layers // GROUP
    barrier = pltpu.get_barrier_semaphore()
    peers = [{"tp": (z + step) % plan.tp} for step in range(1, plan.tp)]
    peers += [{"dp": (dp + step) % plan.dp} for step in range(1, plan.dp)]
    for peer in peers:
        pl.semaphore_signal(barrier, inc=1, device_id=peer, device_id_type=MESH)
    for group in range(groups):
        collect(group)
    pl.semaphore_wait(barrier, len(peers))

    whole_out()
    exchange_layers(0)
    share_in_plane()
    for group in range(1, groups):
        exchange_layers(group)
    for index in range(layers, AHEAD):
        start_exchange(index)

    def step(index, _):
        slot = index % 2

        @pl.when(index + AHEAD < plan.chunks)
        def _():
            start_exchange(index + AHEAD)

        @pl.when((index >= SHARE_AT) & (index < SHARE_AT + plan.dp))
        def _():
            share_to_rank(index - SHARE_AT)

        @pl.when(index == WHOLE_AT)
        def _():
            whole_keep()
            whole_forward()

        @pl.when(index == WHOLE_AT + 3)
        def _():
            whole_arrive()

        @pl.when((index >= RANKS_AT) & (index < RANKS_AT + (plan.tp - 1) * PARTS))
        def _():
            whole_to_rank((index - RANKS_AT) % (plan.tp - 1) + 1, (index - RANKS_AT) // (plan.tp - 1))

        @pl.when(index < layers)
        def _():
            make_layer(index, slot)

        @pl.when(index >= layers)
        def _():
            make_head(index, slot)

        send_own(slab_view(index), index, slot, chunk)

        @pl.when(index >= LAG)
        def _():
            forward(slab_view(index - LAG), index - LAG, chunk)

        @pl.when(index >= 2 * LAG)
        def _():
            forward_diagonal(slab_view(index - 2 * LAG), index - 2 * LAG, chunk)

        return 0

    lax.fori_loop(0, ring, step, 0)

    make_tail(ring % 2)
    send_own(slab_view(ring), ring, ring % 2, tail)
    make_extra()
    for index in range(ring - LAG, ring):
        forward(slab_view(index), index, chunk)
        if index == ring - LAG:
            whole_to_pair()
    forward(slab_view(ring), ring, tail)
    for index in range(ring - 2 * LAG, ring):
        forward_diagonal(slab_view(index), index, chunk)
        if index == ring - 2:
            sent = pl.ds(0, (plan.tp - 1) * rows)
            wait_for(packed, z_send.at[0])
            wait_for(zbuf.at[pl.ds(layers, last - layers), sent, pl.ds(0, chunk)], z_send.at[1])
            wait_for(zbuf.at[last, sent, pl.ds(0, plan.tail_window)], z_send.at[2])
            whole_finish()
            for n, own in enumerate((own_0, own_1)):
                wait_for(own.at[:, pl.ds(0, plan.cut)], share_recv.at[n])
                for parts in (8, 5):
                    gone = pl.ds(0, parts * (plan.down_rows + plan.out_rows))
                    wait_for(own.at[gone, pl.ds(0, plan.cut)], share_send.at[n])
            for index in range((ring - LAG) // COUNTED):
                finish(index, pl.ds(index * COUNTED, COUNTED), chunk)
    forward_diagonal(slab_view(ring), ring, tail)
    for index in range((ring - LAG) // COUNTED, plan.counts - 1):
        first = index * COUNTED
        finish(index, pl.ds(first, min(COUNTED, ring - first)), chunk)
    finish(plan.counts - 1, pl.ds(ring, 1), tail)


def gather(plan, *args):
    dma = pltpu.SemaphoreType.DMA
    groups = plan.layers // GROUP
    share_rows = plan.down_rows + plan.out_rows
    hbm = pl.BlockSpec(memory_space=pltpu.HBM)
    shapes = [(plan.dp, plan.ring + 1, plan.chunk, LANES), (plan.piece, plan.columns), (plan.piece, plan.columns)]
    shapes += [(plan.layers, plan.piece, plan.whole)] + [(plan.dp, share_rows, plan.cut)] * 2
    shapes += [(plan.tp, plan.layers, count, plan.whole) for count in (plan.down_rows, plan.out_rows)]
    return pl.pallas_call(
        functools.partial(gather_kernel, plan),
        out_shape=[jax.ShapeDtypeStruct(shape, jnp.bfloat16) for shape in shapes],
        in_specs=[hbm] * 8,
        out_specs=[hbm] * len(shapes),
        scratch_shapes=[
            pltpu.VMEM((plan.chunks, plan.tp * plan.rows, plan.layer_window), jnp.bfloat16),
            pltpu.VMEM((2, plan.chunk + 2 * LANES, LANES), jnp.bfloat16),
            dma((groups + plan.head_chunks,)), dma((3,)), dma((2,)),
            dma((SLOTS,)), dma((SLOTS,)), dma((SLOTS,)), dma((SLOTS,)), dma((plan.counts,)), dma((plan.counts,)),
            dma((2, plan.dp)), dma((2,)), dma((2,)),
            dma((8,)), dma((2,)), dma((2,)), dma((2,)), dma((2,)), dma((2,)),
            pltpu.VMEM((plan.layers, plan.down_rows, plan.whole), jnp.bfloat16),
            pltpu.VMEM((plan.layers, plan.out_rows, plan.whole), jnp.bfloat16),
            dma((4,)),
            pltpu.VMEM((plan.layers // GROUP, plan.tp - 1, GROUP, plan.rows, plan.layer_window), jnp.bfloat16),
            dma((plan.layers // GROUP,)),
        ],
        compiler_params=pltpu.CompilerParams(collective_id=0, has_side_effects=True),
        name="gather",
    )(*args)[:4]


def place_slabs(plan, slabs, first, count, shapes, store, held=()):
    hbm = pl.BlockSpec(memory_space=pltpu.HBM)
    depth = min(BUFFERS, count)
    ahead = depth // 2

    def body(slab, *refs):
        outs, (buffers, loads, stores) = refs[len(held):-3], refs[-3:]

        def each_size(chunk, act):
            if first + count > plan.ring:
                pl.when(chunk < plan.ring)(lambda: act(plan.chunk))
                pl.when(chunk == plan.ring)(lambda: act(plan.tail))
            else:
                act(plan.chunk)

        def load(i, rows):
            for owner in range(plan.dp):
                pltpu.make_async_copy(
                    slab.at[owner, first + i, pl.ds(0, rows), :],
                    buffers.at[i % depth, pl.ds(0, rows), pl.ds(owner * LANES, LANES)],
                    loads.at[i % depth],
                ).start()

        def wait(i, rows, sem):
            buffer = buffers.at[i % depth, pl.ds(0, rows), :]
            pltpu.make_async_copy(buffer, buffer, sem.at[i % depth]).wait()

        def write(i, rows):
            wait(i, rows, loads)
            for source, target in store(buffers.at[i % depth], first + i, rows, outs):
                pltpu.make_async_copy(source, target, stores.at[i % depth]).start()

        def step(i, _):
            @pl.when(i >= depth)
            def _():
                each_size(first + i - depth, lambda rows: wait(i - depth, rows, stores))

            @pl.when(i < count)
            def _():
                each_size(first + i, lambda rows: load(i, rows))

            @pl.when((i >= ahead) & (i < count + ahead))
            def _():
                each_size(first + i - ahead, lambda rows: write(i - ahead, rows))

            return 0

        lax.fori_loop(0, count + depth, step, 0)

    outs = [jax.ShapeDtypeStruct(shape, jnp.bfloat16) for shape in shapes]
    return pl.pallas_call(
        body,
        in_specs=[hbm] * (1 + len(held)),
        out_specs=[hbm] * len(outs),
        out_shape=outs,
        scratch_shapes=[
            pltpu.VMEM((depth, plan.chunk, plan.dp * LANES), jnp.bfloat16),
            pltpu.SemaphoreType.DMA((depth,)),
            pltpu.SemaphoreType.DMA((depth,)),
        ],
        input_output_aliases={1 + n: n for n in range(len(held))},
        cost_estimate=pl.CostEstimate(
            flops=10**7, bytes_accessed=4 * count * plan.chunk * plan.dp * LANES, transcendentals=0
        ),
        compiler_params=pltpu.CompilerParams(vmem_limit_bytes=VMEM),
    )(slabs, *held)


def place_layers(plan, slabs):
    narrow, wide, width = 3 * plan.part, 2 * plan.wide, plan.dp * LANES

    def store(buffer, chunk, rows, outs):
        return [
            (buffer.at[pl.ds(0, narrow), :], outs[0].at[chunk]),
            (buffer.at[pl.ds(narrow, wide), :], outs[1].at[chunk]),
        ]

    shapes = [(plan.layers, narrow, width), (plan.layers, wide, width)]
    return place_slabs(plan, slabs, 0, plan.layers, shapes, store)


def place_head(plan, slabs, first, count, *held):
    def store(buffer, chunk, rows, outs):
        at = pl.multiple_of((chunk - plan.layers) * plan.chunk, 16)
        return [(buffer.at[pl.ds(0, rows), :], outs[0].at[pl.ds(at, rows), :])]

    shapes = [(plan.vocab, plan.dp * LANES)]
    return place_slabs(plan, slabs, plan.layers + first, count, shapes, store, held)[0]


def place_rows(plan, arrays, spots, width, column, held):
    count = len(spots([array for array in arrays], 0))
    columns = arrays[0].shape[-1]
    outs = [
        jax.ShapeDtypeStruct((plan.layers, plan.downs, plan.columns), jnp.bfloat16),
        jax.ShapeDtypeStruct((plan.layers, plan.columns, plan.outs), jnp.bfloat16),
        jax.ShapeDtypeStruct((plan.vocab, plan.dp * LANES), jnp.bfloat16),
    ]
    with_head = columns > width
    kept = [n for n in range(3) if n in held]
    made = [n for n in range(3 if with_head else 2)]

    def body(*refs):
        targets = dict(zip(made, refs[len(arrays) + len(kept):-6], strict=True))
        buffers, turned, loads, stores, out_stores, head_stores = refs[-6:]
        moves = spots(refs[: len(arrays)], lax.axis_index("dp"))
        loading = [pltpu.make_async_copy(move[0], buffers.at[n], loads.at[n]) for n, move in enumerate(moves)]
        storing = []
        for load in loading:
            load.start()

        def put(source, target, sem):
            storing.append(pltpu.make_async_copy(source, target, sem))
            storing[-1].start()

        place = pl.ds(column, width)
        for n, (load, (_, layer, owner, part)) in enumerate(zip(loading, moves, strict=True)):
            load.wait()
            put(buffers.at[n, pl.ds(0, plan.downs), pl.ds(0, width)], targets[0].at[layer, :, place], stores.at[n])
            for j in range((columns - width) // LANES):
                row = plan.extra_first + (part * WHOLE + j) * plan.piece
                put(
                    buffers.at[n, :, pl.ds(width + j * LANES, LANES)],
                    targets[2].at[pl.ds(row, plan.piece), pl.ds(pl.multiple_of(owner * LANES, LANES), LANES)],
                    head_stores.at[n, j],
                )
        for n, (_, layer, _, _) in enumerate(moves):
            for i in range(plan.outs // LANES):
                for j in range(width // LANES):
                    turned[n, pl.ds(j * LANES, LANES), pl.ds(i * LANES, LANES)] = buffers[
                        n, pl.ds(plan.downs + i * LANES, LANES), pl.ds(j * LANES, LANES)
                    ].T
            put(turned.at[n], targets[1].at[layer, place, :], out_stores.at[n])
        for store in storing:
            store.wait()

    hbm = pl.BlockSpec(memory_space=pltpu.HBM)
    dma = pltpu.SemaphoreType.DMA((count,))
    result = pl.pallas_call(
        body,
        out_shape=[outs[n] for n in made],
        in_specs=[hbm] * (len(arrays) + len(kept)),
        out_specs=[hbm] * len(made),
        scratch_shapes=[
            pltpu.VMEM((count, plan.piece, columns), jnp.bfloat16),
            pltpu.VMEM((count, width, plan.outs), jnp.bfloat16),
            dma, dma, dma, pltpu.SemaphoreType.DMA((count, max(WHOLE, 1))),
        ],
        input_output_aliases={len(arrays) + i: n for i, n in enumerate(kept)},
        cost_estimate=pl.CostEstimate(flops=10**7, bytes_accessed=4 * count * plan.piece * columns, transcendentals=0),
        compiler_params=pltpu.CompilerParams(vmem_limit_bytes=VMEM),
    )(*arrays, *(held[n] for n in kept))
    return dict(zip(made, result, strict=True))


def place_whole(plan, whole):
    def spots(refs, dp):
        return [(refs[0].at[layer], layer, 0, 0) for layer in range(plan.layers)]

    return place_rows(plan, [whole], spots, plan.whole, 0, {})


def place_shares(plan, shares, held):
    which = [(owner, part) for owner, arrays in shares.items() for part in arrays]
    arrays = [shares[owner][part] for owner, part in which]

    def spots(refs, dp):
        core, x, y = dp % 2, (dp // 2) % 2, dp // 4
        found = []
        for ref, ((flip_x, flip_y, flip_core), part) in zip(refs, which, strict=True):
            owner = (y + flip_y * (1 - 2 * y)) * 4 + (x + flip_x * (1 - 2 * x)) * 2 + core + flip_core * (1 - 2 * core)
            found.append((ref, owner * plan.share + part, owner, part))
        return found

    return place_rows(plan, arrays, spots, plan.cut, plan.whole, held)


def solution(mesh):
    train_stack = P(None, ("dp", "tp"), None)
    train_head = P(("dp", "tp"), None)
    fused_stack = P(None, "tp", None)
    last_stack = P(None, None, "tp")
    head_rows = P("tp", None)

    def local_sync(w_query, w_key, w_value, w_out, w_gate, w_up, w_down, w_head):
        plan = Plan(mesh.shape["tp"], mesh.shape["dp"], w_query, w_gate, w_out, w_down, w_head)
        slabs, own_0, own_1, whole = gather(plan, w_query, w_key, w_value, w_out, w_gate, w_up, w_down, w_head)

        def swap(bit, array):
            return lax.ppermute(array, "dp", [(i, i ^ bit) for i in range(plan.dp)])

        pair, along_x, along_y = (functools.partial(swap, bit) for bit in (1, 2, 4))
        hold = lax.optimization_barrier

        x_1, y_0 = along_x(own_1), along_y(own_0)
        x_0, y_1 = along_x(own_0), along_y(own_1)
        pair_own = [pair(own_0), pair(own_1)]
        qkv_block, gate_up_block = place_layers(plan, slabs)
        x_1, y_0, qkv_block, slabs = hold((x_1, y_0, qkv_block, slabs))
        diagonal_0 = along_x(y_0)
        diagonal_1 = along_y(x_1)
        pair_x_1, pair_y_0 = pair(x_1), pair(y_0)
        head_chunks = plan.ring + 1 - plan.layers
        early = head_chunks // 4
        head_block = place_head(plan, slabs, early, head_chunks - early)
        x_0, y_1, head_block, slabs, whole = hold((x_0, y_1, head_block, slabs, whole))
        pair_x_0, pair_y_1 = pair(x_0), pair(y_1)
        placed = place_whole(plan, whole)
        slabs, *placed = hold((slabs, placed[0], placed[1]))
        head_block = place_head(plan, slabs, 0, early, head_block)
        own_0, own_1, head_block = hold((own_0, own_1, head_block))
        near = {
            (0, 0, 0): {0: own_0, 1: own_1}, (0, 0, 1): dict(enumerate(pair_own)),
            (1, 0, 0): {0: x_0, 1: x_1}, (1, 0, 1): {0: pair_x_0, 1: pair_x_1},
            (0, 1, 0): {0: y_0, 1: y_1}, (0, 1, 1): {0: pair_y_0, 1: pair_y_1},
        }
        placed = place_shares(plan, near, {0: placed[0], 1: placed[1], 2: head_block})
        diagonal_0, head_block = hold((diagonal_0, placed[2]))
        pair_diagonal_0 = pair(diagonal_0)
        diagonal_1, down_block = hold((diagonal_1, placed[0]))
        pair_diagonal_1 = pair(diagonal_1)
        placed = {0: down_block, 1: placed[1], 2: head_block}
        placed = place_shares(plan, {(1, 1, 0): {0: diagonal_0, 1: diagonal_1}}, placed)
        placed = place_shares(plan, {(1, 1, 1): {0: pair_diagonal_0}}, placed)
        placed = place_shares(plan, {(1, 1, 1): {1: pair_diagonal_1}}, placed)
        down_block, o_block, head_block = placed[0], placed[1], placed[2]
        return (
            qkv_block,
            o_block,
            gate_up_block,
            jnp.swapaxes(down_block, 1, 2),
            head_block,
        )

    return jax.shard_map(
        local_sync,
        mesh=mesh,
        in_specs=(train_stack,) * 7 + (train_head,),
        out_specs=(fused_stack, last_stack, fused_stack, last_stack, head_rows),
        check_vma=False,
    )
```

```python
import functools

import jax
import jax.numpy as jnp
from jax import lax
from jax.experimental import pallas as pl
from jax.experimental.pallas import tpu as pltpu
from jax.sharding import PartitionSpec as P


MESH = pl.DeviceIdType.MESH
LANES = 128
VMEM = 67_000_000
AHEAD = 14
BUFFERS = 6
LAG = 1
SHARE_AT = 20
SLOTS = 8
COUNTED = 4
WHOLE = 3
WHOLE_AT = 2
RANKS_AT = 10
PARTS = 4
GROUP = 4


class Plan:
    def __init__(self, tp, dp, w_query, w_gate, w_out, w_down, w_head):
        self.tp, self.dp = tp, dp
        self.layers, self.rows, columns = w_query.shape
        self.part = columns // tp
        self.wide = w_gate.shape[2] // tp
        self.vocab = w_head.shape[1] // tp
        self.head_tiles = w_head.shape[1] // LANES
        self.chunk = 3 * self.part + 2 * self.wide
        self.wide_window = -(-self.wide // LANES) * LANES
        self.layer_window = 3 * self.part + 2 * self.wide_window
        self.head_chunks = -(-self.vocab // self.chunk)
        self.chunks = self.layers + self.head_chunks
        end = self.vocab - (self.head_chunks - 1) * self.chunk
        self.tail_window = -(-(end + LANES) // LANES) * LANES
        self.window_tiles = (self.head_chunks - 1) * self.chunk // LANES + self.tail_window // LANES
        self.shift = max(self.vocab * r - self.head_base(r) * LANES for r in range(tp))
        self.out_rows, self.down_rows = w_out.shape[1], w_down.shape[1]
        self.downs, self.outs = 2 * tp * self.down_rows, 2 * tp * self.out_rows
        self.piece = self.downs + self.outs
        self.share = self.layers // dp
        self.columns = w_out.shape[2]
        self.whole = WHOLE * LANES
        self.cut = self.columns - self.whole
        self.extra_first = self.vocab - self.share * WHOLE * self.piece
        self.ring = self.layers + self.extra_first // self.chunk
        self.tail = self.extra_first % self.chunk
        self.counts = -(-self.ring // COUNTED) + 1

    def wide_base(self, rank):
        return (self.wide * rank) // LANES

    def head_base(self, rank):
        base = (self.vocab * rank) // LANES
        return base - (rank // (self.tp - 1)) * (self.vocab * (self.tp - 1) // LANES + self.window_tiles - self.head_tiles)


def gather_kernel(plan, q, k, v, o, g, u, d, h, slabs, own_0, own_1, whole, stop_0, stop_1, land_d, land_o, zbuf, tbuf,
                  z_recv, z_send, local, x_recv, y_recv, a_recv, b_recv, pair_recv, send, stop_recv, share_recv,
                  share_send, land_recv, land_send, whole_recv, whole_send, whole_pair_recv, whole_pair_send,
                  keep_d, keep_o, keep_sem, packed, pack_sem):
    z, dp = lax.axis_index("tp"), lax.axis_index("dp")
    core, x, y = dp % 2, (dp // 2) % 2, dp // 4
    x_peer = y * 4 + (1 - x) * 2 + core
    y_peer = (1 - y) * 4 + x * 2 + core
    diagonal = (1 - y) * 4 + (1 - x) * 2 + core
    pair = dp + 1 - 2 * core
    rows, chunk, tail = plan.rows, plan.chunk, plan.tail
    layers, ring, last = plan.layers, plan.ring, plan.chunks - 1
    my_rows = pl.ds(pl.multiple_of(z * rows, rows), rows)

    def lanes(first_tile, width):
        return pl.ds(pl.multiple_of(first_tile * LANES, LANES), width)

    def remote(source, target, send_sem, recv_sem, **to):
        pltpu.make_async_remote_copy(source, target, send_sem, recv_sem, device_id=to, device_id_type=MESH).start()

    def wait_for(ref, sem):
        pltpu.make_async_copy(ref, ref, sem).wait()


    def z_slot(index):
        return index - layers + layers // GROUP

    def rank_at(step):
        return (z + step + core * (plan.tp - 2 * step)) % plan.tp

    def layer_pieces(first, rank):
        some, part, wide = pl.ds(first, GROUP), plan.part, plan.wide_window
        narrow = lanes(rank * (part // LANES), part)
        window = lanes(plan.wide_base(rank), wide)
        return [
            (q.at[some, :, narrow], 0, part),
            (k.at[some, :, narrow], part, part),
            (v.at[some, :, narrow], 2 * part, part),
            (g.at[some, :, window], 3 * part, wide),
            (u.at[some, :, window], 3 * part + wide, wide),
        ]

    def collect(group):
        for step in range(1, plan.tp):
            for source, column, width in layer_pieces(group * GROUP, rank_at(step)):
                target = packed.at[group, step - 1, :, :, pl.ds(column, width)]
                pltpu.make_async_copy(source, target, pack_sem.at[group]).start()
        for source, column, width in layer_pieces(group * GROUP, z):
            target = zbuf.at[pl.ds(group * GROUP, GROUP), my_rows, pl.ds(column, width)]
            pltpu.make_async_copy(source, target, z_recv.at[group]).start()

    def exchange_layers(group):
        wait_for(packed.at[group], pack_sem.at[group])
        for step in range(1, plan.tp):
            index = group * GROUP
            target = zbuf.at[pl.ds(index, GROUP), my_rows, :]
            remote(packed.at[group, step - 1], target, z_send.at[0], z_recv.at[group], tp=rank_at(step))

    def exchange_head(index, width):
        def piece(rank):
            return h.at[:, lanes(plan.head_base(rank) + (index - layers) * (chunk // LANES), width)]

        target = zbuf.at[index, my_rows, pl.ds(0, width)]
        sent = z_send.at[1 if width == chunk else 2]
        for step in range(1, plan.tp):
            remote(piece(rank_at(step)), target, sent, z_recv.at[z_slot(index)], tp=rank_at(step))
        pltpu.make_async_copy(piece(z), target, z_recv.at[z_slot(index)]).start()

    def start_exchange(index):
        @pl.when((index >= layers) & (index < last))
        def _():
            exchange_head(index, chunk)

        @pl.when(index == last)
        def _():
            exchange_head(last, plan.tail_window)

    def wait_exchange(index, width):
        wait_for(zbuf.at[index, :, pl.ds(0, width)], z_recv.at[z_slot(index)])


    def turn(slot, tile, index, source_tile):
        tbuf[slot, pl.ds(tile * LANES, LANES), :] = zbuf[index, :, pl.ds(source_tile * LANES, LANES)].T

    def store(slot, first, index, to, count):
        pltpu.make_async_copy(
            tbuf.at[slot, pl.ds(first, count), :], slabs.at[dp, index, pl.ds(to, count), :], local.at[slot]
        ).start()

    def make_layer(index, slot):
        @pl.when(index % GROUP == 0)
        def _():
            wait_for(zbuf.at[pl.ds(index, GROUP), :, pl.ds(0, plan.layer_window)], z_recv.at[index // GROUP])

        for tile in range(plan.layer_window // LANES):
            turn(slot, tile, index, tile)
        shift = plan.wide * z - plan.wide_base(z) * LANES
        narrow, wide, window = 3 * plan.part, plan.wide, plan.wide_window
        store(slot, 0, index, 0, narrow)
        store(slot, pl.multiple_of(narrow + shift, 16), index, narrow, wide)
        store(slot, pl.multiple_of(narrow + window + shift, 16), index, narrow + wide, wide)

    head_shift = plan.vocab * z - plan.head_base(z) * LANES

    def make_head(index, slot):
        @pl.when(index == layers)
        def _():
            wait_exchange(index, chunk)

        wait_exchange(index + 1, chunk)
        tiles = chunk // LANES
        for tile in range(tiles):
            turn(slot, tile, index, tile)
        for tile in range(2):
            turn(slot, tiles + tile, index + 1, tile)
        store(slot, pl.multiple_of(head_shift, 16), index, 0, chunk)

    def turn_rows(slot, first, count):
        start = first // LANES
        for tile in range(-(-(first % LANES + plan.shift + count) // LANES)):
            at = start + tile
            turn(slot, tile, layers + at // (chunk // LANES), at % (chunk // LANES))
        return pl.multiple_of(first % LANES + head_shift, 16)

    def make_tail(slot):
        wait_exchange(ring + 1, chunk)
        store(slot, turn_rows(slot, (ring - layers) * chunk, tail), ring, 0, tail)

    def make_extra():
        for index in range(ring + 2, last):
            wait_exchange(index, chunk)
        wait_exchange(last, plan.tail_window)
        blocks = plan.share * WHOLE

        def stored(n, own):
            wait_for(own.at[:, pl.ds(plan.cut, LANES)], local.at[n % 2])

        for n in range(blocks):
            own = (own_0, own_1)[n // WHOLE]
            if n >= 2:
                stored(n, own)
            at = turn_rows(n % 2, plan.extra_first + n * plan.piece, plan.piece)
            pltpu.make_async_copy(
                tbuf.at[n % 2, pl.ds(at, plan.piece), :],
                own.at[:, pl.ds(plan.cut + n % WHOLE * LANES, LANES)], local.at[n % 2],
            ).start()
        for n in range(blocks - min(2, blocks), blocks):
            stored(n, own_0)


    def slab_view(index):
        return lambda owner, first, count: slabs.at[owner, index, pl.ds(first, count), :]

    def push(part, index, recv, to):
        remote(part, part, send.at[counted(index)], recv.at[index % SLOTS], dp=to)

    def push_pair(part, index):
        remote(part, part, send.at[counted(index)], pair_recv.at[counted(index)], dp=pair)

    def counted(index):
        return plan.counts - 1 if index is ring else index // COUNTED

    def send_own(view, index, slot, count):
        own = view(dp, 0, count)
        wait_for(own, local.at[slot])
        push(own, index, x_recv, x_peer)
        push(own, index, y_recv, y_peer)
        push_pair(own, index)

    def forward(view, index, count):
        half = count // 2
        slot = index % SLOTS
        wait_for(view(x_peer, 0, count), x_recv.at[slot])
        push(view(x_peer, half, half), index, b_recv, y_peer)
        push_pair(view(x_peer, 0, count), index)
        wait_for(view(y_peer, 0, count), y_recv.at[slot])
        push(view(y_peer, 0, half), index, a_recv, x_peer)
        push_pair(view(y_peer, 0, count), index)

    def forward_diagonal(view, index, count):
        half = count // 2
        slot = index % SLOTS
        wait_for(view(diagonal, 0, half), a_recv.at[slot])
        wait_for(view(diagonal, half, half), b_recv.at[slot])
        push_pair(view(diagonal, 0, count), index)

    def finish(index, some, count):
        wait_for(slabs.at[pl.ds(0, 7), some, pl.ds(0, count), :], send.at[index])
        wait_for(slabs.at[pl.ds(0, 4), some, pl.ds(0, count), :], pair_recv.at[index])


    def pieces(source_dp, to, place):
        all_rows = plan.downs
        downs = pl.ds(pl.multiple_of(place * plan.down_rows, 8), plan.down_rows)
        outs = pl.ds(pl.multiple_of(all_rows + place * plan.out_rows, 8), plan.out_rows)
        stop_downs, stop_outs = pl.ds(0, plan.down_rows), pl.ds(plan.down_rows, plan.out_rows)
        cut, home = pl.ds(plan.whole, plan.cut), pl.ds(0, plan.cut)
        found = []
        for n, (stop, own) in enumerate(((stop_0, own_0), (stop_1, own_1))):
            layer = to * 2 + n
            found.append((d.at[layer, :, cut], stop.at[source_dp, stop_downs, :], own.at[downs, home], n))
            found.append((o.at[layer, :, cut], stop.at[source_dp, stop_outs, :], own.at[outs, home], n))
        return found

    my_rank = dp // 2
    my_place = (dp % 2) * plan.tp + z
    stays = my_rank == z

    def share_in_plane():
        for step in range(1, plan.dp):
            to = (dp + step) % plan.dp

            @pl.when(stays)
            def _(to=to):
                for part, _, final, n in pieces(dp, to, my_place):
                    remote(part, final, share_send.at[n], share_recv.at[n], dp=to)

            @pl.when(jnp.logical_not(stays))
            def _(to=to):
                for part, stop, _, n in pieces(dp, to, my_place):
                    remote(part, stop, share_send.at[n], stop_recv.at[n, dp], dp=to)

        @pl.when(stays)
        def _():
            for part, _, final, n in pieces(dp, dp, my_place):
                pltpu.make_async_copy(part, final, share_recv.at[n]).start()

    def share_to_rank(source_dp):
        rank, place = source_dp // 2, (source_dp % 2) * plan.tp + z

        @pl.when((rank != z) & (source_dp == dp))
        def _():
            for part, _, final, n in pieces(dp, dp, place):
                remote(part, final, share_send.at[n], share_recv.at[n], tp=rank)

        @pl.when((rank != z) & (source_dp != dp))
        def _():
            for n, stop in enumerate((stop_0, stop_1)):
                wait_for(stop.at[source_dp], stop_recv.at[n, source_dp])
            for _, stop, final, n in pieces(source_dp, dp, place):
                remote(stop, final, share_send.at[n], share_recv.at[n], tp=rank)


    whole_columns = pl.ds(0, plan.whole)
    keep = (keep_d, keep_o)
    mine = ((d, land_d, plan.down_rows, 0), (o, land_o, plan.out_rows, plan.downs))
    half = layers // 2

    def whole_home(n, row):
        _, _, count, first = mine[n]
        return pl.ds(pl.multiple_of(first + row * count, 8), count)

    def landing(rank, some, act):
        pl.when(rank == z)(lambda: act([whole.at[some, whole_home(n, core * plan.tp + z), :] for n in range(2)]))
        pl.when(rank != z)(lambda: act([land.at[rank, some] for _, land, _, _ in mine]))

    every = pl.ds(0, layers)

    def whole_out():
        def act(places):
            for n, (source, _, _, _) in enumerate(mine):
                for to, at in ((x_peer, 0), (y_peer, 2)):
                    remote(source.at[:, :, whole_columns], places[n], land_send.at[n], land_recv.at[at + n], dp=to)

        landing(my_rank, every, act)

        @pl.when(stays)
        def _():
            for n, (source, _, _, _) in enumerate(mine):
                pltpu.make_async_copy(source.at[:, :, whole_columns], keep[n], keep_sem.at[n]).start()

    def whole_keep():
        @pl.when(stays)
        def _():
            for n in range(2):
                wait_for(keep[n], keep_sem.at[n])
                target = whole.at[:, whole_home(n, core * plan.tp + z), :]
                pltpu.make_async_copy(keep[n], target, keep_sem.at[2 + n]).start()

    def whole_forward():
        for owner, at, first, to, then in ((x_peer, 0, half, y_peer, 6), (y_peer, 2, 0, x_peer, 4)):
            def arrived(places, at=at):
                for n in range(2):
                    wait_for(places[n], land_recv.at[at + n])

            def on(places, to=to, then=then):
                for n in range(2):
                    remote(places[n], places[n], land_send.at[n], land_recv.at[then + n], dp=to)

            landing(owner // 2, every, arrived)
            landing(owner // 2, pl.ds(first, half), on)

    def whole_arrive():
        for first, at in ((0, 4), (half, 6)):
            def arrived(places, at=at):
                for n in range(2):
                    wait_for(places[n], land_recv.at[at + n])

            landing(diagonal // 2, pl.ds(first, half), arrived)

    def whole_to_rank(shift, part):
        rank = (z + shift + core * (plan.tp - 2 * shift)) % plan.tp
        some = pl.ds(part * (layers // PARTS), layers // PARTS)

        def move(sources):
            for n, source in enumerate(sources):
                target = whole.at[some, whole_home(n, core * plan.tp + z), :]
                remote(source, target, whole_send.at[n], whole_recv.at[n], tp=rank)

        pl.when(rank == my_rank)(lambda: move([source.at[some, :, whole_columns] for source, _, _, _ in mine]))
        pl.when(rank != my_rank)(lambda: move([land.at[rank, some] for _, land, _, _ in mine]))

    def whole_rows(which):
        return [
            whole.at[:, pl.ds(pl.multiple_of(first + which * plan.tp * count, 8), plan.tp * count), :]
            for _, _, count, first in mine
        ]

    def whole_to_pair():
        for n, part in enumerate(whole_rows(core)):
            away = pl.ds(0, (plan.tp - 1) * mine[n][2])
            wait_for(whole.at[:, away, :], whole_recv.at[n])

            @pl.when(stays)
            def _(n=n):
                wait_for(keep[n], keep_sem.at[2 + n])

            remote(part, part, whole_pair_send.at[n], whole_pair_recv.at[n], dp=pair)

    def whole_finish():
        for n, (_, land, count, first) in enumerate(mine):
            wait_for(land.at[pl.ds(0, 3)], land_send.at[n])
            wait_for(whole.at[:, pl.ds(first, (plan.tp - 1) * count), :], whole_send.at[n])
            wait_for(whole_rows(core)[n], whole_pair_send.at[n])
            wait_for(whole_rows(1 - core)[n], whole_pair_recv.at[n])

    groups = layers // GROUP
    barrier = pltpu.get_barrier_semaphore()
    peers = [{"tp": (z + step) % plan.tp} for step in range(1, plan.tp)]
    peers += [{"dp": (dp + step) % plan.dp} for step in range(1, plan.dp)]
    for peer in peers:
        pl.semaphore_signal(barrier, inc=1, device_id=peer, device_id_type=MESH)
    for group in range(groups):
        collect(group)
    pl.semaphore_wait(barrier, len(peers))

    whole_out()
    exchange_layers(0)
    share_in_plane()
    for group in range(1, groups):
        exchange_layers(group)
    for index in range(layers, AHEAD):
        start_exchange(index)

    def step(index, _):
        slot = index % 2

        @pl.when(index + AHEAD < plan.chunks)
        def _():
            start_exchange(index + AHEAD)

        @pl.when((index >= SHARE_AT) & (index < SHARE_AT + plan.dp))
        def _():
            share_to_rank(index - SHARE_AT)

        @pl.when(index == WHOLE_AT)
        def _():
            whole_keep()
            whole_forward()

        @pl.when(index == WHOLE_AT + 3)
        def _():
            whole_arrive()

        @pl.when((index >= RANKS_AT) & (index < RANKS_AT + (plan.tp - 1) * PARTS))
        def _():
            whole_to_rank((index - RANKS_AT) % (plan.tp - 1) + 1, (index - RANKS_AT) // (plan.tp - 1))

        @pl.when(index < layers)
        def _():
            make_layer(index, slot)

        @pl.when(index >= layers)
        def _():
            make_head(index, slot)

        send_own(slab_view(index), index, slot, chunk)

        @pl.when(index >= LAG)
        def _():
            forward(slab_view(index - LAG), index - LAG, chunk)

        @pl.when(index >= 2 * LAG)
        def _():
            forward_diagonal(slab_view(index - 2 * LAG), index - 2 * LAG, chunk)

        return 0

    lax.fori_loop(0, ring, step, 0)

    make_tail(ring % 2)
    send_own(slab_view(ring), ring, ring % 2, tail)
    make_extra()
    for index in range(ring - LAG, ring):
        forward(slab_view(index), index, chunk)
        if index == ring - LAG:
            whole_to_pair()
    forward(slab_view(ring), ring, tail)
    for index in range(ring - 2 * LAG, ring):
        forward_diagonal(slab_view(index), index, chunk)
        if index == ring - 2:
            sent = pl.ds(0, (plan.tp - 1) * rows)
            wait_for(packed, z_send.at[0])
            wait_for(zbuf.at[pl.ds(layers, last - layers), sent, pl.ds(0, chunk)], z_send.at[1])
            wait_for(zbuf.at[last, sent, pl.ds(0, plan.tail_window)], z_send.at[2])
            whole_finish()
            for n, own in enumerate((own_0, own_1)):
                wait_for(own.at[:, pl.ds(0, plan.cut)], share_recv.at[n])
                for parts in (8, 5):
                    gone = pl.ds(0, parts * (plan.down_rows + plan.out_rows))
                    wait_for(own.at[gone, pl.ds(0, plan.cut)], share_send.at[n])
            for index in range((ring - LAG) // COUNTED):
                finish(index, pl.ds(index * COUNTED, COUNTED), chunk)
    forward_diagonal(slab_view(ring), ring, tail)
    for index in range((ring - LAG) // COUNTED, plan.counts - 1):
        first = index * COUNTED
        finish(index, pl.ds(first, min(COUNTED, ring - first)), chunk)
    finish(plan.counts - 1, pl.ds(ring, 1), tail)


def gather(plan, *args):
    dma = pltpu.SemaphoreType.DMA
    groups = plan.layers // GROUP
    share_rows = plan.down_rows + plan.out_rows
    hbm = pl.BlockSpec(memory_space=pltpu.HBM)
    shapes = [(plan.dp, plan.ring + 1, plan.chunk, LANES), (plan.piece, plan.columns), (plan.piece, plan.columns)]
    shapes += [(plan.layers, plan.piece, plan.whole)] + [(plan.dp, share_rows, plan.cut)] * 2
    shapes += [(plan.tp, plan.layers, count, plan.whole) for count in (plan.down_rows, plan.out_rows)]
    return pl.pallas_call(
        functools.partial(gather_kernel, plan),
        out_shape=[jax.ShapeDtypeStruct(shape, jnp.bfloat16) for shape in shapes],
        in_specs=[hbm] * 8,
        out_specs=[hbm] * len(shapes),
        scratch_shapes=[
            pltpu.VMEM((plan.chunks, plan.tp * plan.rows, plan.layer_window), jnp.bfloat16),
            pltpu.VMEM((2, plan.chunk + 2 * LANES, LANES), jnp.bfloat16),
            dma((groups + plan.head_chunks,)), dma((3,)), dma((2,)),
            dma((SLOTS,)), dma((SLOTS,)), dma((SLOTS,)), dma((SLOTS,)), dma((plan.counts,)), dma((plan.counts,)),
            dma((2, plan.dp)), dma((2,)), dma((2,)),
            dma((8,)), dma((2,)), dma((2,)), dma((2,)), dma((2,)), dma((2,)),
            pltpu.VMEM((plan.layers, plan.down_rows, plan.whole), jnp.bfloat16),
            pltpu.VMEM((plan.layers, plan.out_rows, plan.whole), jnp.bfloat16),
            dma((4,)),
            pltpu.VMEM((plan.layers // GROUP, plan.tp - 1, GROUP, plan.rows, plan.layer_window), jnp.bfloat16),
            dma((plan.layers // GROUP,)),
        ],
        compiler_params=pltpu.CompilerParams(collective_id=0, has_side_effects=True),
        name="gather",
    )(*args)[:4]


def place_slabs(plan, slabs, first, count, shapes, store, held=()):
    hbm = pl.BlockSpec(memory_space=pltpu.HBM)
    depth = min(BUFFERS, count)
    ahead = depth // 2

    def body(slab, *refs):
        outs, (buffers, loads, stores) = refs[len(held):-3], refs[-3:]

        def each_size(chunk, act):
            if first + count > plan.ring:
                pl.when(chunk < plan.ring)(lambda: act(plan.chunk))
                pl.when(chunk == plan.ring)(lambda: act(plan.tail))
            else:
                act(plan.chunk)

        def load(i, rows):
            for owner in range(plan.dp):
                pltpu.make_async_copy(
                    slab.at[owner, first + i, pl.ds(0, rows), :],
                    buffers.at[i % depth, pl.ds(0, rows), pl.ds(owner * LANES, LANES)],
                    loads.at[i % depth],
                ).start()

        def wait(i, rows, sem):
            buffer = buffers.at[i % depth, pl.ds(0, rows), :]
            pltpu.make_async_copy(buffer, buffer, sem.at[i % depth]).wait()

        def write(i, rows):
            wait(i, rows, loads)
            for source, target in store(buffers.at[i % depth], first + i, rows, outs):
                pltpu.make_async_copy(source, target, stores.at[i % depth]).start()

        def step(i, _):
            @pl.when(i >= depth)
            def _():
                each_size(first + i - depth, lambda rows: wait(i - depth, rows, stores))

            @pl.when(i < count)
            def _():
                each_size(first + i, lambda rows: load(i, rows))

            @pl.when((i >= ahead) & (i < count + ahead))
            def _():
                each_size(first + i - ahead, lambda rows: write(i - ahead, rows))

            return 0

        lax.fori_loop(0, count + depth, step, 0)

    outs = [jax.ShapeDtypeStruct(shape, jnp.bfloat16) for shape in shapes]
    return pl.pallas_call(
        body,
        in_specs=[hbm] * (1 + len(held)),
        out_specs=[hbm] * len(outs),
        out_shape=outs,
        scratch_shapes=[
            pltpu.VMEM((depth, plan.chunk, plan.dp * LANES), jnp.bfloat16),
            pltpu.SemaphoreType.DMA((depth,)),
            pltpu.SemaphoreType.DMA((depth,)),
        ],
        input_output_aliases={1 + n: n for n in range(len(held))},
        cost_estimate=pl.CostEstimate(
            flops=10**7, bytes_accessed=4 * count * plan.chunk * plan.dp * LANES, transcendentals=0
        ),
        compiler_params=pltpu.CompilerParams(vmem_limit_bytes=VMEM),
    )(slabs, *held)


def place_layers(plan, slabs):
    narrow, wide, width = 3 * plan.part, 2 * plan.wide, plan.dp * LANES

    def store(buffer, chunk, rows, outs):
        return [
            (buffer.at[pl.ds(0, narrow), :], outs[0].at[chunk]),
            (buffer.at[pl.ds(narrow, wide), :], outs[1].at[chunk]),
        ]

    shapes = [(plan.layers, narrow, width), (plan.layers, wide, width)]
    return place_slabs(plan, slabs, 0, plan.layers, shapes, store)


def place_head(plan, slabs, first, count, *held):
    def store(buffer, chunk, rows, outs):
        at = pl.multiple_of((chunk - plan.layers) * plan.chunk, 16)
        return [(buffer.at[pl.ds(0, rows), :], outs[0].at[pl.ds(at, rows), :])]

    shapes = [(plan.vocab, plan.dp * LANES)]
    return place_slabs(plan, slabs, plan.layers + first, count, shapes, store, held)[0]


def place_rows(plan, arrays, spots, width, column, held):
    count = len(spots([array for array in arrays], 0))
    columns = arrays[0].shape[-1]
    outs = [
        jax.ShapeDtypeStruct((plan.layers, plan.downs, plan.columns), jnp.bfloat16),
        jax.ShapeDtypeStruct((plan.layers, plan.columns, plan.outs), jnp.bfloat16),
        jax.ShapeDtypeStruct((plan.vocab, plan.dp * LANES), jnp.bfloat16),
    ]
    with_head = columns > width
    kept = [n for n in range(3) if n in held]
    made = [n for n in range(3 if with_head else 2)]

    blocks = [(plan.downs, plan.outs), (0, plan.downs // 2), (plan.downs // 2, plan.downs // 2)]

    def body(*refs):
        targets = dict(zip(made, refs[len(arrays) + len(kept):-4], strict=True))
        buffers, turned, loads, stored = refs[-4:]
        moves = spots(refs[: len(arrays)], lax.axis_index("dp"))
        place = pl.ds(column, width)
        loading, storing = [], []
        for n, (source, _, _, _) in enumerate(moves):
            for b, (first, height) in enumerate(blocks):
                some = pl.ds(first, height)
                loading.append(pltpu.make_async_copy(source.at[some, :], buffers.at[n, some, :], loads.at[n, b]))
                loading[-1].start()

        def put(source, target):
            storing.append(pltpu.make_async_copy(source, target, stored.at[0]))
            storing[-1].start()

        for n, (_, layer, owner, part) in enumerate(moves):
            for b, (first, height) in enumerate(blocks):
                loading[n * len(blocks) + b].wait()
                some = pl.ds(first, height)
                if b:
                    put(buffers.at[n, some, pl.ds(0, width)], targets[0].at[layer, some, place])
                for j in range((columns - width) // LANES):
                    row = plan.extra_first + (part * WHOLE + j) * plan.piece + first
                    put(
                        buffers.at[n, some, pl.ds(width + j * LANES, LANES)],
                        targets[2].at[pl.ds(row, height), pl.ds(pl.multiple_of(owner * LANES, LANES), LANES)],
                    )
                if b:
                    continue
                for i in range(plan.outs // LANES):
                    for j in range(width // LANES):
                        turned[n, pl.ds(j * LANES, LANES), pl.ds(i * LANES, LANES)] = buffers[
                            n, pl.ds(plan.downs + i * LANES, LANES), pl.ds(j * LANES, LANES)
                        ].T
                put(turned.at[n], targets[1].at[layer, place, :])
        for store in storing:
            store.wait()

    hbm = pl.BlockSpec(memory_space=pltpu.HBM)
    dma = pltpu.SemaphoreType.DMA
    result = pl.pallas_call(
        body,
        out_shape=[outs[n] for n in made],
        in_specs=[hbm] * (len(arrays) + len(kept)),
        out_specs=[hbm] * len(made),
        scratch_shapes=[
            pltpu.VMEM((count, plan.piece, columns), jnp.bfloat16),
            pltpu.VMEM((count, width, plan.outs), jnp.bfloat16),
            dma((count, len(blocks))), dma((1,)),
        ],
        input_output_aliases={len(arrays) + i: n for i, n in enumerate(kept)},
        cost_estimate=pl.CostEstimate(flops=10**7, bytes_accessed=4 * count * plan.piece * columns, transcendentals=0),
        compiler_params=pltpu.CompilerParams(vmem_limit_bytes=VMEM),
    )(*arrays, *(held[n] for n in kept))
    return dict(zip(made, result, strict=True))


def place_whole(plan, whole):
    def spots(refs, dp):
        return [(refs[0].at[layer], layer, 0, 0) for layer in range(plan.layers)]

    return place_rows(plan, [whole], spots, plan.whole, 0, {})


def place_shares(plan, shares, held):
    which = [(owner, part) for owner, arrays in shares.items() for part in arrays]
    arrays = [shares[owner][part] for owner, part in which]

    def spots(refs, dp):
        core, x, y = dp % 2, (dp // 2) % 2, dp // 4
        found = []
        for ref, ((flip_x, flip_y, flip_core), part) in zip(refs, which, strict=True):
            owner = (y + flip_y * (1 - 2 * y)) * 4 + (x + flip_x * (1 - 2 * x)) * 2 + core + flip_core * (1 - 2 * core)
            found.append((ref, owner * plan.share + part, owner, part))
        return found

    return place_rows(plan, arrays, spots, plan.cut, plan.whole, held)


def solution(mesh):
    train_stack = P(None, ("dp", "tp"), None)
    train_head = P(("dp", "tp"), None)
    fused_stack = P(None, "tp", None)
    last_stack = P(None, None, "tp")
    head_rows = P("tp", None)

    def local_sync(w_query, w_key, w_value, w_out, w_gate, w_up, w_down, w_head):
        plan = Plan(mesh.shape["tp"], mesh.shape["dp"], w_query, w_gate, w_out, w_down, w_head)
        slabs, own_0, own_1, whole = gather(plan, w_query, w_key, w_value, w_out, w_gate, w_up, w_down, w_head)

        def swap(bit, array):
            return lax.ppermute(array, "dp", [(i, i ^ bit) for i in range(plan.dp)])

        pair, along_x, along_y = (functools.partial(swap, bit) for bit in (1, 2, 4))
        hold = lax.optimization_barrier

        x_1, y_0 = along_x(own_1), along_y(own_0)
        x_0, y_1 = along_x(own_0), along_y(own_1)
        pair_own = [pair(own_0), pair(own_1)]
        qkv_block, gate_up_block = place_layers(plan, slabs)
        x_1, y_0, qkv_block, slabs = hold((x_1, y_0, qkv_block, slabs))
        diagonal_0 = along_x(y_0)
        diagonal_1 = along_y(x_1)
        pair_x_1, pair_y_0 = pair(x_1), pair(y_0)
        head_chunks = plan.ring + 1 - plan.layers
        early = head_chunks // 4
        head_block = place_head(plan, slabs, early, head_chunks - early)
        x_0, y_1, head_block, slabs, whole = hold((x_0, y_1, head_block, slabs, whole))
        pair_x_0, pair_y_1 = pair(x_0), pair(y_1)
        placed = place_whole(plan, whole)
        slabs, *placed = hold((slabs, placed[0], placed[1]))
        head_block = place_head(plan, slabs, 0, early, head_block)
        own_0, own_1, head_block = hold((own_0, own_1, head_block))
        near = {
            (0, 0, 0): {0: own_0, 1: own_1}, (0, 0, 1): dict(enumerate(pair_own)),
            (1, 0, 0): {0: x_0, 1: x_1}, (1, 0, 1): {0: pair_x_0, 1: pair_x_1},
            (0, 1, 0): {0: y_0, 1: y_1}, (0, 1, 1): {0: pair_y_0, 1: pair_y_1},
        }
        placed = place_shares(plan, near, {0: placed[0], 1: placed[1], 2: head_block})
        diagonal_0, head_block = hold((diagonal_0, placed[2]))
        pair_diagonal_0 = pair(diagonal_0)
        diagonal_1, down_block = hold((diagonal_1, placed[0]))
        pair_diagonal_1 = pair(diagonal_1)
        placed = {0: down_block, 1: placed[1], 2: head_block}
        placed = place_shares(plan, {(1, 1, 0): {0: diagonal_0, 1: diagonal_1}}, placed)
        placed = place_shares(plan, {(1, 1, 1): {0: pair_diagonal_0}}, placed)
        placed = place_shares(plan, {(1, 1, 1): {1: pair_diagonal_1}}, placed)
        down_block, o_block, head_block = placed[0], placed[1], placed[2]
        return (
            qkv_block,
            o_block,
            gate_up_block,
            jnp.swapaxes(down_block, 1, 2),
            head_block,
        )

    return jax.shard_map(
        local_sync,
        mesh=mesh,
        in_specs=(train_stack,) * 7 + (train_head,),
        out_specs=(fused_stack, last_stack, fused_stack, last_stack, head_rows),
        check_vma=False,
    )
```

```python
import functools

import jax
import jax.numpy as jnp
from jax import lax
from jax.experimental import pallas as pl
from jax.experimental.pallas import tpu as pltpu
from jax.sharding import PartitionSpec as P


MESH = pl.DeviceIdType.MESH
LANES = 128
VMEM = 67_000_000
AHEAD = 14
BUFFERS = 6
LAG = 1
SHARE_AT = 20
SLOTS = 4
COUNTED = 4
WHOLE = 3
WHOLE_AT = 2
RANKS_AT = 10
PARTS = 4
GROUP = 4


class Plan:
    def __init__(self, tp, dp, w_query, w_gate, w_out, w_down, w_head):
        self.tp, self.dp = tp, dp
        self.layers, self.rows, columns = w_query.shape
        self.part = columns // tp
        self.wide = w_gate.shape[2] // tp
        self.vocab = w_head.shape[1] // tp
        self.head_tiles = w_head.shape[1] // LANES
        self.chunk = 3 * self.part + 2 * self.wide
        self.wide_window = -(-self.wide // LANES) * LANES
        self.layer_window = 3 * self.part + 2 * self.wide_window
        self.head_chunks = -(-self.vocab // self.chunk)
        self.chunks = self.layers + self.head_chunks
        end = self.vocab - (self.head_chunks - 1) * self.chunk
        self.tail_window = -(-(end + LANES) // LANES) * LANES
        self.window_tiles = (self.head_chunks - 1) * self.chunk // LANES + self.tail_window // LANES
        self.shift = max(self.vocab * r - self.head_base(r) * LANES for r in range(tp))
        self.out_rows, self.down_rows = w_out.shape[1], w_down.shape[1]
        self.downs, self.outs = 2 * tp * self.down_rows, 2 * tp * self.out_rows
        self.piece = self.downs + self.outs
        self.share = self.layers // dp
        self.columns = w_out.shape[2]
        self.whole = WHOLE * LANES
        self.cut = self.columns - self.whole
        self.extra_first = self.vocab - self.share * WHOLE * self.piece
        self.ring = self.layers + self.extra_first // self.chunk
        self.tail = self.extra_first % self.chunk
        self.counts = -(-self.ring // COUNTED) + 1

    def wide_base(self, rank):
        return (self.wide * rank) // LANES

    def head_base(self, rank):
        base = (self.vocab * rank) // LANES
        return base - (rank // (self.tp - 1)) * (self.vocab * (self.tp - 1) // LANES + self.window_tiles - self.head_tiles)


def gather_kernel(plan, q, k, v, o, g, u, d, h, slabs, own_0, own_1, whole, stop, land_d, land_o, zbuf, tbuf,
                  z_recv, z_send, local, x_recv, y_recv, a_recv, b_recv, pair_recv, send, stop_recv, share_recv,
                  share_send, land_recv, land_send, whole_recv, whole_send, whole_pair_recv, whole_pair_send,
                  keep_d, keep_o, keep_sem, packed, pack_sem):
    z, dp = lax.axis_index("tp"), lax.axis_index("dp")
    core, x, y = dp % 2, (dp // 2) % 2, dp // 4
    x_peer = y * 4 + (1 - x) * 2 + core
    y_peer = (1 - y) * 4 + x * 2 + core
    diagonal = (1 - y) * 4 + (1 - x) * 2 + core
    pair = dp + 1 - 2 * core
    rows, chunk, tail = plan.rows, plan.chunk, plan.tail
    layers, ring, last = plan.layers, plan.ring, plan.chunks - 1
    my_rows = pl.ds(pl.multiple_of(z * rows, rows), rows)

    def lanes(first_tile, width):
        return pl.ds(pl.multiple_of(first_tile * LANES, LANES), width)

    def remote(source, target, send_sem, recv_sem, **to):
        pltpu.make_async_remote_copy(source, target, send_sem, recv_sem, device_id=to, device_id_type=MESH).start()

    def wait_for(ref, sem):
        pltpu.make_async_copy(ref, ref, sem).wait()


    def z_slot(index):
        return index - layers + layers // GROUP

    def rank_at(step):
        return (z + step + core * (plan.tp - 2 * step)) % plan.tp

    def layer_pieces(first, rank):
        some, part, wide = pl.ds(first, GROUP), plan.part, plan.wide_window
        narrow = lanes(rank * (part // LANES), part)
        window = lanes(plan.wide_base(rank), wide)
        return [
            (q.at[some, :, narrow], 0, part),
            (k.at[some, :, narrow], part, part),
            (v.at[some, :, narrow], 2 * part, part),
            (g.at[some, :, window], 3 * part, wide),
            (u.at[some, :, window], 3 * part + wide, wide),
        ]

    def collect(group):
        for step in range(1, plan.tp):
            for source, column, width in layer_pieces(group * GROUP, rank_at(step)):
                target = packed.at[group, step - 1, :, :, pl.ds(column, width)]
                pltpu.make_async_copy(source, target, pack_sem.at[group]).start()
        for source, column, width in layer_pieces(group * GROUP, z):
            target = zbuf.at[pl.ds(group * GROUP, GROUP), my_rows, pl.ds(column, width)]
            pltpu.make_async_copy(source, target, z_recv.at[group]).start()

    def exchange_layers(group):
        wait_for(packed.at[group], pack_sem.at[group])
        for step in range(1, plan.tp):
            index = group * GROUP
            target = zbuf.at[pl.ds(index, GROUP), my_rows, :]
            remote(packed.at[group, step - 1], target, z_send.at[0], z_recv.at[group], tp=rank_at(step))

    def exchange_head(index, width):
        def piece(rank):
            return h.at[:, lanes(plan.head_base(rank) + (index - layers) * (chunk // LANES), width)]

        target = zbuf.at[index, my_rows, pl.ds(0, width)]
        sent = z_send.at[1 if width == chunk else 2]
        for step in range(1, plan.tp):
            remote(piece(rank_at(step)), target, sent, z_recv.at[z_slot(index)], tp=rank_at(step))
        pltpu.make_async_copy(piece(z), target, z_recv.at[z_slot(index)]).start()

    def start_exchange(index):
        @pl.when((index >= layers) & (index < last))
        def _():
            exchange_head(index, chunk)

        @pl.when(index == last)
        def _():
            exchange_head(last, plan.tail_window)

    def wait_exchange(index, width):
        wait_for(zbuf.at[index, :, pl.ds(0, width)], z_recv.at[z_slot(index)])


    def turn(slot, tile, index, source_tile):
        tbuf[slot, pl.ds(tile * LANES, LANES), :] = zbuf[index, :, pl.ds(source_tile * LANES, LANES)].T

    def store(slot, first, index, to, count):
        pltpu.make_async_copy(
            tbuf.at[slot, pl.ds(first, count), :], slabs.at[dp, index, pl.ds(to, count), :], local.at[slot]
        ).start()

    def make_layer(index, slot):
        @pl.when(index % GROUP == 0)
        def _():
            wait_for(zbuf.at[pl.ds(index, GROUP), :, pl.ds(0, plan.layer_window)], z_recv.at[index // GROUP])

        for tile in range(plan.layer_window // LANES):
            turn(slot, tile, index, tile)
        shift = plan.wide * z - plan.wide_base(z) * LANES
        narrow, wide, window = 3 * plan.part, plan.wide, plan.wide_window
        store(slot, 0, index, 0, narrow)
        store(slot, pl.multiple_of(narrow + shift, 16), index, narrow, wide)
        store(slot, pl.multiple_of(narrow + window + shift, 16), index, narrow + wide, wide)

    head_shift = plan.vocab * z - plan.head_base(z) * LANES

    def make_head(index, slot):
        @pl.when(index == layers)
        def _():
            wait_exchange(index, chunk)

        wait_exchange(index + 1, chunk)
        tiles = chunk // LANES
        for tile in range(tiles):
            turn(slot, tile, index, tile)
        for tile in range(2):
            turn(slot, tiles + tile, index + 1, tile)
        store(slot, pl.multiple_of(head_shift, 16), index, 0, chunk)

    def turn_rows(slot, first, count):
        start = first // LANES
        for tile in range(-(-(first % LANES + plan.shift + count) // LANES)):
            at = start + tile
            turn(slot, tile, layers + at // (chunk // LANES), at % (chunk // LANES))
        return pl.multiple_of(first % LANES + head_shift, 16)

    def make_tail(slot):
        wait_exchange(ring + 1, chunk)
        store(slot, turn_rows(slot, (ring - layers) * chunk, tail), ring, 0, tail)

    def make_extra():
        for index in range(ring + 2, last):
            wait_exchange(index, chunk)
        wait_exchange(last, plan.tail_window)
        blocks = plan.share * WHOLE

        def stored(n, own):
            wait_for(own.at[:, pl.ds(plan.cut, LANES)], local.at[n % 2])

        for n in range(blocks):
            own = (own_0, own_1)[n // WHOLE]
            if n >= 2:
                stored(n, own)
            at = turn_rows(n % 2, plan.extra_first + n * plan.piece, plan.piece)
            pltpu.make_async_copy(
                tbuf.at[n % 2, pl.ds(at, plan.piece), :],
                own.at[:, pl.ds(plan.cut + n % WHOLE * LANES, LANES)], local.at[n % 2],
            ).start()
        for n in range(blocks - min(2, blocks), blocks):
            stored(n, own_0)


    def slab_view(index):
        return lambda owner, first, count: slabs.at[owner, index, pl.ds(first, count), :]

    def push(part, index, recv, to):
        remote(part, part, send.at[counted(index)], recv.at[index % SLOTS], dp=to)

    def push_pair(part, index):
        remote(part, part, send.at[counted(index)], pair_recv.at[counted(index)], dp=pair)

    def counted(index):
        return plan.counts - 1 if index is ring else index // COUNTED

    def send_own(view, index, slot, count):
        own = view(dp, 0, count)
        wait_for(own, local.at[slot])
        push(own, index, x_recv, x_peer)
        push(own, index, y_recv, y_peer)
        push_pair(own, index)

    def forward(view, index, count):
        half = count // 2
        slot = index % SLOTS
        wait_for(view(x_peer, 0, count), x_recv.at[slot])
        push(view(x_peer, half, half), index, b_recv, y_peer)
        push_pair(view(x_peer, 0, count), index)
        wait_for(view(y_peer, 0, count), y_recv.at[slot])
        push(view(y_peer, 0, half), index, a_recv, x_peer)
        push_pair(view(y_peer, 0, count), index)

    def forward_diagonal(view, index, count):
        half = count // 2
        slot = index % SLOTS
        wait_for(view(diagonal, 0, half), a_recv.at[slot])
        wait_for(view(diagonal, half, half), b_recv.at[slot])
        push_pair(view(diagonal, 0, count), index)

    def finish(index, some, count):
        wait_for(slabs.at[pl.ds(0, 7), some, pl.ds(0, count), :], send.at[index])
        wait_for(slabs.at[pl.ds(0, 4), some, pl.ds(0, count), :], pair_recv.at[index])


    def pieces(source_dp, to, place):
        all_rows = plan.downs
        downs = pl.ds(pl.multiple_of(place * plan.down_rows, 8), plan.down_rows)
        outs = pl.ds(pl.multiple_of(all_rows + place * plan.out_rows, 8), plan.out_rows)
        stop_downs, stop_outs = pl.ds(0, plan.down_rows), pl.ds(plan.down_rows, plan.out_rows)
        cut, home = pl.ds(plan.whole, plan.cut), pl.ds(0, plan.cut)
        found = []
        for n, own in enumerate((own_0, own_1)):
            layer = to * 2 + n
            found.append((d.at[layer, :, cut], stop.at[source_dp, n, stop_downs, :], own.at[downs, home], n))
            found.append((o.at[layer, :, cut], stop.at[source_dp, n, stop_outs, :], own.at[outs, home], n))
        return found

    my_rank = dp // 2
    my_place = (dp % 2) * plan.tp + z
    stays = my_rank == z

    def share_in_plane():
        for step in range(1, plan.dp):
            to = (dp + step) % plan.dp

            @pl.when(stays)
            def _(to=to):
                for part, _, final, n in pieces(dp, to, my_place):
                    remote(part, final, share_send.at[n], share_recv.at[n], dp=to)

            @pl.when(jnp.logical_not(stays))
            def _(to=to):
                for part, waiting, _, n in pieces(dp, to, my_place):
                    remote(part, waiting, share_send.at[n], stop_recv.at[dp], dp=to)

        @pl.when(stays)
        def _():
            for part, _, final, n in pieces(dp, dp, my_place):
                pltpu.make_async_copy(part, final, share_recv.at[n]).start()

    def share_to_rank(source_dp):
        rank, place = source_dp // 2, (source_dp % 2) * plan.tp + z

        @pl.when((rank != z) & (source_dp == dp))
        def _():
            for part, _, final, n in pieces(dp, dp, place):
                remote(part, final, share_send.at[n], share_recv.at[n], tp=rank)

        @pl.when((rank != z) & (source_dp != dp))
        def _():
            wait_for(stop.at[source_dp], stop_recv.at[source_dp])
            for _, waiting, final, n in pieces(source_dp, dp, place):
                remote(waiting, final, share_send.at[n], share_recv.at[n], tp=rank)


    whole_columns = pl.ds(0, plan.whole)
    keep = (keep_d, keep_o)
    mine = ((d, land_d, plan.down_rows, 0), (o, land_o, plan.out_rows, plan.downs))
    half = layers // 2

    def whole_home(n, row):
        _, _, count, first = mine[n]
        return pl.ds(pl.multiple_of(first + row * count, 8), count)

    def landing(rank, some, act):
        pl.when(rank == z)(lambda: act([whole.at[some, whole_home(n, core * plan.tp + z), :] for n in range(2)]))
        pl.when(rank != z)(lambda: act([land.at[rank, some] for _, land, _, _ in mine]))

    every = pl.ds(0, layers)

    def whole_out():
        def act(places):
            for n, (source, _, _, _) in enumerate(mine):
                for to, at in ((x_peer, 0), (y_peer, 2)):
                    remote(source.at[:, :, whole_columns], places[n], land_send.at[n], land_recv.at[at + n], dp=to)

        landing(my_rank, every, act)

        @pl.when(stays)
        def _():
            for n, (source, _, _, _) in enumerate(mine):
                pltpu.make_async_copy(source.at[:, :, whole_columns], keep[n], keep_sem.at[n]).start()

    def whole_keep():
        @pl.when(stays)
        def _():
            for n in range(2):
                wait_for(keep[n], keep_sem.at[n])
                target = whole.at[:, whole_home(n, core * plan.tp + z), :]
                pltpu.make_async_copy(keep[n], target, keep_sem.at[2 + n]).start()

    def whole_forward():
        for owner, at, first, to, then in ((x_peer, 0, half, y_peer, 6), (y_peer, 2, 0, x_peer, 4)):
            def arrived(places, at=at):
                for n in range(2):
                    wait_for(places[n], land_recv.at[at + n])

            def on(places, to=to, then=then):
                for n in range(2):
                    remote(places[n], places[n], land_send.at[n], land_recv.at[then + n], dp=to)

            landing(owner // 2, every, arrived)
            landing(owner // 2, pl.ds(first, half), on)

    def whole_arrive():
        for first, at in ((0, 4), (half, 6)):
            def arrived(places, at=at):
                for n in range(2):
                    wait_for(places[n], land_recv.at[at + n])

            landing(diagonal // 2, pl.ds(first, half), arrived)

    def whole_to_rank(shift, part):
        rank = (z + shift + core * (plan.tp - 2 * shift)) % plan.tp
        some = pl.ds(part * (layers // PARTS), layers // PARTS)

        def move(sources):
            for n, source in enumerate(sources):
                target = whole.at[some, whole_home(n, core * plan.tp + z), :]
                remote(source, target, whole_send.at[n], whole_recv.at[n], tp=rank)

        pl.when(rank == my_rank)(lambda: move([source.at[some, :, whole_columns] for source, _, _, _ in mine]))
        pl.when(rank != my_rank)(lambda: move([land.at[rank, some] for _, land, _, _ in mine]))

    def whole_rows(which):
        return [
            whole.at[:, pl.ds(pl.multiple_of(first + which * plan.tp * count, 8), plan.tp * count), :]
            for _, _, count, first in mine
        ]

    def whole_to_pair():
        for n, part in enumerate(whole_rows(core)):
            away = pl.ds(0, (plan.tp - 1) * mine[n][2])
            wait_for(whole.at[:, away, :], whole_recv.at[n])

            @pl.when(stays)
            def _(n=n):
                wait_for(keep[n], keep_sem.at[2 + n])

            remote(part, part, whole_pair_send.at[n], whole_pair_recv.at[n], dp=pair)

    def whole_finish():
        for n, (_, land, count, first) in enumerate(mine):
            wait_for(land.at[pl.ds(0, 3)], land_send.at[n])
            wait_for(whole.at[:, pl.ds(first, (plan.tp - 1) * count), :], whole_send.at[n])
            wait_for(whole_rows(core)[n], whole_pair_send.at[n])
            wait_for(whole_rows(1 - core)[n], whole_pair_recv.at[n])

    groups = layers // GROUP
    barrier = pltpu.get_barrier_semaphore()
    peers = [{"tp": (z + step) % plan.tp} for step in range(1, plan.tp)]
    peers += [{"dp": (dp + step) % plan.dp} for step in range(1, plan.dp)]
    for peer in peers:
        pl.semaphore_signal(barrier, inc=1, device_id=peer, device_id_type=MESH)
    for group in range(groups):
        collect(group)
    pl.semaphore_wait(barrier, len(peers))

    whole_out()
    exchange_layers(0)
    share_in_plane()
    for group in range(1, groups):
        exchange_layers(group)
    for index in range(layers, AHEAD):
        start_exchange(index)

    def step(index, _):
        slot = index % 2

        @pl.when(index + AHEAD < plan.chunks)
        def _():
            start_exchange(index + AHEAD)

        @pl.when((index >= SHARE_AT) & (index < SHARE_AT + plan.dp))
        def _():
            share_to_rank(index - SHARE_AT)

        @pl.when(index == WHOLE_AT)
        def _():
            whole_keep()
            whole_forward()

        @pl.when(index == WHOLE_AT + 3)
        def _():
            whole_arrive()

        @pl.when((index >= RANKS_AT) & (index < RANKS_AT + (plan.tp - 1) * PARTS))
        def _():
            whole_to_rank((index - RANKS_AT) % (plan.tp - 1) + 1, (index - RANKS_AT) // (plan.tp - 1))

        @pl.when(index < layers)
        def _():
            make_layer(index, slot)

        @pl.when(index >= layers)
        def _():
            make_head(index, slot)

        send_own(slab_view(index), index, slot, chunk)

        @pl.when(index >= LAG)
        def _():
            forward(slab_view(index - LAG), index - LAG, chunk)

        @pl.when(index >= 2 * LAG)
        def _():
            forward_diagonal(slab_view(index - 2 * LAG), index - 2 * LAG, chunk)

        return 0

    lax.fori_loop(0, ring, step, 0)

    make_tail(ring % 2)
    send_own(slab_view(ring), ring, ring % 2, tail)
    make_extra()
    for index in range(ring - LAG, ring):
        forward(slab_view(index), index, chunk)
        if index == ring - LAG:
            whole_to_pair()
    forward(slab_view(ring), ring, tail)
    for index in range(ring - 2 * LAG, ring):
        forward_diagonal(slab_view(index), index, chunk)
        if index == ring - 2:
            sent = pl.ds(0, (plan.tp - 1) * rows)
            wait_for(packed, z_send.at[0])
            wait_for(zbuf.at[pl.ds(layers, last - layers), sent, pl.ds(0, chunk)], z_send.at[1])
            wait_for(zbuf.at[last, sent, pl.ds(0, plan.tail_window)], z_send.at[2])
            whole_finish()
            for n, own in enumerate((own_0, own_1)):
                wait_for(own.at[:, pl.ds(0, plan.cut)], share_recv.at[n])
                for parts in (8, 5):
                    gone = pl.ds(0, parts * (plan.down_rows + plan.out_rows))
                    wait_for(own.at[gone, pl.ds(0, plan.cut)], share_send.at[n])
            for index in range((ring - LAG) // COUNTED):
                finish(index, pl.ds(index * COUNTED, COUNTED), chunk)
    forward_diagonal(slab_view(ring), ring, tail)
    for index in range((ring - LAG) // COUNTED, plan.counts - 1):
        first = index * COUNTED
        finish(index, pl.ds(first, min(COUNTED, ring - first)), chunk)
    finish(plan.counts - 1, pl.ds(ring, 1), tail)


def gather(plan, *args):
    dma = pltpu.SemaphoreType.DMA
    groups = plan.layers // GROUP
    share_rows = plan.down_rows + plan.out_rows
    hbm = pl.BlockSpec(memory_space=pltpu.HBM)
    shapes = [(plan.dp, plan.ring + 1, plan.chunk, LANES), (plan.piece, plan.columns), (plan.piece, plan.columns)]
    shapes += [(plan.layers, plan.piece, plan.whole), (plan.dp, plan.share, share_rows, plan.cut)]
    shapes += [(plan.tp, plan.layers, count, plan.whole) for count in (plan.down_rows, plan.out_rows)]
    return pl.pallas_call(
        functools.partial(gather_kernel, plan),
        out_shape=[jax.ShapeDtypeStruct(shape, jnp.bfloat16) for shape in shapes],
        in_specs=[hbm] * 8,
        out_specs=[hbm] * len(shapes),
        scratch_shapes=[
            pltpu.VMEM((plan.chunks, plan.tp * plan.rows, plan.layer_window), jnp.bfloat16),
            pltpu.VMEM((2, plan.chunk + 2 * LANES, LANES), jnp.bfloat16),
            dma((groups + plan.head_chunks,)), dma((3,)), dma((2,)),
            dma((SLOTS,)), dma((SLOTS,)), dma((SLOTS,)), dma((SLOTS,)), dma((plan.counts,)), dma((plan.counts,)),
            dma((plan.dp,)), dma((2,)), dma((2,)),
            dma((8,)), dma((2,)), dma((2,)), dma((2,)), dma((2,)), dma((2,)),
            pltpu.VMEM((plan.layers, plan.down_rows, plan.whole), jnp.bfloat16),
            pltpu.VMEM((plan.layers, plan.out_rows, plan.whole), jnp.bfloat16),
            dma((4,)),
            pltpu.VMEM((plan.layers // GROUP, plan.tp - 1, GROUP, plan.rows, plan.layer_window), jnp.bfloat16),
            dma((plan.layers // GROUP,)),
        ],
        compiler_params=pltpu.CompilerParams(collective_id=0, has_side_effects=True),
        name="gather",
    )(*args)[:4]


def place_slabs(plan, slabs, first, count, shapes, store, held=()):
    hbm = pl.BlockSpec(memory_space=pltpu.HBM)
    depth = min(BUFFERS, count)
    ahead = depth // 2

    def body(slab, *refs):
        outs, (buffers, loads, stores) = refs[len(held):-3], refs[-3:]

        def each_size(chunk, act):
            if first + count > plan.ring:
                pl.when(chunk < plan.ring)(lambda: act(plan.chunk))
                pl.when(chunk == plan.ring)(lambda: act(plan.tail))
            else:
                act(plan.chunk)

        def load(i, rows):
            for owner in range(plan.dp):
                pltpu.make_async_copy(
                    slab.at[owner, first + i, pl.ds(0, rows), :],
                    buffers.at[i % depth, pl.ds(0, rows), pl.ds(owner * LANES, LANES)],
                    loads.at[i % depth],
                ).start()

        def wait(i, rows, sem):
            buffer = buffers.at[i % depth, pl.ds(0, rows), :]
            pltpu.make_async_copy(buffer, buffer, sem.at[i % depth]).wait()

        def write(i, rows):
            wait(i, rows, loads)
            for source, target in store(buffers.at[i % depth], first + i, rows, outs):
                pltpu.make_async_copy(source, target, stores.at[i % depth]).start()

        def step(i, _):
            @pl.when(i >= depth)
            def _():
                each_size(first + i - depth, lambda rows: wait(i - depth, rows, stores))

            @pl.when(i < count)
            def _():
                each_size(first + i, lambda rows: load(i, rows))

            @pl.when((i >= ahead) & (i < count + ahead))
            def _():
                each_size(first + i - ahead, lambda rows: write(i - ahead, rows))

            return 0

        lax.fori_loop(0, count + depth, step, 0)

    outs = [jax.ShapeDtypeStruct(shape, jnp.bfloat16) for shape in shapes]
    return pl.pallas_call(
        body,
        in_specs=[hbm] * (1 + len(held)),
        out_specs=[hbm] * len(outs),
        out_shape=outs,
        scratch_shapes=[
            pltpu.VMEM((depth, plan.chunk, plan.dp * LANES), jnp.bfloat16),
            pltpu.SemaphoreType.DMA((depth,)),
            pltpu.SemaphoreType.DMA((depth,)),
        ],
        input_output_aliases={1 + n: n for n in range(len(held))},
        cost_estimate=pl.CostEstimate(
            flops=10**7, bytes_accessed=4 * count * plan.chunk * plan.dp * LANES, transcendentals=0
        ),
        compiler_params=pltpu.CompilerParams(vmem_limit_bytes=VMEM),
    )(slabs, *held)


def place_layers(plan, slabs):
    narrow, wide, width = 3 * plan.part, 2 * plan.wide, plan.dp * LANES

    def store(buffer, chunk, rows, outs):
        return [
            (buffer.at[pl.ds(0, narrow), :], outs[0].at[chunk]),
            (buffer.at[pl.ds(narrow, wide), :], outs[1].at[chunk]),
        ]

    shapes = [(plan.layers, narrow, width), (plan.layers, wide, width)]
    return place_slabs(plan, slabs, 0, plan.layers, shapes, store)


def place_head(plan, slabs, first, count, *held):
    def store(buffer, chunk, rows, outs):
        at = pl.multiple_of((chunk - plan.layers) * plan.chunk, 16)
        return [(buffer.at[pl.ds(0, rows), :], outs[0].at[pl.ds(at, rows), :])]

    shapes = [(plan.vocab, plan.dp * LANES)]
    return place_slabs(plan, slabs, plan.layers + first, count, shapes, store, held)[0]


def place_rows(plan, arrays, spots, width, column, held):
    count = len(spots([array for array in arrays], 0))
    columns = arrays[0].shape[-1]
    outs = [
        jax.ShapeDtypeStruct((plan.layers, plan.downs, plan.columns), jnp.bfloat16),
        jax.ShapeDtypeStruct((plan.layers, plan.columns, plan.outs), jnp.bfloat16),
        jax.ShapeDtypeStruct((plan.vocab, plan.dp * LANES), jnp.bfloat16),
    ]
    with_head = columns > width
    kept = [n for n in range(3) if n in held]
    made = [n for n in range(3 if with_head else 2)]

    blocks = [(plan.downs, plan.outs), (0, plan.downs // 2), (plan.downs // 2, plan.downs // 2)]

    def body(*refs):
        targets = dict(zip(made, refs[len(arrays) + len(kept):-4], strict=True))
        buffers, turned, loads, stored = refs[-4:]
        moves = spots(refs[: len(arrays)], lax.axis_index("dp"))
        place = pl.ds(column, width)
        loading, storing = [], []
        for n, (source, _, _, _) in enumerate(moves):
            for b, (first, height) in enumerate(blocks):
                some = pl.ds(first, height)
                loading.append(pltpu.make_async_copy(source.at[some, :], buffers.at[n, some, :], loads.at[n, b]))
                loading[-1].start()

        def put(source, target):
            storing.append(pltpu.make_async_copy(source, target, stored.at[0]))
            storing[-1].start()

        for n, (_, layer, owner, part) in enumerate(moves):
            for b, (first, height) in enumerate(blocks):
                loading[n * len(blocks) + b].wait()
                some = pl.ds(first, height)
                if b:
                    put(buffers.at[n, some, pl.ds(0, width)], targets[0].at[layer, some, place])
                for j in range((columns - width) // LANES):
                    row = plan.extra_first + (part * WHOLE + j) * plan.piece + first
                    put(
                        buffers.at[n, some, pl.ds(width + j * LANES, LANES)],
                        targets[2].at[pl.ds(row, height), pl.ds(pl.multiple_of(owner * LANES, LANES), LANES)],
                    )
                if b:
                    continue
                for i in range(plan.outs // LANES):
                    for j in range(width // LANES):
                        turned[n, pl.ds(j * LANES, LANES), pl.ds(i * LANES, LANES)] = buffers[
                            n, pl.ds(plan.downs + i * LANES, LANES), pl.ds(j * LANES, LANES)
                        ].T
                put(turned.at[n], targets[1].at[layer, place, :])
        for store in storing:
            store.wait()

    hbm = pl.BlockSpec(memory_space=pltpu.HBM)
    dma = pltpu.SemaphoreType.DMA
    result = pl.pallas_call(
        body,
        out_shape=[outs[n] for n in made],
        in_specs=[hbm] * (len(arrays) + len(kept)),
        out_specs=[hbm] * len(made),
        scratch_shapes=[
            pltpu.VMEM((count, plan.piece, columns), jnp.bfloat16),
            pltpu.VMEM((count, width, plan.outs), jnp.bfloat16),
            dma((count, len(blocks))), dma((1,)),
        ],
        input_output_aliases={len(arrays) + i: n for i, n in enumerate(kept)},
        cost_estimate=pl.CostEstimate(flops=10**7, bytes_accessed=4 * count * plan.piece * columns, transcendentals=0),
        compiler_params=pltpu.CompilerParams(vmem_limit_bytes=VMEM),
    )(*arrays, *(held[n] for n in kept))
    return dict(zip(made, result, strict=True))


def place_whole(plan, whole):
    def spots(refs, dp):
        return [(refs[0].at[layer], layer, 0, 0) for layer in range(plan.layers)]

    return place_rows(plan, [whole], spots, plan.whole, 0, {})


def place_shares(plan, shares, held):
    which = [(owner, part) for owner, arrays in shares.items() for part in arrays]
    arrays = [shares[owner][part] for owner, part in which]

    def spots(refs, dp):
        core, x, y = dp % 2, (dp // 2) % 2, dp // 4
        found = []
        for ref, ((flip_x, flip_y, flip_core), part) in zip(refs, which, strict=True):
            owner = (y + flip_y * (1 - 2 * y)) * 4 + (x + flip_x * (1 - 2 * x)) * 2 + core + flip_core * (1 - 2 * core)
            found.append((ref, owner * plan.share + part, owner, part))
        return found

    return place_rows(plan, arrays, spots, plan.cut, plan.whole, held)


def solution(mesh):
    train_stack = P(None, ("dp", "tp"), None)
    train_head = P(("dp", "tp"), None)
    fused_stack = P(None, "tp", None)
    last_stack = P(None, None, "tp")
    head_rows = P("tp", None)

    def local_sync(w_query, w_key, w_value, w_out, w_gate, w_up, w_down, w_head):
        plan = Plan(mesh.shape["tp"], mesh.shape["dp"], w_query, w_gate, w_out, w_down, w_head)
        slabs, own_0, own_1, whole = gather(plan, w_query, w_key, w_value, w_out, w_gate, w_up, w_down, w_head)

        def swap(bit, array):
            return lax.ppermute(array, "dp", [(i, i ^ bit) for i in range(plan.dp)])

        pair, along_x, along_y = (functools.partial(swap, bit) for bit in (1, 2, 4))
        hold = lax.optimization_barrier

        x_1, y_0 = along_x(own_1), along_y(own_0)
        x_0, y_1 = along_x(own_0), along_y(own_1)
        pair_own = [pair(own_0), pair(own_1)]
        qkv_block, gate_up_block = place_layers(plan, slabs)
        x_1, y_0, qkv_block, slabs = hold((x_1, y_0, qkv_block, slabs))
        diagonal_0 = along_x(y_0)
        diagonal_1 = along_y(x_1)
        pair_x_1, pair_y_0 = pair(x_1), pair(y_0)
        head_chunks = plan.ring + 1 - plan.layers
        early = head_chunks // 4
        head_block = place_head(plan, slabs, early, head_chunks - early)
        x_0, y_1, head_block, slabs, whole = hold((x_0, y_1, head_block, slabs, whole))
        pair_x_0, pair_y_1 = pair(x_0), pair(y_1)
        placed = place_whole(plan, whole)
        slabs, *placed = hold((slabs, placed[0], placed[1]))
        head_block = place_head(plan, slabs, 0, early, head_block)
        own_0, own_1, head_block = hold((own_0, own_1, head_block))
        near = {
            (0, 0, 0): {0: own_0, 1: own_1}, (0, 0, 1): dict(enumerate(pair_own)),
            (1, 0, 0): {0: x_0, 1: x_1}, (1, 0, 1): {0: pair_x_0, 1: pair_x_1},
            (0, 1, 0): {0: y_0, 1: y_1}, (0, 1, 1): {0: pair_y_0, 1: pair_y_1},
        }
        placed = place_shares(plan, near, {0: placed[0], 1: placed[1], 2: head_block})
        diagonal_0, head_block = hold((diagonal_0, placed[2]))
        pair_diagonal_0 = pair(diagonal_0)
        diagonal_1, down_block = hold((diagonal_1, placed[0]))
        pair_diagonal_1 = pair(diagonal_1)
        placed = {0: down_block, 1: placed[1], 2: head_block}
        placed = place_shares(plan, {(1, 1, 0): {0: diagonal_0, 1: diagonal_1}}, placed)
        placed = place_shares(plan, {(1, 1, 1): {0: pair_diagonal_0}}, placed)
        placed = place_shares(plan, {(1, 1, 1): {1: pair_diagonal_1}}, placed)
        down_block, o_block, head_block = placed[0], placed[1], placed[2]
        return (
            qkv_block,
            o_block,
            gate_up_block,
            jnp.swapaxes(down_block, 1, 2),
            head_block,
        )

    return jax.shard_map(
        local_sync,
        mesh=mesh,
        in_specs=(train_stack,) * 7 + (train_head,),
        out_specs=(fused_stack, last_stack, fused_stack, last_stack, head_rows),
        check_vma=False,
    )
```

```python
import functools

import jax
import jax.numpy as jnp
from jax import lax
from jax.experimental import pallas as pl
from jax.experimental.pallas import tpu as pltpu
from jax.sharding import PartitionSpec as P


MESH = pl.DeviceIdType.MESH
LANES = 128
VMEM = 67_000_000
AHEAD = 14
BUFFERS = 6
LAG = 1
SHARE_AT = 20
LAST = 256
SLOTS = 5
COUNTED = 4
WHOLE = 3
WHOLE_AT = 2
RANKS_AT = 10
PARTS = 4
GROUP = 4


class Plan:
    def __init__(self, tp, dp, w_query, w_gate, w_out, w_down, w_head):
        self.tp, self.dp = tp, dp
        self.layers, self.rows, columns = w_query.shape
        self.part = columns // tp
        self.wide = w_gate.shape[2] // tp
        self.vocab = w_head.shape[1] // tp
        self.head_tiles = w_head.shape[1] // LANES
        self.chunk = 3 * self.part + 2 * self.wide
        self.wide_window = -(-self.wide // LANES) * LANES
        self.layer_window = 3 * self.part + 2 * self.wide_window
        self.head_chunks = -(-self.vocab // self.chunk)
        self.chunks = self.layers + self.head_chunks
        end = self.vocab - (self.head_chunks - 1) * self.chunk
        self.tail_window = -(-(end + LANES) // LANES) * LANES
        self.window_tiles = (self.head_chunks - 1) * self.chunk // LANES + self.tail_window // LANES
        self.shift = max(self.vocab * r - self.head_base(r) * LANES for r in range(tp))
        self.out_rows, self.down_rows = w_out.shape[1], w_down.shape[1]
        self.downs, self.outs = 2 * tp * self.down_rows, 2 * tp * self.out_rows
        self.piece = self.downs + self.outs
        self.share = self.layers // dp
        self.columns = w_out.shape[2]
        self.whole = WHOLE * LANES
        self.cut = self.columns - self.whole
        self.extra_first = self.vocab - self.share * WHOLE * self.piece
        self.ring = self.layers + self.extra_first // self.chunk
        self.tail = self.extra_first % self.chunk
        self.counts = -(-self.ring // COUNTED) + 1

    def wide_base(self, rank):
        return (self.wide * rank) // LANES

    def head_base(self, rank):
        base = (self.vocab * rank) // LANES
        return base - (rank // (self.tp - 1)) * (self.vocab * (self.tp - 1) // LANES + self.window_tiles - self.head_tiles)


def gather_kernel(plan, q, k, v, o, g, u, d, h, slabs, own_0, own_1, whole, stop, land_d, land_o, zbuf, tbuf,
                  z_recv, z_send, local, x_recv, y_recv, a_recv, b_recv, pair_recv, send, stop_recv, share_recv,
                  share_send, land_recv, land_send, whole_recv, whole_send, whole_pair_recv, whole_pair_send,
                  keep_d, keep_o, keep_sem, packed, pack_sem):
    z, dp = lax.axis_index("tp"), lax.axis_index("dp")
    core, x, y = dp % 2, (dp // 2) % 2, dp // 4
    x_peer = y * 4 + (1 - x) * 2 + core
    y_peer = (1 - y) * 4 + x * 2 + core
    diagonal = (1 - y) * 4 + (1 - x) * 2 + core
    pair = dp + 1 - 2 * core
    rows, chunk, tail = plan.rows, plan.chunk, plan.tail
    layers, ring, last = plan.layers, plan.ring, plan.chunks - 1
    my_rows = pl.ds(pl.multiple_of(z * rows, rows), rows)

    def lanes(first_tile, width):
        return pl.ds(pl.multiple_of(first_tile * LANES, LANES), width)

    def remote(source, target, send_sem, recv_sem, **to):
        pltpu.make_async_remote_copy(source, target, send_sem, recv_sem, device_id=to, device_id_type=MESH).start()

    def wait_for(ref, sem):
        pltpu.make_async_copy(ref, ref, sem).wait()


    def z_slot(index):
        return index - layers + layers // GROUP

    def rank_at(step):
        return (z + step + core * (plan.tp - 2 * step)) % plan.tp

    def layer_pieces(first, rank):
        some, part, wide = pl.ds(first, GROUP), plan.part, plan.wide_window
        narrow = lanes(rank * (part // LANES), part)
        window = lanes(plan.wide_base(rank), wide)
        return [
            (q.at[some, :, narrow], 0, part),
            (k.at[some, :, narrow], part, part),
            (v.at[some, :, narrow], 2 * part, part),
            (g.at[some, :, window], 3 * part, wide),
            (u.at[some, :, window], 3 * part + wide, wide),
        ]

    def collect(group):
        for step in range(1, plan.tp):
            for source, column, width in layer_pieces(group * GROUP, rank_at(step)):
                target = packed.at[group, step - 1, :, :, pl.ds(column, width)]
                pltpu.make_async_copy(source, target, pack_sem.at[group]).start()
        for source, column, width in layer_pieces(group * GROUP, z):
            target = zbuf.at[pl.ds(group * GROUP, GROUP), my_rows, pl.ds(column, width)]
            pltpu.make_async_copy(source, target, z_recv.at[group]).start()

    def exchange_layers(group):
        wait_for(packed.at[group], pack_sem.at[group])
        for step in range(1, plan.tp):
            index = group * GROUP
            target = zbuf.at[pl.ds(index, GROUP), my_rows, :]
            remote(packed.at[group, step - 1], target, z_send.at[0], z_recv.at[group], tp=rank_at(step))

    def exchange_head(index, width):
        def piece(rank):
            return h.at[:, lanes(plan.head_base(rank) + (index - layers) * (chunk // LANES), width)]

        target = zbuf.at[index, my_rows, pl.ds(0, width)]
        sent = z_send.at[1 if width == chunk else 2]
        for step in range(1, plan.tp):
            remote(piece(rank_at(step)), target, sent, z_recv.at[z_slot(index)], tp=rank_at(step))
        pltpu.make_async_copy(piece(z), target, z_recv.at[z_slot(index)]).start()

    def start_exchange(index):
        @pl.when((index >= layers) & (index < last))
        def _():
            exchange_head(index, chunk)

        @pl.when(index == last)
        def _():
            exchange_head(last, plan.tail_window)

    def wait_exchange(index, width):
        wait_for(zbuf.at[index, :, pl.ds(0, width)], z_recv.at[z_slot(index)])


    def turn(slot, tile, index, source_tile):
        tbuf[slot, pl.ds(tile * LANES, LANES), :] = zbuf[index, :, pl.ds(source_tile * LANES, LANES)].T

    def store(slot, first, index, to, count):
        pltpu.make_async_copy(
            tbuf.at[slot, pl.ds(first, count), :], slabs.at[dp, index, pl.ds(to, count), :], local.at[slot]
        ).start()

    def make_layer(index, slot):
        @pl.when(index % GROUP == 0)
        def _():
            wait_for(zbuf.at[pl.ds(index, GROUP), :, pl.ds(0, plan.layer_window)], z_recv.at[index // GROUP])

        for tile in range(plan.layer_window // LANES):
            turn(slot, tile, index, tile)
        shift = plan.wide * z - plan.wide_base(z) * LANES
        narrow, wide, window = 3 * plan.part, plan.wide, plan.wide_window
        store(slot, 0, index, 0, narrow)
        store(slot, pl.multiple_of(narrow + shift, 16), index, narrow, wide)
        store(slot, pl.multiple_of(narrow + window + shift, 16), index, narrow + wide, wide)

    head_shift = plan.vocab * z - plan.head_base(z) * LANES

    def make_head(index, slot):
        @pl.when(index == layers)
        def _():
            wait_exchange(index, chunk)

        wait_exchange(index + 1, chunk)
        tiles = chunk // LANES
        for tile in range(tiles):
            turn(slot, tile, index, tile)
        for tile in range(2):
            turn(slot, tiles + tile, index + 1, tile)
        store(slot, pl.multiple_of(head_shift, 16), index, 0, chunk)

    def turn_rows(slot, first, count):
        start = first // LANES
        for tile in range(-(-(first % LANES + plan.shift + count) // LANES)):
            at = start + tile
            turn(slot, tile, layers + at // (chunk // LANES), at % (chunk // LANES))
        return pl.multiple_of(first % LANES + head_shift, 16)

    def make_tail(slot):
        wait_exchange(ring + 1, chunk)
        store(slot, turn_rows(slot, (ring - layers) * chunk, tail), ring, 0, tail)

    def make_extra():
        for index in range(ring + 2, last):
            wait_exchange(index, chunk)
        wait_exchange(last, plan.tail_window)
        blocks = plan.share * WHOLE

        def stored(n, own):
            wait_for(own.at[:, pl.ds(plan.cut, LANES)], local.at[n % 2])

        for n in range(blocks):
            own = (own_0, own_1)[n // WHOLE]
            if n >= 2:
                stored(n, own)
            at = turn_rows(n % 2, plan.extra_first + n * plan.piece, plan.piece)
            pltpu.make_async_copy(
                tbuf.at[n % 2, pl.ds(at, plan.piece), :],
                own.at[:, pl.ds(plan.cut + n % WHOLE * LANES, LANES)], local.at[n % 2],
            ).start()
        for n in range(blocks - min(2, blocks), blocks):
            stored(n, own_0)


    def slab_view(index):
        return lambda owner, first, count: slabs.at[owner, index, pl.ds(first, count), :]

    def push(part, index, recv, to):
        remote(part, part, send.at[counted(index)], recv.at[index % SLOTS], dp=to)

    def push_pair(part, index):
        remote(part, part, send.at[counted(index)], pair_recv.at[counted(index)], dp=pair)

    def counted(index):
        return plan.counts - 1 if isinstance(index, int) and index >= ring else index // COUNTED

    def send_own(view, index, slot, count):
        own = view(dp, 0, count)
        wait_for(own, local.at[slot])
        push_own(own, index)

    def push_own(own, index):
        push(own, index, x_recv, x_peer)
        push(own, index, y_recv, y_peer)
        push_pair(own, index)

    def forward(view, index, count):
        half = count // 2
        slot = index % SLOTS
        wait_for(view(x_peer, 0, count), x_recv.at[slot])
        push(view(x_peer, half, half), index, b_recv, y_peer)
        push_pair(view(x_peer, 0, count), index)
        wait_for(view(y_peer, 0, count), y_recv.at[slot])
        push(view(y_peer, 0, half), index, a_recv, x_peer)
        push_pair(view(y_peer, 0, count), index)

    def forward_diagonal(view, index, count):
        half = count // 2
        slot = index % SLOTS
        wait_for(view(diagonal, 0, half), a_recv.at[slot])
        wait_for(view(diagonal, half, half), b_recv.at[slot])
        push_pair(view(diagonal, 0, count), index)

    def finish(index, some, count):
        wait_for(slabs.at[pl.ds(0, 7), some, pl.ds(0, count), :], send.at[index])
        wait_for(slabs.at[pl.ds(0, 4), some, pl.ds(0, count), :], pair_recv.at[index])


    def pieces(source_dp, to, place):
        all_rows = plan.downs
        downs = pl.ds(pl.multiple_of(place * plan.down_rows, 8), plan.down_rows)
        outs = pl.ds(pl.multiple_of(all_rows + place * plan.out_rows, 8), plan.out_rows)
        stop_downs, stop_outs = pl.ds(0, plan.down_rows), pl.ds(plan.down_rows, plan.out_rows)
        cut, home = pl.ds(plan.whole, plan.cut), pl.ds(0, plan.cut)
        found = []
        for n, own in enumerate((own_0, own_1)):
            layer = to * 2 + n
            found.append((d.at[layer, :, cut], stop.at[source_dp, n, stop_downs, :], own.at[downs, home], n))
            found.append((o.at[layer, :, cut], stop.at[source_dp, n, stop_outs, :], own.at[outs, home], n))
        return found

    my_rank = dp // 2
    my_place = (dp % 2) * plan.tp + z
    stays = my_rank == z

    def share_in_plane():
        for step in range(1, plan.dp):
            to = (dp + step) % plan.dp

            @pl.when(stays)
            def _(to=to):
                for part, _, final, n in pieces(dp, to, my_place):
                    remote(part, final, share_send.at[n], share_recv.at[n], dp=to)

            @pl.when(jnp.logical_not(stays))
            def _(to=to):
                for part, waiting, _, n in pieces(dp, to, my_place):
                    remote(part, waiting, share_send.at[n], stop_recv.at[dp], dp=to)

        @pl.when(stays)
        def _():
            for part, _, final, n in pieces(dp, dp, my_place):
                pltpu.make_async_copy(part, final, share_recv.at[n]).start()

    def share_to_rank(source_dp):
        rank, place = source_dp // 2, (source_dp % 2) * plan.tp + z

        @pl.when((rank != z) & (source_dp == dp))
        def _():
            for part, _, final, n in pieces(dp, dp, place):
                remote(part, final, share_send.at[n], share_recv.at[n], tp=rank)

        @pl.when((rank != z) & (source_dp != dp))
        def _():
            wait_for(stop.at[source_dp], stop_recv.at[source_dp])
            for _, waiting, final, n in pieces(source_dp, dp, place):
                remote(waiting, final, share_send.at[n], share_recv.at[n], tp=rank)


    whole_columns = pl.ds(0, plan.whole)
    keep = (keep_d, keep_o)
    mine = ((d, land_d, plan.down_rows, 0), (o, land_o, plan.out_rows, plan.downs))
    half = layers // 2

    def whole_home(n, row):
        _, _, count, first = mine[n]
        return pl.ds(pl.multiple_of(first + row * count, 8), count)

    def landing(rank, some, act):
        pl.when(rank == z)(lambda: act([whole.at[some, whole_home(n, core * plan.tp + z), :] for n in range(2)]))
        pl.when(rank != z)(lambda: act([land.at[rank, some] for _, land, _, _ in mine]))

    every = pl.ds(0, layers)

    def whole_out():
        def act(places):
            for n, (source, _, _, _) in enumerate(mine):
                for to, at in ((x_peer, 0), (y_peer, 2)):
                    remote(source.at[:, :, whole_columns], places[n], land_send.at[n], land_recv.at[at + n], dp=to)

        landing(my_rank, every, act)

        @pl.when(stays)
        def _():
            for n, (source, _, _, _) in enumerate(mine):
                pltpu.make_async_copy(source.at[:, :, whole_columns], keep[n], keep_sem.at[n]).start()

    def whole_keep():
        @pl.when(stays)
        def _():
            for n in range(2):
                wait_for(keep[n], keep_sem.at[n])
                target = whole.at[:, whole_home(n, core * plan.tp + z), :]
                pltpu.make_async_copy(keep[n], target, keep_sem.at[2 + n]).start()

    def whole_forward():
        for owner, at, first, to, then in ((x_peer, 0, half, y_peer, 6), (y_peer, 2, 0, x_peer, 4)):
            def arrived(places, at=at):
                for n in range(2):
                    wait_for(places[n], land_recv.at[at + n])

            def on(places, to=to, then=then):
                for n in range(2):
                    remote(places[n], places[n], land_send.at[n], land_recv.at[then + n], dp=to)

            landing(owner // 2, every, arrived)
            landing(owner // 2, pl.ds(first, half), on)

    def whole_arrive():
        for first, at in ((0, 4), (half, 6)):
            def arrived(places, at=at):
                for n in range(2):
                    wait_for(places[n], land_recv.at[at + n])

            landing(diagonal // 2, pl.ds(first, half), arrived)

    def whole_to_rank(shift, part):
        rank = (z + shift + core * (plan.tp - 2 * shift)) % plan.tp
        some = pl.ds(part * (layers // PARTS), layers // PARTS)

        def move(sources):
            for n, source in enumerate(sources):
                target = whole.at[some, whole_home(n, core * plan.tp + z), :]
                remote(source, target, whole_send.at[n], whole_recv.at[n], tp=rank)

        pl.when(rank == my_rank)(lambda: move([source.at[some, :, whole_columns] for source, _, _, _ in mine]))
        pl.when(rank != my_rank)(lambda: move([land.at[rank, some] for _, land, _, _ in mine]))

    def whole_rows(which):
        return [
            whole.at[:, pl.ds(pl.multiple_of(first + which * plan.tp * count, 8), plan.tp * count), :]
            for _, _, count, first in mine
        ]

    def whole_to_pair():
        for n, part in enumerate(whole_rows(core)):
            away = pl.ds(0, (plan.tp - 1) * mine[n][2])
            wait_for(whole.at[:, away, :], whole_recv.at[n])

            @pl.when(stays)
            def _(n=n):
                wait_for(keep[n], keep_sem.at[2 + n])

            remote(part, part, whole_pair_send.at[n], whole_pair_recv.at[n], dp=pair)

    def whole_finish():
        for n, (_, land, count, first) in enumerate(mine):
            wait_for(land.at[pl.ds(0, 3)], land_send.at[n])
            wait_for(whole.at[:, pl.ds(first, (plan.tp - 1) * count), :], whole_send.at[n])
            wait_for(whole_rows(core)[n], whole_pair_send.at[n])
            wait_for(whole_rows(1 - core)[n], whole_pair_recv.at[n])

    groups = layers // GROUP
    barrier = pltpu.get_barrier_semaphore()
    peers = [{"tp": (z + step) % plan.tp} for step in range(1, plan.tp)]
    peers += [{"dp": (dp + step) % plan.dp} for step in range(1, plan.dp)]
    for peer in peers:
        pl.semaphore_signal(barrier, inc=1, device_id=peer, device_id_type=MESH)
    for group in range(groups):
        collect(group)
    pl.semaphore_wait(barrier, len(peers))

    whole_out()
    exchange_layers(0)
    share_in_plane()
    for group in range(1, groups):
        exchange_layers(group)
    for index in range(layers, AHEAD):
        start_exchange(index)

    def step(index, _):
        slot = index % 2

        @pl.when(index + AHEAD < plan.chunks)
        def _():
            start_exchange(index + AHEAD)

        @pl.when((index >= SHARE_AT) & (index < SHARE_AT + plan.dp))
        def _():
            share_to_rank(index - SHARE_AT)

        @pl.when(index == WHOLE_AT)
        def _():
            whole_keep()
            whole_forward()

        @pl.when(index == WHOLE_AT + 3)
        def _():
            whole_arrive()

        @pl.when((index >= RANKS_AT) & (index < RANKS_AT + (plan.tp - 1) * PARTS))
        def _():
            whole_to_rank((index - RANKS_AT) % (plan.tp - 1) + 1, (index - RANKS_AT) // (plan.tp - 1))

        @pl.when(index < layers)
        def _():
            make_layer(index, slot)

        @pl.when(index >= layers)
        def _():
            make_head(index, slot)

        send_own(slab_view(index), index, slot, chunk)

        @pl.when(index >= LAG)
        def _():
            forward(slab_view(index - LAG), index - LAG, chunk)

        @pl.when(index >= 2 * LAG)
        def _():
            forward_diagonal(slab_view(index - 2 * LAG), index - 2 * LAG, chunk)

        return 0

    lax.fori_loop(0, ring, step, 0)

    def part_view(start):
        return lambda owner, first, count: slabs.at[owner, ring, pl.ds(start + first, count), :]

    tail_parts = [(part_view(0), ring, tail - LAST), (part_view(tail - LAST), ring + 1, LAST)]
    make_tail(ring % 2)
    wait_for(slabs.at[dp, ring, pl.ds(0, tail), :], local.at[ring % 2])
    for view, index, count in tail_parts:
        push_own(view(dp, 0, count), index)
    make_extra()
    for index in range(ring - LAG, ring):
        forward(slab_view(index), index, chunk)
        if index == ring - LAG:
            whole_to_pair()
    for part in tail_parts:
        forward(*part)
    for index in range(ring - 2 * LAG, ring):
        forward_diagonal(slab_view(index), index, chunk)
        if index == ring - 2:
            sent = pl.ds(0, (plan.tp - 1) * rows)
            wait_for(packed, z_send.at[0])
            wait_for(zbuf.at[pl.ds(layers, last - layers), sent, pl.ds(0, chunk)], z_send.at[1])
            wait_for(zbuf.at[last, sent, pl.ds(0, plan.tail_window)], z_send.at[2])
            whole_finish()
            for n, own in enumerate((own_0, own_1)):
                wait_for(own.at[:, pl.ds(0, plan.cut)], share_recv.at[n])
                for parts in (8, 5):
                    gone = pl.ds(0, parts * (plan.down_rows + plan.out_rows))
                    wait_for(own.at[gone, pl.ds(0, plan.cut)], share_send.at[n])
            for index in range((ring - LAG) // COUNTED):
                finish(index, pl.ds(index * COUNTED, COUNTED), chunk)
    for part in tail_parts:
        forward_diagonal(*part)
    for index in range((ring - LAG) // COUNTED, plan.counts - 1):
        first = index * COUNTED
        finish(index, pl.ds(first, min(COUNTED, ring - first)), chunk)
    finish(plan.counts - 1, pl.ds(ring, 1), tail)


def gather(plan, *args):
    dma = pltpu.SemaphoreType.DMA
    groups = plan.layers // GROUP
    share_rows = plan.down_rows + plan.out_rows
    hbm = pl.BlockSpec(memory_space=pltpu.HBM)
    shapes = [(plan.dp, plan.ring + 1, plan.chunk, LANES), (plan.piece, plan.columns), (plan.piece, plan.columns)]
    shapes += [(plan.layers, plan.piece, plan.whole), (plan.dp, plan.share, share_rows, plan.cut)]
    shapes += [(plan.tp, plan.layers, count, plan.whole) for count in (plan.down_rows, plan.out_rows)]
    return pl.pallas_call(
        functools.partial(gather_kernel, plan),
        out_shape=[jax.ShapeDtypeStruct(shape, jnp.bfloat16) for shape in shapes],
        in_specs=[hbm] * 8,
        out_specs=[hbm] * len(shapes),
        scratch_shapes=[
            pltpu.VMEM((plan.chunks, plan.tp * plan.rows, plan.layer_window), jnp.bfloat16),
            pltpu.VMEM((2, plan.chunk + 2 * LANES, LANES), jnp.bfloat16),
            dma((groups + plan.head_chunks,)), dma((3,)), dma((2,)),
            dma((SLOTS,)), dma((SLOTS,)), dma((SLOTS,)), dma((SLOTS,)), dma((plan.counts,)), dma((plan.counts,)),
            dma((plan.dp,)), dma((2,)), dma((2,)),
            dma((8,)), dma((2,)), dma((2,)), dma((2,)), dma((2,)), dma((2,)),
            pltpu.VMEM((plan.layers, plan.down_rows, plan.whole), jnp.bfloat16),
            pltpu.VMEM((plan.layers, plan.out_rows, plan.whole), jnp.bfloat16),
            dma((4,)),
            pltpu.VMEM((plan.layers // GROUP, plan.tp - 1, GROUP, plan.rows, plan.layer_window), jnp.bfloat16),
            dma((plan.layers // GROUP,)),
        ],
        compiler_params=pltpu.CompilerParams(collective_id=0, has_side_effects=True),
        name="gather",
    )(*args)[:4]


def place_slabs(plan, slabs, first, count, shapes, store, held=()):
    hbm = pl.BlockSpec(memory_space=pltpu.HBM)
    depth = min(BUFFERS, count)
    ahead = depth // 2

    def body(slab, *refs):
        outs, (buffers, loads, stores) = refs[len(held):-3], refs[-3:]

        def each_size(chunk, act):
            if first + count > plan.ring:
                pl.when(chunk < plan.ring)(lambda: act(plan.chunk))
                pl.when(chunk == plan.ring)(lambda: act(plan.tail))
            else:
                act(plan.chunk)

        def load(i, rows):
            for owner in range(plan.dp):
                pltpu.make_async_copy(
                    slab.at[owner, first + i, pl.ds(0, rows), :],
                    buffers.at[i % depth, pl.ds(0, rows), pl.ds(owner * LANES, LANES)],
                    loads.at[i % depth],
                ).start()

        def wait(i, rows, sem):
            buffer = buffers.at[i % depth, pl.ds(0, rows), :]
            pltpu.make_async_copy(buffer, buffer, sem.at[i % depth]).wait()

        def write(i, rows):
            wait(i, rows, loads)
            for source, target in store(buffers.at[i % depth], first + i, rows, outs):
                pltpu.make_async_copy(source, target, stores.at[i % depth]).start()

        def step(i, _):
            @pl.when(i >= depth)
            def _():
                each_size(first + i - depth, lambda rows: wait(i - depth, rows, stores))

            @pl.when(i < count)
            def _():
                each_size(first + i, lambda rows: load(i, rows))

            @pl.when((i >= ahead) & (i < count + ahead))
            def _():
                each_size(first + i - ahead, lambda rows: write(i - ahead, rows))

            return 0

        lax.fori_loop(0, count + depth, step, 0)

    outs = [jax.ShapeDtypeStruct(shape, jnp.bfloat16) for shape in shapes]
    return pl.pallas_call(
        body,
        in_specs=[hbm] * (1 + len(held)),
        out_specs=[hbm] * len(outs),
        out_shape=outs,
        scratch_shapes=[
            pltpu.VMEM((depth, plan.chunk, plan.dp * LANES), jnp.bfloat16),
            pltpu.SemaphoreType.DMA((depth,)),
            pltpu.SemaphoreType.DMA((depth,)),
        ],
        input_output_aliases={1 + n: n for n in range(len(held))},
        cost_estimate=pl.CostEstimate(
            flops=10**7, bytes_accessed=4 * count * plan.chunk * plan.dp * LANES, transcendentals=0
        ),
        compiler_params=pltpu.CompilerParams(vmem_limit_bytes=VMEM),
    )(slabs, *held)


def place_layers(plan, slabs):
    narrow, wide, width = 3 * plan.part, 2 * plan.wide, plan.dp * LANES

    def store(buffer, chunk, rows, outs):
        return [
            (buffer.at[pl.ds(0, narrow), :], outs[0].at[chunk]),
            (buffer.at[pl.ds(narrow, wide), :], outs[1].at[chunk]),
        ]

    shapes = [(plan.layers, narrow, width), (plan.layers, wide, width)]
    return place_slabs(plan, slabs, 0, plan.layers, shapes, store)


def place_head(plan, slabs, first, count, *held):
    def store(buffer, chunk, rows, outs):
        at = pl.multiple_of((chunk - plan.layers) * plan.chunk, 16)
        return [(buffer.at[pl.ds(0, rows), :], outs[0].at[pl.ds(at, rows), :])]

    shapes = [(plan.vocab, plan.dp * LANES)]
    return place_slabs(plan, slabs, plan.layers + first, count, shapes, store, held)[0]


def place_rows(plan, arrays, spots, width, column, held):
    count = len(spots([array for array in arrays], 0))
    columns = arrays[0].shape[-1]
    outs = [
        jax.ShapeDtypeStruct((plan.layers, plan.downs, plan.columns), jnp.bfloat16),
        jax.ShapeDtypeStruct((plan.layers, plan.columns, plan.outs), jnp.bfloat16),
        jax.ShapeDtypeStruct((plan.vocab, plan.dp * LANES), jnp.bfloat16),
    ]
    with_head = columns > width
    kept = [n for n in range(3) if n in held]
    made = [n for n in range(3 if with_head else 2)]

    blocks = [(plan.downs, plan.outs), (0, plan.downs // 2), (plan.downs // 2, plan.downs // 2)]

    def body(*refs):
        targets = dict(zip(made, refs[len(arrays) + len(kept):-4], strict=True))
        buffers, turned, loads, stored = refs[-4:]
        moves = spots(refs[: len(arrays)], lax.axis_index("dp"))
        place = pl.ds(column, width)
        loading, storing = [], []
        for n, (source, _, _, _) in enumerate(moves):
            for b, (first, height) in enumerate(blocks):
                some = pl.ds(first, height)
                loading.append(pltpu.make_async_copy(source.at[some, :], buffers.at[n, some, :], loads.at[n, b]))
                loading[-1].start()

        def put(source, target):
            storing.append(pltpu.make_async_copy(source, target, stored.at[0]))
            storing[-1].start()

        for n, (_, layer, owner, part) in enumerate(moves):
            for b, (first, height) in enumerate(blocks):
                loading[n * len(blocks) + b].wait()
                some = pl.ds(first, height)
                if b:
                    put(buffers.at[n, some, pl.ds(0, width)], targets[0].at[layer, some, place])
                for j in range((columns - width) // LANES):
                    row = plan.extra_first + (part * WHOLE + j) * plan.piece + first
                    put(
                        buffers.at[n, some, pl.ds(width + j * LANES, LANES)],
                        targets[2].at[pl.ds(row, height), pl.ds(pl.multiple_of(owner * LANES, LANES), LANES)],
                    )
                if b:
                    continue
                for i in range(plan.outs // LANES):
                    for j in range(width // LANES):
                        turned[n, pl.ds(j * LANES, LANES), pl.ds(i * LANES, LANES)] = buffers[
                            n, pl.ds(plan.downs + i * LANES, LANES), pl.ds(j * LANES, LANES)
                        ].T
                put(turned.at[n], targets[1].at[layer, place, :])
        for store in storing:
            store.wait()

    hbm = pl.BlockSpec(memory_space=pltpu.HBM)
    dma = pltpu.SemaphoreType.DMA
    result = pl.pallas_call(
        body,
        out_shape=[outs[n] for n in made],
        in_specs=[hbm] * (len(arrays) + len(kept)),
        out_specs=[hbm] * len(made),
        scratch_shapes=[
            pltpu.VMEM((count, plan.piece, columns), jnp.bfloat16),
            pltpu.VMEM((count, width, plan.outs), jnp.bfloat16),
            dma((count, len(blocks))), dma((1,)),
        ],
        input_output_aliases={len(arrays) + i: n for i, n in enumerate(kept)},
        cost_estimate=pl.CostEstimate(flops=10**7, bytes_accessed=4 * count * plan.piece * columns, transcendentals=0),
        compiler_params=pltpu.CompilerParams(vmem_limit_bytes=VMEM),
    )(*arrays, *(held[n] for n in kept))
    return dict(zip(made, result, strict=True))


def place_whole(plan, whole):
    def spots(refs, dp):
        return [(refs[0].at[layer], layer, 0, 0) for layer in range(plan.layers)]

    return place_rows(plan, [whole], spots, plan.whole, 0, {})


def place_shares(plan, shares, held):
    which = [(owner, part) for owner, arrays in shares.items() for part in arrays]
    arrays = [shares[owner][part] for owner, part in which]

    def spots(refs, dp):
        core, x, y = dp % 2, (dp // 2) % 2, dp // 4
        found = []
        for ref, ((flip_x, flip_y, flip_core), part) in zip(refs, which, strict=True):
            owner = (y + flip_y * (1 - 2 * y)) * 4 + (x + flip_x * (1 - 2 * x)) * 2 + core + flip_core * (1 - 2 * core)
            found.append((ref, owner * plan.share + part, owner, part))
        return found

    return place_rows(plan, arrays, spots, plan.cut, plan.whole, held)


def solution(mesh):
    train_stack = P(None, ("dp", "tp"), None)
    train_head = P(("dp", "tp"), None)
    fused_stack = P(None, "tp", None)
    last_stack = P(None, None, "tp")
    head_rows = P("tp", None)

    def local_sync(w_query, w_key, w_value, w_out, w_gate, w_up, w_down, w_head):
        plan = Plan(mesh.shape["tp"], mesh.shape["dp"], w_query, w_gate, w_out, w_down, w_head)
        slabs, own_0, own_1, whole = gather(plan, w_query, w_key, w_value, w_out, w_gate, w_up, w_down, w_head)

        def swap(bit, array):
            return lax.ppermute(array, "dp", [(i, i ^ bit) for i in range(plan.dp)])

        pair, along_x, along_y = (functools.partial(swap, bit) for bit in (1, 2, 4))
        hold = lax.optimization_barrier

        x_1, y_0 = along_x(own_1), along_y(own_0)
        x_0, y_1 = along_x(own_0), along_y(own_1)
        pair_own = [pair(own_0), pair(own_1)]
        qkv_block, gate_up_block = place_layers(plan, slabs)
        x_1, y_0, qkv_block, slabs = hold((x_1, y_0, qkv_block, slabs))
        diagonal_0 = along_x(y_0)
        diagonal_1 = along_y(x_1)
        pair_x_1, pair_y_0 = pair(x_1), pair(y_0)
        head_chunks = plan.ring + 1 - plan.layers
        early = head_chunks // 4
        head_block = place_head(plan, slabs, early, head_chunks - early)
        x_0, y_1, head_block, slabs, whole = hold((x_0, y_1, head_block, slabs, whole))
        pair_x_0, pair_y_1 = pair(x_0), pair(y_1)
        placed = place_whole(plan, whole)
        slabs, *placed = hold((slabs, placed[0], placed[1]))
        head_block = place_head(plan, slabs, 0, early, head_block)
        own_0, own_1, head_block = hold((own_0, own_1, head_block))
        near = {
            (0, 0, 0): {0: own_0, 1: own_1}, (0, 0, 1): dict(enumerate(pair_own)),
            (1, 0, 0): {0: x_0, 1: x_1}, (1, 0, 1): {0: pair_x_0, 1: pair_x_1},
            (0, 1, 0): {0: y_0, 1: y_1}, (0, 1, 1): {0: pair_y_0, 1: pair_y_1},
        }
        placed = place_shares(plan, near, {0: placed[0], 1: placed[1], 2: head_block})
        diagonal_0, head_block = hold((diagonal_0, placed[2]))
        pair_diagonal_0 = pair(diagonal_0)
        diagonal_1, down_block = hold((diagonal_1, placed[0]))
        pair_diagonal_1 = pair(diagonal_1)
        placed = {0: down_block, 1: placed[1], 2: head_block}
        placed = place_shares(plan, {(1, 1, 0): {0: diagonal_0, 1: diagonal_1}}, placed)
        placed = place_shares(plan, {(1, 1, 1): {0: pair_diagonal_0}}, placed)
        placed = place_shares(plan, {(1, 1, 1): {1: pair_diagonal_1}}, placed)
        down_block, o_block, head_block = placed[0], placed[1], placed[2]
        return (
            qkv_block,
            o_block,
            gate_up_block,
            jnp.swapaxes(down_block, 1, 2),
            head_block,
        )

    return jax.shard_map(
        local_sync,
        mesh=mesh,
        in_specs=(train_stack,) * 7 + (train_head,),
        out_specs=(fused_stack, last_stack, fused_stack, last_stack, head_rows),
        check_vma=False,
    )
```
